8 devices in a mesh: dp: 2 (over z, y), emb: 4 (over x, core).
Axes of the slice: x: 2, y: 2, z: 1, core: 2. Of those that a mesh axis runs over, the one named last changes fastest.
Arguments:
- tok_ids: int32 [4096], P(('dp', 'emb'))
- resid_in: bfloat16 [4096, 3072], P(('dp', 'emb'))
- cot_out: bfloat16 [4096, 3072], P(('dp', 'emb'))
- tables: bfloat16 [4, 128256, 256], P(None, 'emb')
- w_up: bfloat16 [4, 3072, 8192], replicated
- w_down: bfloat16 [4, 8192, 3072], replicated
- w_gate: bfloat16 [4, 3072, 256], replicated
- w_proj: bfloat16 [4, 256, 3072], replicated
Outputs:
- output 1: bfloat16 [4096, 3072], P(('dp', 'emb'))
- output 2: float32 [4, 128256, 256], P(None, 'emb')
All inputs are finite; a program needn't handle non-finite values.
Results may differ from the reference program's by a relative error of at most 0.0110832.
Values are sent between devices in bfloat16 or wider.
A program may use at most 2.5 GiB of HBM per device.

```python
import jax
import jax.numpy as jnp
from jax import lax

TOKENS_DEV = 512
LAYERS = 4
D_MODEL = 3072
FFN_DIM = 8192
EMB_DIM = 256
VOCAB_SIZE = 128256
NUM_DP = 2
NUM_EMB = 4
CAP_ROWS = 256

N_TOKENS = TOKENS_DEV * NUM_DP * NUM_EMB
RANGE_ROWS = VOCAB_SIZE // NUM_EMB
HOT_SET = min(16, RANGE_ROWS)
NORM_EPS = 1e-6


def draw_ids(id_key):
    key_list = jax.random.split(id_key, 9)
    n_dev = NUM_DP * NUM_EMB
    draw_shape = (n_dev, TOKENS_DEV)
    tok_pos = jnp.arange(TOKENS_DEV, dtype=jnp.int32)[None, :]
    hot_top = jax.random.randint(key_list[0], (n_dev, 1), 1, NUM_EMB + 1)
    hot_owner = jax.random.randint(key_list[1], (n_dev, 1), 0, hot_top)
    shift_by = jax.random.randint(key_list[2], (n_dev, 1), 0, NUM_EMB - 1)
    spread = (hot_owner + 1 + (tok_pos - CAP_ROWS + shift_by) % (NUM_EMB - 1)) % NUM_EMB
    owner_seq = jnp.where(tok_pos < CAP_ROWS, hot_owner, spread)
    scores = jax.random.randint(key_list[3], draw_shape, 0, TOKENS_DEV) * TOKENS_DEV + tok_pos
    perm_order = jnp.argsort(scores, axis=1)
    owner_ids = jnp.take_along_axis(owner_seq, perm_order, axis=1)
    is_hot = jax.random.randint(key_list[4], draw_shape, 0, 4) == 0
    hot_off = jax.random.randint(key_list[5], draw_shape, 0, HOT_SET)
    span_a = jax.random.randint(key_list[6], draw_shape, 1, RANGE_ROWS + 1)
    span_b = jax.random.randint(key_list[7], draw_shape, 1, span_a + 1)
    tail_off = jax.random.randint(key_list[8], draw_shape, 0, span_b)
    offset = jnp.where(is_hot, hot_off, tail_off)
    return (owner_ids * RANGE_ROWS + offset).reshape(-1).astype(jnp.int32)


def setup_inputs(seed: int = 0) -> dict:
    root_key = jax.random.key(seed)
    key_list = jax.random.split(root_key, 8)
    tok_ids = draw_ids(key_list[0])
    resid_in = jax.random.normal(key_list[1], (N_TOKENS, D_MODEL), jnp.float32).astype(jnp.bfloat16)
    cot_out = jax.random.normal(key_list[2], (N_TOKENS, D_MODEL), jnp.float32).astype(jnp.bfloat16)
    tables = (0.5 * jax.random.normal(key_list[3], (LAYERS, VOCAB_SIZE, EMB_DIM), jnp.float32)).astype(jnp.bfloat16)
    w_up = (jax.random.normal(key_list[4], (LAYERS, D_MODEL, FFN_DIM), jnp.float32) * D_MODEL ** -0.5).astype(jnp.bfloat16)
    w_down = (jax.random.normal(key_list[5], (LAYERS, FFN_DIM, D_MODEL), jnp.float32) * (0.5 * FFN_DIM ** -0.5)).astype(jnp.bfloat16)
    w_gate = (jax.random.normal(key_list[6], (LAYERS, D_MODEL, EMB_DIM), jnp.float32) * D_MODEL ** -0.5).astype(jnp.bfloat16)
    w_proj = (jax.random.normal(key_list[7], (LAYERS, EMB_DIM, D_MODEL), jnp.float32) * EMB_DIM ** -0.5).astype(jnp.bfloat16)
    return {'tok_ids': tok_ids, 'resid_in': resid_in, 'cot_out': cot_out, 'tables': tables, 'w_up': w_up, 'w_down': w_down, 'w_gate': w_gate, 'w_proj': w_proj}


def rms_norm(x_f32):
    return x_f32 * lax.rsqrt(jnp.mean(x_f32 * x_f32, axis=-1, keepdims=True) + NORM_EPS)


def layer_forward(resid_cur, fetched, w_up_l, w_down_l, w_gate_l, w_proj_l):
    x_f32 = resid_cur.astype(jnp.float32)
    normed = rms_norm(x_f32).astype(jnp.bfloat16)
    hidden = jax.nn.gelu(jnp.dot(normed, w_up_l, preferred_element_type=jnp.float32)).astype(jnp.bfloat16)
    mlp_out = jnp.dot(hidden, w_down_l, preferred_element_type=jnp.float32)
    gate_act = jax.nn.gelu(jnp.dot(normed, w_gate_l, preferred_element_type=jnp.float32))
    mixed_in = (gate_act * fetched).astype(jnp.bfloat16)
    proj_out = jnp.dot(mixed_in, w_proj_l, preferred_element_type=jnp.float32)
    return (x_f32 + mlp_out + proj_out).astype(jnp.bfloat16)


def reference(tok_ids, resid_in, cot_out, tables, w_up, w_down, w_gate, w_proj):
    def fwd_step(resid_cur, layer_params):
        table_l, w_up_l, w_down_l, w_gate_l, w_proj_l = layer_params
        fetched = jnp.take(table_l, tok_ids, axis=0).astype(jnp.float32)
        resid_next = layer_forward(resid_cur, fetched, w_up_l, w_down_l, w_gate_l, w_proj_l)
        return resid_next, resid_cur

    resid_out, resid_saved = lax.scan(fwd_step, resid_in, (tables, w_up, w_down, w_gate, w_proj))

    def bwd_step(cot_next, layer_params):
        resid_cur, table_l, w_up_l, w_down_l, w_gate_l, w_proj_l = layer_params
        fetched = jnp.take(table_l, tok_ids, axis=0).astype(jnp.float32)

        def local_layer(resid_arg, fetched_arg):
            return layer_forward(resid_arg, fetched_arg, w_up_l, w_down_l, w_gate_l, w_proj_l)

        pullback = jax.vjp(local_layer, resid_cur, fetched)[1]
        cot_cur, d_fetched = pullback(cot_next)
        d_table = jax.ops.segment_sum(d_fetched, tok_ids, num_segments=VOCAB_SIZE)
        return cot_cur, d_table

    cot_first, d_tables = lax.scan(bwd_step, cot_out, (resid_saved, tables, w_up, w_down, w_gate, w_proj), reverse=True)
    return resid_out, d_tables
```

```python
import functools

import jax
import jax.numpy as jnp
from jax import lax
from jax.experimental import pallas as pl
from jax.experimental.pallas import tpu as pltpu
from jax.sharding import PartitionSpec as P

NORM_EPS = 1e-6
BF = jnp.bfloat16
F32 = jnp.float32
I32 = jnp.int32
VMEM_BYTES = 67043328
GELU_C = 0.7978845608028654
GELU_A = 0.044715

MESH_AXES = ('dp', 'emb')
CAP = 256


def gelu(x):
    return 0.5 * x * (1.0 + jnp.tanh(GELU_C * (x + GELU_A * (x * x * x))))


def gelu_slope(x):
    sq = x * x
    th = jnp.tanh(GELU_C * (x + GELU_A * (x * sq)))
    return 0.5 * (1.0 + th) + (0.5 * GELU_C) * x * (1.0 - th * th) * (1.0 + (3 * GELU_A) * sq)


def dot(a, b):
    return jnp.dot(a, b, preferred_element_type=F32)


def dot_t(a, b):
    return lax.dot_general(a, b, (((1,), (1,)), ((), ())), preferred_element_type=F32)


def row_loop(rows, slab, unroll=2):
    def run(body):
        def step(i, carry):
            body(pl.ds(pl.multiple_of(i * slab, slab), slab))
            return carry

        lax.fori_loop(0, rows // slab, step, 0, unroll=unroll)

    return run


def forward_kernel(cfg, x_hbm, cot_hbm, fet_ref, wg_ref, wp_ref, wu_ref, wd_ref,
                   out_hbm, saved_hbm, up_ref, gate_ref, rows_ref, dgp_ref, dtab_hbm,
                   x_s, u_s, acc_s, h_s, zero_s, in_sem, out_sem, z_sem):
    n_layers, n_blk, cw, nw, slab, z_per, z_chunks = cfg
    layer, blk = pl.program_id(0), pl.program_id(1)
    tok, dim = x_s.shape
    fb = wu_ref.shape[2]
    step = layer * n_blk + blk
    z_rows = zero_s.shape[0]

    def z_copy(j):
        c = step * z_per + j
        zl = c // z_chunks
        zc = c - zl * z_chunks
        return pltpu.make_async_copy(zero_s, dtab_hbm.at[zl, pl.ds(pl.multiple_of(zc * z_rows, 8), z_rows), :], z_sem.at[j])

    def norm_rows(sl, x):
        scale = lax.rsqrt(jnp.mean(x * x, axis=-1, keepdims=True) + NORM_EPS)
        u_s[sl, :] = (x * scale).astype(BF)
        acc_s[sl, :] = x

    @pl.when(step == 0)
    def _():
        fetch = pltpu.make_async_copy(x_hbm, x_s, in_sem)
        fetch.start()
        row_loop(z_rows, 8, 1)(lambda sl: zero_s.__setitem__((sl, slice(None)), jnp.zeros((8, zero_s.shape[1]), F32)))
        fetch.wait()
        row_loop(tok, slab)(lambda sl: norm_rows(sl, x_s[sl, :].astype(F32)))

    for j in range(z_per):
        @pl.when(step > 0)
        def _():
            z_copy(j).wait()

        z_copy(j).start()

    @pl.when(blk == 0)
    def _():
        gate_ref[0] = dot(u_s[...], wg_ref[0])

    for c in range(fb // cw):
        cs = slice(c * cw, (c + 1) * cw)
        up = dot(u_s[...], wu_ref[0, :, cs])
        up_ref[0, :, cs] = up
        h_s[:, cs] = gelu(up).astype(BF)
    for n in range(dim // nw):
        ns = slice(n * nw, (n + 1) * nw)
        acc_s[:, ns] += dot(h_s[...], wd_ref[0, :, ns])

    @pl.when(blk == n_blk - 1)
    def _():
        mixed = (gelu(gate_ref[0]) * fet_ref[0].astype(F32)).astype(BF)
        for n in range(dim // nw):
            ns = slice(n * nw, (n + 1) * nw)
            acc_s[:, ns] += dot(mixed, wp_ref[0, :, ns])

        @pl.when(layer > 0)
        def _():
            pltpu.make_async_copy(x_s, saved_hbm.at[layer - 1], out_sem).wait()

        def next_rows(sl):
            x_new = acc_s[sl, :].astype(BF)
            x_s[sl, :] = x_new
            norm_rows(sl, x_new.astype(F32))

        row_loop(tok, slab)(next_rows)

        @pl.when(layer < n_layers - 1)
        def _():
            pltpu.make_async_copy(x_s, saved_hbm.at[layer], out_sem).start()

        @pl.when(layer == n_layers - 1)
        def _():
            put = pltpu.make_async_copy(x_s, out_hbm, out_sem)
            put.start()
            get = pltpu.make_async_copy(cot_hbm, u_s, in_sem)
            get.start()
            for j in range(z_per):
                z_copy(j).wait()
            get.wait()
            d_mixed = dot_t(u_s[...], wp_ref[0]).astype(BF).astype(F32)
            gate_grads(gate_ref[0], fet_ref[0], d_mixed, rows_ref, dgp_ref)
            put.wait()


def gate_grads(gate_pre, fetched, d_mixed, rows_ref, dgp_ref):
    rows_ref[...] = gelu(gate_pre) * d_mixed
    dgp_ref[...] = (d_mixed * fetched.astype(F32) * gelu_slope(gate_pre)).astype(BF)


def backward_kernel(cfg, cot_ref, x_ref, up_ref, wu_ref, wd_ref, wg_ref, wp_ref, gate_ref, fet_ref, dgp_in_ref,
                    cot_out_ref, rows_ref, dgp_ref, acc_s, dup_s, dng_s):
    n_blk, cw, nw, slab = cfg
    blk = pl.program_id(0)
    tok, dim = cot_ref.shape
    fb = wu_ref.shape[2]

    @pl.when(blk == 0)
    def _():
        for n in range(dim // nw):
            ns = slice(n * nw, (n + 1) * nw)
            dng_s[:, ns] = dot_t(dgp_in_ref[...], wg_ref[0, ns, :]).astype(BF)

        def clear(sl):
            acc_s[sl, :] = jnp.zeros((slab, dim), F32)

        row_loop(tok, slab)(clear)

    for c in range(fb // cw):
        cs = slice(c * cw, (c + 1) * cw)
        d_hid = dot_t(cot_ref[...], wd_ref[0, cs, :]).astype(BF).astype(F32)
        dup_s[:, cs] = (d_hid * gelu_slope(up_ref[0, :, cs])).astype(BF)
    for n in range(dim // nw):
        ns = slice(n * nw, (n + 1) * nw)
        acc_s[:, ns] += dot_t(dup_s[...], wu_ref[0, ns, :])

    @pl.when(blk == n_blk - 1)
    def _():
        def rows_back(sl):
            x = x_ref[0, sl, :].astype(F32)
            scale = lax.rsqrt(jnp.mean(x * x, axis=-1, keepdims=True) + NORM_EPS)
            d_n = (acc_s[sl, :].astype(BF).astype(F32) + dng_s[sl, :].astype(F32)).astype(BF).astype(F32)
            proj = jnp.mean(d_n * x, axis=-1, keepdims=True)
            d_x = d_n * scale - x * (proj * (scale * scale * scale))
            cot_out_ref[sl, :] = (cot_ref[sl, :].astype(F32) + d_x).astype(BF)

        row_loop(tok, slab)(rows_back)
        d_mixed = dot_t(cot_out_ref[...], wp_ref[0]).astype(BF).astype(F32)
        gate_grads(gate_ref[0], fet_ref[0], d_mixed, rows_ref, dgp_ref)


def gather_kernel(cfg, loc_ref, pick_ref, tables_hbm, out_ref, buf, sems):
    n_layers, n_slots, per_sem, per_dot, group = cfg

    def issue(s, carry):
        base = pl.multiple_of(jnp.left_shift(jnp.right_shift(loc_ref[s], 3), 3), 8)
        pltpu.make_async_copy(
            tables_hbm.at[:, pl.ds(base, 8), :], buf.at[:, pl.ds(pl.multiple_of(s * 8, 8), 8), :], sems.at[s // per_sem]
        ).start()
        return carry

    lax.fori_loop(0, n_slots, issue, 0, unroll=8)
    per_trip = per_dot * group

    def pick(g, carry):
        @pl.when(lax.rem(g * per_trip, per_sem) == 0)
        def _():
            part = buf.at[:, pl.ds(pl.multiple_of(g * per_trip * 8, 8), per_sem * 8), :]
            pltpu.make_async_copy(part, part, sems.at[g * per_trip // per_sem]).wait()

        for k in range(group):
            s0 = pl.multiple_of(g * per_trip + k * per_dot, per_dot)
            want = pick_ref[pl.ds(s0, per_dot), :]
            sel = (lax.broadcasted_iota(I32, (per_dot, per_dot * 8), 1) == want).astype(BF)
            for l in range(n_layers):
                rows = buf[l, pl.ds(pl.multiple_of(s0 * 8, 8), per_dot * 8), :]
                out_ref[l, pl.ds(s0, per_dot), :] = dot(sel, rows).astype(BF)
        return carry

    lax.fori_loop(0, n_slots // per_trip, pick, 0)


def scatter_kernel(cfg, keys_ref, meta_ref, rows_ref, dt_in, dt_out, sums, sem):
    first_layer, slot_bits = cfg
    layer = first_layer - pl.program_id(0)
    count = meta_ref[0]

    def add(j, carry):
        acc, prev = carry
        key = keys_ref[j]
        slot = jnp.bitwise_and(key, (1 << slot_bits) - 1)
        row = jnp.right_shift(key, slot_bits)
        acc = jnp.where(row == prev, acc, 0.0) + rows_ref[0, pl.ds(slot, 1), :]
        sums[pl.ds(j, 1), :] = acc
        return acc, row

    lax.fori_loop(0, count, add, (jnp.zeros((1, rows_ref.shape[2]), F32), jnp.int32(-1)))

    def put(j, n):
        row = jnp.right_shift(keys_ref[j], slot_bits)
        last = row != jnp.right_shift(keys_ref[j + 1], slot_bits)

        @pl.when(last)
        def _():
            pltpu.make_async_copy(sums.at[pl.ds(j, 1), :], dt_out.at[layer, pl.ds(row, 1), :], sem).start()

        return n + last.astype(I32)

    n_rows = lax.fori_loop(0, count, put, jnp.int32(0))

    def drain(j, carry):
        pltpu.make_async_copy(sums.at[pl.ds(0, 1), :], dt_out.at[layer, pl.ds(0, 1), :], sem).wait()
        return carry

    lax.fori_loop(0, n_rows, drain, 0)


def solution(mesh):
    n_emb, n_dp = mesh.shape['emb'], mesh.shape['dp']
    n_dev = n_emb * n_dp
    tok_spec = P(('dp', 'emb'))
    act_spec = P(('dp', 'emb'), None)
    table_spec = P(None, 'emb', None)
    full_spec = P(None, None, None)
    hbm = pl.BlockSpec(memory_space=pl.ANY)
    vm = pl.BlockSpec(memory_space=pltpu.VMEM)
    sm = pl.BlockSpec(memory_space=pltpu.SMEM)

    def device_body(tok_ids, resid_in, cot_out, tables, w_up, w_down, w_gate, w_proj):
        n_layers, range_rows, e_dim = tables.shape
        tok = tok_ids.shape[0]
        dim, ffn = w_up.shape[1:]
        n_slots = n_dev * CAP
        my_emb, my_dp = lax.axis_index('emb'), lax.axis_index('dp')

        ids8 = lax.all_gather(tok_ids, MESH_AXES, tiled=True).reshape(n_dev, tok)
        mine = (ids8 // range_rows) == my_emb
        t_iota = jnp.arange(tok, dtype=I32)
        before = t_iota[None, :] < t_iota[:, None]
        rank8 = jnp.sum((mine[:, None, :] & before[None]).astype(I32), axis=-1)
        c_iota = jnp.arange(CAP, dtype=I32)
        hit = mine[:, None, :] & (rank8[:, None, :] == c_iota[None, :, None])
        recv_loc = jnp.sum(jnp.where(hit, (ids8 - my_emb * range_rows)[:, None, :], 0), axis=-1)
        counts = jnp.sum(mine.astype(I32), axis=-1)
        valid = c_iota[None, :] < counts[:, None]
        slot_bits = (n_slots - 1).bit_length()
        keys = jnp.where(valid, recv_loc * n_slots + jnp.arange(n_slots, dtype=I32).reshape(n_dev, CAP), jnp.iinfo(jnp.int32).max)
        skeys = jnp.concatenate([lax.sort(keys.reshape(-1)), jnp.full((8,), jnp.iinfo(jnp.int32).max, I32)])
        total = jnp.sum(counts).reshape(1)

        my_owner = tok_ids // range_rows
        rank = jnp.sum(((my_owner[None, :] == my_owner[:, None]) & before).astype(I32), axis=-1)
        slot_of = my_owner * CAP + rank
        sel_in = slot_of[:, None] == jnp.arange(n_emb * CAP, dtype=I32)[None, :]

        want = lax.dynamic_slice_in_dim(recv_loc, my_dp * n_emb, n_emb, 0).reshape(-1)
        n_serve = n_emb * CAP
        per_dot, group, per_sem = 32, 4, 128
        pick = (jnp.bitwise_and(want, 7) + 8 * (jnp.arange(n_serve, dtype=I32) % per_dot))[:, None]
        served = pl.pallas_call(
            functools.partial(gather_kernel, (n_layers, n_serve, per_sem, per_dot, group)),
            out_shape=jax.ShapeDtypeStruct((n_layers, n_serve, e_dim), BF),
            in_specs=[sm, vm, hbm],
            out_specs=vm,
            scratch_shapes=[pltpu.VMEM((n_layers, n_serve * 8, e_dim), BF), pltpu.SemaphoreType.DMA((n_serve // per_sem,))],
            compiler_params=pltpu.CompilerParams(vmem_limit_bytes=VMEM_BYTES),
            name='table_rows',
        )(want, pick, tables)
        returned = lax.all_to_all(served.reshape(n_layers, n_emb, CAP, e_dim), 'emb', 1, 1, tiled=True)
        fetched = jnp.einsum('tc,lce->lte', sel_in.astype(BF), returned.reshape(n_layers, n_serve, e_dim),
                             preferred_element_type=F32).astype(BF)

        fb = 1024
        n_blk = ffn // fb
        cw, nw, slab = 512, 512, 16
        z_rows = 1336
        z_chunks = range_rows // z_rows
        z_per = n_layers * z_chunks // (n_layers * n_blk)
        assert z_chunks * z_rows == range_rows and z_per * n_blk == z_chunks

        def lsp(*shape):
            return pl.BlockSpec((1,) + shape, lambda l, f: (l, 0, 0))

        matmul_flops = 4 * tok * dim * ffn
        out, saved, ups, gates, rows, dgp, dtab = pl.pallas_call(
            functools.partial(forward_kernel, (n_layers, n_blk, cw, nw, slab, z_per, z_chunks)),
            grid=(n_layers, n_blk),
            out_shape=[
                jax.ShapeDtypeStruct((tok, dim), BF),
                jax.ShapeDtypeStruct((n_layers - 1, tok, dim), BF),
                jax.ShapeDtypeStruct((n_layers - 1, tok, ffn), F32),
                jax.ShapeDtypeStruct((n_layers, tok, e_dim), F32),
                jax.ShapeDtypeStruct((tok, e_dim), F32),
                jax.ShapeDtypeStruct((tok, e_dim), BF),
                jax.ShapeDtypeStruct((n_layers, range_rows, e_dim), F32),
            ],
            in_specs=[hbm, hbm, lsp(tok, e_dim), lsp(dim, e_dim), lsp(e_dim, dim),
                      pl.BlockSpec((1, dim, fb), lambda l, f: (l, 0, f)), pl.BlockSpec((1, fb, dim), lambda l, f: (l, f, 0))],
            out_specs=[hbm, hbm,
                       pl.BlockSpec((1, tok, fb), lambda l, f: (jnp.maximum(l - 1, 0), 0, jnp.where(l > 0, f, 0))),
                       lsp(tok, e_dim),
                       pl.BlockSpec((tok, e_dim), lambda l, f: (0, 0)), pl.BlockSpec((tok, e_dim), lambda l, f: (0, 0)), hbm],
            scratch_shapes=[
                pltpu.VMEM((tok, dim), BF), pltpu.VMEM((tok, dim), BF), pltpu.VMEM((tok, dim), F32), pltpu.VMEM((tok, fb), BF),
                pltpu.VMEM((z_rows, e_dim), F32), pltpu.SemaphoreType.DMA, pltpu.SemaphoreType.DMA, pltpu.SemaphoreType.DMA((z_per,)),
            ],
            compiler_params=pltpu.CompilerParams(vmem_limit_bytes=VMEM_BYTES, dimension_semantics=('arbitrary', 'arbitrary')),
            cost_estimate=pl.CostEstimate(flops=n_layers * matmul_flops, bytes_accessed=400 << 20, transcendentals=0),
            name='forward',
        )(resid_in, cot_out, fetched, w_gate, w_proj, w_up, w_down)

        sel_out = (jnp.arange(n_serve, dtype=I32)[:, None] == slot_of[None, :]).astype(F32)

        def exchange(grad_rows):
            slots = jnp.dot(sel_out, grad_rows, precision=lax.Precision.HIGHEST, preferred_element_type=F32)
            slots = jnp.broadcast_to(slots.reshape(1, n_emb, CAP, e_dim), (n_dp, n_emb, CAP, e_dim)).reshape(n_dev, CAP, e_dim)
            return lax.all_to_all(slots, MESH_AXES, 0, 0, tiled=True).reshape(n_slots, e_dim)

        def backward(layer, cot, dgp):
            def at(l, *shape):
                return pl.BlockSpec((1,) + shape, lambda f: (l, 0, 0), pipeline_mode=pl.Buffered(1))

            def flat(*shape):
                return pl.BlockSpec(shape, lambda f: (0, 0), pipeline_mode=pl.Buffered(1))

            return pl.pallas_call(
                functools.partial(backward_kernel, (n_blk, cw, nw, slab)),
                grid=(n_blk,),
                out_shape=[jax.ShapeDtypeStruct((tok, dim), BF), jax.ShapeDtypeStruct((tok, e_dim), F32), jax.ShapeDtypeStruct((tok, e_dim), BF)],
                in_specs=[flat(tok, dim), at(layer - 1, tok, dim),
                          pl.BlockSpec((1, tok, fb), lambda f: (layer - 1, 0, f)),
                          pl.BlockSpec((1, dim, fb), lambda f: (layer, 0, f)), pl.BlockSpec((1, fb, dim), lambda f: (layer, f, 0)),
                          at(layer, dim, e_dim), at(layer - 1, e_dim, dim), at(layer - 1, tok, e_dim), at(layer - 1, tok, e_dim),
                          flat(tok, e_dim)],
                out_specs=[flat(tok, dim), flat(tok, e_dim), flat(tok, e_dim)],
                scratch_shapes=[pltpu.VMEM((tok, dim), F32), pltpu.VMEM((tok, fb), BF), pltpu.VMEM((tok, dim), BF)],
                compiler_params=pltpu.CompilerParams(vmem_limit_bytes=VMEM_BYTES, dimension_semantics=('arbitrary',)),
                cost_estimate=pl.CostEstimate(flops=matmul_flops, bytes_accessed=100 << 20, transcendentals=0),
                name=f'backward_{layer}',
            )(cot, saved, ups, w_up, w_down, w_gate, w_proj, gates, fetched, dgp)

        def scatter(first_layer, rows_in, dtab):
            n = rows_in.shape[0]
            return pl.pallas_call(
                functools.partial(scatter_kernel, (first_layer, slot_bits)),
                grid=(n,),
                out_shape=jax.ShapeDtypeStruct(dtab.shape, F32),
                in_specs=[sm, sm, pl.BlockSpec((1, n_slots, e_dim), lambda i: (i, 0, 0)), hbm],
                out_specs=hbm,
                input_output_aliases={3: 0},
                scratch_shapes=[pltpu.VMEM((n_slots, e_dim), F32), pltpu.SemaphoreType.DMA],
                compiler_params=pltpu.CompilerParams(vmem_limit_bytes=VMEM_BYTES, dimension_semantics=('arbitrary',)),
                cost_estimate=pl.CostEstimate(flops=n * 20_000_000_000, bytes_accessed=n << 22, transcendentals=0),
                name=f'scatter_{first_layer}',
            )(skeys, total, rows_in, dtab)

        cot = cot_out
        for layer in reversed(range(1, n_layers)):
            got = exchange(rows)
            cot, rows, dgp = backward(layer, cot, dgp)
            dtab = scatter(layer, got[None], dtab)
        dtab = scatter(0, exchange(rows)[None], dtab)
        return out, dtab

    return jax.shard_map(device_body, mesh=mesh, in_specs=(tok_spec, act_spec, act_spec, table_spec, full_spec, full_spec, full_spec, full_spec), out_specs=(act_spec, table_spec), check_vma=False)
```

```python
import functools

import jax
import jax.numpy as jnp
from jax import lax
from jax.experimental import pallas as pl
from jax.experimental.pallas import tpu as pltpu
from jax.sharding import PartitionSpec as P

NORM_EPS = 1e-6
BF = jnp.bfloat16
F32 = jnp.float32
I32 = jnp.int32
VMEM_BYTES = 67043328
GELU_C = 0.7978845608028654
GELU_A = 0.044715

MESH_AXES = ('dp', 'emb')
CAP = 256


def gelu(x):
    return 0.5 * x * (1.0 + jnp.tanh(GELU_C * (x + GELU_A * (x * x * x))))


def gelu_slope(x):
    sq = x * x
    th = jnp.tanh(GELU_C * (x + GELU_A * (x * sq)))
    return 0.5 * (1.0 + th) + (0.5 * GELU_C) * x * (1.0 - th * th) * (1.0 + (3 * GELU_A) * sq)


def dot(a, b):
    return jnp.dot(a, b, preferred_element_type=F32)


def dot_t(a, b):
    return lax.dot_general(a, b, (((1,), (1,)), ((), ())), preferred_element_type=F32)


def row_loop(rows, slab, unroll=2):
    def run(body):
        def step(i, carry):
            body(pl.ds(pl.multiple_of(i * slab, slab), slab))
            return carry

        lax.fori_loop(0, rows // slab, step, 0, unroll=unroll)

    return run


def peer_of(n_emb, index):
    dp = index // n_emb
    return {'dp': dp, 'emb': index - dp * n_emb}


def remote(src, dst, send_sem, recv_sem, device):
    return pltpu.make_async_remote_copy(src_ref=src, dst_ref=dst, send_sem=send_sem, recv_sem=recv_sem,
                                        device_id=device, device_id_type=pl.DeviceIdType.MESH)


def meet(devices):
    barrier = pltpu.get_barrier_semaphore()
    for device in devices:
        pl.semaphore_signal(barrier, inc=1, device_id=device, device_id_type=pl.DeviceIdType.MESH)
    pl.semaphore_wait(barrier, len(devices))


def ids_kernel(cfg, in_ref, out_ref, send_sem, recv_sem):
    n_dp, n_emb = cfg
    n_dev = n_dp * n_emb
    me = lax.axis_index('dp') * n_emb + lax.axis_index('emb')
    peers = [peer_of(n_emb, lax.rem(me + k, n_dev)) for k in range(1, n_dev)]
    meet(peers)
    copies = [remote(in_ref, out_ref.at[me], send_sem.at[k], recv_sem.at[k], peer) for k, peer in enumerate(peers)]
    for copy in copies:
        copy.start()
    out_ref[me] = in_ref[...]
    for copy in copies:
        copy.wait()


def gather_kernel(cfg, loc_ref, counts_ref, pick_ref, tables_hbm, out_ref, buf, sems):
    n_layers, n_dest, cap, per_dot, group = cfg
    trip = per_dot * group
    n_trips = [(counts_ref[d] + (trip - 1)) // trip for d in range(n_dest)]

    def row_copy(d, s):
        base = pl.multiple_of(jnp.left_shift(jnp.right_shift(loc_ref[s], 3), 3), 8)
        return pltpu.make_async_copy(
            tables_hbm.at[:, pl.ds(base, 8), :], buf.at[:, pl.ds(pl.multiple_of(s * 8, 8), 8), :], sems.at[d])

    for d in range(n_dest):
        def issue(i, carry, d=d):
            for k in range(8):
                row_copy(d, d * cap + i * 8 + k).start()
            return carry

        lax.fori_loop(0, n_trips[d] * (trip // 8), issue, 0)

    for d in range(n_dest):
        def drain(i, carry, d=d):
            part = buf.at[:, pl.ds(pl.multiple_of((d * cap + i * trip) * 8, 8), trip * 8), :]
            pltpu.make_async_copy(part, part, sems.at[d]).wait()
            return carry

        lax.fori_loop(0, n_trips[d], drain, 0)

        def pick(i, carry, d=d):
            for k in range(group):
                s0 = pl.multiple_of(d * cap + i * trip + k * per_dot, per_dot)
                want = pick_ref[pl.ds(s0, per_dot), :]
                sel = (lax.broadcasted_iota(I32, (per_dot, per_dot * 8), 1) == want).astype(BF)
                for l in range(n_layers):
                    rows = buf[l, pl.ds(pl.multiple_of(s0 * 8, 8), per_dot * 8), :]
                    out_ref[l, pl.ds(s0, per_dot), :] = dot(sel, rows).astype(BF)
            return carry

        lax.fori_loop(0, n_trips[d], pick, 0)

        def blank(i, carry, d=d):
            s0 = pl.multiple_of(d * cap + i * trip, trip)
            for l in range(n_layers):
                out_ref[l, pl.ds(s0, trip), :] = jnp.zeros((trip, out_ref.shape[2]), BF)
            return carry

        lax.fori_loop(n_trips[d], cap // trip, blank, 0)


def mlp_block(cfg, u_s, h_s, acc_s, wu_ref, wd_ref, up_ref):
    cw, nw = cfg
    for c in range(wu_ref.shape[2] // cw):
        cs = slice(c * cw, (c + 1) * cw)
        up = dot(u_s[...], wu_ref[0, :, cs])
        if up_ref is not None:
            up_ref[0, :, cs] = up
        h_s[:, cs] = gelu(up).astype(BF)
    for n in range(acc_s.shape[1] // nw):
        ns = slice(n * nw, (n + 1) * nw)
        acc_s[:, ns] += dot(h_s[...], wd_ref[0, :, ns])


def norm_rows(x, sl, u_s, acc_s):
    scale = lax.rsqrt(jnp.mean(x * x, axis=-1, keepdims=True) + NORM_EPS)
    u_s[sl, :] = (x * scale).astype(BF)
    acc_s[sl, :] = x


def add_proj(nw, acc_s, mixed, wp_ref):
    for n in range(acc_s.shape[1] // nw):
        ns = slice(n * nw, (n + 1) * nw)
        acc_s[:, ns] += dot(mixed, wp_ref[0, :, ns])


def first_kernel(cfg, x_hbm, slot_ref, served_hbm, wg_ref, wp_ref, wu_ref, wd_ref,
                 x_out_ref, gate_ref, fet_ref,
                 u_s, acc_s, h_s, ret_s, in_sem, self_sem, send_sem, recv_sem):
    n_dp, n_emb, cap, cw, nw, slab = cfg
    n_blk = pl.num_programs(0)
    blk = pl.program_id(0)
    tok, dim = u_s.shape
    my_emb = lax.axis_index('emb')
    my_dp = lax.axis_index('dp')
    here = ret_s.at[:, pl.ds(pl.multiple_of(my_emb * cap, cap), cap), :]
    own = pltpu.make_async_copy(served_hbm.at[:, pl.ds(pl.multiple_of(my_emb * cap, cap), cap), :], here, self_sem)
    peers = [lax.rem(my_emb + k, n_emb) for k in range(1, n_emb)]
    copies = [remote(served_hbm.at[:, pl.ds(pl.multiple_of(p * cap, cap), cap), :], here,
                     send_sem.at[k], recv_sem.at[k], {'dp': my_dp, 'emb': p}) for k, p in enumerate(peers)]

    @pl.when(blk == 0)
    def _():
        fetch = pltpu.make_async_copy(x_hbm, x_out_ref, in_sem)
        fetch.start()
        meet([{'dp': my_dp, 'emb': p} for p in peers])
        own.start()
        for copy in copies:
            copy.start()
        fetch.wait()
        row_loop(tok, slab)(lambda sl: norm_rows(x_out_ref[sl, :].astype(F32), sl, u_s, acc_s))
        gate_ref[0] = dot(u_s[...], wg_ref[0])

    mlp_block((cw, nw), u_s, h_s, acc_s, wu_ref, wd_ref, None)

    @pl.when(blk == n_blk - 1)
    def _():
        own.wait()
        for copy in copies:
            copy.wait()
        sel = (lax.broadcasted_iota(I32, (tok, n_emb * cap), 1) == slot_ref[...]).astype(BF)
        for l in range(fet_ref.shape[0]):
            fet_ref[l] = dot(sel, ret_s[l]).astype(BF)
        add_proj(nw, acc_s, (gelu(gate_ref[0]) * fet_ref[0].astype(F32)).astype(BF), wp_ref)

        def finish(sl):
            x_out_ref[sl, :] = acc_s[sl, :].astype(BF)

        row_loop(tok, slab)(finish)


def forward_kernel(cfg, x_hbm, cot_hbm, fet_ref, wg_ref, wp_ref, wu_ref, wd_ref,
                   out_hbm, saved_hbm, up_ref, gate_ref, rows_ref, dgp_ref, dtab_hbm,
                   x_s, u_s, acc_s, h_s, zero_s, in_sem, out_sem, z_sem):
    n_layers, n_blk, cw, nw, slab, z_per, z_chunks = cfg
    layer, blk = pl.program_id(0), pl.program_id(1)
    tok, dim = x_s.shape
    step = layer * n_blk + blk
    z_rows = zero_s.shape[0]

    def z_copy(j):
        c = step * z_per + j
        zl = c // z_chunks
        zc = c - zl * z_chunks
        return pltpu.make_async_copy(zero_s, dtab_hbm.at[zl, pl.ds(pl.multiple_of(zc * z_rows, 8), z_rows), :], z_sem.at[j])

    @pl.when(step == 0)
    def _():
        fetch = pltpu.make_async_copy(x_hbm, x_s, in_sem)
        fetch.start()
        row_loop(z_rows, 8, 1)(lambda sl: zero_s.__setitem__((sl, slice(None)), jnp.zeros((8, zero_s.shape[1]), F32)))
        fetch.wait()
        row_loop(tok, slab)(lambda sl: norm_rows(x_s[sl, :].astype(F32), sl, u_s, acc_s))

    for j in range(z_per):
        @pl.when(step > 0)
        def _():
            z_copy(j).wait()

        z_copy(j).start()

    @pl.when(blk == 0)
    def _():
        gate_ref[0] = dot(u_s[...], wg_ref[0])

    mlp_block((cw, nw), u_s, h_s, acc_s, wu_ref, wd_ref, up_ref)

    @pl.when(blk == n_blk - 1)
    def _():
        add_proj(nw, acc_s, (gelu(gate_ref[0]) * fet_ref[0].astype(F32)).astype(BF), wp_ref)

        @pl.when(layer > 0)
        def _():
            pltpu.make_async_copy(x_s, saved_hbm.at[layer - 1], out_sem).wait()

        def next_rows(sl):
            x_new = acc_s[sl, :].astype(BF)
            x_s[sl, :] = x_new
            norm_rows(x_new.astype(F32), sl, u_s, acc_s)

        row_loop(tok, slab)(next_rows)

        @pl.when(layer < n_layers - 1)
        def _():
            pltpu.make_async_copy(x_s, saved_hbm.at[layer], out_sem).start()

        @pl.when(layer == n_layers - 1)
        def _():
            put = pltpu.make_async_copy(x_s, out_hbm, out_sem)
            put.start()
            get = pltpu.make_async_copy(cot_hbm, u_s, in_sem)
            get.start()
            for j in range(z_per):
                z_copy(j).wait()
            get.wait()
            d_mixed = dot_t(u_s[...], wp_ref[0]).astype(BF).astype(F32)
            gate_grads(gate_ref[0], fet_ref[0], d_mixed, rows_ref, dgp_ref)
            put.wait()


def gate_grads(gate_pre, fetched, d_mixed, rows_ref, dgp_ref):
    rows_ref[...] = gelu(gate_pre) * d_mixed
    dgp_ref[...] = (d_mixed * fetched.astype(F32) * gelu_slope(gate_pre)).astype(BF)


def to_slots(rows, slot_ref, slots_s):
    hi = rows.astype(BF)
    rest = rows - hi.astype(F32)
    mid = rest.astype(BF)
    low = (rest - mid.astype(F32)).astype(BF)
    n, tok = slots_s.shape[0], rows.shape[0]
    sel = (lax.broadcasted_iota(I32, (n, tok), 0) == slot_ref[...]).astype(BF)
    slots_s[...] = (dot(sel, hi) + dot(sel, mid)) + dot(sel, low)


def backward_kernel(cfg, cot_hbm, x1_hbm, saved_hbm, rows_in_ref, dgp_in_ref, slot_ref, gate0_ref,
                    up_ref, wu_ref, wd_ref, wg_ref, wp_ref, gate_ref, fet_ref,
                    got_hbm, slots0_hbm,
                    cot_s, x_s, acc_s, dup_s, dng_s, slots_s, rows_s, dgp_s, in_sem, x_sem, put_sem, send_sem, self_sem, recv_sem):
    n_layers, n_blk, n_dp, n_emb, cap, cw, nw, slab = cfg
    i, blk = pl.program_id(0), pl.program_id(1)
    layer = n_layers - i
    tok, dim = cot_s.shape
    fb = wu_ref.shape[2]
    n_dev = n_dp * n_emb
    me = lax.axis_index('dp') * n_emb + lax.axis_index('emb')
    peers = [peer_of(n_emb, lax.rem(me + k, n_dev)) for k in range(1, n_dev)]
    here = got_hbm.at[layer - 1, pl.ds(pl.multiple_of(me * cap, cap), cap), :]

    def part(emb):
        return slots_s.at[pl.ds(pl.multiple_of(emb * cap, cap), cap), :]

    own = pltpu.make_async_copy(part(lax.axis_index('emb')), here, self_sem)
    copies = [remote(part(peer['emb']), here, send_sem.at[k], recv_sem.at[i, k], peer) for k, peer in enumerate(peers)]

    @pl.when(blk == 0)
    def _():
        @pl.when(i == 0)
        def _():
            fetch = pltpu.make_async_copy(cot_hbm, cot_s, in_sem)
            fetch.start()
            rows_s[...] = rows_in_ref[...]
            dgp_s[...] = dgp_in_ref[...]
            meet(peers)
            fetch.wait()

        @pl.when(i < n_layers - 1)
        def _():
            pltpu.make_async_copy(saved_hbm.at[n_layers - 2 - i], x_s, x_sem).start()

        @pl.when(i == n_layers - 1)
        def _():
            pltpu.make_async_copy(x1_hbm, x_s, x_sem).start()

        to_slots(rows_s[...], slot_ref, slots_s)
        for n in range(dim // nw):
            ns = slice(n * nw, (n + 1) * nw)
            dng_s[:, ns] = dot_t(dgp_s[...], wg_ref[0, ns, :]).astype(BF)

        def clear(sl):
            acc_s[sl, :] = jnp.zeros((slab, dim), F32)

        row_loop(tok, slab)(clear)

    @pl.when(blk == 1)
    def _():
        own.start()
        for copy in copies:
            copy.start()

    for c in range(fb // cw):
        cs = slice(c * cw, (c + 1) * cw)
        d_hid = dot_t(cot_s[...], wd_ref[0, cs, :]).astype(BF).astype(F32)
        dup_s[:, cs] = (d_hid * gelu_slope(up_ref[0, :, cs])).astype(BF)
    for n in range(dim // nw):
        ns = slice(n * nw, (n + 1) * nw)
        acc_s[:, ns] += dot_t(dup_s[...], wu_ref[0, ns, :])

    @pl.when(blk == n_blk - 1)
    def _():
        pltpu.make_async_copy(x1_hbm, x_s, x_sem).wait()

        def rows_back(sl):
            x = x_s[sl, :].astype(F32)
            scale = lax.rsqrt(jnp.mean(x * x, axis=-1, keepdims=True) + NORM_EPS)
            d_n = (acc_s[sl, :].astype(BF).astype(F32) + dng_s[sl, :].astype(F32)).astype(BF).astype(F32)
            proj = jnp.mean(d_n * x, axis=-1, keepdims=True)
            d_x = d_n * scale - x * (proj * (scale * scale * scale))
            cot_s[sl, :] = (cot_s[sl, :].astype(F32) + d_x).astype(BF)

        row_loop(tok, slab)(rows_back)
        d_mixed = dot_t(cot_s[...], wp_ref[0]).astype(BF).astype(F32)
        gate = jnp.where(i < n_layers - 1, gate_ref[0], gate0_ref[0])
        gate_grads(gate, fet_ref[0], d_mixed, rows_s, dgp_s)
        own.wait()
        for copy in copies:
            copy.wait()

        @pl.when(i == n_layers - 1)
        def _():
            to_slots(rows_s[...], slot_ref, slots_s)
            puts = [pltpu.make_async_copy(slots_s, slots0_hbm.at[d], put_sem.at[d]) for d in range(n_dp)]
            for put in puts:
                put.start()
            for put in puts:
                put.wait()


def scatter_kernel(cfg, keys_ref, meta_ref, rows_ref, dt_in, dt_out, sums, sem):
    first_layer, slot_bits, unroll, bulk = cfg
    count = meta_ref[0]
    n_layers, _, e_dim = rows_ref.shape
    trips = (count + (unroll - 1)) // unroll

    def add(t, carry):
        prev, accs = carry
        for k in range(unroll):
            j = t * unroll + k
            key = keys_ref[j]
            slot = jnp.bitwise_and(key, (1 << slot_bits) - 1)
            row = jnp.right_shift(key, slot_bits)
            same = row == prev
            accs = tuple(jnp.where(same, acc, 0.0) + rows_ref[l, pl.ds(slot, 1), :] for l, acc in enumerate(accs))
            for l in range(n_layers):
                sums[l, pl.ds(j, 1), :] = accs[l]
            prev = row
        return prev, accs

    lax.fori_loop(0, trips, add, (jnp.int32(-1), tuple(jnp.zeros((1, e_dim), F32) for _ in range(n_layers))))

    def move(j, row, n):
        return pltpu.make_async_copy(sums.at[:, pl.ds(j, n), :], dt_out.at[pl.ds(first_layer, n_layers), pl.ds(row, n), :], sem)

    def put(t, carry):
        n, row = carry
        for k in range(unroll):
            j = t * unroll + k
            follow = jnp.right_shift(keys_ref[j + 1], slot_bits)
            last = jnp.logical_and(row != follow, j < count)

            @pl.when(last)
            def _(j=j, row=row):
                move(j, row, 1).start()

            n = n + last.astype(I32)
            row = follow
        return n, row

    n_rows, _ = lax.fori_loop(0, trips, put, (jnp.int32(0), jnp.right_shift(keys_ref[0], slot_bits)))

    def drain_bulk(j, carry):
        move(0, 0, bulk).wait()
        return carry

    def drain(j, carry):
        move(0, 0, 1).wait()
        return carry

    lax.fori_loop(0, n_rows // bulk, drain_bulk, 0)
    lax.fori_loop(0, lax.rem(n_rows, bulk), drain, 0)


def solution(mesh):
    n_emb, n_dp = mesh.shape['emb'], mesh.shape['dp']
    n_dev = n_emb * n_dp
    tok_spec = P(('dp', 'emb'))
    act_spec = P(('dp', 'emb'), None)
    table_spec = P(None, 'emb', None)
    full_spec = P(None, None, None)
    hbm = pl.BlockSpec(memory_space=pl.ANY)
    vm = pl.BlockSpec(memory_space=pltpu.VMEM)
    sm = pl.BlockSpec(memory_space=pltpu.SMEM)
    big = jnp.iinfo(jnp.int32).max

    def params(n_grid, **kw):
        return pltpu.CompilerParams(vmem_limit_bytes=VMEM_BYTES, dimension_semantics=('arbitrary',) * n_grid if n_grid else None, **kw)

    def device_body(tok_ids, resid_in, cot_out, tables, w_up, w_down, w_gate, w_proj):
        n_layers, range_rows, e_dim = tables.shape
        tok = tok_ids.shape[0]
        dim, ffn = w_up.shape[1:]
        n_slots, n_serve = n_dev * CAP, n_emb * CAP
        my_emb, my_dp = lax.axis_index('emb'), lax.axis_index('dp')

        lanes = 128
        ids8 = pl.pallas_call(
            functools.partial(ids_kernel, (n_dp, n_emb)),
            out_shape=jax.ShapeDtypeStruct((n_dev, tok // lanes, lanes), I32),
            in_specs=[vm], out_specs=vm,
            scratch_shapes=[pltpu.SemaphoreType.DMA((n_dev - 1,)), pltpu.SemaphoreType.DMA((n_dev - 1,))],
            compiler_params=pltpu.CompilerParams(collective_id=0, has_side_effects=True),
            name='all_ids',
        )(tok_ids.reshape(tok // lanes, lanes)).reshape(n_dev, tok)
        mine = (ids8 // range_rows) == my_emb
        t_iota = jnp.arange(tok, dtype=I32)
        before = t_iota[None, :] < t_iota[:, None]
        rank8 = jnp.sum((mine[:, None, :] & before[None]).astype(I32), axis=-1)
        c_iota = jnp.arange(CAP, dtype=I32)
        hit = mine[:, None, :] & (rank8[:, None, :] == c_iota[None, :, None])
        recv_loc = jnp.sum(jnp.where(hit, (ids8 - my_emb * range_rows)[:, None, :], 0), axis=-1)
        counts = jnp.sum(mine.astype(I32), axis=-1)
        valid = c_iota[None, :] < counts[:, None]
        slot_bits = (n_slots - 1).bit_length()
        slot_ids = jnp.arange(n_slots, dtype=I32).reshape(n_dev, CAP)
        keys = jnp.where(valid, recv_loc * (1 << slot_bits) + slot_ids, big)
        skeys = jnp.concatenate([lax.sort(keys.reshape(-1)), jnp.full((16,), big, I32)])
        total = jnp.sum(counts).reshape(1)

        my_owner = tok_ids // range_rows
        rank = jnp.sum(((my_owner[None, :] == my_owner[:, None]) & before).astype(I32), axis=-1)
        slot_of = my_owner * CAP + rank

        spread = jnp.where(valid, recv_loc, lax.rem(slot_ids * 8, range_rows))
        want = lax.dynamic_slice_in_dim(spread, my_dp * n_emb, n_emb, 0).reshape(-1)
        n_want = lax.dynamic_slice_in_dim(counts, my_dp * n_emb, n_emb, 0)
        per_dot, group = 32, 2
        pick = (jnp.bitwise_and(want, 7) + 8 * (jnp.arange(n_serve, dtype=I32) % per_dot))[:, None]
        served = pl.pallas_call(
            functools.partial(gather_kernel, (n_layers, n_emb, CAP, per_dot, group)),
            out_shape=jax.ShapeDtypeStruct((n_layers, n_serve, e_dim), BF),
            in_specs=[sm, sm, vm, hbm],
            out_specs=vm,
            scratch_shapes=[pltpu.VMEM((n_layers, n_serve * 8, e_dim), BF), pltpu.SemaphoreType.DMA((n_emb,))],
            compiler_params=params(0),
            name='table_rows',
        )(want, n_want, pick, tables)

        fb = 1024
        n_blk = ffn // fb
        cw, nw, slab = 512, 512, 16
        n_back = n_layers - 1
        z_rows = 1336
        z_chunks = range_rows // z_rows
        z_per = n_layers * z_chunks // (n_back * n_blk)
        assert z_chunks * z_rows == range_rows and z_per * n_blk * n_back == z_chunks * n_layers

        def flat(*shape):
            return pl.BlockSpec(shape, lambda *_: (0,) * len(shape), pipeline_mode=pl.Buffered(1))

        matmul_flops = 4 * tok * dim * ffn
        x1, gate0, fetched = pl.pallas_call(
            functools.partial(first_kernel, (n_dp, n_emb, CAP, cw, nw, slab)),
            grid=(n_blk,),
            out_shape=[
                jax.ShapeDtypeStruct((tok, dim), BF),
                jax.ShapeDtypeStruct((1, tok, e_dim), F32),
                jax.ShapeDtypeStruct((n_layers, tok, e_dim), BF),
            ],
            in_specs=[hbm, flat(tok, 1), hbm, flat(1, dim, e_dim), flat(1, e_dim, dim),
                      pl.BlockSpec((1, dim, fb), lambda f: (0, 0, f)), pl.BlockSpec((1, fb, dim), lambda f: (0, f, 0))],
            out_specs=[flat(tok, dim), flat(1, tok, e_dim), flat(n_layers, tok, e_dim)],
            scratch_shapes=[
                pltpu.VMEM((tok, dim), BF), pltpu.VMEM((tok, dim), F32), pltpu.VMEM((tok, fb), BF),
                pltpu.VMEM((n_layers, n_serve, e_dim), BF), pltpu.SemaphoreType.DMA, pltpu.SemaphoreType.DMA,
                pltpu.SemaphoreType.DMA((n_emb - 1,)), pltpu.SemaphoreType.DMA((n_emb - 1,)),
            ],
            compiler_params=params(1, collective_id=1, has_side_effects=True),
            cost_estimate=pl.CostEstimate(flops=matmul_flops, bytes_accessed=100 << 20, transcendentals=0),
            name='first_layer',
        )(resid_in, slot_of[:, None], served, w_gate, w_proj, w_up, w_down)

        def lsp(*shape):
            return pl.BlockSpec((1,) + shape, lambda l, f: (l + 1, 0, 0))

        out, saved, ups, gates, rows, dgp, dtab = pl.pallas_call(
            functools.partial(forward_kernel, (n_back, n_blk, cw, nw, slab, z_per, z_chunks)),
            grid=(n_back, n_blk),
            out_shape=[
                jax.ShapeDtypeStruct((tok, dim), BF),
                jax.ShapeDtypeStruct((n_back - 1, tok, dim), BF),
                jax.ShapeDtypeStruct((n_back, tok, ffn), F32),
                jax.ShapeDtypeStruct((n_back, tok, e_dim), F32),
                jax.ShapeDtypeStruct((tok, e_dim), F32),
                jax.ShapeDtypeStruct((tok, e_dim), BF),
                jax.ShapeDtypeStruct((n_layers, range_rows, e_dim), F32),
            ],
            in_specs=[hbm, hbm, lsp(tok, e_dim), lsp(dim, e_dim), lsp(e_dim, dim),
                      pl.BlockSpec((1, dim, fb), lambda l, f: (l + 1, 0, f)), pl.BlockSpec((1, fb, dim), lambda l, f: (l + 1, f, 0))],
            out_specs=[hbm, hbm,
                       pl.BlockSpec((1, tok, fb), lambda l, f: (l, 0, f)),
                       pl.BlockSpec((1, tok, e_dim), lambda l, f: (l, 0, 0)),
                       flat(tok, e_dim), flat(tok, e_dim), hbm],
            scratch_shapes=[
                pltpu.VMEM((tok, dim), BF), pltpu.VMEM((tok, dim), BF), pltpu.VMEM((tok, dim), F32), pltpu.VMEM((tok, fb), BF),
                pltpu.VMEM((z_rows, e_dim), F32), pltpu.SemaphoreType.DMA, pltpu.SemaphoreType.DMA, pltpu.SemaphoreType.DMA((z_per,)),
            ],
            compiler_params=params(2),
            cost_estimate=pl.CostEstimate(flops=n_back * matmul_flops, bytes_accessed=400 << 20, transcendentals=0),
            name='forward',
        )(x1, cot_out, fetched, w_gate, w_proj, w_up, w_down)

        def of_layer(off, *shape):
            return pl.BlockSpec((1,) + shape, lambda i, f: (jnp.maximum(n_back - i + off, 0), 0, 0))

        got, slots0 = pl.pallas_call(
            functools.partial(backward_kernel, (n_back, n_blk, n_dp, n_emb, CAP, cw, nw, slab)),
            grid=(n_back, n_blk),
            out_shape=[jax.ShapeDtypeStruct((n_back, n_slots, e_dim), F32), jax.ShapeDtypeStruct((n_dp, n_serve, e_dim), F32)],
            in_specs=[hbm, hbm, hbm, flat(tok, e_dim), flat(tok, e_dim), flat(1, tok), flat(1, tok, e_dim),
                      pl.BlockSpec((1, tok, fb), lambda i, f: (n_back - 1 - i, 0, f)),
                      pl.BlockSpec((1, dim, fb), lambda i, f: (n_back - i, 0, f)), pl.BlockSpec((1, fb, dim), lambda i, f: (n_back - i, f, 0)),
                      of_layer(0, dim, e_dim), of_layer(-1, e_dim, dim), of_layer(-2, tok, e_dim), of_layer(-1, tok, e_dim)],
            out_specs=[hbm, hbm],
            scratch_shapes=[
                pltpu.VMEM((tok, dim), BF), pltpu.VMEM((tok, dim), BF), pltpu.VMEM((tok, dim), F32), pltpu.VMEM((tok, fb), BF),
                pltpu.VMEM((tok, dim), BF), pltpu.VMEM((n_serve, e_dim), F32), pltpu.VMEM((tok, e_dim), F32), pltpu.VMEM((tok, e_dim), BF),
                pltpu.SemaphoreType.DMA, pltpu.SemaphoreType.DMA, pltpu.SemaphoreType.DMA((n_dp,)),
                pltpu.SemaphoreType.DMA((n_dev - 1,)), pltpu.SemaphoreType.DMA, pltpu.SemaphoreType.DMA((n_back, n_dev - 1)),
            ],
            compiler_params=params(2, collective_id=2, has_side_effects=True),
            cost_estimate=pl.CostEstimate(flops=n_back * matmul_flops, bytes_accessed=400 << 20, transcendentals=0),
            name='backward',
        )(cot_out, x1, saved, rows, dgp, slot_of[None, :], gate0, ups, w_up, w_down, w_gate, w_proj, gates, fetched)

        def scatter(first_layer, rows_in, dtab):
            n = rows_in.shape[0]
            return pl.pallas_call(
                functools.partial(scatter_kernel, (first_layer, slot_bits, 8, 64)),
                out_shape=jax.ShapeDtypeStruct(dtab.shape, F32),
                in_specs=[sm, sm, vm, hbm],
                out_specs=hbm,
                input_output_aliases={3: 0},
                scratch_shapes=[pltpu.VMEM((n, n_slots + 8, e_dim), F32), pltpu.SemaphoreType.DMA],
                compiler_params=params(0),
                cost_estimate=pl.CostEstimate(flops=n * 20_000_000_000, bytes_accessed=n << 22, transcendentals=0),
                name=f'scatter_{first_layer}',
            )(skeys, total, rows_in, dtab)

        got0 = lax.all_to_all(slots0.reshape(n_dev, CAP, e_dim), MESH_AXES, 0, 0, tiled=True).reshape(1, n_slots, e_dim)
        dtab = scatter(1, got, dtab)
        dtab = scatter(0, got0, dtab)
        return out, dtab

    return jax.shard_map(device_body, mesh=mesh, in_specs=(tok_spec, act_spec, act_spec, table_spec, full_spec, full_spec, full_spec, full_spec), out_specs=(act_spec, table_spec), check_vma=False)
```

```python
import functools

import jax
import jax.numpy as jnp
from jax import lax
from jax.experimental import pallas as pl
from jax.experimental.pallas import tpu as pltpu
from jax.sharding import PartitionSpec as P

NORM_EPS = 1e-6
BF = jnp.bfloat16
F32 = jnp.float32
I32 = jnp.int32
VMEM_BYTES = 67043328
GELU_C = 0.7978845608028654
GELU_A = 0.044715

MESH_AXES = ('dp', 'emb')
CAP = 256


def gelu(x):
    return 0.5 * x * (1.0 + jnp.tanh(GELU_C * (x + GELU_A * (x * x * x))))


def gelu_slope(x):
    sq = x * x
    th = jnp.tanh(GELU_C * (x + GELU_A * (x * sq)))
    return 0.5 * (1.0 + th) + (0.5 * GELU_C) * x * (1.0 - th * th) * (1.0 + (3 * GELU_A) * sq)


def dot(a, b):
    return jnp.dot(a, b, preferred_element_type=F32)


def dot_t(a, b):
    return lax.dot_general(a, b, (((1,), (1,)), ((), ())), preferred_element_type=F32)


def row_loop(rows, slab, unroll=2):
    def run(body):
        def step(i, carry):
            body(pl.ds(pl.multiple_of(i * slab, slab), slab))
            return carry

        lax.fori_loop(0, rows // slab, step, 0, unroll=unroll)

    return run


def peer_of(n_emb, index):
    dp = index // n_emb
    return {'dp': dp, 'emb': index - dp * n_emb}


def remote(src, dst, send_sem, recv_sem, device):
    return pltpu.make_async_remote_copy(src_ref=src, dst_ref=dst, send_sem=send_sem, recv_sem=recv_sem,
                                        device_id=device, device_id_type=pl.DeviceIdType.MESH)


def meet(devices):
    barrier = pltpu.get_barrier_semaphore()
    for device in devices:
        pl.semaphore_signal(barrier, inc=1, device_id=device, device_id_type=pl.DeviceIdType.MESH)
    pl.semaphore_wait(barrier, len(devices))


def ids_kernel(cfg, in_ref, out_ref, send_sem, recv_sem):
    n_dp, n_emb = cfg
    n_dev = n_dp * n_emb
    me = lax.axis_index('dp') * n_emb + lax.axis_index('emb')
    peers = [peer_of(n_emb, lax.rem(me + k, n_dev)) for k in range(1, n_dev)]
    meet(peers)
    copies = [remote(in_ref, out_ref.at[me], send_sem.at[k], recv_sem.at[k], peer) for k, peer in enumerate(peers)]
    for copy in copies:
        copy.start()
    out_ref[me] = in_ref[...]
    for copy in copies:
        copy.wait()


def gather_kernel(cfg, loc_ref, counts_ref, pick_ref, tables_hbm, out_ref, buf, sems):
    n_layers, n_dest, cap, per_dot, group = cfg
    trip = per_dot * group
    n_trips = [(counts_ref[d] + (trip - 1)) // trip for d in range(n_dest)]

    def row_copy(d, s):
        base = pl.multiple_of(jnp.left_shift(jnp.right_shift(loc_ref[s], 3), 3), 8)
        return pltpu.make_async_copy(
            tables_hbm.at[:, pl.ds(base, 8), :], buf.at[:, pl.ds(pl.multiple_of(s * 8, 8), 8), :], sems.at[d])

    for d in range(n_dest):
        def issue(i, carry, d=d):
            for k in range(8):
                row_copy(d, d * cap + i * 8 + k).start()
            return carry

        lax.fori_loop(0, n_trips[d] * (trip // 8), issue, 0)

    for d in range(n_dest):
        def drain(i, carry, d=d):
            part = buf.at[:, pl.ds(pl.multiple_of((d * cap + i * trip) * 8, 8), trip * 8), :]
            pltpu.make_async_copy(part, part, sems.at[d]).wait()
            return carry

        lax.fori_loop(0, n_trips[d], drain, 0)

        def pick(i, carry, d=d):
            for k in range(group):
                s0 = pl.multiple_of(d * cap + i * trip + k * per_dot, per_dot)
                want = pick_ref[pl.ds(s0, per_dot), :]
                sel = (lax.broadcasted_iota(I32, (per_dot, per_dot * 8), 1) == want).astype(BF)
                for l in range(n_layers):
                    rows = buf[l, pl.ds(pl.multiple_of(s0 * 8, 8), per_dot * 8), :]
                    out_ref[l, pl.ds(s0, per_dot), :] = dot(sel, rows).astype(BF)
            return carry

        lax.fori_loop(0, n_trips[d], pick, 0)

        def blank(i, carry, d=d):
            s0 = pl.multiple_of(d * cap + i * trip, trip)
            for l in range(n_layers):
                out_ref[l, pl.ds(s0, trip), :] = jnp.zeros((trip, out_ref.shape[2]), BF)
            return carry

        lax.fori_loop(n_trips[d], cap // trip, blank, 0)


def mlp_block(cfg, u_s, h_s, acc_s, wu_ref, wd_ref, up_ref):
    cw, nw = cfg
    gw = 128
    fb = wu_ref.shape[2]

    def act(c):
        for g in range(cw // gw):
            gs = slice(c * cw + g * gw, c * cw + (g + 1) * gw)
            h_s[:, gs] = gelu(up_ref[0, :, gs]).astype(BF)

    n_c = fb // cw
    for c in range(n_c):
        cs = slice(c * cw, (c + 1) * cw)
        up_ref[0, :, cs] = dot(u_s[...], wu_ref[0, :, cs])
        if c > 0:
            act(c - 1)
    for c in range(n_c):
        cs = slice(c * cw, (c + 1) * cw)
        for n in range(acc_s.shape[1] // nw):
            ns = slice(n * nw, (n + 1) * nw)
            acc_s[:, ns] += dot(h_s[:, cs], wd_ref[0, cs, ns])
        if c == 0:
            act(n_c - 1)


def norm_rows(x, sl, u_s, acc_s):
    scale = lax.rsqrt(jnp.mean(x * x, axis=-1, keepdims=True) + NORM_EPS)
    u_s[sl, :] = (x * scale).astype(BF)
    acc_s[sl, :] = x


def add_proj(nw, acc_s, mixed, wp_ref):
    for n in range(acc_s.shape[1] // nw):
        ns = slice(n * nw, (n + 1) * nw)
        acc_s[:, ns] += dot(mixed, wp_ref[0, :, ns])


def first_kernel(cfg, x_hbm, slot_ref, served_hbm, wg_ref, wp_ref, wu_ref, wd_ref,
                 x_out_ref, gate_ref, fet_ref,
                 u_s, acc_s, h_s, up_s, ret_s, in_sem, self_sem, send_sem, recv_sem):
    n_dp, n_emb, cap, cw, nw, slab = cfg
    n_blk = pl.num_programs(0)
    blk = pl.program_id(0)
    tok, dim = u_s.shape
    my_emb = lax.axis_index('emb')
    my_dp = lax.axis_index('dp')
    here = ret_s.at[:, pl.ds(pl.multiple_of(my_emb * cap, cap), cap), :]
    own = pltpu.make_async_copy(served_hbm.at[:, pl.ds(pl.multiple_of(my_emb * cap, cap), cap), :], here, self_sem)
    peers = [lax.rem(my_emb + k, n_emb) for k in range(1, n_emb)]
    copies = [remote(served_hbm.at[:, pl.ds(pl.multiple_of(p * cap, cap), cap), :], here,
                     send_sem.at[k], recv_sem.at[k], {'dp': my_dp, 'emb': p}) for k, p in enumerate(peers)]

    @pl.when(blk == 0)
    def _():
        fetch = pltpu.make_async_copy(x_hbm, x_out_ref, in_sem)
        fetch.start()
        meet([{'dp': my_dp, 'emb': p} for p in peers])
        own.start()
        for copy in copies:
            copy.start()
        fetch.wait()
        row_loop(tok, slab)(lambda sl: norm_rows(x_out_ref[sl, :].astype(F32), sl, u_s, acc_s))
        gate_ref[0] = dot(u_s[...], wg_ref[0])

    mlp_block((cw, nw), u_s, h_s, acc_s, wu_ref, wd_ref, up_s)

    @pl.when(blk == n_blk - 1)
    def _():
        own.wait()
        for copy in copies:
            copy.wait()
        sel = (lax.broadcasted_iota(I32, (tok, n_emb * cap), 1) == slot_ref[...]).astype(BF)
        for l in range(fet_ref.shape[0]):
            fet_ref[l] = dot(sel, ret_s[l]).astype(BF)
        add_proj(nw, acc_s, (gelu(gate_ref[0]) * fet_ref[0].astype(F32)).astype(BF), wp_ref)

        def finish(sl):
            x_out_ref[sl, :] = acc_s[sl, :].astype(BF)

        row_loop(tok, slab)(finish)


def forward_kernel(cfg, x_hbm, cot_hbm, fet_ref, wg_ref, wp_ref, wu_ref, wd_ref,
                   out_hbm, saved_hbm, up_ref, gate_ref, rows_ref, dgp_ref, dtab_hbm,
                   x_s, u_s, acc_s, h_s, zero_s, in_sem, out_sem, z_sem):
    n_layers, n_blk, cw, nw, slab, z_per, z_chunks = cfg
    layer, blk = pl.program_id(0), pl.program_id(1)
    tok, dim = x_s.shape
    step = layer * n_blk + blk
    z_rows = zero_s.shape[0]

    def z_copy(j):
        c = step * z_per + j
        zl = c // z_chunks
        zc = c - zl * z_chunks
        return pltpu.make_async_copy(zero_s, dtab_hbm.at[zl, pl.ds(pl.multiple_of(zc * z_rows, 8), z_rows), :], z_sem.at[j])

    @pl.when(step == 0)
    def _():
        fetch = pltpu.make_async_copy(x_hbm, x_s, in_sem)
        fetch.start()
        row_loop(z_rows, 8, 1)(lambda sl: zero_s.__setitem__((sl, slice(None)), jnp.zeros((8, zero_s.shape[1]), F32)))
        fetch.wait()
        row_loop(tok, slab)(lambda sl: norm_rows(x_s[sl, :].astype(F32), sl, u_s, acc_s))

    for j in range(z_per):
        @pl.when(step > 0)
        def _():
            z_copy(j).wait()

        z_copy(j).start()

    @pl.when(blk == 0)
    def _():
        gate_ref[0] = dot(u_s[...], wg_ref[0])

    mlp_block((cw, nw), u_s, h_s, acc_s, wu_ref, wd_ref, up_ref)

    @pl.when(blk == n_blk - 1)
    def _():
        add_proj(nw, acc_s, (gelu(gate_ref[0]) * fet_ref[0].astype(F32)).astype(BF), wp_ref)

        @pl.when(layer > 0)
        def _():
            pltpu.make_async_copy(x_s, saved_hbm.at[layer - 1], out_sem).wait()

        def next_rows(sl):
            x_new = acc_s[sl, :].astype(BF)
            x_s[sl, :] = x_new
            norm_rows(x_new.astype(F32), sl, u_s, acc_s)

        row_loop(tok, slab)(next_rows)

        @pl.when(layer < n_layers - 1)
        def _():
            pltpu.make_async_copy(x_s, saved_hbm.at[layer], out_sem).start()

        @pl.when(layer == n_layers - 1)
        def _():
            put = pltpu.make_async_copy(x_s, out_hbm, out_sem)
            put.start()
            get = pltpu.make_async_copy(cot_hbm, u_s, in_sem)
            get.start()
            for j in range(z_per):
                z_copy(j).wait()
            get.wait()
            d_mixed = dot_t(u_s[...], wp_ref[0]).astype(BF).astype(F32)
            gate_grads(gate_ref[0], fet_ref[0], d_mixed, rows_ref, dgp_ref)
            put.wait()


def gate_grads(gate_pre, fetched, d_mixed, rows_ref, dgp_ref):
    rows_ref[...] = gelu(gate_pre) * d_mixed
    dgp_ref[...] = (d_mixed * fetched.astype(F32) * gelu_slope(gate_pre)).astype(BF)


def to_slots(rows, slot_ref, slots_s):
    hi = rows.astype(BF)
    rest = rows - hi.astype(F32)
    mid = rest.astype(BF)
    low = (rest - mid.astype(F32)).astype(BF)
    sel = slot_pick(slots_s.shape[0], slot_ref)
    slots_s[...] = (dot(sel, hi) + dot(sel, mid)) + dot(sel, low)


def slot_pick(n, slot_ref):
    return (lax.broadcasted_iota(I32, (n, slot_ref.shape[1]), 0) == slot_ref[...]).astype(BF)


def backward_kernel(cfg, cot_hbm, x1_hbm, saved_hbm, rows_in_ref, dgp_in_ref, slot_ref, gate0_ref,
                    up_ref, wu_ref, wd_ref, wg_ref, wp_ref, gate_ref, fet_ref,
                    got_hbm, gate_hbm, slots0_ref,
                    cot_s, x_s, acc_s, dup_s, dh_s, dng_s, slots_s, gslots_s, rows_s, dgp_s, in_sem, x_sem, send_sem, self_sem, recv_sem):
    n_layers, n_blk, n_dp, n_emb, cap, cw, nw, slab = cfg
    i, blk = pl.program_id(0), pl.program_id(1)
    layer = n_layers - i
    tok, dim = cot_s.shape
    fb = wu_ref.shape[2]
    n_dev = n_dp * n_emb
    me = lax.axis_index('dp') * n_emb + lax.axis_index('emb')
    peers = [peer_of(n_emb, lax.rem(me + k, n_dev)) for k in range(1, n_dev)]
    here = got_hbm.at[layer - 1, pl.ds(pl.multiple_of(me * cap, cap), cap), :]

    g_here = gate_hbm.at[pl.ds(pl.multiple_of(me * cap, cap), cap), :]

    def part(ref, emb):
        return ref.at[pl.ds(pl.multiple_of(emb * cap, cap), cap), :]

    own = pltpu.make_async_copy(part(slots_s, lax.axis_index('emb')), here, self_sem.at[0])
    copies = [remote(part(slots_s, peer['emb']), here, send_sem.at[0, k], recv_sem.at[i, k], peer) for k, peer in enumerate(peers)]
    g_own = pltpu.make_async_copy(part(gslots_s, lax.axis_index('emb')), g_here, self_sem.at[1])
    g_copies = [remote(part(gslots_s, peer['emb']), g_here, send_sem.at[1, k], recv_sem.at[n_layers, k], peer)
                for k, peer in enumerate(peers)]

    @pl.when(blk == 0)
    def _():
        @pl.when(i == 0)
        def _():
            fetch = pltpu.make_async_copy(cot_hbm, cot_s, in_sem)
            fetch.start()
            rows_s[...] = rows_in_ref[...]
            dgp_s[...] = dgp_in_ref[...]
            meet(peers)
            fetch.wait()

        @pl.when(i < n_layers - 1)
        def _():
            pltpu.make_async_copy(saved_hbm.at[n_layers - 2 - i], x_s, x_sem).start()

        @pl.when(i == n_layers - 1)
        def _():
            pltpu.make_async_copy(x1_hbm, x_s, x_sem).start()

        to_slots(rows_s[...], slot_ref, slots_s)
        for n in range(dim // nw):
            ns = slice(n * nw, (n + 1) * nw)
            dng_s[:, ns] = dot_t(dgp_s[...], wg_ref[0, ns, :]).astype(BF)

        def clear(sl):
            acc_s[sl, :] = jnp.zeros((slab, dim), F32)

        row_loop(tok, slab)(clear)

    @pl.when(blk == 1)
    def _():
        own.start()
        for copy in copies:
            copy.start()

    @pl.when((blk == 2) & (i == 0))
    def _():
        to_slots(gelu(gate0_ref[0]), slot_ref, gslots_s)

    @pl.when((blk == 3) & (i == 0))
    def _():
        g_own.start()
        for copy in g_copies:
            copy.start()

    gw = 128

    def act(c):
        for g in range(cw // gw):
            gs = slice(c * cw + g * gw, c * cw + (g + 1) * gw)
            dup_s[:, gs] = (dh_s[:, gs].astype(F32) * gelu_slope(up_ref[0, :, gs])).astype(BF)

    for c in range(fb // cw):
        cs = slice(c * cw, (c + 1) * cw)
        dh_s[:, cs] = dot_t(cot_s[...], wd_ref[0, cs, :]).astype(BF)
        if c > 0:
            act(c - 1)
    for c in range(fb // cw):
        cs = slice(c * cw, (c + 1) * cw)
        for n in range(dim // nw):
            ns = slice(n * nw, (n + 1) * nw)
            acc_s[:, ns] += dot_t(dup_s[:, cs], wu_ref[0, ns, cs])
        if c == 0:
            act(fb // cw - 1)

    @pl.when(blk == n_blk - 1)
    def _():
        pltpu.make_async_copy(x1_hbm, x_s, x_sem).wait()

        def rows_back(sl):
            x = x_s[sl, :].astype(F32)
            scale = lax.rsqrt(jnp.mean(x * x, axis=-1, keepdims=True) + NORM_EPS)
            d_n = (acc_s[sl, :].astype(BF).astype(F32) + dng_s[sl, :].astype(F32)).astype(BF).astype(F32)
            proj = jnp.mean(d_n * x, axis=-1, keepdims=True)
            d_x = d_n * scale - x * (proj * (scale * scale * scale))
            cot_s[sl, :] = (cot_s[sl, :].astype(F32) + d_x).astype(BF)

        row_loop(tok, slab)(rows_back)
        d_mixed = dot_t(cot_s[...], wp_ref[0]).astype(BF)
        own.wait()
        for copy in copies:
            copy.wait()

        @pl.when(i == 0)
        def _():
            g_own.wait()
            for copy in g_copies:
                copy.wait()

        @pl.when(i < n_layers - 1)
        def _():
            gate_grads(gate_ref[0], fet_ref[0], d_mixed.astype(F32), rows_s, dgp_s)

        @pl.when(i == n_layers - 1)
        def _():
            slots = dot(slot_pick(slots_s.shape[0], slot_ref), d_mixed).astype(BF)
            for d in range(n_dp):
                slots0_ref[d] = slots


def scatter_kernel(cfg, keys_ref, meta_ref, *refs):
    first_layer, n_layers, slot_bits, unroll, window, bulk = cfg
    if first_layer == 0:
        gate_ref, mixed_ref, dt_in, dt_out, groups, spots, prod, sems = refs
        n_rows = mixed_ref.shape[0]

        def product(sl):
            prod[0, sl, :] = gate_ref[sl, :] * mixed_ref[sl, :].astype(F32)

        row_loop(n_rows, 64, 4)(product)
        rows_ref = prod
    else:
        rows_ref, dt_in, dt_out, groups, spots, sems = refs
    count = meta_ref[0]
    e_dim = rows_ref.shape[2]
    sub = 8
    n_win = (count + (window - 1)) // window
    lane_row = lax.broadcasted_iota(I32, (sub, e_dim), 0)
    mask = (1 << slot_bits) - 1

    def move(buf, spot, group, n):
        return pltpu.make_async_copy(groups.at[buf, :, pl.ds(spot, n)],
                                     dt_out.at[pl.ds(first_layer, n_layers), pl.ds(group, n)], sems.at[buf])

    def settle(buf, n):
        def drain_bulk(j, carry):
            move(buf, 0, 0, bulk).wait()
            return carry

        def drain(j, carry):
            move(buf, 0, 0, 1).wait()
            return carry

        lax.fori_loop(0, n // bulk, drain_bulk, 0)
        lax.fori_loop(0, lax.rem(n, bulk), drain, 0)

    def run_window(w, carry):
        buf = lax.rem(w, 2)
        prev, accs, older, old = carry
        settle(buf, older)
        stop = jnp.minimum(count, (w + 1) * window)
        trips = (stop - w * window + (unroll - 1)) // unroll

        def add(t, carry):
            prev, n, accs = carry
            for k in range(unroll):
                key = keys_ref[w * window + t * unroll + k]
                slot = jnp.bitwise_and(key, mask)
                row = jnp.right_shift(key, slot_bits)
                group = jnp.right_shift(row, 3)
                same = group == prev
                n = n + jnp.where(same, 0, 1)
                spots[jnp.maximum(n, 0)] = group
                here = lane_row == jnp.bitwise_and(row, sub - 1)
                new = []
                for l, acc in enumerate(accs):
                    row_l = jnp.broadcast_to(rows_ref[l, pl.ds(slot, 1), :], (sub, e_dim))
                    new.append(jnp.where(same, acc, 0.0) + jnp.where(here, row_l, 0.0))
                    groups[buf, l, jnp.maximum(n, 0)] = new[l]
                accs = tuple(new)
                prev = group
            return prev, n, accs

        n0 = jnp.where(jnp.right_shift(keys_ref[w * window], slot_bits + 3) == prev, 0, -1)
        prev, n, accs = lax.fori_loop(0, trips, add, (prev, n0, accs))
        follow = jnp.right_shift(keys_ref[(w + 1) * window], slot_bits + 3)
        padded = trips * unroll > stop - w * window
        goes_on = jnp.logical_and(stop < count, follow == prev)
        n_groups = n + 1 - jnp.where(jnp.logical_or(padded, goes_on), 1, 0)

        def put(u, carry):
            move(buf, u, spots[u], 1).start()
            return carry

        lax.fori_loop(0, n_groups, put, 0)
        return prev, accs, old, n_groups

    zero = jnp.int32(0)
    accs = tuple(jnp.zeros((sub, e_dim), F32) for _ in range(n_layers))
    _, _, older, old = lax.fori_loop(0, n_win, run_window, (jnp.int32(-1), accs, zero, zero))
    settle(lax.rem(n_win, 2), older)
    settle(lax.rem(n_win + 1, 2), old)


def solution(mesh):
    n_emb, n_dp = mesh.shape['emb'], mesh.shape['dp']
    n_dev = n_emb * n_dp
    tok_spec = P(('dp', 'emb'))
    act_spec = P(('dp', 'emb'), None)
    table_spec = P(None, 'emb', None)
    full_spec = P(None, None, None)
    hbm = pl.BlockSpec(memory_space=pl.ANY)
    vm = pl.BlockSpec(memory_space=pltpu.VMEM)
    sm = pl.BlockSpec(memory_space=pltpu.SMEM)
    big = jnp.iinfo(jnp.int32).max

    def params(n_grid, **kw):
        return pltpu.CompilerParams(vmem_limit_bytes=VMEM_BYTES, dimension_semantics=('arbitrary',) * n_grid if n_grid else None, **kw)

    def device_body(tok_ids, resid_in, cot_out, tables, w_up, w_down, w_gate, w_proj):
        n_layers, range_rows, e_dim = tables.shape
        tok = tok_ids.shape[0]
        dim, ffn = w_up.shape[1:]
        n_slots, n_serve = n_dev * CAP, n_emb * CAP
        my_emb, my_dp = lax.axis_index('emb'), lax.axis_index('dp')

        lanes = 128
        ids8 = pl.pallas_call(
            functools.partial(ids_kernel, (n_dp, n_emb)),
            out_shape=jax.ShapeDtypeStruct((n_dev, tok // lanes, lanes), I32),
            in_specs=[vm], out_specs=vm,
            scratch_shapes=[pltpu.SemaphoreType.DMA((n_dev - 1,)), pltpu.SemaphoreType.DMA((n_dev - 1,))],
            compiler_params=pltpu.CompilerParams(collective_id=0, has_side_effects=True),
            name='all_ids',
        )(tok_ids.reshape(tok // lanes, lanes)).reshape(n_dev, tok)
        mine = (ids8 // range_rows) == my_emb
        t_iota = jnp.arange(tok, dtype=I32)
        before = t_iota[None, :] < t_iota[:, None]
        rank8 = jnp.sum((mine[:, None, :] & before[None]).astype(I32), axis=-1)
        c_iota = jnp.arange(CAP, dtype=I32)
        hit = mine[:, None, :] & (rank8[:, None, :] == c_iota[None, :, None])
        recv_loc = jnp.sum(jnp.where(hit, (ids8 - my_emb * range_rows)[:, None, :], 0), axis=-1)
        counts = jnp.sum(mine.astype(I32), axis=-1)
        valid = c_iota[None, :] < counts[:, None]
        slot_bits = (n_slots - 1).bit_length()
        slot_ids = jnp.arange(n_slots, dtype=I32).reshape(n_dev, CAP)
        keys = jnp.where(valid, recv_loc * (1 << slot_bits) + slot_ids, big)
        skeys = jnp.concatenate([lax.sort(keys.reshape(-1)), jnp.full((128,), big, I32)])
        total = jnp.sum(counts).reshape(1)

        my_owner = tok_ids // range_rows
        rank = jnp.sum(((my_owner[None, :] == my_owner[:, None]) & before).astype(I32), axis=-1)
        slot_of = my_owner * CAP + rank

        spread = jnp.where(valid, recv_loc, lax.rem(slot_ids * 8, range_rows))
        want = lax.dynamic_slice_in_dim(spread, my_dp * n_emb, n_emb, 0).reshape(-1)
        n_want = lax.dynamic_slice_in_dim(counts, my_dp * n_emb, n_emb, 0)
        per_dot, group = 32, 2
        pick = (jnp.bitwise_and(want, 7) + 8 * (jnp.arange(n_serve, dtype=I32) % per_dot))[:, None]
        served = pl.pallas_call(
            functools.partial(gather_kernel, (n_layers, n_emb, CAP, per_dot, group)),
            out_shape=jax.ShapeDtypeStruct((n_layers, n_serve, e_dim), BF),
            in_specs=[sm, sm, vm, hbm],
            out_specs=vm,
            scratch_shapes=[pltpu.VMEM((n_layers, n_serve * 8, e_dim), BF), pltpu.SemaphoreType.DMA((n_emb,))],
            compiler_params=params(0),
            name='table_rows',
        )(want, n_want, pick, tables)

        fb = 1024
        n_blk = ffn // fb
        cw, nw, slab = 512, 512, 16
        n_back = n_layers - 1
        z_rows = 1336
        z_chunks = range_rows // z_rows
        z_per = n_layers * z_chunks // (n_back * n_blk)
        assert z_chunks * z_rows == range_rows and z_per * n_blk * n_back == z_chunks * n_layers

        def flat(*shape):
            return pl.BlockSpec(shape, lambda *_: (0,) * len(shape), pipeline_mode=pl.Buffered(1))

        matmul_flops = 4 * tok * dim * ffn
        x1, gate0, fetched = pl.pallas_call(
            functools.partial(first_kernel, (n_dp, n_emb, CAP, cw, nw, slab)),
            grid=(n_blk,),
            out_shape=[
                jax.ShapeDtypeStruct((tok, dim), BF),
                jax.ShapeDtypeStruct((1, tok, e_dim), F32),
                jax.ShapeDtypeStruct((n_layers, tok, e_dim), BF),
            ],
            in_specs=[hbm, flat(tok, 1), hbm, flat(1, dim, e_dim), flat(1, e_dim, dim),
                      pl.BlockSpec((1, dim, fb), lambda f: (0, 0, f)), pl.BlockSpec((1, fb, dim), lambda f: (0, f, 0))],
            out_specs=[flat(tok, dim), flat(1, tok, e_dim), flat(n_layers, tok, e_dim)],
            scratch_shapes=[
                pltpu.VMEM((tok, dim), BF), pltpu.VMEM((tok, dim), F32), pltpu.VMEM((tok, fb), BF), pltpu.VMEM((1, tok, fb), F32),
                pltpu.VMEM((n_layers, n_serve, e_dim), BF), pltpu.SemaphoreType.DMA, pltpu.SemaphoreType.DMA,
                pltpu.SemaphoreType.DMA((n_emb - 1,)), pltpu.SemaphoreType.DMA((n_emb - 1,)),
            ],
            compiler_params=params(1, collective_id=1, has_side_effects=True),
            cost_estimate=pl.CostEstimate(flops=matmul_flops, bytes_accessed=100 << 20, transcendentals=0),
            name='first_layer',
        )(resid_in, slot_of[:, None], served, w_gate, w_proj, w_up, w_down)

        def lsp(*shape):
            return pl.BlockSpec((1,) + shape, lambda l, f: (l + 1, 0, 0))

        out, saved, ups, gates, rows, dgp, dtab = pl.pallas_call(
            functools.partial(forward_kernel, (n_back, n_blk, cw, nw, slab, z_per, z_chunks)),
            grid=(n_back, n_blk),
            out_shape=[
                jax.ShapeDtypeStruct((tok, dim), BF),
                jax.ShapeDtypeStruct((n_back - 1, tok, dim), BF),
                jax.ShapeDtypeStruct((n_back, tok, ffn), F32),
                jax.ShapeDtypeStruct((n_back, tok, e_dim), F32),
                jax.ShapeDtypeStruct((tok, e_dim), F32),
                jax.ShapeDtypeStruct((tok, e_dim), BF),
                jax.ShapeDtypeStruct((n_layers, range_rows, e_dim), F32),
            ],
            in_specs=[hbm, hbm, lsp(tok, e_dim), lsp(dim, e_dim), lsp(e_dim, dim),
                      pl.BlockSpec((1, dim, fb), lambda l, f: (l + 1, 0, f)), pl.BlockSpec((1, fb, dim), lambda l, f: (l + 1, f, 0))],
            out_specs=[hbm, hbm,
                       pl.BlockSpec((1, tok, fb), lambda l, f: (l, 0, f)),
                       pl.BlockSpec((1, tok, e_dim), lambda l, f: (l, 0, 0)),
                       flat(tok, e_dim), flat(tok, e_dim), hbm],
            scratch_shapes=[
                pltpu.VMEM((tok, dim), BF), pltpu.VMEM((tok, dim), BF), pltpu.VMEM((tok, dim), F32), pltpu.VMEM((tok, fb), BF),
                pltpu.VMEM((z_rows, e_dim), F32), pltpu.SemaphoreType.DMA, pltpu.SemaphoreType.DMA, pltpu.SemaphoreType.DMA((z_per,)),
            ],
            compiler_params=params(2),
            cost_estimate=pl.CostEstimate(flops=n_back * matmul_flops, bytes_accessed=400 << 20, transcendentals=0),
            name='forward',
        )(x1, cot_out, fetched, w_gate, w_proj, w_up, w_down)

        def of_layer(off, *shape):
            return pl.BlockSpec((1,) + shape, lambda i, f: (jnp.maximum(n_back - i + off, 0), 0, 0))

        got, got_gate, slots0 = pl.pallas_call(
            functools.partial(backward_kernel, (n_back, n_blk, n_dp, n_emb, CAP, cw, nw, slab)),
            grid=(n_back, n_blk),
            out_shape=[jax.ShapeDtypeStruct((n_back, n_slots, e_dim), F32), jax.ShapeDtypeStruct((n_slots, e_dim), F32),
                       jax.ShapeDtypeStruct((n_dp, n_serve, e_dim), BF)],
            in_specs=[hbm, hbm, hbm, flat(tok, e_dim), flat(tok, e_dim), flat(1, tok), flat(1, tok, e_dim),
                      pl.BlockSpec((1, tok, fb), lambda i, f: (n_back - 1 - i, 0, f)),
                      pl.BlockSpec((1, dim, fb), lambda i, f: (n_back - i, 0, f)), pl.BlockSpec((1, fb, dim), lambda i, f: (n_back - i, f, 0)),
                      of_layer(0, dim, e_dim), of_layer(-1, e_dim, dim), of_layer(-2, tok, e_dim), of_layer(-1, tok, e_dim)],
            out_specs=[hbm, hbm, flat(n_dp, n_serve, e_dim)],
            scratch_shapes=[
                pltpu.VMEM((tok, dim), BF), pltpu.VMEM((tok, dim), BF), pltpu.VMEM((tok, dim), F32), pltpu.VMEM((tok, fb), BF), pltpu.VMEM((tok, fb), BF),
                pltpu.VMEM((tok, dim), BF), pltpu.VMEM((n_serve, e_dim), F32), pltpu.VMEM((n_serve, e_dim), F32),
                pltpu.VMEM((tok, e_dim), F32), pltpu.VMEM((tok, e_dim), BF),
                pltpu.SemaphoreType.DMA, pltpu.SemaphoreType.DMA,
                pltpu.SemaphoreType.DMA((2, n_dev - 1)), pltpu.SemaphoreType.DMA((2,)), pltpu.SemaphoreType.DMA((n_back + 1, n_dev - 1)),
            ],
            compiler_params=params(2, collective_id=2, has_side_effects=True),
            cost_estimate=pl.CostEstimate(flops=n_back * matmul_flops, bytes_accessed=400 << 20, transcendentals=0),
            name='backward',
        )(cot_out, x1, saved, rows, dgp, slot_of[None, :], gate0, ups, w_up, w_down, w_gate, w_proj, gates, fetched)

        window, sub = 512, 8

        def scatter(first_layer, n, rows_in, dtab):
            scratch = [pltpu.VMEM((2, n, window, sub, e_dim), F32), pltpu.SMEM((window,), I32)]
            if first_layer == 0:
                scratch.append(pltpu.VMEM((1, n_slots, e_dim), F32))
            return pl.pallas_call(
                functools.partial(scatter_kernel, (first_layer, n, slot_bits, 8, window, 32)),
                out_shape=jax.ShapeDtypeStruct(dtab.shape, F32),
                in_specs=[sm, sm] + [vm] * len(rows_in) + [hbm],
                out_specs=hbm,
                input_output_aliases={2 + len(rows_in): 0},
                scratch_shapes=scratch + [pltpu.SemaphoreType.DMA((2,))],
                compiler_params=params(0),
                cost_estimate=pl.CostEstimate(flops=n * 20_000_000_000, bytes_accessed=n << 22, transcendentals=0),
                name=f'scatter_{first_layer}',
            )(skeys, total, *rows_in, dtab)

        mixed0 = lax.all_to_all(slots0.reshape(n_dev, CAP, e_dim), MESH_AXES, 0, 0, tiled=True).reshape(n_slots, e_dim)
        dtab = dtab.reshape(n_layers, range_rows // sub, sub, e_dim)
        dtab = scatter(1, n_back, (got,), dtab)
        dtab = scatter(0, 1, (got_gate, mixed0), dtab)
        dtab = dtab.reshape(n_layers, range_rows, e_dim)
        return out, dtab

    return jax.shard_map(device_body, mesh=mesh, in_specs=(tok_spec, act_spec, act_spec, table_spec, full_spec, full_spec, full_spec, full_spec), out_specs=(act_spec, table_spec), check_vma=False)
```

```python
import functools

import jax
import jax.numpy as jnp
from jax import lax
from jax.experimental import pallas as pl
from jax.experimental.pallas import tpu as pltpu
from jax.sharding import PartitionSpec as P

NORM_EPS = 1e-6
BF = jnp.bfloat16
F32 = jnp.float32
I32 = jnp.int32
VMEM_BYTES = 67043328
GELU_C = 0.7978845608028654
GELU_A = 0.044715

MESH_AXES = ('dp', 'emb')
CAP = 256


def gelu(x):
    return 0.5 * x * (1.0 + jnp.tanh(GELU_C * (x + GELU_A * (x * x * x))))


def gelu_slope(x):
    sq = x * x
    th = jnp.tanh(GELU_C * (x + GELU_A * (x * sq)))
    return 0.5 * (1.0 + th) + (0.5 * GELU_C) * x * (1.0 - th * th) * (1.0 + (3 * GELU_A) * sq)


def dot(a, b):
    return jnp.dot(a, b, preferred_element_type=F32)


def dot_t(a, b):
    return lax.dot_general(a, b, (((1,), (1,)), ((), ())), preferred_element_type=F32)


def row_loop(rows, slab, unroll=2):
    def run(body):
        def step(i, carry):
            body(pl.ds(pl.multiple_of(i * slab, slab), slab))
            return carry

        lax.fori_loop(0, rows // slab, step, 0, unroll=unroll)

    return run


def peer_of(n_emb, index):
    dp = index // n_emb
    return {'dp': dp, 'emb': index - dp * n_emb}


def remote(src, dst, send_sem, recv_sem, device):
    return pltpu.make_async_remote_copy(src_ref=src, dst_ref=dst, send_sem=send_sem, recv_sem=recv_sem,
                                        device_id=device, device_id_type=pl.DeviceIdType.MESH)


def meet(devices):
    barrier = pltpu.get_barrier_semaphore()
    for device in devices:
        pl.semaphore_signal(barrier, inc=1, device_id=device, device_id_type=pl.DeviceIdType.MESH)
    pl.semaphore_wait(barrier, len(devices))


def ids_kernel(cfg, in_ref, out_ref, send_sem, recv_sem):
    n_dp, n_emb = cfg
    n_dev = n_dp * n_emb
    me = lax.axis_index('dp') * n_emb + lax.axis_index('emb')
    peers = [peer_of(n_emb, lax.rem(me + k, n_dev)) for k in range(1, n_dev)]
    meet(peers)
    copies = [remote(in_ref, out_ref.at[me], send_sem.at[k], recv_sem.at[k], peer) for k, peer in enumerate(peers)]
    for copy in copies:
        copy.start()
    out_ref[me] = in_ref[...]
    for copy in copies:
        copy.wait()


def gather_kernel(cfg, loc_ref, counts_ref, pick_ref, tables_hbm, out_ref, buf, sems):
    n_layers, n_dest, cap, per_dot, group = cfg
    trip = per_dot * group
    n_trips = [(counts_ref[d] + (trip - 1)) // trip for d in range(n_dest)]

    def row_copy(d, s):
        base = pl.multiple_of(jnp.left_shift(jnp.right_shift(loc_ref[s], 3), 3), 8)
        return pltpu.make_async_copy(
            tables_hbm.at[:, pl.ds(base, 8), :], buf.at[:, pl.ds(pl.multiple_of(s * 8, 8), 8), :], sems.at[d])

    for d in range(n_dest):
        def issue(i, carry, d=d):
            for k in range(8):
                row_copy(d, d * cap + i * 8 + k).start()
            return carry

        lax.fori_loop(0, n_trips[d] * (trip // 8), issue, 0)

    for d in range(n_dest):
        def drain(i, carry, d=d):
            part = buf.at[:, pl.ds(pl.multiple_of((d * cap + i * trip) * 8, 8), trip * 8), :]
            pltpu.make_async_copy(part, part, sems.at[d]).wait()
            return carry

        lax.fori_loop(0, n_trips[d], drain, 0)

        def pick(i, carry, d=d):
            for k in range(group):
                s0 = pl.multiple_of(d * cap + i * trip + k * per_dot, per_dot)
                want = pick_ref[pl.ds(s0, per_dot), :]
                sel = (lax.broadcasted_iota(I32, (per_dot, per_dot * 8), 1) == want).astype(BF)
                for l in range(n_layers):
                    rows = buf[l, pl.ds(pl.multiple_of(s0 * 8, 8), per_dot * 8), :]
                    out_ref[l, pl.ds(s0, per_dot), :] = dot(sel, rows).astype(BF)
            return carry

        lax.fori_loop(0, n_trips[d], pick, 0)

        def blank(i, carry, d=d):
            s0 = pl.multiple_of(d * cap + i * trip, trip)
            for l in range(n_layers):
                out_ref[l, pl.ds(s0, trip), :] = jnp.zeros((trip, out_ref.shape[2]), BF)
            return carry

        lax.fori_loop(n_trips[d], cap // trip, blank, 0)


def weight_copies(wu_hbm, wd_hbm, wu_s, wd_s, sems):
    fb = wu_s.shape[2]

    def copies(layer, blk, slot):
        at = pl.multiple_of(blk * fb, fb)
        return (pltpu.make_async_copy(wu_hbm.at[layer, :, pl.ds(at, fb)], wu_s.at[slot], sems.at[0, slot]),
                pltpu.make_async_copy(wd_hbm.at[layer, pl.ds(at, fb), :], wd_s.at[slot], sems.at[1, slot]))

    return copies


def start(copies):
    for copy in copies:
        copy.start()


def wait(copies):
    for copy in copies:
        copy.wait()


def mlp_block(cfg, u_s, h_s, acc_s, wu_ref, wd_ref, up_ref):
    cw, nw = cfg
    gw = 128
    n_c = wu_ref.shape[1] // cw

    def act(c):
        for g in range(cw // gw):
            gs = slice(c * cw + g * gw, c * cw + (g + 1) * gw)
            h_s[:, gs] = gelu(up_ref[:, gs]).astype(BF)

    for c in range(n_c):
        cs = slice(c * cw, (c + 1) * cw)
        up_ref[:, cs] = dot(u_s[...], wu_ref[:, cs])
        if c > 0:
            act(c - 1)
    for c in range(n_c):
        cs = slice(c * cw, (c + 1) * cw)
        for n in range(acc_s.shape[1] // nw):
            ns = slice(n * nw, (n + 1) * nw)
            acc_s[:, ns] += dot(h_s[:, cs], wd_ref[cs, ns])
        if c == 0:
            act(n_c - 1)


def norm_rows(x, sl, u_s, acc_s):
    scale = lax.rsqrt(jnp.mean(x * x, axis=-1, keepdims=True) + NORM_EPS)
    u_s[sl, :] = (x * scale).astype(BF)
    acc_s[sl, :] = x


def add_proj(nw, acc_s, mixed, wp_ref):
    for n in range(acc_s.shape[1] // nw):
        ns = slice(n * nw, (n + 1) * nw)
        acc_s[:, ns] += dot(mixed, wp_ref[:, ns])


def first_kernel(cfg, x_hbm, slot_ref, served_hbm, wg_hbm, wp_hbm, wu_hbm, wd_hbm,
                 x_out_ref, gate_ref, fet_ref,
                 u_s, acc_s, h_s, up_s, ret_s, wu_s, wd_s, wg_s, wp_s, in_sem, w_sem, self_sem, send_sem, recv_sem):
    n_dp, n_emb, cap, n_blk, cw, nw, slab = cfg
    tok, dim = u_s.shape
    my_emb = lax.axis_index('emb')
    my_dp = lax.axis_index('dp')
    here = ret_s.at[:, pl.ds(pl.multiple_of(my_emb * cap, cap), cap), :]
    own = pltpu.make_async_copy(served_hbm.at[:, pl.ds(pl.multiple_of(my_emb * cap, cap), cap), :], here, self_sem)
    peers = [lax.rem(my_emb + k, n_emb) for k in range(1, n_emb)]
    copies = [remote(served_hbm.at[:, pl.ds(pl.multiple_of(p * cap, cap), cap), :], here,
                     send_sem.at[k], recv_sem.at[k], {'dp': my_dp, 'emb': p}) for k, p in enumerate(peers)]
    weights = weight_copies(wu_hbm, wd_hbm, wu_s, wd_s, w_sem)
    first = [pltpu.make_async_copy(x_hbm, x_out_ref, in_sem.at[0]),
             pltpu.make_async_copy(wg_hbm.at[0], wg_s, in_sem.at[1]),
             pltpu.make_async_copy(wp_hbm.at[0], wp_s, in_sem.at[2])]
    start(first[:2])
    start(weights(0, 0, 0))
    start(first[2:])
    meet([{'dp': my_dp, 'emb': p} for p in peers])
    own.start()
    start(copies)
    first[0].wait()
    row_loop(tok, slab)(lambda sl: norm_rows(x_out_ref[sl, :].astype(F32), sl, u_s, acc_s))
    first[1].wait()
    gate_ref[0] = dot(u_s[...], wg_s[...])

    def block(f, carry):
        slot = lax.rem(f, 2)

        @pl.when(f + 1 < n_blk)
        def _():
            start(weights(0, f + 1, 1 - slot))

        wait(weights(0, f, slot))
        mlp_block((cw, nw), u_s, h_s, acc_s, wu_s.at[slot], wd_s.at[slot], up_s)
        return carry

    lax.fori_loop(0, n_blk, block, 0)
    own.wait()
    wait(copies)
    first[2].wait()
    sel = (lax.broadcasted_iota(I32, (tok, n_emb * cap), 1) == slot_ref[...]).astype(BF)
    for l in range(fet_ref.shape[0]):
        fet_ref[l] = dot(sel, ret_s[l]).astype(BF)
    add_proj(nw, acc_s, (gelu(gate_ref[0]) * fet_ref[0].astype(F32)).astype(BF), wp_s)

    def finish(sl):
        x_out_ref[sl, :] = acc_s[sl, :].astype(BF)

    row_loop(tok, slab)(finish)


def forward_kernel(cfg, x_hbm, cot_hbm, fet_ref, wg_hbm, wp_hbm, wu_hbm, wd_hbm,
                   out_hbm, saved_hbm, ups_hbm, gate_ref, rows_ref, dgp_ref, dtab_hbm,
                   x_s, u_s, acc_s, h_s, up_s, zero_s, wu_s, wd_s, wg_s, wp_s, in_sem, w_sem, up_sem, out_sem, z_sem):
    n_layers, n_blk, cw, nw, slab, z_per, z_chunks = cfg
    tok, dim = x_s.shape
    fb = wu_s.shape[2]
    z_rows = zero_s.shape[0]
    n_steps = n_layers * n_blk
    weights = weight_copies(wu_hbm, wd_hbm, wu_s, wd_s, w_sem)

    def z_copies(step):
        found = []
        for j in range(z_per):
            c = step * z_per + j
            zl = c // z_chunks
            zc = c - zl * z_chunks
            found.append(pltpu.make_async_copy(
                zero_s, dtab_hbm.at[zl, pl.ds(pl.multiple_of(zc * z_rows, 8), z_rows), :], z_sem.at[j]))
        return found

    def up_copy(layer, blk, slot):
        return pltpu.make_async_copy(up_s.at[slot], ups_hbm.at[layer, :, pl.ds(pl.multiple_of(blk * fb, fb), fb)], up_sem.at[slot])

    def gate_copy(layer):
        return pltpu.make_async_copy(wg_hbm.at[layer + 1], wg_s, in_sem.at[1])

    def proj_copy(layer):
        return pltpu.make_async_copy(wp_hbm.at[layer + 1], wp_s, in_sem.at[2])

    fetch = pltpu.make_async_copy(x_hbm, x_s, in_sem.at[0])
    fetch.start()
    gate_copy(0).start()
    start(weights(1, 0, 0))
    proj_copy(0).start()
    row_loop(z_rows, 8, 1)(lambda sl: zero_s.__setitem__((sl, slice(None)), jnp.zeros((8, zero_s.shape[1]), F32)))
    fetch.wait()
    row_loop(tok, slab)(lambda sl: norm_rows(x_s[sl, :].astype(F32), sl, u_s, acc_s))

    def one_layer(layer, carry):
        gate_copy(layer).wait()
        gate_ref[layer] = dot(u_s[...], wg_s[...])

        @pl.when(layer + 1 < n_layers)
        def _():
            gate_copy(layer + 1).start()

        def block(f, carry):
            step = layer * n_blk + f
            slot = lax.rem(step, 2)

            @pl.when(step + 1 < n_steps)
            def _():
                nxt = step + 1
                start(weights(1 + nxt // n_blk, lax.rem(nxt, n_blk), 1 - slot))

            @pl.when(step > 0)
            def _():
                wait(z_copies(step - 1))

            start(z_copies(step))

            @pl.when(step > 1)
            def _():
                up_copy(layer, f, slot).wait()

            wait(weights(1 + layer, f, slot))
            mlp_block((cw, nw), u_s, h_s, acc_s, wu_s.at[slot], wd_s.at[slot], up_s.at[slot])
            up_copy(layer, f, slot).start()
            return carry

        lax.fori_loop(0, n_blk, block, 0)
        proj_copy(layer).wait()
        add_proj(nw, acc_s, (gelu(gate_ref[layer]) * fet_ref[layer + 1].astype(F32)).astype(BF), wp_s)

        @pl.when(layer > 0)
        def _():
            pltpu.make_async_copy(x_s, saved_hbm.at[layer - 1], out_sem).wait()

        def next_rows(sl):
            x_new = acc_s[sl, :].astype(BF)
            x_s[sl, :] = x_new
            norm_rows(x_new.astype(F32), sl, u_s, acc_s)

        row_loop(tok, slab)(next_rows)

        @pl.when(layer < n_layers - 1)
        def _():
            pltpu.make_async_copy(x_s, saved_hbm.at[layer], out_sem).start()
            proj_copy(layer + 1).start()

        return carry

    lax.fori_loop(0, n_layers, one_layer, 0)
    put = pltpu.make_async_copy(x_s, out_hbm, out_sem)
    put.start()
    get = pltpu.make_async_copy(cot_hbm, u_s, in_sem.at[0])
    get.start()
    wait(z_copies(n_steps - 1))
    up_copy(0, 0, 0).wait()
    up_copy(0, 0, 1).wait()
    get.wait()
    d_mixed = dot_t(u_s[...], wp_s[...]).astype(BF).astype(F32)
    gate_grads(gate_ref[n_layers - 1], fet_ref[n_layers], d_mixed, rows_ref, dgp_ref)
    put.wait()


def gate_grads(gate_pre, fetched, d_mixed, rows_ref, dgp_ref):
    rows_ref[...] = gelu(gate_pre) * d_mixed
    dgp_ref[...] = (d_mixed * fetched.astype(F32) * gelu_slope(gate_pre)).astype(BF)


def to_slots(rows, slot_ref, slots_s):
    hi = rows.astype(BF)
    rest = rows - hi.astype(F32)
    mid = rest.astype(BF)
    low = (rest - mid.astype(F32)).astype(BF)
    sel = slot_pick(slots_s.shape[0], slot_ref)
    slots_s[...] = (dot(sel, hi) + dot(sel, mid)) + dot(sel, low)


def slot_pick(n, slot_ref):
    return (lax.broadcasted_iota(I32, (n, slot_ref.shape[1]), 0) == slot_ref[...]).astype(BF)


def backward_kernel(cfg, cot_hbm, x1_hbm, saved_hbm, rows_in_ref, dgp_in_ref, slot_ref, gate0_ref, gate_ref, fet_ref,
                    ups_hbm, wu_hbm, wd_hbm, wg_hbm, wp_hbm,
                    got_hbm, gate_hbm, slots0_ref,
                    cot_s, x_s, acc_s, dup_s, dh_s, dng_s, slots_s, gslots_s, rows_s, dgp_s, up_s, wu_s, wd_s, wg_s, wp_s,
                    in_sem, w_sem, up_sem, send_sem, self_sem, recv_sem):
    n_layers, n_blk, n_dp, n_emb, cap, cw, nw, slab = cfg
    tok, dim = cot_s.shape
    fb = wu_s.shape[2]
    gw = 128
    n_dev = n_dp * n_emb
    n_steps = n_layers * n_blk
    my_emb = lax.axis_index('emb')
    me = lax.axis_index('dp') * n_emb + my_emb
    peers = [peer_of(n_emb, lax.rem(me + k, n_dev)) for k in range(1, n_dev)]
    weights = weight_copies(wu_hbm, wd_hbm, wu_s, wd_s, w_sem)

    def part(ref, emb):
        return ref.at[pl.ds(pl.multiple_of(emb * cap, cap), cap), :]

    def sends(ref, there, which, got):
        return [pltpu.make_async_copy(part(ref, my_emb), there, self_sem.at[which])] + [
            remote(part(ref, peer['emb']), there, send_sem.at[which, k], recv_sem.at[got, k], peer) for k, peer in enumerate(peers)]

    def row_sends(i):
        return sends(slots_s, part(got_hbm.at[n_layers - 1 - i], me), 0, i)

    gate_sends = sends(gslots_s, part(gate_hbm, me), 1, n_layers)

    def up_copy(step, slot):
        i = step // n_blk
        blk = step - i * n_blk
        return pltpu.make_async_copy(ups_hbm.at[n_layers - 1 - i, :, pl.ds(pl.multiple_of(blk * fb, fb), fb)], up_s.at[slot], up_sem.at[slot])

    def load(step, slot):
        i = step // n_blk
        return weights(n_layers - i, step - i * n_blk, slot) + (up_copy(step, slot),)

    def gate_copy(i):
        return pltpu.make_async_copy(wg_hbm.at[n_layers - i], wg_s, in_sem.at[1])

    def proj_copy(i):
        return pltpu.make_async_copy(wp_hbm.at[n_layers - 1 - i], wp_s, in_sem.at[2])

    def x_copy(i):
        return pltpu.make_async_copy(saved_hbm.at[n_layers - 2 - i], x_s, in_sem.at[3])

    fetch = pltpu.make_async_copy(cot_hbm, cot_s, in_sem.at[0])
    gate_copy(0).start()
    fetch.start()
    start(load(0, 0))
    proj_copy(0).start()
    rows_s[...] = rows_in_ref[...]
    dgp_s[...] = dgp_in_ref[...]

    def clear(sl):
        acc_s[sl, :] = jnp.zeros((slab, dim), F32)

    row_loop(tok, slab)(clear)
    meet(peers)
    to_slots(gelu(gate0_ref[0]), slot_ref, gslots_s)

    def one_layer(i, carry):
        @pl.when(i < n_layers - 1)
        def _():
            x_copy(i).start()

        @pl.when(i == n_layers - 1)
        def _():
            pltpu.make_async_copy(x1_hbm, x_s, in_sem.at[3]).start()

        to_slots(rows_s[...], slot_ref, slots_s)
        gate_copy(i).wait()
        for n in range(dim // nw):
            ns = slice(n * nw, (n + 1) * nw)
            dng_s[:, ns] = dot_t(dgp_s[...], wg_s[ns, :]).astype(BF)
        start(row_sends(i))

        @pl.when(i < n_layers - 1)
        def _():
            gate_copy(i + 1).start()

        @pl.when(i == 0)
        def _():
            start(gate_sends)
            fetch.wait()

        def block(f, carry):
            step = i * n_blk + f
            slot = lax.rem(step, 2)

            @pl.when(step + 1 < n_steps)
            def _():
                start(load(step + 1, 1 - slot))

            wait(load(step, slot))
            wu_ref, wd_ref, up_ref = wu_s.at[slot], wd_s.at[slot], up_s.at[slot]

            def act(c):
                for g in range(cw // gw):
                    gs = slice(c * cw + g * gw, c * cw + (g + 1) * gw)
                    dup_s[:, gs] = (dh_s[:, gs].astype(F32) * gelu_slope(up_ref[:, gs])).astype(BF)

            n_c = fb // cw
            for c in range(n_c):
                cs = slice(c * cw, (c + 1) * cw)
                dh_s[:, cs] = dot_t(cot_s[...], wd_ref[cs, :]).astype(BF)
                if c > 0:
                    act(c - 1)
            for c in range(n_c):
                cs = slice(c * cw, (c + 1) * cw)
                for n in range(dim // nw):
                    ns = slice(n * nw, (n + 1) * nw)
                    acc_s[:, ns] += dot_t(dup_s[:, cs], wu_ref[ns, cs])
                if c == 0:
                    act(n_c - 1)
            return carry

        lax.fori_loop(0, n_blk, block, 0)
        pltpu.make_async_copy(x1_hbm, x_s, in_sem.at[3]).wait()

        def rows_back(sl):
            x = x_s[sl, :].astype(F32)
            scale = lax.rsqrt(jnp.mean(x * x, axis=-1, keepdims=True) + NORM_EPS)
            d_n = (acc_s[sl, :].astype(BF).astype(F32) + dng_s[sl, :].astype(F32)).astype(BF).astype(F32)
            acc_s[sl, :] = jnp.zeros((slab, dim), F32)
            proj = jnp.mean(d_n * x, axis=-1, keepdims=True)
            d_x = d_n * scale - x * (proj * (scale * scale * scale))
            cot_s[sl, :] = (cot_s[sl, :].astype(F32) + d_x).astype(BF)

        row_loop(tok, slab)(rows_back)
        proj_copy(i).wait()
        d_mixed = dot_t(cot_s[...], wp_s[...]).astype(BF)
        wait(row_sends(i))

        @pl.when(i < n_layers - 1)
        def _():
            proj_copy(i + 1).start()
            gate_grads(gate_ref[jnp.maximum(n_layers - 2 - i, 0)], fet_ref[n_layers - 1 - i], d_mixed.astype(F32), rows_s, dgp_s)

        @pl.when(i == n_layers - 1)
        def _():
            slots = dot(slot_pick(slots_s.shape[0], slot_ref), d_mixed).astype(BF)
            for d in range(n_dp):
                slots0_ref[d] = slots

        return carry

    lax.fori_loop(0, n_layers, one_layer, 0)
    wait(gate_sends)


def scatter_kernel(cfg, keys_ref, meta_ref, *refs):
    first_layer, n_layers, slot_bits, unroll, window, bulk = cfg
    if first_layer == 0:
        gate_ref, mixed_ref, dt_in, dt_out, groups, spots, prod, sems = refs
        n_rows = mixed_ref.shape[0]

        def product(sl):
            prod[0, sl, :] = gate_ref[sl, :] * mixed_ref[sl, :].astype(F32)

        row_loop(n_rows, 64, 4)(product)
        rows_ref = prod
    else:
        rows_ref, dt_in, dt_out, groups, spots, sems = refs
    count = meta_ref[0]
    e_dim = rows_ref.shape[2]
    sub = 8
    n_win = (count + (window - 1)) // window
    lane_row = lax.broadcasted_iota(I32, (sub, e_dim), 0)
    mask = (1 << slot_bits) - 1

    def move(buf, spot, group, n):
        return pltpu.make_async_copy(groups.at[buf, :, pl.ds(spot, n)],
                                     dt_out.at[pl.ds(first_layer, n_layers), pl.ds(group, n)], sems.at[buf])

    def settle(buf, n):
        def drain_bulk(j, carry):
            move(buf, 0, 0, bulk).wait()
            return carry

        def drain(j, carry):
            move(buf, 0, 0, 1).wait()
            return carry

        lax.fori_loop(0, n // bulk, drain_bulk, 0)
        lax.fori_loop(0, lax.rem(n, bulk), drain, 0)

    def run_window(w, carry):
        buf = lax.rem(w, 2)
        prev, accs, older, old = carry
        settle(buf, older)
        stop = jnp.minimum(count, (w + 1) * window)
        trips = (stop - w * window + (unroll - 1)) // unroll

        def add(t, carry):
            prev, n, accs = carry
            for k in range(unroll):
                key = keys_ref[w * window + t * unroll + k]
                slot = jnp.bitwise_and(key, mask)
                row = jnp.right_shift(key, slot_bits)
                group = jnp.right_shift(row, 3)
                same = group == prev
                n = n + jnp.where(same, 0, 1)
                spots[jnp.maximum(n, 0)] = group
                here = lane_row == jnp.bitwise_and(row, sub - 1)
                new = []
                for l, acc in enumerate(accs):
                    row_l = jnp.broadcast_to(rows_ref[l, pl.ds(slot, 1), :], (sub, e_dim))
                    new.append(jnp.where(same, acc, 0.0) + jnp.where(here, row_l, 0.0))
                    groups[buf, l, jnp.maximum(n, 0)] = new[l]
                accs = tuple(new)
                prev = group
            return prev, n, accs

        n0 = jnp.where(jnp.right_shift(keys_ref[w * window], slot_bits + 3) == prev, 0, -1)
        prev, n, accs = lax.fori_loop(0, trips, add, (prev, n0, accs))
        follow = jnp.right_shift(keys_ref[(w + 1) * window], slot_bits + 3)
        padded = trips * unroll > stop - w * window
        goes_on = jnp.logical_and(stop < count, follow == prev)
        n_groups = n + 1 - jnp.where(jnp.logical_or(padded, goes_on), 1, 0)

        def put(u, carry):
            move(buf, u, spots[u], 1).start()
            return carry

        lax.fori_loop(0, n_groups, put, 0)
        return prev, accs, old, n_groups

    zero = jnp.int32(0)
    accs = tuple(jnp.zeros((sub, e_dim), F32) for _ in range(n_layers))
    _, _, older, old = lax.fori_loop(0, n_win, run_window, (jnp.int32(-1), accs, zero, zero))
    settle(lax.rem(n_win, 2), older)
    settle(lax.rem(n_win + 1, 2), old)


def solution(mesh):
    n_emb, n_dp = mesh.shape['emb'], mesh.shape['dp']
    n_dev = n_emb * n_dp
    tok_spec = P(('dp', 'emb'))
    act_spec = P(('dp', 'emb'), None)
    table_spec = P(None, 'emb', None)
    full_spec = P(None, None, None)
    hbm = pl.BlockSpec(memory_space=pl.ANY)
    vm = pl.BlockSpec(memory_space=pltpu.VMEM)
    sm = pl.BlockSpec(memory_space=pltpu.SMEM)
    big = jnp.iinfo(jnp.int32).max

    def params(n_grid, **kw):
        return pltpu.CompilerParams(vmem_limit_bytes=VMEM_BYTES, dimension_semantics=('arbitrary',) * n_grid if n_grid else None, **kw)

    def device_body(tok_ids, resid_in, cot_out, tables, w_up, w_down, w_gate, w_proj):
        n_layers, range_rows, e_dim = tables.shape
        tok = tok_ids.shape[0]
        dim, ffn = w_up.shape[1:]
        n_slots, n_serve = n_dev * CAP, n_emb * CAP
        my_emb, my_dp = lax.axis_index('emb'), lax.axis_index('dp')

        lanes = 128
        ids8 = pl.pallas_call(
            functools.partial(ids_kernel, (n_dp, n_emb)),
            out_shape=jax.ShapeDtypeStruct((n_dev, tok // lanes, lanes), I32),
            in_specs=[vm], out_specs=vm,
            scratch_shapes=[pltpu.SemaphoreType.DMA((n_dev - 1,)), pltpu.SemaphoreType.DMA((n_dev - 1,))],
            compiler_params=pltpu.CompilerParams(collective_id=0, has_side_effects=True),
            name='all_ids',
        )(tok_ids.reshape(tok // lanes, lanes)).reshape(n_dev, tok)
        mine = (ids8 // range_rows) == my_emb
        t_iota = jnp.arange(tok, dtype=I32)
        before = t_iota[None, :] < t_iota[:, None]
        rank8 = jnp.sum((mine[:, None, :] & before[None]).astype(I32), axis=-1)
        c_iota = jnp.arange(CAP, dtype=I32)
        hit = mine[:, None, :] & (rank8[:, None, :] == c_iota[None, :, None])
        recv_loc = jnp.sum(jnp.where(hit, (ids8 - my_emb * range_rows)[:, None, :], 0), axis=-1)
        counts = jnp.sum(mine.astype(I32), axis=-1)
        valid = c_iota[None, :] < counts[:, None]
        slot_bits = (n_slots - 1).bit_length()
        slot_ids = jnp.arange(n_slots, dtype=I32).reshape(n_dev, CAP)
        keys = jnp.where(valid, recv_loc * (1 << slot_bits) + slot_ids, big)
        skeys = jnp.concatenate([lax.sort(keys.reshape(-1)), jnp.full((128,), big, I32)])
        total = jnp.sum(counts).reshape(1)

        my_owner = tok_ids // range_rows
        rank = jnp.sum(((my_owner[None, :] == my_owner[:, None]) & before).astype(I32), axis=-1)
        slot_of = my_owner * CAP + rank

        spread = jnp.where(valid, recv_loc, lax.rem(slot_ids * 8, range_rows))
        want = lax.dynamic_slice_in_dim(spread, my_dp * n_emb, n_emb, 0).reshape(-1)
        n_want = lax.dynamic_slice_in_dim(counts, my_dp * n_emb, n_emb, 0)
        per_dot, group = 32, 2
        pick = (jnp.bitwise_and(want, 7) + 8 * (jnp.arange(n_serve, dtype=I32) % per_dot))[:, None]
        served = pl.pallas_call(
            functools.partial(gather_kernel, (n_layers, n_emb, CAP, per_dot, group)),
            out_shape=jax.ShapeDtypeStruct((n_layers, n_serve, e_dim), BF),
            in_specs=[sm, sm, vm, hbm],
            out_specs=vm,
            scratch_shapes=[pltpu.VMEM((n_layers, n_serve * 8, e_dim), BF), pltpu.SemaphoreType.DMA((n_emb,))],
            compiler_params=params(0),
            name='table_rows',
        )(want, n_want, pick, tables)

        fb = 1024
        n_blk = ffn // fb
        cw, nw, slab = 512, 512, 16
        n_back = n_layers - 1
        z_rows = 1336
        z_chunks = range_rows // z_rows
        z_per = n_layers * z_chunks // (n_back * n_blk)
        assert z_chunks * z_rows == range_rows and z_per * n_blk * n_back == z_chunks * n_layers

        matmul_flops = 4 * tok * dim * ffn
        w_bufs = [pltpu.VMEM((2, dim, fb), BF), pltpu.VMEM((2, fb, dim), BF), pltpu.VMEM((dim, e_dim), BF), pltpu.VMEM((e_dim, dim), BF)]
        dma = pltpu.SemaphoreType.DMA
        x1, gate0, fetched = pl.pallas_call(
            functools.partial(first_kernel, (n_dp, n_emb, CAP, n_blk, cw, nw, slab)),
            out_shape=[
                jax.ShapeDtypeStruct((tok, dim), BF),
                jax.ShapeDtypeStruct((1, tok, e_dim), F32),
                jax.ShapeDtypeStruct((n_layers, tok, e_dim), BF),
            ],
            in_specs=[hbm, vm, hbm, hbm, hbm, hbm, hbm],
            out_specs=[vm, vm, vm],
            scratch_shapes=[
                pltpu.VMEM((tok, dim), BF), pltpu.VMEM((tok, dim), F32), pltpu.VMEM((tok, fb), BF), pltpu.VMEM((tok, fb), F32),
                pltpu.VMEM((n_layers, n_serve, e_dim), BF), *w_bufs, dma((3,)), dma((2, 2)), dma, dma((n_emb - 1,)), dma((n_emb - 1,)),
            ],
            compiler_params=params(0, collective_id=1, has_side_effects=True),
            cost_estimate=pl.CostEstimate(flops=matmul_flops, bytes_accessed=100 << 20, transcendentals=0),
            name='first_layer',
        )(resid_in, slot_of[:, None], served, w_gate, w_proj, w_up, w_down)

        out, saved, ups, gates, rows, dgp, dtab = pl.pallas_call(
            functools.partial(forward_kernel, (n_back, n_blk, cw, nw, slab, z_per, z_chunks)),
            out_shape=[
                jax.ShapeDtypeStruct((tok, dim), BF),
                jax.ShapeDtypeStruct((n_back - 1, tok, dim), BF),
                jax.ShapeDtypeStruct((n_back, tok, ffn), F32),
                jax.ShapeDtypeStruct((n_back, tok, e_dim), F32),
                jax.ShapeDtypeStruct((tok, e_dim), F32),
                jax.ShapeDtypeStruct((tok, e_dim), BF),
                jax.ShapeDtypeStruct((n_layers, range_rows, e_dim), F32),
            ],
            in_specs=[hbm, hbm, vm, hbm, hbm, hbm, hbm],
            out_specs=[hbm, hbm, hbm, vm, vm, vm, hbm],
            scratch_shapes=[
                pltpu.VMEM((tok, dim), BF), pltpu.VMEM((tok, dim), BF), pltpu.VMEM((tok, dim), F32), pltpu.VMEM((tok, fb), BF),
                pltpu.VMEM((2, tok, fb), F32), pltpu.VMEM((z_rows, e_dim), F32), *w_bufs,
                dma((3,)), dma((2, 2)), dma((2,)), dma, dma((z_per,)),
            ],
            compiler_params=params(0),
            cost_estimate=pl.CostEstimate(flops=n_back * matmul_flops, bytes_accessed=400 << 20, transcendentals=0),
            name='forward',
        )(x1, cot_out, fetched, w_gate, w_proj, w_up, w_down)

        got, got_gate, slots0 = pl.pallas_call(
            functools.partial(backward_kernel, (n_back, n_blk, n_dp, n_emb, CAP, cw, nw, slab)),
            out_shape=[jax.ShapeDtypeStruct((n_back, n_slots, e_dim), F32), jax.ShapeDtypeStruct((n_slots, e_dim), F32),
                       jax.ShapeDtypeStruct((n_dp, n_serve, e_dim), BF)],
            in_specs=[hbm, hbm, hbm, vm, vm, vm, vm, vm, vm, hbm, hbm, hbm, hbm, hbm],
            out_specs=[hbm, hbm, vm],
            scratch_shapes=[
                pltpu.VMEM((tok, dim), BF), pltpu.VMEM((tok, dim), BF), pltpu.VMEM((tok, dim), F32), pltpu.VMEM((tok, fb), BF), pltpu.VMEM((tok, fb), BF),
                pltpu.VMEM((tok, dim), BF), pltpu.VMEM((n_serve, e_dim), F32), pltpu.VMEM((n_serve, e_dim), F32),
                pltpu.VMEM((tok, e_dim), F32), pltpu.VMEM((tok, e_dim), BF), pltpu.VMEM((2, tok, fb), F32), *w_bufs,
                dma((4,)), dma((2, 2)), dma((2,)), dma((2, n_dev - 1)), dma((2,)), dma((n_back + 1, n_dev - 1)),
            ],
            compiler_params=params(0, collective_id=2, has_side_effects=True),
            cost_estimate=pl.CostEstimate(flops=n_back * matmul_flops, bytes_accessed=400 << 20, transcendentals=0),
            name='backward',
        )(cot_out, x1, saved, rows, dgp, slot_of[None, :], gate0, gates, fetched, ups, w_up, w_down, w_gate, w_proj)

        window, sub = 512, 8

        def scatter(first_layer, n, rows_in, dtab):
            scratch = [pltpu.VMEM((2, n, window, sub, e_dim), F32), pltpu.SMEM((window,), I32)]
            if first_layer == 0:
                scratch.append(pltpu.VMEM((1, n_slots, e_dim), F32))
            return pl.pallas_call(
                functools.partial(scatter_kernel, (first_layer, n, slot_bits, 8, window, 32)),
                out_shape=jax.ShapeDtypeStruct(dtab.shape, F32),
                in_specs=[sm, sm] + [vm] * len(rows_in) + [hbm],
                out_specs=hbm,
                input_output_aliases={2 + len(rows_in): 0},
                scratch_shapes=scratch + [pltpu.SemaphoreType.DMA((2,))],
                compiler_params=params(0),
                cost_estimate=pl.CostEstimate(flops=n * 20_000_000_000, bytes_accessed=n << 22, transcendentals=0),
                name=f'scatter_{first_layer}',
            )(skeys, total, *rows_in, dtab)

        mixed0 = lax.all_to_all(slots0.reshape(n_dev, CAP, e_dim), MESH_AXES, 0, 0, tiled=True).reshape(n_slots, e_dim)
        dtab = dtab.reshape(n_layers, range_rows // sub, sub, e_dim)
        dtab = scatter(1, n_back, (got,), dtab)
        dtab = scatter(0, 1, (got_gate, mixed0), dtab)
        dtab = dtab.reshape(n_layers, range_rows, e_dim)
        return out, dtab

    return jax.shard_map(device_body, mesh=mesh, in_specs=(tok_spec, act_spec, act_spec, table_spec, full_spec, full_spec, full_spec, full_spec), out_specs=(act_spec, table_spec), check_vma=False)
```

```python
import functools

import jax
import jax.numpy as jnp
from jax import lax
from jax.experimental import pallas as pl
from jax.experimental.pallas import tpu as pltpu
from jax.sharding import PartitionSpec as P

NORM_EPS = 1e-6
BF = jnp.bfloat16
F32 = jnp.float32
I32 = jnp.int32
VMEM_BYTES = 67043328
GELU_C = 0.7978845608028654
GELU_A = 0.044715

MESH_AXES = ('dp', 'emb')
CAP = 256


def gelu(x):
    return 0.5 * x * (1.0 + jnp.tanh(GELU_C * (x + GELU_A * (x * x * x))))


def gelu_slope(x):
    sq = x * x
    th = jnp.tanh(GELU_C * (x + GELU_A * (x * sq)))
    return 0.5 * (1.0 + th) + (0.5 * GELU_C) * x * (1.0 - th * th) * (1.0 + (3 * GELU_A) * sq)


def dot(a, b):
    return jnp.dot(a, b, preferred_element_type=F32)


def dot_t(a, b):
    return lax.dot_general(a, b, (((1,), (1,)), ((), ())), preferred_element_type=F32)


def row_loop(rows, slab, unroll=2):
    def run(body):
        def step(i, carry):
            body(pl.ds(pl.multiple_of(i * slab, slab), slab))
            return carry

        lax.fori_loop(0, rows // slab, step, 0, unroll=unroll)

    return run


def peer_of(n_emb, index):
    dp = index // n_emb
    return {'dp': dp, 'emb': index - dp * n_emb}


def remote(src, dst, send_sem, recv_sem, device):
    return pltpu.make_async_remote_copy(src_ref=src, dst_ref=dst, send_sem=send_sem, recv_sem=recv_sem,
                                        device_id=device, device_id_type=pl.DeviceIdType.MESH)


def meet(devices):
    barrier = pltpu.get_barrier_semaphore()
    for device in devices:
        pl.semaphore_signal(barrier, inc=1, device_id=device, device_id_type=pl.DeviceIdType.MESH)
    pl.semaphore_wait(barrier, len(devices))


def ids_kernel(cfg, in_ref, out_ref, send_sem, recv_sem):
    n_dp, n_emb = cfg
    n_dev = n_dp * n_emb
    me = lax.axis_index('dp') * n_emb + lax.axis_index('emb')
    peers = [peer_of(n_emb, lax.rem(me + k, n_dev)) for k in range(1, n_dev)]
    meet(peers)
    copies = [remote(in_ref, out_ref.at[me], send_sem.at[k], recv_sem.at[k], peer) for k, peer in enumerate(peers)]
    for copy in copies:
        copy.start()
    out_ref[me] = in_ref[...]
    for copy in copies:
        copy.wait()


def gather_kernel(cfg, loc_ref, counts_ref, pick_ref, tables_hbm, out_ref, buf, sems):
    n_layers, n_dest, cap, per_dot, group = cfg
    trip = per_dot * group
    n_trips = [(counts_ref[d] + (trip - 1)) // trip for d in range(n_dest)]

    def row_copy(d, s):
        base = pl.multiple_of(jnp.left_shift(jnp.right_shift(loc_ref[s], 3), 3), 8)
        return pltpu.make_async_copy(
            tables_hbm.at[:, pl.ds(base, 8), :], buf.at[:, pl.ds(pl.multiple_of(s * 8, 8), 8), :], sems.at[d])

    for d in range(n_dest):
        def issue(i, carry, d=d):
            for k in range(8):
                row_copy(d, d * cap + i * 8 + k).start(priority=k % 2)
            return carry

        lax.fori_loop(0, n_trips[d] * (trip // 8), issue, 0)

    for d in range(n_dest):
        def drain(i, carry, d=d):
            part = buf.at[:, pl.ds(pl.multiple_of((d * cap + i * trip) * 8, 8), trip * 8), :]
            pltpu.make_async_copy(part, part, sems.at[d]).wait()
            return carry

        lax.fori_loop(0, n_trips[d], drain, 0)

        def pick(i, carry, d=d):
            for k in range(group):
                s0 = pl.multiple_of(d * cap + i * trip + k * per_dot, per_dot)
                want = pick_ref[pl.ds(s0, per_dot), :]
                sel = (lax.broadcasted_iota(I32, (per_dot, per_dot * 8), 1) == want).astype(BF)
                for l in range(n_layers):
                    rows = buf[l, pl.ds(pl.multiple_of(s0 * 8, 8), per_dot * 8), :]
                    out_ref[l, pl.ds(s0, per_dot), :] = dot(sel, rows).astype(BF)
            return carry

        lax.fori_loop(0, n_trips[d], pick, 0)

        def blank(i, carry, d=d):
            s0 = pl.multiple_of(d * cap + i * trip, trip)
            for l in range(n_layers):
                out_ref[l, pl.ds(s0, trip), :] = jnp.zeros((trip, out_ref.shape[2]), BF)
            return carry

        lax.fori_loop(n_trips[d], cap // trip, blank, 0)


def weight_copies(wu_hbm, wd_hbm, wu_s, wd_s, sems):
    fb = wu_s.shape[2]

    def copies(layer, blk, slot):
        at = pl.multiple_of(blk * fb, fb)
        return (pltpu.make_async_copy(wu_hbm.at[layer, :, pl.ds(at, fb)], wu_s.at[slot], sems.at[0, slot]),
                pltpu.make_async_copy(wd_hbm.at[layer, pl.ds(at, fb), :], wd_s.at[slot], sems.at[1, slot]))

    return copies


def start(copies):
    for copy in copies:
        copy.start()


def wait(copies):
    for copy in copies:
        copy.wait()


def mlp_block(cfg, u_s, h_s, acc_s, wu_ref, wd_ref, up_ref):
    cw, nw = cfg
    gw = 128
    n_c = wu_ref.shape[1] // cw

    def act(c):
        for g in range(cw // gw):
            gs = slice(c * cw + g * gw, c * cw + (g + 1) * gw)
            h_s[:, gs] = gelu(up_ref[:, gs]).astype(BF)

    for c in range(n_c):
        cs = slice(c * cw, (c + 1) * cw)
        up_ref[:, cs] = dot(u_s[...], wu_ref[:, cs])
        if c > 0:
            act(c - 1)
    for c in range(n_c):
        cs = slice(c * cw, (c + 1) * cw)
        for n in range(acc_s.shape[1] // nw):
            ns = slice(n * nw, (n + 1) * nw)
            acc_s[:, ns] += dot(h_s[:, cs], wd_ref[cs, ns])
        if c == 0:
            act(n_c - 1)


def norm_rows(x, sl, u_s, acc_s):
    scale = lax.rsqrt(jnp.mean(x * x, axis=-1, keepdims=True) + NORM_EPS)
    u_s[sl, :] = (x * scale).astype(BF)
    acc_s[sl, :] = x


def add_proj(nw, acc_s, mixed, wp_ref):
    for n in range(acc_s.shape[1] // nw):
        ns = slice(n * nw, (n + 1) * nw)
        acc_s[:, ns] += dot(mixed, wp_ref[:, ns])


def first_kernel(cfg, x_hbm, slot_ref, served_hbm, wg_hbm, wp_hbm, wu_hbm, wd_hbm,
                 x_out_ref, gate_ref, fet_ref,
                 u_s, acc_s, h_s, up_s, ret_s, wu_s, wd_s, wg_s, wp_s, in_sem, w_sem, self_sem, send_sem, recv_sem):
    n_dp, n_emb, cap, n_blk, cw, nw, slab = cfg
    tok, dim = u_s.shape
    my_emb = lax.axis_index('emb')
    my_dp = lax.axis_index('dp')
    here = ret_s.at[:, pl.ds(pl.multiple_of(my_emb * cap, cap), cap), :]
    own = pltpu.make_async_copy(served_hbm.at[:, pl.ds(pl.multiple_of(my_emb * cap, cap), cap), :], here, self_sem)
    peers = [lax.rem(my_emb + k, n_emb) for k in range(1, n_emb)]
    copies = [remote(served_hbm.at[:, pl.ds(pl.multiple_of(p * cap, cap), cap), :], here,
                     send_sem.at[k], recv_sem.at[k], {'dp': my_dp, 'emb': p}) for k, p in enumerate(peers)]
    weights = weight_copies(wu_hbm, wd_hbm, wu_s, wd_s, w_sem)
    first = [pltpu.make_async_copy(x_hbm, x_out_ref, in_sem.at[0]),
             pltpu.make_async_copy(wg_hbm.at[0], wg_s, in_sem.at[1]),
             pltpu.make_async_copy(wp_hbm.at[0], wp_s, in_sem.at[2])]
    start(first[:2])
    start(weights(0, 0, 0))
    start(first[2:])
    meet([{'dp': my_dp, 'emb': p} for p in peers])
    own.start()
    start(copies)
    first[0].wait()
    row_loop(tok, slab)(lambda sl: norm_rows(x_out_ref[sl, :].astype(F32), sl, u_s, acc_s))
    first[1].wait()
    gate_ref[0] = dot(u_s[...], wg_s[...])

    def block(f, carry):
        slot = lax.rem(f, 2)

        @pl.when(f + 1 < n_blk)
        def _():
            start(weights(0, f + 1, 1 - slot))

        wait(weights(0, f, slot))
        mlp_block((cw, nw), u_s, h_s, acc_s, wu_s.at[slot], wd_s.at[slot], up_s)
        return carry

    lax.fori_loop(0, n_blk, block, 0)
    own.wait()
    wait(copies)
    first[2].wait()
    sel = (lax.broadcasted_iota(I32, (tok, n_emb * cap), 1) == slot_ref[...]).astype(BF)
    for l in range(fet_ref.shape[0]):
        fet_ref[l] = dot(sel, ret_s[l]).astype(BF)
    add_proj(nw, acc_s, (gelu(gate_ref[0]) * fet_ref[0].astype(F32)).astype(BF), wp_s)

    def finish(sl):
        x_out_ref[sl, :] = acc_s[sl, :].astype(BF)

    row_loop(tok, slab)(finish)


def forward_kernel(cfg, x_hbm, cot_hbm, fet_ref, wg_hbm, wp_hbm, wu_hbm, wd_hbm,
                   out_hbm, saved_hbm, ups_hbm, gate_ref, rows_ref, dgp_ref, dtab_hbm,
                   x_s, u_s, acc_s, h_s, up_s, zero_s, wu_s, wd_s, wg_s, wp_s, in_sem, w_sem, up_sem, out_sem, z_sem):
    n_layers, n_blk, cw, nw, slab, z_per, z_chunks = cfg
    tok, dim = x_s.shape
    fb = wu_s.shape[2]
    z_rows = zero_s.shape[0]
    n_steps = n_layers * n_blk
    weights = weight_copies(wu_hbm, wd_hbm, wu_s, wd_s, w_sem)

    def z_copies(step):
        found = []
        for j in range(z_per):
            c = step * z_per + j
            zl = c // z_chunks
            zc = c - zl * z_chunks
            found.append(pltpu.make_async_copy(
                zero_s, dtab_hbm.at[zl, pl.ds(pl.multiple_of(zc * z_rows, 8), z_rows), :], z_sem.at[j]))
        return found

    def up_copy(layer, blk, slot):
        return pltpu.make_async_copy(up_s.at[slot], ups_hbm.at[layer, :, pl.ds(pl.multiple_of(blk * fb, fb), fb)], up_sem.at[slot])

    def gate_copy(layer):
        return pltpu.make_async_copy(wg_hbm.at[layer + 1], wg_s, in_sem.at[1])

    def proj_copy(layer):
        return pltpu.make_async_copy(wp_hbm.at[layer + 1], wp_s, in_sem.at[2])

    fetch = pltpu.make_async_copy(x_hbm, x_s, in_sem.at[0])
    fetch.start()
    gate_copy(0).start()
    start(weights(1, 0, 0))
    proj_copy(0).start()
    row_loop(z_rows, 8, 1)(lambda sl: zero_s.__setitem__((sl, slice(None)), jnp.zeros((8, zero_s.shape[1]), F32)))
    fetch.wait()
    row_loop(tok, slab)(lambda sl: norm_rows(x_s[sl, :].astype(F32), sl, u_s, acc_s))

    def one_layer(layer, carry):
        gate_copy(layer).wait()
        gate_ref[layer] = dot(u_s[...], wg_s[...])

        @pl.when(layer + 1 < n_layers)
        def _():
            gate_copy(layer + 1).start()

        def block(f, carry):
            step = layer * n_blk + f
            slot = lax.rem(step, 2)

            @pl.when(step + 1 < n_steps)
            def _():
                nxt = step + 1
                start(weights(1 + nxt // n_blk, lax.rem(nxt, n_blk), 1 - slot))

            @pl.when(step > 0)
            def _():
                wait(z_copies(step - 1))

            start(z_copies(step))

            @pl.when(step > 1)
            def _():
                up_copy(layer, f, slot).wait()

            wait(weights(1 + layer, f, slot))
            mlp_block((cw, nw), u_s, h_s, acc_s, wu_s.at[slot], wd_s.at[slot], up_s.at[slot])
            up_copy(layer, f, slot).start()
            return carry

        lax.fori_loop(0, n_blk, block, 0)
        proj_copy(layer).wait()
        add_proj(nw, acc_s, (gelu(gate_ref[layer]) * fet_ref[layer + 1].astype(F32)).astype(BF), wp_s)

        @pl.when(layer > 0)
        def _():
            pltpu.make_async_copy(x_s, saved_hbm.at[layer - 1], out_sem).wait()

        def next_rows(sl):
            x_new = acc_s[sl, :].astype(BF)
            x_s[sl, :] = x_new
            norm_rows(x_new.astype(F32), sl, u_s, acc_s)

        row_loop(tok, slab)(next_rows)

        @pl.when(layer < n_layers - 1)
        def _():
            pltpu.make_async_copy(x_s, saved_hbm.at[layer], out_sem).start()
            proj_copy(layer + 1).start()

        return carry

    lax.fori_loop(0, n_layers, one_layer, 0)
    put = pltpu.make_async_copy(x_s, out_hbm, out_sem)
    put.start()
    get = pltpu.make_async_copy(cot_hbm, u_s, in_sem.at[0])
    get.start()
    wait(z_copies(n_steps - 1))
    up_copy(0, 0, 0).wait()
    up_copy(0, 0, 1).wait()
    get.wait()
    d_mixed = dot_t(u_s[...], wp_s[...]).astype(BF).astype(F32)
    gate_grads(gate_ref[n_layers - 1], fet_ref[n_layers], d_mixed, rows_ref, dgp_ref)
    put.wait()


def gate_grads(gate_pre, fetched, d_mixed, rows_ref, dgp_ref):
    rows_ref[...] = gelu(gate_pre) * d_mixed
    dgp_ref[...] = (d_mixed * fetched.astype(F32) * gelu_slope(gate_pre)).astype(BF)


def to_slots(rows, slot_ref, slots_s):
    hi = rows.astype(BF)
    rest = rows - hi.astype(F32)
    mid = rest.astype(BF)
    low = (rest - mid.astype(F32)).astype(BF)
    n = slots_s.shape[0] * slots_s.shape[2]
    sel = slot_pick(n, slot_ref)
    slots = (dot(sel, hi) + dot(sel, mid)) + dot(sel, low)
    for h in range(slots_s.shape[1]):
        slots_s[:, h] = slots[:, h * 128:(h + 1) * 128].reshape(n // 8, 8, 128)


def slot_pick(n, slot_ref):
    return (lax.broadcasted_iota(I32, (n, slot_ref.shape[1]), 0) == slot_ref[...]).astype(BF)


def backward_kernel(cfg, cot_hbm, x1_hbm, saved_hbm, rows_in_ref, dgp_in_ref, slot_ref, gate0_ref, gate_ref, fet_ref,
                    ups_hbm, wu_hbm, wd_hbm, wg_hbm, wp_hbm,
                    got_hbm, gate_hbm, slots0_ref,
                    cot_s, x_s, acc_s, dup_s, dh_s, dng_s, slots_s, gslots_s, rows_s, dgp_s, up_s, wu_s, wd_s, wg_s, wp_s,
                    in_sem, w_sem, up_sem, send_sem, self_sem, recv_sem):
    n_layers, n_blk, n_dp, n_emb, cap, cw, nw, slab = cfg
    tok, dim = cot_s.shape
    fb = wu_s.shape[2]
    gw = 128
    n_dev = n_dp * n_emb
    n_steps = n_layers * n_blk
    my_emb = lax.axis_index('emb')
    me = lax.axis_index('dp') * n_emb + my_emb
    peers = [peer_of(n_emb, lax.rem(me + k, n_dev)) for k in range(1, n_dev)]
    weights = weight_copies(wu_hbm, wd_hbm, wu_s, wd_s, w_sem)

    def part(ref, emb):
        return ref.at[pl.ds(emb * (cap // 8), cap // 8)]

    def sends(ref, there, which, got):
        return [pltpu.make_async_copy(part(ref, my_emb), there, self_sem.at[which])] + [
            remote(part(ref, peer['emb']), there, send_sem.at[which, k], recv_sem.at[got, k], peer) for k, peer in enumerate(peers)]

    def row_sends(i):
        return sends(slots_s, part(got_hbm.at[n_layers - 1 - i], me), 0, i)

    gate_sends = sends(gslots_s, part(gate_hbm, me), 1, n_layers)

    def up_copy(step, slot):
        i = step // n_blk
        blk = step - i * n_blk
        return pltpu.make_async_copy(ups_hbm.at[n_layers - 1 - i, :, pl.ds(pl.multiple_of(blk * fb, fb), fb)], up_s.at[slot], up_sem.at[slot])

    def load(step, slot):
        i = step // n_blk
        return weights(n_layers - i, step - i * n_blk, slot) + (up_copy(step, slot),)

    def gate_copy(i):
        return pltpu.make_async_copy(wg_hbm.at[n_layers - i], wg_s, in_sem.at[1])

    def proj_copy(i):
        return pltpu.make_async_copy(wp_hbm.at[n_layers - 1 - i], wp_s, in_sem.at[2])

    def x_copy(i):
        return pltpu.make_async_copy(saved_hbm.at[n_layers - 2 - i], x_s, in_sem.at[3])

    fetch = pltpu.make_async_copy(cot_hbm, cot_s, in_sem.at[0])
    gate_copy(0).start()
    fetch.start()
    start(load(0, 0))
    proj_copy(0).start()
    rows_s[...] = rows_in_ref[...]
    dgp_s[...] = dgp_in_ref[...]

    def clear(sl):
        acc_s[sl, :] = jnp.zeros((slab, dim), F32)

    row_loop(tok, slab)(clear)
    meet(peers)
    to_slots(gelu(gate0_ref[0]), slot_ref, gslots_s)

    def one_layer(i, carry):
        @pl.when(i < n_layers - 1)
        def _():
            x_copy(i).start()

        @pl.when(i == n_layers - 1)
        def _():
            pltpu.make_async_copy(x1_hbm, x_s, in_sem.at[3]).start()

        to_slots(rows_s[...], slot_ref, slots_s)
        gate_copy(i).wait()
        for n in range(dim // nw):
            ns = slice(n * nw, (n + 1) * nw)
            dng_s[:, ns] = dot_t(dgp_s[...], wg_s[ns, :]).astype(BF)
        start(row_sends(i))

        @pl.when(i < n_layers - 1)
        def _():
            gate_copy(i + 1).start()

        @pl.when(i == 0)
        def _():
            start(gate_sends)
            fetch.wait()

        def block(f, carry):
            step = i * n_blk + f
            slot = lax.rem(step, 2)

            @pl.when(step + 1 < n_steps)
            def _():
                start(load(step + 1, 1 - slot))

            wait(load(step, slot))
            wu_ref, wd_ref, up_ref = wu_s.at[slot], wd_s.at[slot], up_s.at[slot]

            def act(c):
                for g in range(cw // gw):
                    gs = slice(c * cw + g * gw, c * cw + (g + 1) * gw)
                    dup_s[:, gs] = (dh_s[:, gs].astype(F32) * gelu_slope(up_ref[:, gs])).astype(BF)

            n_c = fb // cw
            for c in range(n_c):
                cs = slice(c * cw, (c + 1) * cw)
                dh_s[:, cs] = dot_t(cot_s[...], wd_ref[cs, :]).astype(BF)
                if c > 0:
                    act(c - 1)
            for c in range(n_c):
                cs = slice(c * cw, (c + 1) * cw)
                for n in range(dim // nw):
                    ns = slice(n * nw, (n + 1) * nw)
                    acc_s[:, ns] += dot_t(dup_s[:, cs], wu_ref[ns, cs])
                if c == 0:
                    act(n_c - 1)
            return carry

        lax.fori_loop(0, n_blk, block, 0)
        pltpu.make_async_copy(x1_hbm, x_s, in_sem.at[3]).wait()

        def rows_back(sl):
            x = x_s[sl, :].astype(F32)
            scale = lax.rsqrt(jnp.mean(x * x, axis=-1, keepdims=True) + NORM_EPS)
            d_n = (acc_s[sl, :].astype(BF).astype(F32) + dng_s[sl, :].astype(F32)).astype(BF).astype(F32)
            acc_s[sl, :] = jnp.zeros((slab, dim), F32)
            proj = jnp.mean(d_n * x, axis=-1, keepdims=True)
            d_x = d_n * scale - x * (proj * (scale * scale * scale))
            cot_s[sl, :] = (cot_s[sl, :].astype(F32) + d_x).astype(BF)

        row_loop(tok, slab)(rows_back)
        proj_copy(i).wait()
        d_mixed = dot_t(cot_s[...], wp_s[...]).astype(BF)
        wait(row_sends(i))

        @pl.when(i < n_layers - 1)
        def _():
            proj_copy(i + 1).start()
            gate_grads(gate_ref[jnp.maximum(n_layers - 2 - i, 0)], fet_ref[n_layers - 1 - i], d_mixed.astype(F32), rows_s, dgp_s)

        @pl.when(i == n_layers - 1)
        def _():
            slots = dot(slot_pick(n_emb * cap, slot_ref), d_mixed).astype(BF)
            for d in range(n_dp):
                slots0_ref[d] = slots

        return carry

    lax.fori_loop(0, n_layers, one_layer, 0)
    wait(gate_sends)


def scatter_kernel(cfg, read_ref, write_ref, group_ref, meta_ref, rows_ref, gate_ref, mixed_ref, dt_in, dt_out, groups, prod, sems):
    unroll, window, bulk = cfg
    n_layers = groups.shape[1]
    n_slots = mixed_ref.shape[0]
    count = meta_ref[0]

    def product(i, carry):
        step = 64
        mixed = mixed_ref[pl.ds(pl.multiple_of(i * step, step), step), :].astype(F32)
        for h in range(2):
            at = pl.ds(i * (step // 8), step // 8)
            prod[at, h] = gate_ref[at, h] * mixed[:, h * 128:(h + 1) * 128].reshape(step // 8, 8, 128)
        return carry

    lax.fori_loop(0, n_slots // 64, product, 0, unroll=4)
    words = prod.reshape(n_slots * 2, 128)
    sub_iota = lax.broadcasted_iota(I32, (8, 128), 0)

    def move(buf, spot, group, n):
        return pltpu.make_async_copy(groups.at[buf, :, pl.ds(spot, n)], dt_out.at[:, pl.ds(group, n)], sems.at[buf])

    def settle(w):
        n = meta_ref[1 + w]

        def drain_bulk(j, carry):
            move(w % 2, 0, 0, bulk).wait()
            return carry

        def drain(j, carry):
            move(w % 2, 0, 0, 1).wait()
            return carry

        lax.fori_loop(0, n // bulk, drain_bulk, 0)
        lax.fori_loop(0, lax.rem(n, bulk), drain, 0)

    n_win = n_slots // window
    accs = tuple(jnp.zeros((8, 128), F32) for _ in range(2 * n_layers))
    for w in range(n_win):
        buf = w % 2
        if w >= 2:
            settle(w - 2)
        left = jnp.clip(count - w * window, 0, window)
        trips = (left + (unroll - 1)) // unroll

        def add(t, accs, w=w, buf=buf):
            for k in range(unroll):
                j = w * window + t * unroll + k
                word = read_ref[j]
                at = jnp.bitwise_and(word, n_slots * 2 - 1)
                sub = jnp.bitwise_and(jnp.right_shift(word, 12), 7)
                same = word < 0
                here = sub_iota == sub
                spot = jnp.bitwise_and(write_ref[j], window - 1)
                new = []
                for l in range(n_layers):
                    for h in range(2):
                        src = words if l == 0 else rows_ref.at[l - 1]
                        row = jnp.broadcast_to(src[pl.ds(at + 8 * h, 1), :], (8, 128))
                        acc = jnp.where(same, accs[2 * l + h], 0.0) + jnp.where(here, row, 0.0)
                        groups[buf, l, spot, :, h * 128:(h + 1) * 128] = acc
                        new.append(acc)
                accs = tuple(new)
            return accs

        accs = lax.fori_loop(0, trips, add, accs)

        def put(t, carry, w=w, buf=buf):
            for k in range(unroll):
                j = w * window + t * unroll + k
                word = write_ref[j]

                @pl.when(word < 0)
                def _(j=j, word=word):
                    move(buf, jnp.bitwise_and(word, window - 1), group_ref[j], 1).start()

            return carry

        lax.fori_loop(0, trips, put, 0)
    for w in range(max(n_win - 2, 0), n_win):
        settle(w)


def solution(mesh):
    n_emb, n_dp = mesh.shape['emb'], mesh.shape['dp']
    n_dev = n_emb * n_dp
    tok_spec = P(('dp', 'emb'))
    act_spec = P(('dp', 'emb'), None)
    table_spec = P(None, 'emb', None)
    full_spec = P(None, None, None)
    hbm = pl.BlockSpec(memory_space=pl.ANY)
    vm = pl.BlockSpec(memory_space=pltpu.VMEM)
    sm = pl.BlockSpec(memory_space=pltpu.SMEM)
    big = jnp.iinfo(jnp.int32).max

    def params(n_grid, **kw):
        return pltpu.CompilerParams(vmem_limit_bytes=VMEM_BYTES, dimension_semantics=('arbitrary',) * n_grid if n_grid else None, **kw)

    def device_body(tok_ids, resid_in, cot_out, tables, w_up, w_down, w_gate, w_proj):
        n_layers, range_rows, e_dim = tables.shape
        tok = tok_ids.shape[0]
        dim, ffn = w_up.shape[1:]
        n_slots, n_serve = n_dev * CAP, n_emb * CAP
        my_emb, my_dp = lax.axis_index('emb'), lax.axis_index('dp')

        lanes = 128
        ids8 = pl.pallas_call(
            functools.partial(ids_kernel, (n_dp, n_emb)),
            out_shape=jax.ShapeDtypeStruct((n_dev, tok // lanes, lanes), I32),
            in_specs=[vm], out_specs=vm,
            scratch_shapes=[pltpu.SemaphoreType.DMA((n_dev - 1,)), pltpu.SemaphoreType.DMA((n_dev - 1,))],
            compiler_params=pltpu.CompilerParams(collective_id=0, has_side_effects=True),
            name='all_ids',
        )(tok_ids.reshape(tok // lanes, lanes)).reshape(n_dev, tok)
        mine = (ids8 // range_rows) == my_emb
        t_iota = jnp.arange(tok, dtype=I32)
        before = t_iota[None, :] < t_iota[:, None]
        rank8 = jnp.sum((mine[:, None, :] & before[None]).astype(I32), axis=-1)
        c_iota = jnp.arange(CAP, dtype=I32)
        hit = mine[:, None, :] & (rank8[:, None, :] == c_iota[None, :, None])
        recv_loc = jnp.sum(jnp.where(hit, (ids8 - my_emb * range_rows)[:, None, :], 0), axis=-1)
        counts = jnp.sum(mine.astype(I32), axis=-1)
        valid = c_iota[None, :] < counts[:, None]
        slot_bits = (n_slots - 1).bit_length()
        slot_ids = jnp.arange(n_slots, dtype=I32).reshape(n_dev, CAP)
        keys = jnp.where(valid, recv_loc * (1 << slot_bits) + slot_ids, big)
        window, sub = 512, 8
        skeys = lax.sort(keys.reshape(-1))
        total = jnp.sum(counts)
        order = jnp.arange(n_slots, dtype=I32)
        live = order < total
        slot = jnp.bitwise_and(skeys, (1 << slot_bits) - 1)
        row = jnp.right_shift(skeys, slot_bits)
        group = jnp.right_shift(row, 3)
        edge = group[1:] != group[:-1]
        one = jnp.ones((1,), jnp.bool_)
        fresh = jnp.concatenate([one, edge])
        last = jnp.concatenate([edge, one]) & live
        place = jnp.cumsum(fresh.astype(I32)).reshape(-1, window)
        place = (place - place[:, :1]).reshape(-1)
        sign = jnp.int32(-(1 << 31))
        read_word = jnp.right_shift(slot, 3) * 16 + jnp.bitwise_and(slot, 7) + jnp.left_shift(jnp.bitwise_and(row, 7), 12)
        read_word = read_word + jnp.where(fresh, 0, sign)
        write_word = place + jnp.where(last, sign, 0)
        group_word = jnp.where(live, group, 0)
        meta = jnp.concatenate([total.reshape(1), jnp.sum(last.reshape(-1, window).astype(I32), axis=1)])

        my_owner = tok_ids // range_rows
        rank = jnp.sum(((my_owner[None, :] == my_owner[:, None]) & before).astype(I32), axis=-1)
        slot_of = my_owner * CAP + rank

        spread = jnp.where(valid, recv_loc, lax.rem(slot_ids * 8, range_rows))
        want = lax.dynamic_slice_in_dim(spread, my_dp * n_emb, n_emb, 0).reshape(-1)
        n_want = lax.dynamic_slice_in_dim(counts, my_dp * n_emb, n_emb, 0)
        per_dot, group = 32, 2
        pick = (jnp.bitwise_and(want, 7) + 8 * (jnp.arange(n_serve, dtype=I32) % per_dot))[:, None]
        served = pl.pallas_call(
            functools.partial(gather_kernel, (n_layers, n_emb, CAP, per_dot, group)),
            out_shape=jax.ShapeDtypeStruct((n_layers, n_serve, e_dim), BF),
            in_specs=[sm, sm, vm, hbm],
            out_specs=vm,
            scratch_shapes=[pltpu.VMEM((n_layers, n_serve * 8, e_dim), BF), pltpu.SemaphoreType.DMA((n_emb,))],
            compiler_params=params(0),
            name='table_rows',
        )(want, n_want, pick, tables)

        fb = 1024
        n_blk = ffn // fb
        cw, nw, slab = 512, 512, 16
        n_back = n_layers - 1
        z_rows = 1336
        z_chunks = range_rows // z_rows
        z_per = n_layers * z_chunks // (n_back * n_blk)
        assert z_chunks * z_rows == range_rows and z_per * n_blk * n_back == z_chunks * n_layers

        matmul_flops = 4 * tok * dim * ffn
        w_bufs = [pltpu.VMEM((2, dim, fb), BF), pltpu.VMEM((2, fb, dim), BF), pltpu.VMEM((dim, e_dim), BF), pltpu.VMEM((e_dim, dim), BF)]
        dma = pltpu.SemaphoreType.DMA
        x1, gate0, fetched = pl.pallas_call(
            functools.partial(first_kernel, (n_dp, n_emb, CAP, n_blk, cw, nw, slab)),
            out_shape=[
                jax.ShapeDtypeStruct((tok, dim), BF),
                jax.ShapeDtypeStruct((1, tok, e_dim), F32),
                jax.ShapeDtypeStruct((n_layers, tok, e_dim), BF),
            ],
            in_specs=[hbm, vm, hbm, hbm, hbm, hbm, hbm],
            out_specs=[vm, vm, vm],
            scratch_shapes=[
                pltpu.VMEM((tok, dim), BF), pltpu.VMEM((tok, dim), F32), pltpu.VMEM((tok, fb), BF), pltpu.VMEM((tok, fb), F32),
                pltpu.VMEM((n_layers, n_serve, e_dim), BF), *w_bufs, dma((3,)), dma((2, 2)), dma, dma((n_emb - 1,)), dma((n_emb - 1,)),
            ],
            compiler_params=params(0, collective_id=1, has_side_effects=True),
            cost_estimate=pl.CostEstimate(flops=matmul_flops, bytes_accessed=100 << 20, transcendentals=0),
            name='first_layer',
        )(resid_in, slot_of[:, None], served, w_gate, w_proj, w_up, w_down)

        out, saved, ups, gates, rows, dgp, dtab = pl.pallas_call(
            functools.partial(forward_kernel, (n_back, n_blk, cw, nw, slab, z_per, z_chunks)),
            out_shape=[
                jax.ShapeDtypeStruct((tok, dim), BF),
                jax.ShapeDtypeStruct((n_back - 1, tok, dim), BF),
                jax.ShapeDtypeStruct((n_back, tok, ffn), F32),
                jax.ShapeDtypeStruct((n_back, tok, e_dim), F32),
                jax.ShapeDtypeStruct((tok, e_dim), F32),
                jax.ShapeDtypeStruct((tok, e_dim), BF),
                jax.ShapeDtypeStruct((n_layers, range_rows, e_dim), F32),
            ],
            in_specs=[hbm, hbm, vm, hbm, hbm, hbm, hbm],
            out_specs=[hbm, hbm, hbm, vm, vm, vm, hbm],
            scratch_shapes=[
                pltpu.VMEM((tok, dim), BF), pltpu.VMEM((tok, dim), BF), pltpu.VMEM((tok, dim), F32), pltpu.VMEM((tok, fb), BF),
                pltpu.VMEM((2, tok, fb), F32), pltpu.VMEM((z_rows, e_dim), F32), *w_bufs,
                dma((3,)), dma((2, 2)), dma((2,)), dma, dma((z_per,)),
            ],
            compiler_params=params(0),
            cost_estimate=pl.CostEstimate(flops=n_back * matmul_flops, bytes_accessed=400 << 20, transcendentals=0),
            name='forward',
        )(x1, cot_out, fetched, w_gate, w_proj, w_up, w_down)

        got, got_gate, slots0 = pl.pallas_call(
            functools.partial(backward_kernel, (n_back, n_blk, n_dp, n_emb, CAP, cw, nw, slab)),
            out_shape=[jax.ShapeDtypeStruct((n_back, n_slots // 8, e_dim // 128, 8, 128), F32), jax.ShapeDtypeStruct((n_slots // 8, e_dim // 128, 8, 128), F32),
                       jax.ShapeDtypeStruct((n_dp, n_serve, e_dim), BF)],
            in_specs=[hbm, hbm, hbm, vm, vm, vm, vm, vm, vm, hbm, hbm, hbm, hbm, hbm],
            out_specs=[hbm, hbm, vm],
            scratch_shapes=[
                pltpu.VMEM((tok, dim), BF), pltpu.VMEM((tok, dim), BF), pltpu.VMEM((tok, dim), F32), pltpu.VMEM((tok, fb), BF), pltpu.VMEM((tok, fb), BF),
                pltpu.VMEM((tok, dim), BF), pltpu.VMEM((n_serve // 8, e_dim // 128, 8, 128), F32), pltpu.VMEM((n_serve // 8, e_dim // 128, 8, 128), F32),
                pltpu.VMEM((tok, e_dim), F32), pltpu.VMEM((tok, e_dim), BF), pltpu.VMEM((2, tok, fb), F32), *w_bufs,
                dma((4,)), dma((2, 2)), dma((2,)), dma((2, n_dev - 1)), dma((2,)), dma((n_back + 1, n_dev - 1)),
            ],
            compiler_params=params(0, collective_id=2, has_side_effects=True),
            cost_estimate=pl.CostEstimate(flops=n_back * matmul_flops, bytes_accessed=400 << 20, transcendentals=0),
            name='backward',
        )(cot_out, x1, saved, rows, dgp, slot_of[None, :], gate0, gates, fetched, ups, w_up, w_down, w_gate, w_proj)

        mixed0 = lax.all_to_all(slots0.reshape(n_dev, CAP, e_dim), MESH_AXES, 0, 0, tiled=True).reshape(n_slots, e_dim)
        dtab = pl.pallas_call(
            functools.partial(scatter_kernel, (8, window, 32)),
            out_shape=jax.ShapeDtypeStruct((n_layers, range_rows // sub, sub, e_dim), F32),
            in_specs=[sm, sm, sm, sm, vm, vm, vm, hbm],
            out_specs=hbm,
            input_output_aliases={7: 0},
            scratch_shapes=[pltpu.VMEM((2, n_layers, window, sub, e_dim), F32), pltpu.VMEM((n_slots // 8, e_dim // 128, 8, 128), F32), dma((2,))],
            compiler_params=params(0),
            name='scatter',
        )(read_word, write_word, group_word, meta, got.reshape(n_back, n_slots * 2, 128), got_gate, mixed0,
          dtab.reshape(n_layers, range_rows // sub, sub, e_dim))
        dtab = dtab.reshape(n_layers, range_rows, e_dim)
        return out, dtab

    return jax.shard_map(device_body, mesh=mesh, in_specs=(tok_spec, act_spec, act_spec, table_spec, full_spec, full_spec, full_spec, full_spec), out_specs=(act_spec, table_spec), check_vma=False)
```

```python
import functools

import jax
import jax.numpy as jnp
from jax import lax
from jax.experimental import pallas as pl
from jax.experimental.pallas import tpu as pltpu
from jax.sharding import PartitionSpec as P

NORM_EPS = 1e-6
BF = jnp.bfloat16
F32 = jnp.float32
I32 = jnp.int32
VMEM_BYTES = 67043328
GELU_C = 0.7978845608028654
GELU_A = 0.044715

MESH_AXES = ('dp', 'emb')
CAP = 256


def gelu(x):
    return 0.5 * x * (1.0 + jnp.tanh(GELU_C * (x + GELU_A * (x * x * x))))


def gelu_slope(x):
    sq = x * x
    th = jnp.tanh(GELU_C * (x + GELU_A * (x * sq)))
    return 0.5 * (1.0 + th) + (0.5 * GELU_C) * x * (1.0 - th * th) * (1.0 + (3 * GELU_A) * sq)


def dot(a, b):
    return jnp.dot(a, b, preferred_element_type=F32)


def dot_t(a, b):
    return lax.dot_general(a, b, (((1,), (1,)), ((), ())), preferred_element_type=F32)


def row_loop(rows, slab, unroll=2):
    def run(body):
        def step(i, carry):
            body(pl.ds(pl.multiple_of(i * slab, slab), slab))
            return carry

        lax.fori_loop(0, rows // slab, step, 0, unroll=unroll)

    return run


def peer_of(n_emb, index):
    dp = index // n_emb
    return {'dp': dp, 'emb': index - dp * n_emb}


def remote(src, dst, send_sem, recv_sem, device):
    return pltpu.make_async_remote_copy(src_ref=src, dst_ref=dst, send_sem=send_sem, recv_sem=recv_sem,
                                        device_id=device, device_id_type=pl.DeviceIdType.MESH)


def meet(devices):
    barrier = pltpu.get_barrier_semaphore()
    for device in devices:
        pl.semaphore_signal(barrier, inc=1, device_id=device, device_id_type=pl.DeviceIdType.MESH)
    pl.semaphore_wait(barrier, len(devices))


def plan_kernel(cfg, in_ref, ids_ref, recv_ref, counts_ref, pick_ref, slot_row_ref, slot_col_ref, rank_s, send_sem, recv_sem):
    n_dp, n_emb, cap, range_rows, per_dot = cfg
    n_dev = n_dp * n_emb
    my_dp, my_emb = lax.axis_index('dp'), lax.axis_index('emb')
    me = my_dp * n_emb + my_emb
    n_sub, lanes = in_ref.shape
    tok = n_sub * lanes
    peers = [peer_of(n_emb, lax.rem(me + k, n_dev)) for k in range(1, n_dev)]
    meet(peers)
    copies = [remote(in_ref, ids_ref.at[me], send_sem.at[k], recv_sem.at[k], peer) for k, peer in enumerate(peers)]
    start(copies)
    ids_ref[me] = in_ref[...]

    def line(ref):
        return jnp.concatenate([ref[..., j, :] for j in range(n_sub)], axis=-1)

    def ones(cond):
        return jnp.where(cond, 1.0, 0.0)

    def digits(x):
        return jnp.concatenate([jnp.right_shift(x, 8), jnp.bitwise_and(x, 255)], axis=0).astype(F32).astype(BF)

    square = (tok, tok)
    down, right = lax.broadcasted_iota(I32, square, 0), lax.broadcasted_iota(I32, square, 1)
    earlier = ones(down < right).astype(BF)
    own = jnp.broadcast_to(jnp.concatenate([in_ref[j:j + 1, :] for j in range(n_sub)], axis=-1), (8, tok))
    owner = sum(jnp.where(own >= e * range_rows, 1, 0) for e in range(1, n_emb))
    is_owner = owner == lax.broadcasted_iota(I32, (8, tok), 0)
    own_rank = dot(ones(is_owner).astype(BF), earlier).astype(I32)
    slot_row = jnp.sum(jnp.where(is_owner, own_rank + owner * cap, 0).astype(F32), axis=0, keepdims=True).astype(I32)
    slot_row_ref[...] = slot_row
    turned = dot_t(ones(down == right).astype(BF), digits(jnp.broadcast_to(slot_row, (8, tok))))
    slot_col_ref[...] = (turned[:, 0:1] * 256.0 + turned[:, 8:9]).astype(I32)

    wait(copies)
    ids8 = line(ids_ref)
    low = my_emb * range_rows
    mine = jnp.logical_and(ids8 >= low, ids8 < low + range_rows)
    mine_f = ones(mine)
    rank_s[...] = jnp.where(mine, dot(mine_f.astype(BF), earlier), -1.0)
    counts = jnp.sum(mine_f, axis=1, keepdims=True).astype(I32)
    counts_ref[...] = jnp.broadcast_to(counts, counts_ref.shape)
    loc = digits(jnp.where(mine, ids8 - low, 0))
    c_iota = lax.broadcasted_iota(I32, (cap, tok), 0).astype(F32)
    dev_iota = lax.broadcasted_iota(I32, (n_dev, cap), 0)
    recv = jnp.zeros((n_dev, cap), F32)
    for d in range(n_dev):
        found = dot_t(loc, ones(rank_s[d:d + 1, :] == c_iota).astype(BF))
        recv = jnp.where(dev_iota == d, found[:n_dev] * 256.0 + found[n_dev:], recv)
    slot = dev_iota * cap + lax.broadcasted_iota(I32, (n_dev, cap), 1)
    recv_ref[...] = jnp.where(slot - dev_iota * cap < counts, recv.astype(I32), slot * 8)
    lane16 = lax.broadcasted_iota(I32, (cap, 2 * n_dev), 1)
    row1 = lax.broadcasted_iota(I32, (cap, 1), 0)
    for e in range(n_emb):
        d = my_dp * n_emb + e
        found = dot_t(ones(rank_s[pl.ds(d, 1), :] == c_iota).astype(BF), loc)
        low8 = jnp.sum(jnp.where(lane16 == n_dev + d, found, 0.0), axis=1, keepdims=True).astype(I32)
        pick_ref[e * cap:(e + 1) * cap, :] = jnp.bitwise_and(low8, 7) + 8 * jnp.bitwise_and(row1, per_dot - 1)


def gather_kernel(cfg, loc_ref, counts_ref, pick_ref, tables_hbm, out_ref, dtab_hbm, buf, zero_s, sems, z_sem):
    n_layers, n_dest, cap, per_dot, group, z_chunks = cfg
    trip = per_dot * group
    z_rows = zero_s.shape[0]
    first = lax.axis_index('dp') * n_dest
    n_trips = [(counts_ref[first + d, 0] + (trip - 1)) // trip for d in range(n_dest)]

    def row_copy(d, c):
        base = pl.multiple_of(jnp.left_shift(jnp.right_shift(loc_ref[first + d, c], 3), 3), 8)
        at = pl.multiple_of(d * cap * 8 + c * 8, 8)
        return pltpu.make_async_copy(tables_hbm.at[:, pl.ds(base, 8), :], buf.at[:, pl.ds(at, 8), :], sems.at[d])

    def z_copy(c):
        return pltpu.make_async_copy(zero_s, dtab_hbm.at[0, pl.ds(pl.multiple_of(c * z_rows, 8), z_rows), :], z_sem)

    for d in range(n_dest):
        def issue(i, carry, d=d):
            for k in range(8):
                row_copy(d, i * 8 + k).start()
            return carry

        lax.fori_loop(0, n_trips[d] * (trip // 8), issue, 0)

    clear_rows(zero_s)

    def z_start(c, carry):
        z_copy(c).start(priority=1)
        return carry

    lax.fori_loop(0, z_chunks, z_start, 0)
    for d in range(n_dest):
        def drain(i, carry, d=d):
            part = buf.at[:, pl.ds(pl.multiple_of((d * cap + i * trip) * 8, 8), trip * 8), :]
            pltpu.make_async_copy(part, part, sems.at[d]).wait()
            return carry

        lax.fori_loop(0, n_trips[d], drain, 0)

        def pick(i, carry, d=d):
            for k in range(group):
                s0 = pl.multiple_of(d * cap + i * trip + k * per_dot, per_dot)
                want = pick_ref[pl.ds(s0, per_dot), :]
                sel = (lax.broadcasted_iota(I32, (per_dot, per_dot * 8), 1) == want).astype(BF)
                for l in range(n_layers):
                    rows = buf[l, pl.ds(pl.multiple_of(s0 * 8, 8), per_dot * 8), :]
                    out_ref[l, pl.ds(s0, per_dot), :] = dot(sel, rows).astype(BF)
            return carry

        lax.fori_loop(0, n_trips[d], pick, 0)

        def blank(i, carry, d=d):
            s0 = pl.multiple_of(d * cap + i * trip, trip)
            for l in range(n_layers):
                out_ref[l, pl.ds(s0, trip), :] = jnp.zeros((trip, out_ref.shape[2]), BF)
            return carry

        lax.fori_loop(n_trips[d], cap // trip, blank, 0)

    def z_wait(c, carry):
        z_copy(c).wait()
        return carry

    lax.fori_loop(0, z_chunks, z_wait, 0)


def clear_rows(ref):
    row_loop(ref.shape[0], 8, 1)(lambda sl: ref.__setitem__((sl, slice(None)), jnp.zeros((8, ref.shape[1]), F32)))


def weight_copies(wu_hbm, wd_hbm, wu_s, wd_s, sems):
    fb = wu_s.shape[2]

    def copies(layer, blk, slot):
        at = pl.multiple_of(blk * fb, fb)
        return (pltpu.make_async_copy(wu_hbm.at[layer, :, pl.ds(at, fb)], wu_s.at[slot], sems.at[0, slot]),
                pltpu.make_async_copy(wd_hbm.at[layer, pl.ds(at, fb), :], wd_s.at[slot], sems.at[1, slot]))

    return copies


def start(copies):
    for copy in copies:
        copy.start()


def wait(copies):
    for copy in copies:
        copy.wait()


def mlp_block(cfg, u_s, h_s, acc_s, wu_ref, wd_ref, up_ref):
    cw, nw = cfg
    gw = 128
    n_c = wu_ref.shape[1] // cw

    def act(c):
        for g in range(cw // gw):
            gs = slice(c * cw + g * gw, c * cw + (g + 1) * gw)
            h_s[:, gs] = gelu(up_ref[:, gs]).astype(BF)

    for c in range(n_c):
        cs = slice(c * cw, (c + 1) * cw)
        up_ref[:, cs] = dot(u_s[...], wu_ref[:, cs])
        if c > 0:
            act(c - 1)
    for c in range(n_c):
        cs = slice(c * cw, (c + 1) * cw)
        for n in range(acc_s.shape[1] // nw):
            ns = slice(n * nw, (n + 1) * nw)
            acc_s[:, ns] += dot(h_s[:, cs], wd_ref[cs, ns])
        if c == 0:
            act(n_c - 1)


def norm_rows(x, sl, u_s, acc_s):
    scale = lax.rsqrt(jnp.mean(x * x, axis=-1, keepdims=True) + NORM_EPS)
    u_s[sl, :] = (x * scale).astype(BF)
    acc_s[sl, :] = x


def add_proj(nw, acc_s, mixed, wp_ref):
    for n in range(acc_s.shape[1] // nw):
        ns = slice(n * nw, (n + 1) * nw)
        acc_s[:, ns] += dot(mixed, wp_ref[:, ns])


def first_kernel(cfg, x_hbm, slot_ref, served_hbm, wg_hbm, wp_hbm, wu_hbm, wd_hbm,
                 x_out_ref, gate_ref, fet_ref,
                 u_s, acc_s, h_s, up_s, ret_s, wu_s, wd_s, wg_s, wp_s, in_sem, w_sem, self_sem, send_sem, recv_sem):
    n_dp, n_emb, cap, n_blk, cw, nw, slab = cfg
    tok, dim = u_s.shape
    my_emb = lax.axis_index('emb')
    my_dp = lax.axis_index('dp')
    here = ret_s.at[:, pl.ds(pl.multiple_of(my_emb * cap, cap), cap), :]
    own = pltpu.make_async_copy(served_hbm.at[:, pl.ds(pl.multiple_of(my_emb * cap, cap), cap), :], here, self_sem)
    peers = [lax.rem(my_emb + k, n_emb) for k in range(1, n_emb)]
    copies = [remote(served_hbm.at[:, pl.ds(pl.multiple_of(p * cap, cap), cap), :], here,
                     send_sem.at[k], recv_sem.at[k], {'dp': my_dp, 'emb': p}) for k, p in enumerate(peers)]
    weights = weight_copies(wu_hbm, wd_hbm, wu_s, wd_s, w_sem)
    first = [pltpu.make_async_copy(x_hbm, x_out_ref, in_sem.at[0]),
             pltpu.make_async_copy(wg_hbm.at[0], wg_s, in_sem.at[1]),
             pltpu.make_async_copy(wp_hbm.at[0], wp_s, in_sem.at[2])]
    start(first[:2])
    start(weights(0, 0, 0))
    start(first[2:])
    meet([{'dp': my_dp, 'emb': p} for p in peers])
    own.start()
    start(copies)
    first[0].wait()
    row_loop(tok, slab)(lambda sl: norm_rows(x_out_ref[sl, :].astype(F32), sl, u_s, acc_s))
    first[1].wait()
    gate_ref[0] = dot(u_s[...], wg_s[...])

    def block(f, carry):
        slot = lax.rem(f, 2)

        @pl.when(f + 1 < n_blk)
        def _():
            start(weights(0, f + 1, 1 - slot))

        wait(weights(0, f, slot))
        mlp_block((cw, nw), u_s, h_s, acc_s, wu_s.at[slot], wd_s.at[slot], up_s)
        return carry

    lax.fori_loop(0, n_blk, block, 0)
    own.wait()
    wait(copies)
    first[2].wait()
    sel = (lax.broadcasted_iota(I32, (tok, n_emb * cap), 1) == slot_ref[...]).astype(BF)
    for l in range(fet_ref.shape[0]):
        fet_ref[l] = dot(sel, ret_s[l]).astype(BF)
    add_proj(nw, acc_s, (gelu(gate_ref[0]) * fet_ref[0].astype(F32)).astype(BF), wp_s)

    def finish(sl):
        x_out_ref[sl, :] = acc_s[sl, :].astype(BF)

    row_loop(tok, slab)(finish)


def forward_kernel(cfg, x_hbm, cot_hbm, fet_ref, wg_hbm, wp_hbm, wu_hbm, wd_hbm, dt_in,
                   out_hbm, saved_hbm, ups_hbm, gate_ref, rows_ref, dgp_ref, dtab_hbm,
                   x_s, u_s, acc_s, h_s, up_s, zero_s, wu_s, wd_s, wg_s, wp_s, in_sem, w_sem, up_sem, out_sem, z_sem):
    n_layers, n_blk, cw, nw, slab, z_per, z_chunks = cfg
    tok, dim = x_s.shape
    fb = wu_s.shape[2]
    z_rows = zero_s.shape[0]
    n_steps = n_layers * n_blk
    weights = weight_copies(wu_hbm, wd_hbm, wu_s, wd_s, w_sem)

    def z_copies(step):
        found = []
        for j in range(z_per):
            c = step * z_per + j
            zl = c // z_chunks
            zc = c - zl * z_chunks
            found.append(pltpu.make_async_copy(
                zero_s, dtab_hbm.at[zl + 1, pl.ds(pl.multiple_of(zc * z_rows, 8), z_rows), :], z_sem.at[j]))
        return found

    def up_copy(layer, blk, slot):
        return pltpu.make_async_copy(up_s.at[slot], ups_hbm.at[layer, :, pl.ds(pl.multiple_of(blk * fb, fb), fb)], up_sem.at[slot])

    def gate_copy(layer):
        return pltpu.make_async_copy(wg_hbm.at[layer + 1], wg_s, in_sem.at[1])

    def proj_copy(layer):
        return pltpu.make_async_copy(wp_hbm.at[layer + 1], wp_s, in_sem.at[2])

    fetch = pltpu.make_async_copy(x_hbm, x_s, in_sem.at[0])
    fetch.start()
    gate_copy(0).start()
    start(weights(1, 0, 0))
    proj_copy(0).start()
    clear_rows(zero_s)
    fetch.wait()
    row_loop(tok, slab)(lambda sl: norm_rows(x_s[sl, :].astype(F32), sl, u_s, acc_s))

    def one_layer(layer, carry):
        gate_copy(layer).wait()
        gate_ref[layer] = dot(u_s[...], wg_s[...])

        @pl.when(layer + 1 < n_layers)
        def _():
            gate_copy(layer + 1).start()

        def block(f, carry):
            step = layer * n_blk + f
            slot = lax.rem(step, 2)

            @pl.when(step + 1 < n_steps)
            def _():
                nxt = step + 1
                start(weights(1 + nxt // n_blk, lax.rem(nxt, n_blk), 1 - slot))

            @pl.when(step > 0)
            def _():
                wait(z_copies(step - 1))

            for copy in z_copies(step):
                copy.start(priority=1)

            @pl.when(step > 1)
            def _():
                up_copy(layer, f, slot).wait()

            wait(weights(1 + layer, f, slot))
            mlp_block((cw, nw), u_s, h_s, acc_s, wu_s.at[slot], wd_s.at[slot], up_s.at[slot])
            up_copy(layer, f, slot).start()
            return carry

        lax.fori_loop(0, n_blk, block, 0)
        proj_copy(layer).wait()
        add_proj(nw, acc_s, (gelu(gate_ref[layer]) * fet_ref[layer + 1].astype(F32)).astype(BF), wp_s)

        @pl.when(layer > 0)
        def _():
            pltpu.make_async_copy(x_s, saved_hbm.at[layer - 1], out_sem).wait()

        def next_rows(sl):
            x_new = acc_s[sl, :].astype(BF)
            x_s[sl, :] = x_new
            norm_rows(x_new.astype(F32), sl, u_s, acc_s)

        row_loop(tok, slab)(next_rows)

        @pl.when(layer < n_layers - 1)
        def _():
            pltpu.make_async_copy(x_s, saved_hbm.at[layer], out_sem).start()
            proj_copy(layer + 1).start()

        return carry

    lax.fori_loop(0, n_layers, one_layer, 0)
    put = pltpu.make_async_copy(x_s, out_hbm, out_sem)
    put.start()
    get = pltpu.make_async_copy(cot_hbm, u_s, in_sem.at[0])
    get.start()
    wait(z_copies(n_steps - 1))
    up_copy(0, 0, 0).wait()
    up_copy(0, 0, 1).wait()
    get.wait()
    d_mixed = dot_t(u_s[...], wp_s[...]).astype(BF).astype(F32)
    gate_grads(gate_ref[n_layers - 1], fet_ref[n_layers], d_mixed, rows_ref, dgp_ref)
    put.wait()


def gate_grads(gate_pre, fetched, d_mixed, rows_ref, dgp_ref):
    rows_ref[...] = gelu(gate_pre) * d_mixed
    dgp_ref[...] = (d_mixed * fetched.astype(F32) * gelu_slope(gate_pre)).astype(BF)


def to_slots(rows, slot_ref, slots_s):
    hi = rows.astype(BF)
    rest = rows - hi.astype(F32)
    mid = rest.astype(BF)
    low = (rest - mid.astype(F32)).astype(BF)
    n = slots_s.shape[0] * slots_s.shape[2]
    sel = slot_pick(n, slot_ref)
    slots = (dot(sel, hi) + dot(sel, mid)) + dot(sel, low)
    for h in range(slots_s.shape[1]):
        slots_s[:, h] = slots[:, h * 128:(h + 1) * 128].reshape(n // 8, 8, 128)


def slot_pick(n, slot_ref):
    return (lax.broadcasted_iota(I32, (n, slot_ref.shape[1]), 0) == slot_ref[...]).astype(BF)


def backward_kernel(cfg, cot_hbm, x1_hbm, saved_hbm, rows_in_ref, dgp_in_ref, slot_ref, gate0_ref, gate_ref, fet_ref,
                    ups_hbm, wu_hbm, wd_hbm, wg_hbm, wp_hbm,
                    got_hbm, gate_hbm, slots0_ref,
                    cot_s, x_s, acc_s, dup_s, dh_s, dng_s, slots_s, gslots_s, rows_s, dgp_s, up_s, wu_s, wd_s, wg_s, wp_s,
                    in_sem, w_sem, up_sem, send_sem, self_sem, recv_sem):
    n_layers, n_blk, n_dp, n_emb, cap, cw, nw, slab = cfg
    tok, dim = cot_s.shape
    fb = wu_s.shape[2]
    gw = 128
    n_dev = n_dp * n_emb
    n_steps = n_layers * n_blk
    my_emb = lax.axis_index('emb')
    me = lax.axis_index('dp') * n_emb + my_emb
    peers = [peer_of(n_emb, lax.rem(me + k, n_dev)) for k in range(1, n_dev)]
    weights = weight_copies(wu_hbm, wd_hbm, wu_s, wd_s, w_sem)

    def part(ref, emb):
        return ref.at[pl.ds(emb * (cap // 8), cap // 8)]

    def sends(ref, there, which, got):
        return [pltpu.make_async_copy(part(ref, my_emb), there, self_sem.at[which])] + [
            remote(part(ref, peer['emb']), there, send_sem.at[which, k], recv_sem.at[got, k], peer) for k, peer in enumerate(peers)]

    def row_sends(i):
        return sends(slots_s, part(got_hbm.at[n_layers - 1 - i], me), 0, i)

    gate_sends = sends(gslots_s, part(gate_hbm, me), 1, n_layers)

    def up_copy(step, slot):
        i = step // n_blk
        blk = step - i * n_blk
        return pltpu.make_async_copy(ups_hbm.at[n_layers - 1 - i, :, pl.ds(pl.multiple_of(blk * fb, fb), fb)], up_s.at[slot], up_sem.at[slot])

    def load(step, slot):
        i = step // n_blk
        return weights(n_layers - i, step - i * n_blk, slot) + (up_copy(step, slot),)

    def gate_copy(i):
        return pltpu.make_async_copy(wg_hbm.at[n_layers - i], wg_s, in_sem.at[1])

    def proj_copy(i):
        return pltpu.make_async_copy(wp_hbm.at[n_layers - 1 - i], wp_s, in_sem.at[2])

    def x_copy(i):
        return pltpu.make_async_copy(saved_hbm.at[n_layers - 2 - i], x_s, in_sem.at[3])

    fetch = pltpu.make_async_copy(cot_hbm, cot_s, in_sem.at[0])
    gate_copy(0).start()
    fetch.start()
    start(load(0, 0))
    proj_copy(0).start()
    rows_s[...] = rows_in_ref[...]
    dgp_s[...] = dgp_in_ref[...]

    def clear(sl):
        acc_s[sl, :] = jnp.zeros((slab, dim), F32)

    row_loop(tok, slab)(clear)
    meet(peers)
    to_slots(gelu(gate0_ref[0]), slot_ref, gslots_s)

    def one_layer(i, carry):
        @pl.when(i < n_layers - 1)
        def _():
            x_copy(i).start()

        @pl.when(i == n_layers - 1)
        def _():
            pltpu.make_async_copy(x1_hbm, x_s, in_sem.at[3]).start()

        gate_copy(i).wait()
        to_slots(rows_s[...], slot_ref, slots_s)
        for n in range(dim // nw):
            ns = slice(n * nw, (n + 1) * nw)
            dng_s[:, ns] = dot_t(dgp_s[...], wg_s[ns, :]).astype(BF)
        start(row_sends(i))

        @pl.when(i < n_layers - 1)
        def _():
            gate_copy(i + 1).start()

        @pl.when(i == 0)
        def _():
            start(gate_sends)
            fetch.wait()

        def block(f, carry):
            step = i * n_blk + f
            slot = lax.rem(step, 2)

            @pl.when(step + 1 < n_steps)
            def _():
                start(load(step + 1, 1 - slot))

            wait(load(step, slot))
            wu_ref, wd_ref, up_ref = wu_s.at[slot], wd_s.at[slot], up_s.at[slot]

            def act(c):
                for g in range(cw // gw):
                    gs = slice(c * cw + g * gw, c * cw + (g + 1) * gw)
                    dup_s[:, gs] = (dh_s[:, gs].astype(F32) * gelu_slope(up_ref[:, gs])).astype(BF)

            n_c = fb // cw
            for c in range(n_c):
                cs = slice(c * cw, (c + 1) * cw)
                dh_s[:, cs] = dot_t(cot_s[...], wd_ref[cs, :]).astype(BF)
                if c > 0:
                    act(c - 1)
            for c in range(n_c):
                cs = slice(c * cw, (c + 1) * cw)
                for n in range(dim // nw):
                    ns = slice(n * nw, (n + 1) * nw)
                    acc_s[:, ns] += dot_t(dup_s[:, cs], wu_ref[ns, cs])
                if c == 0:
                    act(n_c - 1)
            return carry

        lax.fori_loop(0, n_blk, block, 0)
        pltpu.make_async_copy(x1_hbm, x_s, in_sem.at[3]).wait()

        def rows_back(sl):
            x = x_s[sl, :].astype(F32)
            scale = lax.rsqrt(jnp.mean(x * x, axis=-1, keepdims=True) + NORM_EPS)
            d_n = (acc_s[sl, :].astype(BF) + dng_s[sl, :]).astype(F32)
            acc_s[sl, :] = jnp.zeros((slab, dim), F32)
            proj = jnp.mean(d_n * x, axis=-1, keepdims=True)
            d_x = d_n * scale - x * (proj * (scale * scale * scale))
            cot_s[sl, :] = (cot_s[sl, :].astype(F32) + d_x).astype(BF)

        row_loop(tok, slab)(rows_back)
        proj_copy(i).wait()
        d_mixed = dot_t(cot_s[...], wp_s[...]).astype(BF)
        wait(row_sends(i))

        @pl.when(i < n_layers - 1)
        def _():
            proj_copy(i + 1).start()
            gate_grads(gate_ref[jnp.maximum(n_layers - 2 - i, 0)], fet_ref[n_layers - 1 - i], d_mixed.astype(F32), rows_s, dgp_s)

        @pl.when(i == n_layers - 1)
        def _():
            slots = dot(slot_pick(n_emb * cap, slot_ref), d_mixed).astype(BF)
            for d in range(n_dp):
                slots0_ref[d] = slots

        return carry

    lax.fori_loop(0, n_layers, one_layer, 0)
    wait(gate_sends)


def scatter_kernel(cfg, read_ref, write_ref, group_ref, meta_ref, rows_ref, gate_ref, mixed_ref, dt_in, dt_out, groups, prod, sems):
    unroll, window, bulk = cfg
    n_layers = groups.shape[1]
    n_slots = mixed_ref.shape[0]
    count = meta_ref[0]

    def product(i, carry):
        step = 64
        mixed = mixed_ref[pl.ds(pl.multiple_of(i * step, step), step), :].astype(F32)
        for h in range(2):
            at = pl.ds(i * (step // 8), step // 8)
            prod[at, h] = gate_ref[at, h] * mixed[:, h * 128:(h + 1) * 128].reshape(step // 8, 8, 128)
        return carry

    lax.fori_loop(0, n_slots // 64, product, 0, unroll=4)
    words = prod.reshape(n_slots * 2, 128)
    sub_iota = lax.broadcasted_iota(I32, (8, 128), 0)

    def move(buf, spot, group, n):
        return pltpu.make_async_copy(groups.at[buf, :, pl.ds(spot, n)], dt_out.at[:, pl.ds(group, n)], sems.at[buf])

    def settle(w):
        n = meta_ref[1 + w]

        def drain_bulk(j, carry):
            move(w % 2, 0, 0, bulk).wait()
            return carry

        def drain(j, carry):
            move(w % 2, 0, 0, 1).wait()
            return carry

        lax.fori_loop(0, n // bulk, drain_bulk, 0)
        lax.fori_loop(0, lax.rem(n, bulk), drain, 0)

    n_win = n_slots // window
    accs = tuple(jnp.zeros((8, 128), F32) for _ in range(2 * n_layers))
    for w in range(n_win):
        buf = w % 2
        if w >= 2:
            settle(w - 2)
        left = jnp.clip(count - w * window, 0, window)
        trips = (left + (unroll - 1)) // unroll

        def add(t, accs, w=w, buf=buf):
            for k in range(unroll):
                j = w * window + t * unroll + k
                word = read_ref[j]
                at = jnp.bitwise_and(word, n_slots * 2 - 1)
                sub = jnp.bitwise_and(jnp.right_shift(word, 12), 7)
                same = word < 0
                here = sub_iota == sub
                spot = jnp.bitwise_and(write_ref[j], window - 1)
                new = []
                for l in range(n_layers):
                    for h in range(2):
                        src = words if l == 0 else rows_ref.at[l - 1]
                        row = jnp.broadcast_to(src[pl.ds(at + 8 * h, 1), :], (8, 128))
                        acc = jnp.where(same, accs[2 * l + h], 0.0) + jnp.where(here, row, 0.0)
                        groups[buf, l, spot, :, h * 128:(h + 1) * 128] = acc
                        new.append(acc)
                accs = tuple(new)
            return accs

        accs = lax.fori_loop(0, trips, add, accs)

        def put(t, carry, w=w, buf=buf):
            for k in range(unroll):
                j = w * window + t * unroll + k
                word = write_ref[j]

                @pl.when(word < 0)
                def _(j=j, word=word):
                    move(buf, jnp.bitwise_and(word, window - 1), group_ref[j], 1).start()

            return carry

        lax.fori_loop(0, trips, put, 0)
    for w in range(max(n_win - 2, 0), n_win):
        settle(w)


def solution(mesh):
    n_emb, n_dp = mesh.shape['emb'], mesh.shape['dp']
    n_dev = n_emb * n_dp
    tok_spec = P(('dp', 'emb'))
    act_spec = P(('dp', 'emb'), None)
    table_spec = P(None, 'emb', None)
    full_spec = P(None, None, None)
    hbm = pl.BlockSpec(memory_space=pl.ANY)
    vm = pl.BlockSpec(memory_space=pltpu.VMEM)
    sm = pl.BlockSpec(memory_space=pltpu.SMEM)
    big = jnp.iinfo(jnp.int32).max

    def params(n_grid, **kw):
        return pltpu.CompilerParams(vmem_limit_bytes=VMEM_BYTES, dimension_semantics=('arbitrary',) * n_grid if n_grid else None, **kw)

    def device_body(tok_ids, resid_in, cot_out, tables, w_up, w_down, w_gate, w_proj):
        n_layers, range_rows, e_dim = tables.shape
        tok = tok_ids.shape[0]
        dim, ffn = w_up.shape[1:]
        n_slots, n_serve = n_dev * CAP, n_emb * CAP
        my_emb, my_dp = lax.axis_index('emb'), lax.axis_index('dp')

        lanes = 128
        per_dot, dots = 32, 2
        dma = pltpu.SemaphoreType.DMA
        _, recv_loc, counts, pick, slot_row, slot_col = pl.pallas_call(
            functools.partial(plan_kernel, (n_dp, n_emb, CAP, range_rows, per_dot)),
            out_shape=[jax.ShapeDtypeStruct(shape, I32) for shape in (
                (n_dev, tok // lanes, lanes), (n_dev, CAP), (n_dev, lanes), (n_serve, 1), (1, tok), (tok, 1))],
            in_specs=[vm], out_specs=[vm] * 6,
            scratch_shapes=[pltpu.VMEM((n_dev, tok), F32), dma((n_dev - 1,)), dma((n_dev - 1,))],
            compiler_params=pltpu.CompilerParams(collective_id=0, has_side_effects=True),
            name='plan',
        )(tok_ids.reshape(tok // lanes, lanes))
        c_iota = jnp.arange(CAP, dtype=I32)
        valid = c_iota[None, :] < counts[:, :1]
        slot_bits = (n_slots - 1).bit_length()
        slot_ids = jnp.arange(n_slots, dtype=I32).reshape(n_dev, CAP)
        keys = jnp.where(valid, recv_loc * (1 << slot_bits) + slot_ids, big)
        window, sub = 512, 8
        skeys = lax.sort(keys.reshape(-1))
        total = jnp.sum(counts[:, 0])
        order = jnp.arange(n_slots, dtype=I32)
        live = order < total
        slot = jnp.bitwise_and(skeys, (1 << slot_bits) - 1)
        row = jnp.right_shift(skeys, slot_bits)
        group = jnp.right_shift(row, 3)
        edge = group[1:] != group[:-1]
        one = jnp.ones((1,), jnp.bool_)
        fresh = jnp.concatenate([one, edge])
        last = jnp.concatenate([edge, one]) & live
        place = jnp.cumsum(fresh.astype(I32)).reshape(-1, window)
        place = (place - place[:, :1]).reshape(-1)
        sign = jnp.int32(-(1 << 31))
        read_word = jnp.right_shift(slot, 3) * 16 + jnp.bitwise_and(slot, 7) + jnp.left_shift(jnp.bitwise_and(row, 7), 12)
        read_word = read_word + jnp.where(fresh, 0, sign)
        write_word = place + jnp.where(last, sign, 0)
        group_word = jnp.where(live, group, 0)
        meta = jnp.concatenate([total.reshape(1), jnp.sum(last.reshape(-1, window).astype(I32), axis=1)])

        z_rows = 1336
        z_chunks = range_rows // z_rows
        served, dtab = pl.pallas_call(
            functools.partial(gather_kernel, (n_layers, n_emb, CAP, per_dot, dots, z_chunks)),
            out_shape=[jax.ShapeDtypeStruct((n_layers, n_serve, e_dim), BF), jax.ShapeDtypeStruct((n_layers, range_rows, e_dim), F32)],
            in_specs=[sm, sm, vm, hbm],
            out_specs=[vm, hbm],
            scratch_shapes=[pltpu.VMEM((n_layers, n_serve * 8, e_dim), BF), pltpu.VMEM((z_rows, e_dim), F32), dma((n_emb,)), dma],
            compiler_params=params(0),
            name='table_rows',
        )(recv_loc, counts, pick, tables)

        fb = 1024
        n_blk = ffn // fb
        cw, nw, slab = 512, 512, 16
        n_back = n_layers - 1
        z_per = z_chunks // n_blk
        assert z_chunks * z_rows == range_rows and z_per * n_blk == z_chunks
        matmul_flops = 4 * tok * dim * ffn
        w_bufs = [pltpu.VMEM((2, dim, fb), BF), pltpu.VMEM((2, fb, dim), BF), pltpu.VMEM((dim, e_dim), BF), pltpu.VMEM((e_dim, dim), BF)]
        x1, gate0, fetched = pl.pallas_call(
            functools.partial(first_kernel, (n_dp, n_emb, CAP, n_blk, cw, nw, slab)),
            out_shape=[
                jax.ShapeDtypeStruct((tok, dim), BF),
                jax.ShapeDtypeStruct((1, tok, e_dim), F32),
                jax.ShapeDtypeStruct((n_layers, tok, e_dim), BF),
            ],
            in_specs=[hbm, vm, hbm, hbm, hbm, hbm, hbm],
            out_specs=[vm, vm, vm],
            scratch_shapes=[
                pltpu.VMEM((tok, dim), BF), pltpu.VMEM((tok, dim), F32), pltpu.VMEM((tok, fb), BF), pltpu.VMEM((tok, fb), F32),
                pltpu.VMEM((n_layers, n_serve, e_dim), BF), *w_bufs, dma((3,)), dma((2, 2)), dma, dma((n_emb - 1,)), dma((n_emb - 1,)),
            ],
            compiler_params=params(0, collective_id=1, has_side_effects=True),
            cost_estimate=pl.CostEstimate(flops=matmul_flops, bytes_accessed=100 << 20, transcendentals=0),
            name='first_layer',
        )(resid_in, slot_col, served, w_gate, w_proj, w_up, w_down)

        out, saved, ups, gates, rows, dgp, dtab = pl.pallas_call(
            functools.partial(forward_kernel, (n_back, n_blk, cw, nw, slab, z_per, z_chunks)),
            out_shape=[
                jax.ShapeDtypeStruct((tok, dim), BF),
                jax.ShapeDtypeStruct((n_back - 1, tok, dim), BF),
                jax.ShapeDtypeStruct((n_back, tok, ffn), F32),
                jax.ShapeDtypeStruct((n_back, tok, e_dim), F32),
                jax.ShapeDtypeStruct((tok, e_dim), F32),
                jax.ShapeDtypeStruct((tok, e_dim), BF),
                jax.ShapeDtypeStruct((n_layers, range_rows, e_dim), F32),
            ],
            in_specs=[hbm, hbm, vm, hbm, hbm, hbm, hbm, hbm],
            out_specs=[hbm, hbm, hbm, vm, vm, vm, hbm],
            input_output_aliases={7: 6},
            scratch_shapes=[
                pltpu.VMEM((tok, dim), BF), pltpu.VMEM((tok, dim), BF), pltpu.VMEM((tok, dim), F32), pltpu.VMEM((tok, fb), BF),
                pltpu.VMEM((2, tok, fb), F32), pltpu.VMEM((z_rows, e_dim), F32), *w_bufs,
                dma((3,)), dma((2, 2)), dma((2,)), dma, dma((z_per,)),
            ],
            compiler_params=params(0),
            cost_estimate=pl.CostEstimate(flops=n_back * matmul_flops, bytes_accessed=400 << 20, transcendentals=0),
            name='forward',
        )(x1, cot_out, fetched, w_gate, w_proj, w_up, w_down, dtab)

        got, got_gate, slots0 = pl.pallas_call(
            functools.partial(backward_kernel, (n_back, n_blk, n_dp, n_emb, CAP, cw, nw, slab)),
            out_shape=[jax.ShapeDtypeStruct((n_back, n_slots // 8, e_dim // 128, 8, 128), F32), jax.ShapeDtypeStruct((n_slots // 8, e_dim // 128, 8, 128), F32),
                       jax.ShapeDtypeStruct((n_dp, n_serve, e_dim), BF)],
            in_specs=[hbm, hbm, hbm, vm, vm, vm, vm, vm, vm, hbm, hbm, hbm, hbm, hbm],
            out_specs=[hbm, hbm, vm],
            scratch_shapes=[
                pltpu.VMEM((tok, dim), BF), pltpu.VMEM((tok, dim), BF), pltpu.VMEM((tok, dim), F32), pltpu.VMEM((tok, fb), BF), pltpu.VMEM((tok, fb), BF),
                pltpu.VMEM((tok, dim), BF), pltpu.VMEM((n_serve // 8, e_dim // 128, 8, 128), F32), pltpu.VMEM((n_serve // 8, e_dim // 128, 8, 128), F32),
                pltpu.VMEM((tok, e_dim), F32), pltpu.VMEM((tok, e_dim), BF), pltpu.VMEM((2, tok, fb), F32), *w_bufs,
                dma((4,)), dma((2, 2)), dma((2,)), dma((2, n_dev - 1)), dma((2,)), dma((n_back + 1, n_dev - 1)),
            ],
            compiler_params=params(0, collective_id=2, has_side_effects=True),
            cost_estimate=pl.CostEstimate(flops=n_back * matmul_flops, bytes_accessed=400 << 20, transcendentals=0),
            name='backward',
        )(cot_out, x1, saved, rows, dgp, slot_row, gate0, gates, fetched, ups, w_up, w_down, w_gate, w_proj)

        mixed0 = lax.all_to_all(slots0.reshape(n_dev, CAP, e_dim), MESH_AXES, 0, 0, tiled=True).reshape(n_slots, e_dim)
        dtab = pl.pallas_call(
            functools.partial(scatter_kernel, (8, window, 32)),
            out_shape=jax.ShapeDtypeStruct((n_layers, range_rows // sub, sub, e_dim), F32),
            in_specs=[sm, sm, sm, sm, vm, vm, vm, hbm],
            out_specs=hbm,
            input_output_aliases={7: 0},
            scratch_shapes=[pltpu.VMEM((2, n_layers, window, sub, e_dim), F32), pltpu.VMEM((n_slots // 8, e_dim // 128, 8, 128), F32), dma((2,))],
            compiler_params=params(0),
            name='scatter',
        )(read_word, write_word, group_word, meta, got.reshape(n_back, n_slots * 2, 128), got_gate, mixed0,
          dtab.reshape(n_layers, range_rows // sub, sub, e_dim))
        dtab = dtab.reshape(n_layers, range_rows, e_dim)
        return out, dtab

    return jax.shard_map(device_body, mesh=mesh, in_specs=(tok_spec, act_spec, act_spec, table_spec, full_spec, full_spec, full_spec, full_spec), out_specs=(act_spec, table_spec), check_vma=False)
```

```python
import functools

import jax
import jax.numpy as jnp
from jax import lax
from jax.experimental import pallas as pl
from jax.experimental.pallas import tpu as pltpu
from jax.sharding import PartitionSpec as P

NORM_EPS = 1e-6
BF = jnp.bfloat16
F32 = jnp.float32
I32 = jnp.int32
VMEM_BYTES = 67043328
GELU_C = 0.7978845608028654
GELU_A = 0.044715

MESH_AXES = ('dp', 'emb')
CAP = 256


def gelu(x):
    return 0.5 * x * (1.0 + jnp.tanh(GELU_C * (x + GELU_A * (x * x * x))))


def gelu_slope(x):
    sq = x * x
    th = jnp.tanh(GELU_C * (x + GELU_A * (x * sq)))
    return 0.5 * (1.0 + th) + (0.5 * GELU_C) * x * (1.0 - th * th) * (1.0 + (3 * GELU_A) * sq)


def dot(a, b):
    return jnp.dot(a, b, preferred_element_type=F32)


def dot_t(a, b):
    return lax.dot_general(a, b, (((1,), (1,)), ((), ())), preferred_element_type=F32)


def row_loop(rows, slab, unroll=2):
    def run(body):
        def step(i, carry):
            body(pl.ds(pl.multiple_of(i * slab, slab), slab))
            return carry

        lax.fori_loop(0, rows // slab, step, 0, unroll=unroll)

    return run


def peer_of(n_emb, index):
    dp = index // n_emb
    return {'dp': dp, 'emb': index - dp * n_emb}


def remote(src, dst, send_sem, recv_sem, device):
    return pltpu.make_async_remote_copy(src_ref=src, dst_ref=dst, send_sem=send_sem, recv_sem=recv_sem,
                                        device_id=device, device_id_type=pl.DeviceIdType.MESH)


def meet(devices):
    barrier = pltpu.get_barrier_semaphore()
    for device in devices:
        pl.semaphore_signal(barrier, inc=1, device_id=device, device_id_type=pl.DeviceIdType.MESH)
    pl.semaphore_wait(barrier, len(devices))


def plan_kernel(cfg, in_ref, ids_ref, recv_ref, counts_ref, pick_ref, slot_row_ref, slot_col_ref, rank_s, send_sem, recv_sem):
    n_dp, n_emb, cap, range_rows, per_dot = cfg
    n_dev = n_dp * n_emb
    my_dp, my_emb = lax.axis_index('dp'), lax.axis_index('emb')
    me = my_dp * n_emb + my_emb
    n_sub, lanes = in_ref.shape
    tok = n_sub * lanes
    peers = [peer_of(n_emb, lax.rem(me + k, n_dev)) for k in range(1, n_dev)]
    meet(peers)
    copies = [remote(in_ref, ids_ref.at[me], send_sem.at[k], recv_sem.at[k], peer) for k, peer in enumerate(peers)]
    start(copies)
    ids_ref[me] = in_ref[...]

    def line(ref):
        return jnp.concatenate([ref[..., j, :] for j in range(n_sub)], axis=-1)

    def ones(cond):
        return jnp.where(cond, 1.0, 0.0)

    def digits(x):
        return jnp.concatenate([jnp.right_shift(x, 8), jnp.bitwise_and(x, 255)], axis=0).astype(F32).astype(BF)

    square = (tok, tok)
    down, right = lax.broadcasted_iota(I32, square, 0), lax.broadcasted_iota(I32, square, 1)
    earlier = ones(down < right).astype(BF)
    own = jnp.broadcast_to(jnp.concatenate([in_ref[j:j + 1, :] for j in range(n_sub)], axis=-1), (8, tok))
    owner = sum(jnp.where(own >= e * range_rows, 1, 0) for e in range(1, n_emb))
    is_owner = owner == lax.broadcasted_iota(I32, (8, tok), 0)
    own_rank = dot(ones(is_owner).astype(BF), earlier).astype(I32)
    slot_row = jnp.sum(jnp.where(is_owner, own_rank + owner * cap, 0).astype(F32), axis=0, keepdims=True).astype(I32)
    slot_row_ref[...] = slot_row
    turned = dot_t(ones(down == right).astype(BF), digits(jnp.broadcast_to(slot_row, (8, tok))))
    slot_col_ref[...] = (turned[:, 0:1] * 256.0 + turned[:, 8:9]).astype(I32)

    wait(copies)
    ids8 = line(ids_ref)
    low = my_emb * range_rows
    mine = jnp.logical_and(ids8 >= low, ids8 < low + range_rows)
    mine_f = ones(mine)
    rank_s[...] = jnp.where(mine, dot(mine_f.astype(BF), earlier), -1.0)
    counts = jnp.sum(mine_f, axis=1, keepdims=True).astype(I32)
    counts_ref[...] = jnp.broadcast_to(counts, counts_ref.shape)
    loc = digits(jnp.where(mine, ids8 - low, 0))
    c_iota = lax.broadcasted_iota(I32, (cap, tok), 0).astype(F32)
    dev_iota = lax.broadcasted_iota(I32, (n_dev, cap), 0)
    recv = jnp.zeros((n_dev, cap), F32)
    for d in range(n_dev):
        found = dot_t(loc, ones(rank_s[d:d + 1, :] == c_iota).astype(BF))
        recv = jnp.where(dev_iota == d, found[:n_dev] * 256.0 + found[n_dev:], recv)
    slot = dev_iota * cap + lax.broadcasted_iota(I32, (n_dev, cap), 1)
    recv_ref[...] = jnp.where(slot - dev_iota * cap < counts, recv.astype(I32), slot * 8)
    lane16 = lax.broadcasted_iota(I32, (cap, 2 * n_dev), 1)
    row1 = lax.broadcasted_iota(I32, (cap, 1), 0)
    for e in range(n_emb):
        d = my_dp * n_emb + e
        found = dot_t(ones(rank_s[pl.ds(d, 1), :] == c_iota).astype(BF), loc)
        low8 = jnp.sum(jnp.where(lane16 == n_dev + d, found, 0.0), axis=1, keepdims=True).astype(I32)
        pick_ref[e * cap:(e + 1) * cap, :] = jnp.bitwise_and(low8, 7) + 8 * jnp.bitwise_and(row1, per_dot - 1)


def gather_kernel(cfg, loc_ref, counts_ref, pick_ref, tables_hbm, out_ref, dtab_hbm, buf, zero_s, sems, z_sem):
    n_layers, n_dest, cap, per_dot, group, z_chunks = cfg
    trip = per_dot * group
    z_rows = zero_s.shape[0]
    first = lax.axis_index('dp') * n_dest
    n_trips = [(counts_ref[first + d, 0] + (trip - 1)) // trip for d in range(n_dest)]

    def row_copy(d, c):
        base = pl.multiple_of(jnp.left_shift(jnp.right_shift(loc_ref[first + d, c], 3), 3), 8)
        at = pl.multiple_of(d * cap * 8 + c * 8, 8)
        return pltpu.make_async_copy(tables_hbm.at[:, pl.ds(base, 8), :], buf.at[:, pl.ds(at, 8), :], sems.at[d])

    def z_copy(c):
        return pltpu.make_async_copy(zero_s, dtab_hbm.at[0, pl.ds(c * z_rows, z_rows)], z_sem)

    for d in range(n_dest):
        def issue(i, carry, d=d):
            for k in range(8):
                row_copy(d, i * 8 + k).start()
            return carry

        lax.fori_loop(0, n_trips[d] * (trip // 8), issue, 0)

    clear_rows(zero_s)

    def z_start(c, carry):
        z_copy(c).start(priority=1)
        return carry

    lax.fori_loop(0, z_chunks, z_start, 0)
    for d in range(n_dest):
        def drain(i, carry, d=d):
            part = buf.at[:, pl.ds(pl.multiple_of((d * cap + i * trip) * 8, 8), trip * 8), :]
            pltpu.make_async_copy(part, part, sems.at[d]).wait()
            return carry

        lax.fori_loop(0, n_trips[d], drain, 0)

        def pick(i, carry, d=d):
            for k in range(group):
                s0 = pl.multiple_of(d * cap + i * trip + k * per_dot, per_dot)
                want = pick_ref[pl.ds(s0, per_dot), :]
                sel = (lax.broadcasted_iota(I32, (per_dot, per_dot * 8), 1) == want).astype(BF)
                for l in range(n_layers):
                    rows = buf[l, pl.ds(pl.multiple_of(s0 * 8, 8), per_dot * 8), :]
                    out_ref[l, pl.ds(s0, per_dot), :] = dot(sel, rows).astype(BF)
            return carry

        lax.fori_loop(0, n_trips[d], pick, 0)

        def blank(i, carry, d=d):
            s0 = pl.multiple_of(d * cap + i * trip, trip)
            for l in range(n_layers):
                out_ref[l, pl.ds(s0, trip), :] = jnp.zeros((trip, out_ref.shape[2]), BF)
            return carry

        lax.fori_loop(n_trips[d], cap // trip, blank, 0)

    def z_wait(c, carry):
        z_copy(c).wait()
        return carry

    lax.fori_loop(0, z_chunks, z_wait, 0)


def clear_rows(ref):
    def clear(i, carry):
        ref[i] = jnp.zeros(ref.shape[1:], F32)
        return carry

    lax.fori_loop(0, ref.shape[0], clear, 0)


def weight_copies(wu_hbm, wd_hbm, wu_s, wd_s, sems):
    fb = wu_s.shape[2]

    def copies(layer, blk, slot):
        at = pl.multiple_of(blk * fb, fb)
        return (pltpu.make_async_copy(wu_hbm.at[layer, :, pl.ds(at, fb)], wu_s.at[slot], sems.at[0, slot]),
                pltpu.make_async_copy(wd_hbm.at[layer, pl.ds(at, fb), :], wd_s.at[slot], sems.at[1, slot]))

    return copies


def start(copies):
    for copy in copies:
        copy.start()


def wait(copies):
    for copy in copies:
        copy.wait()


def mlp_block(cfg, u_s, h_s, acc_s, wu_ref, wd_ref, up_ref):
    cw, nw = cfg
    gw = 128
    n_c = wu_ref.shape[1] // cw

    def act(c):
        for g in range(cw // gw):
            gs = slice(c * cw + g * gw, c * cw + (g + 1) * gw)
            h_s[:, gs] = gelu(up_ref[:, gs]).astype(BF)

    for c in range(n_c):
        cs = slice(c * cw, (c + 1) * cw)
        up_ref[:, cs] = dot(u_s[...], wu_ref[:, cs])
        if c > 0:
            act(c - 1)
    for c in range(n_c):
        cs = slice(c * cw, (c + 1) * cw)
        for n in range(acc_s.shape[1] // nw):
            ns = slice(n * nw, (n + 1) * nw)
            acc_s[:, ns] += dot(h_s[:, cs], wd_ref[cs, ns])
        if c == 0:
            act(n_c - 1)


def norm_rows(x, sl, u_s, acc_s):
    scale = lax.rsqrt(jnp.mean(x * x, axis=-1, keepdims=True) + NORM_EPS)
    u_s[sl, :] = (x * scale).astype(BF)
    acc_s[sl, :] = x


def add_proj(nw, acc_s, mixed, wp_ref):
    for n in range(acc_s.shape[1] // nw):
        ns = slice(n * nw, (n + 1) * nw)
        acc_s[:, ns] += dot(mixed, wp_ref[:, ns])


def first_kernel(cfg, x_hbm, slot_ref, served_hbm, wg_hbm, wp_hbm, wu_hbm, wd_hbm,
                 x_out_ref, gate_ref, fet_ref,
                 u_s, acc_s, h_s, up_s, ret_s, wu_s, wd_s, wg_s, wp_s, in_sem, w_sem, self_sem, send_sem, recv_sem):
    n_dp, n_emb, cap, n_blk, cw, nw, slab = cfg
    tok, dim = u_s.shape
    my_emb = lax.axis_index('emb')
    my_dp = lax.axis_index('dp')
    here = ret_s.at[:, pl.ds(pl.multiple_of(my_emb * cap, cap), cap), :]
    own = pltpu.make_async_copy(served_hbm.at[:, pl.ds(pl.multiple_of(my_emb * cap, cap), cap), :], here, self_sem)
    peers = [lax.rem(my_emb + k, n_emb) for k in range(1, n_emb)]
    copies = [remote(served_hbm.at[:, pl.ds(pl.multiple_of(p * cap, cap), cap), :], here,
                     send_sem.at[k], recv_sem.at[k], {'dp': my_dp, 'emb': p}) for k, p in enumerate(peers)]
    weights = weight_copies(wu_hbm, wd_hbm, wu_s, wd_s, w_sem)
    first = [pltpu.make_async_copy(x_hbm, x_out_ref, in_sem.at[0]),
             pltpu.make_async_copy(wg_hbm.at[0], wg_s, in_sem.at[1]),
             pltpu.make_async_copy(wp_hbm.at[0], wp_s, in_sem.at[2])]
    start(first[:2])
    start(weights(0, 0, 0))
    start(first[2:])
    meet([{'dp': my_dp, 'emb': p} for p in peers])
    own.start()
    start(copies)
    first[0].wait()
    row_loop(tok, slab)(lambda sl: norm_rows(x_out_ref[sl, :].astype(F32), sl, u_s, acc_s))
    first[1].wait()
    gate_ref[0] = dot(u_s[...], wg_s[...])

    def block(f, carry):
        slot = lax.rem(f, 2)

        @pl.when(f + 1 < n_blk)
        def _():
            start(weights(0, f + 1, 1 - slot))

        wait(weights(0, f, slot))
        mlp_block((cw, nw), u_s, h_s, acc_s, wu_s.at[slot], wd_s.at[slot], up_s)
        return carry

    lax.fori_loop(0, n_blk, block, 0)
    own.wait()
    wait(copies)
    first[2].wait()
    sel = (lax.broadcasted_iota(I32, (tok, n_emb * cap), 1) == slot_ref[...]).astype(BF)
    for l in range(fet_ref.shape[0]):
        fet_ref[l] = dot(sel, ret_s[l]).astype(BF)
    add_proj(nw, acc_s, (gelu(gate_ref[0]) * fet_ref[0].astype(F32)).astype(BF), wp_s)

    def finish(sl):
        x_out_ref[sl, :] = acc_s[sl, :].astype(BF)

    row_loop(tok, slab)(finish)


def forward_kernel(cfg, x_hbm, cot_hbm, fet_ref, wg_hbm, wp_hbm, wu_hbm, wd_hbm, dt_in,
                   out_hbm, saved_hbm, ups_hbm, gate_ref, rows_ref, dgp_ref, dtab_hbm,
                   x_s, u_s, acc_s, h_s, up_s, zero_s, wu_s, wd_s, wg_s, wp_s, in_sem, w_sem, up_sem, out_sem, z_sem):
    n_layers, n_blk, cw, nw, slab, z_per, z_chunks, z_first = cfg
    z_total = (n_layers + 1) * z_chunks
    tok, dim = x_s.shape
    fb = wu_s.shape[2]
    z_rows = zero_s.shape[0]
    n_steps = n_layers * n_blk
    weights = weight_copies(wu_hbm, wd_hbm, wu_s, wd_s, w_sem)

    z_steps = (z_total - z_first) // z_per

    def z_copies(step):
        found = []
        for j in range(z_per):
            c = z_first + step * z_per + j
            zl = c // z_chunks
            found.append(pltpu.make_async_copy(zero_s, dtab_hbm.at[zl, pl.ds((c - zl * z_chunks) * z_rows, z_rows)], z_sem.at[j]))
        return found

    def up_copy(layer, blk, slot):
        return pltpu.make_async_copy(up_s.at[slot], ups_hbm.at[layer, :, pl.ds(pl.multiple_of(blk * fb, fb), fb)], up_sem.at[slot])

    def gate_copy(layer):
        return pltpu.make_async_copy(wg_hbm.at[layer + 1], wg_s, in_sem.at[1])

    def proj_copy(layer):
        return pltpu.make_async_copy(wp_hbm.at[layer + 1], wp_s, in_sem.at[2])

    fetch = pltpu.make_async_copy(x_hbm, x_s, in_sem.at[0])
    fetch.start()
    gate_copy(0).start()
    start(weights(1, 0, 0))
    proj_copy(0).start()
    clear_rows(zero_s)
    fetch.wait()
    row_loop(tok, slab)(lambda sl: norm_rows(x_s[sl, :].astype(F32), sl, u_s, acc_s))

    def one_layer(layer, carry):
        gate_copy(layer).wait()
        gate_ref[layer] = dot(u_s[...], wg_s[...])

        @pl.when(layer + 1 < n_layers)
        def _():
            gate_copy(layer + 1).start()

        def block(f, carry):
            step = layer * n_blk + f
            slot = lax.rem(step, 2)

            @pl.when(step + 1 < n_steps)
            def _():
                nxt = step + 1
                start(weights(1 + nxt // n_blk, lax.rem(nxt, n_blk), 1 - slot))

            @pl.when((step > 0) & (step <= z_steps))
            def _():
                wait(z_copies(step - 1))

            @pl.when(step < z_steps)
            def _():
                for copy in z_copies(step):
                    copy.start(priority=1)

            @pl.when(step > 1)
            def _():
                up_copy(layer, f, slot).wait()

            wait(weights(1 + layer, f, slot))
            mlp_block((cw, nw), u_s, h_s, acc_s, wu_s.at[slot], wd_s.at[slot], up_s.at[slot])
            up_copy(layer, f, slot).start()
            return carry

        lax.fori_loop(0, n_blk, block, 0)
        proj_copy(layer).wait()
        add_proj(nw, acc_s, (gelu(gate_ref[layer]) * fet_ref[layer + 1].astype(F32)).astype(BF), wp_s)

        @pl.when(layer > 0)
        def _():
            pltpu.make_async_copy(x_s, saved_hbm.at[layer - 1], out_sem).wait()

        def next_rows(sl):
            x_new = acc_s[sl, :].astype(BF)
            x_s[sl, :] = x_new
            norm_rows(x_new.astype(F32), sl, u_s, acc_s)

        row_loop(tok, slab)(next_rows)

        @pl.when(layer < n_layers - 1)
        def _():
            pltpu.make_async_copy(x_s, saved_hbm.at[layer], out_sem).start()
            proj_copy(layer + 1).start()

        return carry

    lax.fori_loop(0, n_layers, one_layer, 0)
    put = pltpu.make_async_copy(x_s, out_hbm, out_sem)
    put.start()
    get = pltpu.make_async_copy(cot_hbm, u_s, in_sem.at[0])
    get.start()
    if z_steps == n_steps:
        wait(z_copies(n_steps - 1))
    up_copy(0, 0, 0).wait()
    up_copy(0, 0, 1).wait()
    get.wait()
    d_mixed = dot_t(u_s[...], wp_s[...]).astype(BF).astype(F32)
    gate_grads(gate_ref[n_layers - 1], fet_ref[n_layers], d_mixed, rows_ref, dgp_ref)
    put.wait()


def gate_grads(gate_pre, fetched, d_mixed, rows_ref, dgp_ref):
    rows_ref[...] = gelu(gate_pre) * d_mixed
    dgp_ref[...] = (d_mixed * fetched.astype(F32) * gelu_slope(gate_pre)).astype(BF)


def to_slots(rows, slot_ref, slots_s):
    hi = rows.astype(BF)
    rest = rows - hi.astype(F32)
    mid = rest.astype(BF)
    low = (rest - mid.astype(F32)).astype(BF)
    n = slots_s.shape[0] * slots_s.shape[2]
    sel = slot_pick(n, slot_ref)
    slots = (dot(sel, hi) + dot(sel, mid)) + dot(sel, low)
    for h in range(slots_s.shape[1]):
        slots_s[:, h] = slots[:, h * 128:(h + 1) * 128].reshape(n // 8, 8, 128)


def slot_pick(n, slot_ref):
    return (lax.broadcasted_iota(I32, (n, slot_ref.shape[1]), 0) == slot_ref[...]).astype(BF)


def backward_kernel(cfg, cot_hbm, x1_hbm, saved_hbm, rows_in_ref, dgp_in_ref, slot_ref, gate0_ref, gate_ref, fet_ref,
                    ups_hbm, wu_hbm, wd_hbm, wg_hbm, wp_hbm,
                    got_hbm, gate_hbm, slots0_ref,
                    cot_s, x_s, acc_s, dup_s, dh_s, dng_s, slots_s, gslots_s, rows_s, dgp_s, up_s, wu_s, wd_s, wg_s, wp_s,
                    in_sem, w_sem, up_sem, send_sem, self_sem, recv_sem):
    n_layers, n_blk, n_dp, n_emb, cap, cw, nw, slab = cfg
    tok, dim = cot_s.shape
    fb = wu_s.shape[2]
    gw = 128
    n_dev = n_dp * n_emb
    n_steps = n_layers * n_blk
    my_emb = lax.axis_index('emb')
    me = lax.axis_index('dp') * n_emb + my_emb
    peers = [peer_of(n_emb, lax.rem(me + k, n_dev)) for k in range(1, n_dev)]
    weights = weight_copies(wu_hbm, wd_hbm, wu_s, wd_s, w_sem)

    def part(ref, emb):
        return ref.at[pl.ds(emb * (cap // 8), cap // 8)]

    def sends(ref, there, which, got):
        return [pltpu.make_async_copy(part(ref, my_emb), there, self_sem.at[which])] + [
            remote(part(ref, peer['emb']), there, send_sem.at[which, k], recv_sem.at[got, k], peer) for k, peer in enumerate(peers)]

    def row_sends(i):
        return sends(slots_s, part(got_hbm.at[n_layers - 1 - i], me), 0, i)

    gate_sends = sends(gslots_s, part(gate_hbm, me), 1, n_layers)

    def up_copy(step, slot):
        i = step // n_blk
        blk = step - i * n_blk
        return pltpu.make_async_copy(ups_hbm.at[n_layers - 1 - i, :, pl.ds(pl.multiple_of(blk * fb, fb), fb)], up_s.at[slot], up_sem.at[slot])

    def load(step, slot):
        i = step // n_blk
        return weights(n_layers - i, step - i * n_blk, slot) + (up_copy(step, slot),)

    def gate_copy(i):
        return pltpu.make_async_copy(wg_hbm.at[n_layers - i], wg_s, in_sem.at[1])

    def proj_copy(i):
        return pltpu.make_async_copy(wp_hbm.at[n_layers - 1 - i], wp_s, in_sem.at[2])

    def x_copy(i):
        return pltpu.make_async_copy(saved_hbm.at[n_layers - 2 - i], x_s, in_sem.at[3])

    fetch = pltpu.make_async_copy(cot_hbm, cot_s, in_sem.at[0])
    gate_copy(0).start()
    fetch.start()
    start(load(0, 0))
    proj_copy(0).start()
    rows_s[...] = rows_in_ref[...]
    dgp_s[...] = dgp_in_ref[...]

    def clear(sl):
        acc_s[sl, :] = jnp.zeros((slab, dim), F32)

    row_loop(tok, slab)(clear)
    meet(peers)
    to_slots(gelu(gate0_ref[0]), slot_ref, gslots_s)

    def one_layer(i, carry):
        @pl.when(i < n_layers - 1)
        def _():
            x_copy(i).start()

        @pl.when(i == n_layers - 1)
        def _():
            pltpu.make_async_copy(x1_hbm, x_s, in_sem.at[3]).start()

        gate_copy(i).wait()
        to_slots(rows_s[...], slot_ref, slots_s)
        for n in range(dim // nw):
            ns = slice(n * nw, (n + 1) * nw)
            dng_s[:, ns] = dot_t(dgp_s[...], wg_s[ns, :]).astype(BF)
        start(row_sends(i))

        @pl.when(i < n_layers - 1)
        def _():
            gate_copy(i + 1).start()

        @pl.when(i == 0)
        def _():
            start(gate_sends)
            fetch.wait()

        def block(f, carry):
            step = i * n_blk + f
            slot = lax.rem(step, 2)

            @pl.when(step + 1 < n_steps)
            def _():
                start(load(step + 1, 1 - slot))

            wait(load(step, slot))
            wu_ref, wd_ref, up_ref = wu_s.at[slot], wd_s.at[slot], up_s.at[slot]

            def act(c):
                for g in range(cw // gw):
                    gs = slice(c * cw + g * gw, c * cw + (g + 1) * gw)
                    dup_s[:, gs] = (dh_s[:, gs].astype(F32) * gelu_slope(up_ref[:, gs])).astype(BF)

            n_c = fb // cw
            for c in range(n_c):
                cs = slice(c * cw, (c + 1) * cw)
                dh_s[:, cs] = dot_t(cot_s[...], wd_ref[cs, :]).astype(BF)
                if c > 0:
                    act(c - 1)
            for c in range(n_c):
                cs = slice(c * cw, (c + 1) * cw)
                for n in range(dim // nw):
                    ns = slice(n * nw, (n + 1) * nw)
                    acc_s[:, ns] += dot_t(dup_s[:, cs], wu_ref[ns, cs])
                if c == 0:
                    act(n_c - 1)
            return carry

        lax.fori_loop(0, n_blk, block, 0)
        pltpu.make_async_copy(x1_hbm, x_s, in_sem.at[3]).wait()

        def rows_back(sl):
            x = x_s[sl, :].astype(F32)
            scale = lax.rsqrt(jnp.mean(x * x, axis=-1, keepdims=True) + NORM_EPS)
            d_n = (acc_s[sl, :].astype(BF) + dng_s[sl, :]).astype(F32)
            acc_s[sl, :] = jnp.zeros((slab, dim), F32)
            proj = jnp.mean(d_n * x, axis=-1, keepdims=True)
            d_x = d_n * scale - x * (proj * (scale * scale * scale))
            cot_s[sl, :] = (cot_s[sl, :].astype(F32) + d_x).astype(BF)

        row_loop(tok, slab)(rows_back)
        proj_copy(i).wait()
        d_mixed = dot_t(cot_s[...], wp_s[...]).astype(BF)
        wait(row_sends(i))

        @pl.when(i < n_layers - 1)
        def _():
            proj_copy(i + 1).start()
            gate_grads(gate_ref[jnp.maximum(n_layers - 2 - i, 0)], fet_ref[n_layers - 1 - i], d_mixed.astype(F32), rows_s, dgp_s)

        @pl.when(i == n_layers - 1)
        def _():
            slots = dot(slot_pick(n_emb * cap, slot_ref), d_mixed).astype(BF)
            for d in range(n_dp):
                slots0_ref[d] = slots

        return carry

    lax.fori_loop(0, n_layers, one_layer, 0)
    wait(gate_sends)


def scatter_kernel(cfg, read_ref, write_ref, group_ref, meta_ref, rows_hbm, gate_hbm, mixed_hbm, dt_in, dt_out, rows_ref, gate_ref, mixed_ref, groups, prod, spots, sems, in_sem):
    unroll, window, bulk = cfg
    n_layers = groups.shape[1]
    n_slots = mixed_ref.shape[0]
    n_win = n_slots // window
    count = meta_ref[0]
    loads = [pltpu.make_async_copy(src, dst, in_sem.at[k]) for k, (src, dst) in enumerate(
        ((gate_hbm, gate_ref), (mixed_hbm, mixed_ref), (rows_hbm, rows_ref)))]
    start(loads)
    wait(loads[:2])

    def product(i, carry):
        step = 64
        mixed = mixed_ref[pl.ds(pl.multiple_of(i * step, step), step), :].astype(F32)
        for h in range(2):
            at = pl.ds(i * (step // 8), step // 8)
            prod[at, h] = gate_ref[at, h] * mixed[:, h * 128:(h + 1) * 128].reshape(step // 8, 8, 128)
        return carry

    lax.fori_loop(0, n_slots // 64, product, 0, unroll=4)

    def move(buf, spot, group, n):
        return pltpu.make_async_copy(groups.at[buf, :, pl.ds(spot, n)], dt_out.at[:, pl.ds(group, n)], sems.at[buf])

    def each(n, k, body):
        def trip(t, carry):
            for i in range(k):
                body(t * k + i)
            return carry

        def one(i, carry):
            body(i)
            return carry

        full = n // k
        lax.fori_loop(0, full, trip, 0)
        lax.fori_loop(full * k, n, one, 0)

    def settle(w):
        n = meta_ref[1 + w]

        def drain_bulk(j, carry):
            move(w % 2, 0, 0, bulk).wait()
            return carry

        def drain(j, carry):
            move(w % 2, 0, 0, 1).wait()
            return carry

        lax.fori_loop(0, n // bulk, drain_bulk, 0)
        lax.fori_loop(0, lax.rem(n, bulk), drain, 0)

    blank = jnp.zeros(groups.shape[3:], F32)
    accs = tuple(jnp.zeros((2, 128), F32) for _ in range(n_layers))
    for w in range(n_win):
        buf = w % 2
        if w >= 2:
            settle(w - 2)
        left = jnp.clip(count - w * window, 0, window)
        trips = (left + (unroll - 1)) // unroll
        n_out = meta_ref[1 + w]

        def clear(u, buf=buf):
            for l in range(n_layers):
                groups[buf, l, u] = blank

        each(jnp.where(left > 0, jnp.minimum(n_out + 1, window), 0), 4, clear)
        if w == 0:
            wait(loads[2:])
        else:
            @pl.when(meta_ref[1 + 2 * n_win + w] > 0)
            def _(w=w, buf=buf):
                for l in range(n_layers):
                    groups[buf, l, 0] = groups[1 - buf, l, meta_ref[n_win + w]]

        sums = [groups.at[buf, l].reshape(window * 16, 128) for l in range(n_layers)]
        rows = [prod.reshape(n_slots * 2, 128)] + [rows_ref.at[l] for l in range(n_layers - 1)]

        def add(t, accs, w=w, sums=sums, rows=rows):
            for k in range(unroll):
                j = w * window + t * unroll + k
                word = read_ref[j]
                at = jnp.bitwise_and(word, n_slots * 2 - 1)
                same = word < 0
                to = write_ref[j]
                spots[jnp.right_shift(to, 4)] = group_ref[j]
                accs = tuple(jnp.where(same, acc, 0.0) + src[pl.ds(at, 2, stride=8), :] for acc, src in zip(accs, rows))
                for acc, dst in zip(accs, sums):
                    dst[pl.ds(to, 2, stride=8), :] = acc
            return accs

        accs = lax.fori_loop(0, trips, add, accs)
        each(n_out, 4, lambda u, buf=buf: move(buf, u, spots[u], 1).start())
    for w in range(max(n_win - 2, 0), n_win):
        settle(w)


def solution(mesh):
    n_emb, n_dp = mesh.shape['emb'], mesh.shape['dp']
    n_dev = n_emb * n_dp
    tok_spec = P(('dp', 'emb'))
    act_spec = P(('dp', 'emb'), None)
    table_spec = P(None, 'emb', None)
    full_spec = P(None, None, None)
    hbm = pl.BlockSpec(memory_space=pl.ANY)
    vm = pl.BlockSpec(memory_space=pltpu.VMEM)
    sm = pl.BlockSpec(memory_space=pltpu.SMEM)
    big = jnp.iinfo(jnp.int32).max

    def params(n_grid, **kw):
        return pltpu.CompilerParams(vmem_limit_bytes=VMEM_BYTES, dimension_semantics=('arbitrary',) * n_grid if n_grid else None, **kw)

    def device_body(tok_ids, resid_in, cot_out, tables, w_up, w_down, w_gate, w_proj):
        n_layers, range_rows, e_dim = tables.shape
        tok = tok_ids.shape[0]
        dim, ffn = w_up.shape[1:]
        n_slots, n_serve = n_dev * CAP, n_emb * CAP
        my_emb, my_dp = lax.axis_index('emb'), lax.axis_index('dp')

        lanes = 128
        per_dot, dots = 32, 2
        dma = pltpu.SemaphoreType.DMA
        _, recv_loc, counts, pick, slot_row, slot_col = pl.pallas_call(
            functools.partial(plan_kernel, (n_dp, n_emb, CAP, range_rows, per_dot)),
            out_shape=[jax.ShapeDtypeStruct(shape, I32) for shape in (
                (n_dev, tok // lanes, lanes), (n_dev, CAP), (n_dev, lanes), (n_serve, 1), (1, tok), (tok, 1))],
            in_specs=[vm], out_specs=[vm] * 6,
            scratch_shapes=[pltpu.VMEM((n_dev, tok), F32), dma((n_dev - 1,)), dma((n_dev - 1,))],
            compiler_params=pltpu.CompilerParams(collective_id=0, has_side_effects=True),
            name='plan',
        )(tok_ids.reshape(tok // lanes, lanes))
        c_iota = jnp.arange(CAP, dtype=I32)
        valid = c_iota[None, :] < counts[:, :1]
        slot_bits = (n_slots - 1).bit_length()
        slot_ids = jnp.arange(n_slots, dtype=I32).reshape(n_dev, CAP)
        keys = jnp.where(valid, recv_loc * (1 << slot_bits) + slot_ids, big)
        window, sub = 256, 8
        n_win = n_slots // window
        skeys = lax.sort(keys.reshape(-1))
        total = jnp.sum(counts[:, 0])
        live = jnp.arange(n_slots, dtype=I32) < total
        slot = jnp.bitwise_and(skeys, (1 << slot_bits) - 1)
        row = jnp.right_shift(skeys, slot_bits)
        group = jnp.right_shift(row, 3)
        same_row = jnp.concatenate([jnp.zeros((1,), jnp.bool_), row[1:] == row[:-1]])
        edge = group[1:] != group[:-1]
        one = jnp.ones((1,), jnp.bool_)
        fresh = jnp.concatenate([one, edge])
        last = jnp.concatenate([edge, one]) & live
        place = jnp.cumsum(fresh.astype(I32)).reshape(-1, window)
        place = place - place[:, :1]
        read_word = jnp.right_shift(slot, 3) * 16 + jnp.bitwise_and(slot, 7) + jnp.where(same_row, jnp.int32(-(1 << 31)), 0)
        write_word = place.reshape(-1) * 16 + jnp.bitwise_and(row, 7)
        group_word = jnp.where(live, group, 0)
        goes_on = jnp.logical_not(fresh) & live
        meta = jnp.concatenate([total.reshape(1), jnp.sum(last.reshape(-1, window).astype(I32), axis=1), place[:, -1],
                                goes_on.reshape(-1, window)[:, 0].astype(I32)])

        tab_shape = (n_layers, range_rows // 8, e_dim // 128, 8, 128)
        z_rows = 167
        z_chunks = tab_shape[1] // z_rows
        z_first, z_per = z_chunks // 2, 4
        served, dtab = pl.pallas_call(
            functools.partial(gather_kernel, (n_layers, n_emb, CAP, per_dot, dots, z_first)),
            out_shape=[jax.ShapeDtypeStruct((n_layers, n_serve, e_dim), BF), jax.ShapeDtypeStruct(tab_shape, F32)],
            in_specs=[sm, sm, vm, hbm],
            out_specs=[vm, hbm],
            scratch_shapes=[pltpu.VMEM((n_layers, n_serve * 8, e_dim), BF), pltpu.VMEM((z_rows,) + tab_shape[2:], F32), dma((n_emb,)), dma],
            compiler_params=params(0),
            name='table_rows',
        )(recv_loc, counts, pick, tables)

        fb = 1024
        n_blk = ffn // fb
        cw, nw, slab = 512, 512, 16
        n_back = n_layers - 1
        assert z_chunks * z_rows == tab_shape[1] and (n_layers * z_chunks - z_first) % z_per == 0
        matmul_flops = 4 * tok * dim * ffn
        w_bufs = [pltpu.VMEM((2, dim, fb), BF), pltpu.VMEM((2, fb, dim), BF), pltpu.VMEM((dim, e_dim), BF), pltpu.VMEM((e_dim, dim), BF)]
        x1, gate0, fetched = pl.pallas_call(
            functools.partial(first_kernel, (n_dp, n_emb, CAP, n_blk, cw, nw, slab)),
            out_shape=[
                jax.ShapeDtypeStruct((tok, dim), BF),
                jax.ShapeDtypeStruct((1, tok, e_dim), F32),
                jax.ShapeDtypeStruct((n_layers, tok, e_dim), BF),
            ],
            in_specs=[hbm, vm, hbm, hbm, hbm, hbm, hbm],
            out_specs=[vm, vm, vm],
            scratch_shapes=[
                pltpu.VMEM((tok, dim), BF), pltpu.VMEM((tok, dim), F32), pltpu.VMEM((tok, fb), BF), pltpu.VMEM((tok, fb), F32),
                pltpu.VMEM((n_layers, n_serve, e_dim), BF), *w_bufs, dma((3,)), dma((2, 2)), dma, dma((n_emb - 1,)), dma((n_emb - 1,)),
            ],
            compiler_params=params(0, collective_id=1, has_side_effects=True),
            cost_estimate=pl.CostEstimate(flops=matmul_flops, bytes_accessed=100 << 20, transcendentals=0),
            name='first_layer',
        )(resid_in, slot_col, served, w_gate, w_proj, w_up, w_down)

        out, saved, ups, gates, rows, dgp, dtab = pl.pallas_call(
            functools.partial(forward_kernel, (n_back, n_blk, cw, nw, slab, z_per, z_chunks, z_first)),
            out_shape=[
                jax.ShapeDtypeStruct((tok, dim), BF),
                jax.ShapeDtypeStruct((n_back - 1, tok, dim), BF),
                jax.ShapeDtypeStruct((n_back, tok, ffn), F32),
                jax.ShapeDtypeStruct((n_back, tok, e_dim), F32),
                jax.ShapeDtypeStruct((tok, e_dim), F32),
                jax.ShapeDtypeStruct((tok, e_dim), BF),
                jax.ShapeDtypeStruct(tab_shape, F32),
            ],
            in_specs=[hbm, hbm, vm, hbm, hbm, hbm, hbm, hbm],
            out_specs=[hbm, hbm, hbm, vm, vm, vm, hbm],
            input_output_aliases={7: 6},
            scratch_shapes=[
                pltpu.VMEM((tok, dim), BF), pltpu.VMEM((tok, dim), BF), pltpu.VMEM((tok, dim), F32), pltpu.VMEM((tok, fb), BF),
                pltpu.VMEM((2, tok, fb), F32), pltpu.VMEM((z_rows,) + tab_shape[2:], F32), *w_bufs,
                dma((3,)), dma((2, 2)), dma((2,)), dma, dma((z_per,)),
            ],
            compiler_params=params(0),
            cost_estimate=pl.CostEstimate(flops=n_back * matmul_flops, bytes_accessed=400 << 20, transcendentals=0),
            name='forward',
        )(x1, cot_out, fetched, w_gate, w_proj, w_up, w_down, dtab)

        got, got_gate, slots0 = pl.pallas_call(
            functools.partial(backward_kernel, (n_back, n_blk, n_dp, n_emb, CAP, cw, nw, slab)),
            out_shape=[jax.ShapeDtypeStruct((n_back, n_slots // 8, e_dim // 128, 8, 128), F32), jax.ShapeDtypeStruct((n_slots // 8, e_dim // 128, 8, 128), F32),
                       jax.ShapeDtypeStruct((n_dp, n_serve, e_dim), BF)],
            in_specs=[hbm, hbm, hbm, vm, vm, vm, vm, vm, vm, hbm, hbm, hbm, hbm, hbm],
            out_specs=[hbm, hbm, vm],
            scratch_shapes=[
                pltpu.VMEM((tok, dim), BF), pltpu.VMEM((tok, dim), BF), pltpu.VMEM((tok, dim), F32), pltpu.VMEM((tok, fb), BF), pltpu.VMEM((tok, fb), BF),
                pltpu.VMEM((tok, dim), BF), pltpu.VMEM((n_serve // 8, e_dim // 128, 8, 128), F32), pltpu.VMEM((n_serve // 8, e_dim // 128, 8, 128), F32),
                pltpu.VMEM((tok, e_dim), F32), pltpu.VMEM((tok, e_dim), BF), pltpu.VMEM((2, tok, fb), F32), *w_bufs,
                dma((4,)), dma((2, 2)), dma((2,)), dma((2, n_dev - 1)), dma((2,)), dma((n_back + 1, n_dev - 1)),
            ],
            compiler_params=params(0, collective_id=2, has_side_effects=True),
            cost_estimate=pl.CostEstimate(flops=n_back * matmul_flops, bytes_accessed=400 << 20, transcendentals=0),
            name='backward',
        )(cot_out, x1, saved, rows, dgp, slot_row, gate0, gates, fetched, ups, w_up, w_down, w_gate, w_proj)

        mixed0 = lax.all_to_all(slots0.reshape(n_dev, CAP, e_dim), MESH_AXES, 0, 0, tiled=True).reshape(n_slots, e_dim)
        dtab = pl.pallas_call(
            functools.partial(scatter_kernel, (8, window, 32)),
            out_shape=jax.ShapeDtypeStruct(dtab.shape, F32),
            in_specs=[sm, sm, sm, sm, hbm, hbm, hbm, hbm],
            out_specs=hbm,
            input_output_aliases={7: 0},
            scratch_shapes=[pltpu.VMEM((n_back, n_slots * 2, 128), F32), pltpu.VMEM((n_slots // 8,) + tab_shape[2:], F32),
                            pltpu.VMEM((n_slots, e_dim), BF), pltpu.VMEM((2, n_layers, window, e_dim // 128, sub, 128), F32),
                            pltpu.VMEM((n_slots // 8, e_dim // 128, 8, 128), F32), pltpu.SMEM((window,), I32), dma((2,)), dma((3,))],
            compiler_params=params(0),
            name='scatter',
        )(read_word, write_word, group_word, meta, got.reshape(n_back, n_slots * 2, 128), got_gate, mixed0, dtab)
        dtab = dtab.transpose(0, 1, 3, 2, 4).reshape(n_layers, range_rows, e_dim)
        return out, dtab

    return jax.shard_map(device_body, mesh=mesh, in_specs=(tok_spec, act_spec, act_spec, table_spec, full_spec, full_spec, full_spec, full_spec), out_specs=(act_spec, table_spec), check_vma=False)
```

```python
import functools

import jax
import jax.numpy as jnp
from jax import lax
from jax.experimental import pallas as pl
from jax.experimental.pallas import tpu as pltpu
from jax.sharding import PartitionSpec as P

NORM_EPS = 1e-6
BF = jnp.bfloat16
F32 = jnp.float32
I32 = jnp.int32
VMEM_BYTES = 67043328
GELU_C = 0.7978845608028654
GELU_A = 0.044715

MESH_AXES = ('dp', 'emb')
CAP = 256


def gelu(x):
    return 0.5 * x * (1.0 + jnp.tanh(GELU_C * (x + GELU_A * (x * x * x))))


def gelu_slope(x):
    sq = x * x
    th = jnp.tanh(GELU_C * (x + GELU_A * (x * sq)))
    return 0.5 * (1.0 + th) + (0.5 * GELU_C) * x * (1.0 - th * th) * (1.0 + (3 * GELU_A) * sq)


def dot(a, b):
    return jnp.dot(a, b, preferred_element_type=F32)


def dot_t(a, b):
    return lax.dot_general(a, b, (((1,), (1,)), ((), ())), preferred_element_type=F32)


def row_loop(rows, slab, unroll=2):
    def run(body):
        def step(i, carry):
            body(pl.ds(pl.multiple_of(i * slab, slab), slab))
            return carry

        lax.fori_loop(0, rows // slab, step, 0, unroll=unroll)

    return run


def peer_of(n_emb, index):
    dp = index // n_emb
    return {'dp': dp, 'emb': index - dp * n_emb}


def remote(src, dst, send_sem, recv_sem, device):
    return pltpu.make_async_remote_copy(src_ref=src, dst_ref=dst, send_sem=send_sem, recv_sem=recv_sem,
                                        device_id=device, device_id_type=pl.DeviceIdType.MESH)


def meet(devices):
    barrier = pltpu.get_barrier_semaphore()
    for device in devices:
        pl.semaphore_signal(barrier, inc=1, device_id=device, device_id_type=pl.DeviceIdType.MESH)
    pl.semaphore_wait(barrier, len(devices))


def plan_kernel(cfg, in_ref, ids_ref, recv_ref, counts_ref, pick_ref, slot_row_ref, slot_col_ref, rank_s, send_sem, recv_sem):
    n_dp, n_emb, cap, range_rows, per_dot = cfg
    n_dev = n_dp * n_emb
    my_dp, my_emb = lax.axis_index('dp'), lax.axis_index('emb')
    me = my_dp * n_emb + my_emb
    n_sub, lanes = in_ref.shape
    tok = n_sub * lanes
    peers = [peer_of(n_emb, lax.rem(me + k, n_dev)) for k in range(1, n_dev)]
    meet(peers)
    copies = [remote(in_ref, ids_ref.at[me], send_sem.at[k], recv_sem.at[k], peer) for k, peer in enumerate(peers)]
    start(copies)
    ids_ref[me] = in_ref[...]

    def line(ref):
        return jnp.concatenate([ref[..., j, :] for j in range(n_sub)], axis=-1)

    def ones(cond):
        return jnp.where(cond, 1.0, 0.0)

    def digits(x):
        return jnp.concatenate([jnp.right_shift(x, 8), jnp.bitwise_and(x, 255)], axis=0).astype(F32).astype(BF)

    square = (tok, tok)
    down, right = lax.broadcasted_iota(I32, square, 0), lax.broadcasted_iota(I32, square, 1)
    earlier = ones(down < right).astype(BF)
    own = jnp.broadcast_to(jnp.concatenate([in_ref[j:j + 1, :] for j in range(n_sub)], axis=-1), (8, tok))
    owner = sum(jnp.where(own >= e * range_rows, 1, 0) for e in range(1, n_emb))
    is_owner = owner == lax.broadcasted_iota(I32, (8, tok), 0)
    own_rank = dot(ones(is_owner).astype(BF), earlier).astype(I32)
    slot_row = jnp.sum(jnp.where(is_owner, own_rank + owner * cap, 0).astype(F32), axis=0, keepdims=True).astype(I32)
    slot_row_ref[...] = slot_row
    turned = dot_t(ones(down == right).astype(BF), digits(jnp.broadcast_to(slot_row, (8, tok))))
    slot_col_ref[...] = (turned[:, 0:1] * 256.0 + turned[:, 8:9]).astype(I32)

    wait(copies)
    ids8 = line(ids_ref)
    low = my_emb * range_rows
    mine = jnp.logical_and(ids8 >= low, ids8 < low + range_rows)
    mine_f = ones(mine)
    rank_s[...] = jnp.where(mine, dot(mine_f.astype(BF), earlier), -1.0)
    counts = jnp.sum(mine_f, axis=1, keepdims=True).astype(I32)
    counts_ref[...] = jnp.broadcast_to(counts, counts_ref.shape)
    loc = digits(jnp.where(mine, ids8 - low, 0))
    c_iota = lax.broadcasted_iota(I32, (cap, tok), 0).astype(F32)
    dev_iota = lax.broadcasted_iota(I32, (n_dev, cap), 0)
    recv = jnp.zeros((n_dev, cap), F32)
    for d in range(n_dev):
        found = dot_t(loc, ones(rank_s[d:d + 1, :] == c_iota).astype(BF))
        recv = jnp.where(dev_iota == d, found[:n_dev] * 256.0 + found[n_dev:], recv)
    slot = dev_iota * cap + lax.broadcasted_iota(I32, (n_dev, cap), 1)
    recv_ref[...] = jnp.where(slot - dev_iota * cap < counts, recv.astype(I32), slot * 8)
    lane16 = lax.broadcasted_iota(I32, (cap, 2 * n_dev), 1)
    row1 = lax.broadcasted_iota(I32, (cap, 1), 0)
    for e in range(n_emb):
        d = my_dp * n_emb + e
        found = dot_t(ones(rank_s[pl.ds(d, 1), :] == c_iota).astype(BF), loc)
        low8 = jnp.sum(jnp.where(lane16 == n_dev + d, found, 0.0), axis=1, keepdims=True).astype(I32)
        pick_ref[e * cap:(e + 1) * cap, :] = jnp.bitwise_and(low8, 7) + 8 * jnp.bitwise_and(row1, per_dot - 1)


def gather_kernel(cfg, loc_ref, counts_ref, pick_ref, tables_hbm, out_ref, dtab_hbm, buf, zero_s, sems, z_sem):
    n_layers, n_dest, cap, per_dot, group, z_chunks = cfg
    trip = per_dot * group
    z_rows = zero_s.shape[0]
    first = lax.axis_index('dp') * n_dest
    n_trips = [(counts_ref[first + d, 0] + (trip - 1)) // trip for d in range(n_dest)]

    def row_copy(d, c):
        base = pl.multiple_of(jnp.left_shift(jnp.right_shift(loc_ref[first + d, c], 3), 3), 8)
        at = pl.multiple_of(d * cap * 8 + c * 8, 8)
        return pltpu.make_async_copy(tables_hbm.at[:, pl.ds(base, 8), :], buf.at[:, pl.ds(at, 8), :], sems.at[d])

    def z_copy(c):
        return pltpu.make_async_copy(zero_s, dtab_hbm.at[1, pl.ds(c * z_rows, z_rows)], z_sem)

    for d in range(n_dest):
        def issue(i, carry, d=d):
            for k in range(8):
                row_copy(d, i * 8 + k).start()
            return carry

        lax.fori_loop(0, n_trips[d] * (trip // 8), issue, 0)

    clear_rows(zero_s)

    def z_start(c, carry):
        z_copy(c).start(priority=1)
        return carry

    lax.fori_loop(0, z_chunks, z_start, 0)
    for d in range(n_dest):
        def drain(i, carry, d=d):
            part = buf.at[:, pl.ds(pl.multiple_of((d * cap + i * trip) * 8, 8), trip * 8), :]
            pltpu.make_async_copy(part, part, sems.at[d]).wait()
            return carry

        lax.fori_loop(0, n_trips[d], drain, 0)

        def pick(i, carry, d=d):
            for k in range(group):
                s0 = pl.multiple_of(d * cap + i * trip + k * per_dot, per_dot)
                want = pick_ref[pl.ds(s0, per_dot), :]
                sel = (lax.broadcasted_iota(I32, (per_dot, per_dot * 8), 1) == want).astype(BF)
                for l in range(n_layers):
                    rows = buf[l, pl.ds(pl.multiple_of(s0 * 8, 8), per_dot * 8), :]
                    out_ref[l, pl.ds(s0, per_dot), :] = dot(sel, rows).astype(BF)
            return carry

        lax.fori_loop(0, n_trips[d], pick, 0)

        def blank(i, carry, d=d):
            s0 = pl.multiple_of(d * cap + i * trip, trip)
            for l in range(n_layers):
                out_ref[l, pl.ds(s0, trip), :] = jnp.zeros((trip, out_ref.shape[2]), BF)
            return carry

        lax.fori_loop(n_trips[d], cap // trip, blank, 0)

    def z_wait(c, carry):
        z_copy(c).wait()
        return carry

    lax.fori_loop(0, z_chunks, z_wait, 0)


def clear_rows(ref):
    def clear(i, carry):
        ref[i] = jnp.zeros(ref.shape[1:], F32)
        return carry

    lax.fori_loop(0, ref.shape[0], clear, 0)


def weight_copies(wu_hbm, wd_hbm, wu_s, wd_s, sems):
    fb = wu_s.shape[2]

    def copies(layer, blk, slot):
        at = pl.multiple_of(blk * fb, fb)
        return (pltpu.make_async_copy(wu_hbm.at[layer, :, pl.ds(at, fb)], wu_s.at[slot], sems.at[0, slot]),
                pltpu.make_async_copy(wd_hbm.at[layer, pl.ds(at, fb), :], wd_s.at[slot], sems.at[1, slot]))

    return copies


def start(copies):
    for copy in copies:
        copy.start()


def wait(copies):
    for copy in copies:
        copy.wait()


def mlp_block(cfg, u_s, h_s, acc_s, wu_ref, wd_ref, up_ref, second=None):
    cw, nw = cfg
    gw = 128
    n_c = wu_ref.shape[1] // cw

    def act(c):
        for g in range(cw // gw):
            gs = slice(c * cw + g * gw, c * cw + (g + 1) * gw)
            h_s[:, gs] = gelu(up_ref[:, gs]).astype(BF)

    for c in range(n_c):
        cs = slice(c * cw, (c + 1) * cw)
        up_ref[:, cs] = dot(u_s[...], wu_ref[:, cs])
        if c > 0:
            act(c - 1)
    if second is not None:
        second.wait()
    for c in range(n_c):
        cs = slice(c * cw, (c + 1) * cw)
        for n in range(acc_s.shape[1] // nw):
            ns = slice(n * nw, (n + 1) * nw)
            acc_s[:, ns] += dot(h_s[:, cs], wd_ref[cs, ns])
        if c == 0:
            act(n_c - 1)


def norm_rows(x, sl, u_s, acc_s):
    scale = lax.rsqrt(jnp.mean(x * x, axis=-1, keepdims=True) + NORM_EPS)
    u_s[sl, :] = (x * scale).astype(BF)
    acc_s[sl, :] = x


def add_proj(nw, acc_s, mixed, wp_ref):
    for n in range(acc_s.shape[1] // nw):
        ns = slice(n * nw, (n + 1) * nw)
        acc_s[:, ns] += dot(mixed, wp_ref[:, ns])


def first_kernel(cfg, x_hbm, slot_ref, served_hbm, wg_hbm, wp_hbm, wu_hbm, wd_hbm,
                 x_out_ref, gate_ref, fet_ref,
                 u_s, acc_s, h_s, up_s, ret_s, wu_s, wd_s, wg_s, wp_s, in_sem, w_sem, self_sem, send_sem, recv_sem):
    n_dp, n_emb, cap, n_blk, cw, nw, slab = cfg
    tok, dim = u_s.shape
    my_emb = lax.axis_index('emb')
    my_dp = lax.axis_index('dp')
    here = ret_s.at[:, pl.ds(pl.multiple_of(my_emb * cap, cap), cap), :]
    own = pltpu.make_async_copy(served_hbm.at[:, pl.ds(pl.multiple_of(my_emb * cap, cap), cap), :], here, self_sem)
    peers = [lax.rem(my_emb + k, n_emb) for k in range(1, n_emb)]
    copies = [remote(served_hbm.at[:, pl.ds(pl.multiple_of(p * cap, cap), cap), :], here,
                     send_sem.at[k], recv_sem.at[k], {'dp': my_dp, 'emb': p}) for k, p in enumerate(peers)]
    weights = weight_copies(wu_hbm, wd_hbm, wu_s, wd_s, w_sem)
    first = [pltpu.make_async_copy(x_hbm, x_out_ref, in_sem.at[0]),
             pltpu.make_async_copy(wg_hbm.at[0], wg_s, in_sem.at[1]),
             pltpu.make_async_copy(wp_hbm.at[0], wp_s, in_sem.at[2])]
    start(first[:2])
    start(weights(0, 0, 0))
    start(first[2:])
    meet([{'dp': my_dp, 'emb': p} for p in peers])
    own.start()
    start(copies)
    first[0].wait()
    row_loop(tok, slab)(lambda sl: norm_rows(x_out_ref[sl, :].astype(F32), sl, u_s, acc_s))
    first[1].wait()
    gate_ref[0] = dot(u_s[...], wg_s[...])

    def block(f, carry):
        slot = lax.rem(f, 2)

        @pl.when(f + 1 < n_blk)
        def _():
            start(weights(0, f + 1, 1 - slot))

        up_w, down_w = weights(0, f, slot)
        up_w.wait()
        mlp_block((cw, nw), u_s, h_s, acc_s, wu_s.at[slot], wd_s.at[slot], up_s, down_w)
        return carry

    lax.fori_loop(0, n_blk, block, 0)
    own.wait()
    wait(copies)
    first[2].wait()
    sel = (lax.broadcasted_iota(I32, (tok, n_emb * cap), 1) == slot_ref[...]).astype(BF)
    for l in range(fet_ref.shape[0]):
        fet_ref[l] = dot(sel, ret_s[l]).astype(BF)
    add_proj(nw, acc_s, (gelu(gate_ref[0]) * fet_ref[0].astype(F32)).astype(BF), wp_s)

    def finish(sl):
        x_out_ref[sl, :] = acc_s[sl, :].astype(BF)

    row_loop(tok, slab)(finish)


def forward_kernel(cfg, x_hbm, cot_hbm, fet_ref, wg_hbm, wp_hbm, wu_hbm, wd_hbm, dt_in,
                   out_hbm, saved_hbm, ups_hbm, gate_ref, rows_ref, dgp_ref, dtab_hbm,
                   x_s, u_s, acc_s, h_s, up_s, zero_s, wu_s, wd_s, wg_s, wp_s, in_sem, w_sem, up_sem, out_sem, z_sem):
    n_layers, n_blk, cw, nw, slab, z_pair, z_chunks, z_first = cfg
    tok, dim = x_s.shape
    fb = wu_s.shape[2]
    z_rows = zero_s.shape[0]
    n_steps = n_layers * n_blk
    weights = weight_copies(wu_hbm, wd_hbm, wu_s, wd_s, w_sem)

    def z_copies(step, js):
        found = []
        for j in js:
            c = z_first + jnp.right_shift(step, 1) * z_pair + jnp.bitwise_and(step, 1) * (z_pair // 2) + j
            zl = c // z_chunks
            found.append(pltpu.make_async_copy(zero_s, dtab_hbm.at[zl + 1, pl.ds((c - zl * z_chunks) * z_rows, z_rows)], z_sem.at[j]))
        return found

    few, more = range(z_pair // 2), range(z_pair // 2, z_pair - z_pair // 2)

    def up_copy(layer, blk, slot):
        return pltpu.make_async_copy(up_s.at[slot], ups_hbm.at[layer, :, pl.ds(pl.multiple_of(blk * fb, fb), fb)], up_sem.at[slot])

    def gate_copy(layer):
        return pltpu.make_async_copy(wg_hbm.at[layer + 1], wg_s, in_sem.at[1])

    def proj_copy(layer):
        return pltpu.make_async_copy(wp_hbm.at[layer + 1], wp_s, in_sem.at[2])

    fetch = pltpu.make_async_copy(x_hbm, x_s, in_sem.at[0])
    fetch.start()
    gate_copy(0).start()
    start(weights(1, 0, 0))
    proj_copy(0).start()
    clear_rows(zero_s)
    fetch.wait()
    row_loop(tok, slab)(lambda sl: norm_rows(x_s[sl, :].astype(F32), sl, u_s, acc_s))

    def one_layer(layer, carry):
        gate_copy(layer).wait()
        gate_ref[layer] = dot(u_s[...], wg_s[...])

        @pl.when(layer + 1 < n_layers)
        def _():
            gate_copy(layer + 1).start()

        def block(f, carry):
            step = layer * n_blk + f
            slot = lax.rem(step, 2)

            @pl.when(step + 1 < n_steps)
            def _():
                nxt = step + 1
                start(weights(1 + nxt // n_blk, lax.rem(nxt, n_blk), 1 - slot))

            odd = jnp.bitwise_and(step, 1) == 1

            @pl.when(step > 0)
            def _():
                wait(z_copies(step - 1, few))

            @pl.when((step > 0) & jnp.logical_not(odd))
            def _():
                wait(z_copies(step - 1, more))

            for copy in z_copies(step, few):
                copy.start(priority=1)

            @pl.when(odd)
            def _():
                for copy in z_copies(step, more):
                    copy.start(priority=1)

            @pl.when(step > 1)
            def _():
                up_copy(layer, f, slot).wait()

            wait(weights(1 + layer, f, slot))
            mlp_block((cw, nw), u_s, h_s, acc_s, wu_s.at[slot], wd_s.at[slot], up_s.at[slot])
            up_copy(layer, f, slot).start()
            return carry

        lax.fori_loop(0, n_blk, block, 0)
        proj_copy(layer).wait()
        add_proj(nw, acc_s, (gelu(gate_ref[layer]) * fet_ref[layer + 1].astype(F32)).astype(BF), wp_s)

        @pl.when(layer > 0)
        def _():
            pltpu.make_async_copy(x_s, saved_hbm.at[layer - 1], out_sem).wait()

        def next_rows(sl):
            x_new = acc_s[sl, :].astype(BF)
            x_s[sl, :] = x_new
            norm_rows(x_new.astype(F32), sl, u_s, acc_s)

        row_loop(tok, slab)(next_rows)

        @pl.when(layer < n_layers - 1)
        def _():
            pltpu.make_async_copy(x_s, saved_hbm.at[layer], out_sem).start()
            proj_copy(layer + 1).start()

        return carry

    lax.fori_loop(0, n_layers, one_layer, 0)
    put = pltpu.make_async_copy(x_s, out_hbm, out_sem)
    put.start()
    get = pltpu.make_async_copy(cot_hbm, u_s, in_sem.at[0])
    get.start()
    wait(z_copies(n_steps - 1, few))
    if n_steps % 2 == 0:
        wait(z_copies(n_steps - 1, more))
    up_copy(0, 0, 0).wait()
    up_copy(0, 0, 1).wait()
    get.wait()
    d_mixed = dot_t(u_s[...], wp_s[...]).astype(BF).astype(F32)
    gate_grads(gate_ref[n_layers - 1], fet_ref[n_layers], d_mixed, rows_ref, dgp_ref)
    put.wait()


def gate_grads(gate_pre, fetched, d_mixed, rows_ref, dgp_ref):
    rows_ref[...] = gelu(gate_pre) * d_mixed
    dgp_ref[...] = (d_mixed * fetched.astype(F32) * gelu_slope(gate_pre)).astype(BF)


def to_slots(rows, slot_ref, slots_s):
    hi = rows.astype(BF)
    rest = rows - hi.astype(F32)
    mid = rest.astype(BF)
    low = (rest - mid.astype(F32)).astype(BF)
    n = slots_s.shape[0] * slots_s.shape[2]
    sel = slot_pick(n, slot_ref)
    slots = (dot(sel, hi) + dot(sel, mid)) + dot(sel, low)
    for h in range(slots_s.shape[1]):
        slots_s[:, h] = slots[:, h * 128:(h + 1) * 128].reshape(n // 8, 8, 128)


def slot_pick(n, slot_ref):
    return (lax.broadcasted_iota(I32, (n, slot_ref.shape[1]), 0) == slot_ref[...]).astype(BF)


def backward_kernel(cfg, cot_hbm, x1_hbm, saved_hbm, rows_in_ref, dgp_in_ref, slot_ref, gate0_ref, gate_ref, fet_ref,
                    ups_hbm, wu_hbm, wd_hbm, wg_hbm, wp_hbm,
                    got_hbm, gate_hbm, slots0_ref,
                    cot_s, x_s, acc_s, dup_s, dh_s, dng_s, slots_s, gslots_s, rows_s, dgp_s, up_s, wu_s, wd_s, wg_s, wp_s,
                    in_sem, w_sem, up_sem, send_sem, self_sem, recv_sem):
    n_layers, n_blk, n_dp, n_emb, cap, cw, nw, slab = cfg
    tok, dim = cot_s.shape
    fb = wu_s.shape[2]
    gw = 128
    n_dev = n_dp * n_emb
    n_steps = n_layers * n_blk
    my_emb = lax.axis_index('emb')
    me = lax.axis_index('dp') * n_emb + my_emb
    peers = [peer_of(n_emb, lax.rem(me + k, n_dev)) for k in range(1, n_dev)]
    weights = weight_copies(wu_hbm, wd_hbm, wu_s, wd_s, w_sem)

    def part(ref, emb):
        return ref.at[pl.ds(emb * (cap // 8), cap // 8)]

    def sends(ref, there, which, got):
        return [pltpu.make_async_copy(part(ref, my_emb), there, self_sem.at[which])] + [
            remote(part(ref, peer['emb']), there, send_sem.at[which, k], recv_sem.at[got, k], peer) for k, peer in enumerate(peers)]

    def row_sends(i):
        return sends(slots_s, part(got_hbm.at[n_layers - 1 - i], me), 0, i)

    gate_sends = sends(gslots_s, part(gate_hbm, me), 1, n_layers)

    def up_copy(step, slot):
        i = step // n_blk
        blk = step - i * n_blk
        return pltpu.make_async_copy(ups_hbm.at[n_layers - 1 - i, :, pl.ds(pl.multiple_of(blk * fb, fb), fb)], up_s.at[slot], up_sem.at[slot])

    def load(step, slot):
        i = step // n_blk
        return weights(n_layers - i, step - i * n_blk, slot) + (up_copy(step, slot),)

    def gate_copy(i):
        return pltpu.make_async_copy(wg_hbm.at[n_layers - i], wg_s, in_sem.at[1])

    def proj_copy(i):
        return pltpu.make_async_copy(wp_hbm.at[n_layers - 1 - i], wp_s, in_sem.at[2])

    def x_copy(i):
        return pltpu.make_async_copy(saved_hbm.at[n_layers - 2 - i], x_s, in_sem.at[3])

    fetch = pltpu.make_async_copy(cot_hbm, cot_s, in_sem.at[0])
    gate_copy(0).start()
    fetch.start()
    start(load(0, 0))
    proj_copy(0).start()
    rows_s[...] = rows_in_ref[...]
    dgp_s[...] = dgp_in_ref[...]

    def clear(sl):
        acc_s[sl, :] = jnp.zeros((slab, dim), F32)

    row_loop(tok, slab)(clear)
    meet(peers)
    to_slots(gelu(gate0_ref[0]), slot_ref, gslots_s)

    def one_layer(i, carry):
        @pl.when(i < n_layers - 1)
        def _():
            x_copy(i).start()

        @pl.when(i == n_layers - 1)
        def _():
            pltpu.make_async_copy(x1_hbm, x_s, in_sem.at[3]).start()

        gate_copy(i).wait()
        to_slots(rows_s[...], slot_ref, slots_s)
        for n in range(dim // nw):
            ns = slice(n * nw, (n + 1) * nw)
            dng_s[:, ns] = dot_t(dgp_s[...], wg_s[ns, :]).astype(BF)
        start(row_sends(i))

        @pl.when(i < n_layers - 1)
        def _():
            gate_copy(i + 1).start()

        @pl.when(i == 0)
        def _():
            start(gate_sends)
            fetch.wait()

        def block(f, carry):
            step = i * n_blk + f
            slot = lax.rem(step, 2)

            @pl.when(step + 1 < n_steps)
            def _():
                start(load(step + 1, 1 - slot))

            wait(load(step, slot))
            wu_ref, wd_ref, up_ref = wu_s.at[slot], wd_s.at[slot], up_s.at[slot]

            def act(c):
                for g in range(cw // gw):
                    gs = slice(c * cw + g * gw, c * cw + (g + 1) * gw)
                    dup_s[:, gs] = (dh_s[:, gs].astype(F32) * gelu_slope(up_ref[:, gs])).astype(BF)

            n_c = fb // cw
            for c in range(n_c):
                cs = slice(c * cw, (c + 1) * cw)
                dh_s[:, cs] = dot_t(cot_s[...], wd_ref[cs, :]).astype(BF)
                if c > 0:
                    act(c - 1)
            for c in range(n_c):
                cs = slice(c * cw, (c + 1) * cw)
                for n in range(dim // nw):
                    ns = slice(n * nw, (n + 1) * nw)
                    acc_s[:, ns] += dot_t(dup_s[:, cs], wu_ref[ns, cs])
                if c == 0:
                    act(n_c - 1)
            return carry

        lax.fori_loop(0, n_blk, block, 0)
        pltpu.make_async_copy(x1_hbm, x_s, in_sem.at[3]).wait()

        def rows_back(sl):
            x = x_s[sl, :].astype(F32)
            scale = lax.rsqrt(jnp.mean(x * x, axis=-1, keepdims=True) + NORM_EPS)
            d_n = (acc_s[sl, :].astype(BF) + dng_s[sl, :]).astype(F32)
            acc_s[sl, :] = jnp.zeros((slab, dim), F32)
            proj = jnp.mean(d_n * x, axis=-1, keepdims=True)
            d_x = d_n * scale - x * (proj * (scale * scale * scale))
            cot_s[sl, :] = (cot_s[sl, :].astype(F32) + d_x).astype(BF)

        row_loop(tok, slab)(rows_back)
        proj_copy(i).wait()
        d_mixed = dot_t(cot_s[...], wp_s[...]).astype(BF)
        wait(row_sends(i))

        @pl.when(i < n_layers - 1)
        def _():
            proj_copy(i + 1).start()
            gate_grads(gate_ref[jnp.maximum(n_layers - 2 - i, 0)], fet_ref[n_layers - 1 - i], d_mixed.astype(F32), rows_s, dgp_s)

        @pl.when(i == n_layers - 1)
        def _():
            slots = dot(slot_pick(n_emb * cap, slot_ref), d_mixed).astype(BF)
            for d in range(n_dp):
                slots0_ref[d] = slots

        return carry

    lax.fori_loop(0, n_layers, one_layer, 0)
    wait(gate_sends)


def scatter_kernel(cfg, read_ref, write_ref, group_ref, meta_ref, rows_hbm, gate_hbm, mixed_hbm, dt_in, dt_out,
                   rows_ref, gate_ref, mixed_ref, late, groups, prod, zero_s, spots, sems, in_sem, z_sem):
    unroll, window, bulk, z_chunks = cfg
    n_back = groups.shape[1]
    n_slots = mixed_ref.shape[0]
    n_win = n_slots // window
    z_rows = zero_s.shape[0]
    count = meta_ref[0]
    loads = [pltpu.make_async_copy(src, dst, in_sem.at[k]) for k, (src, dst) in enumerate(
        ((gate_hbm, gate_ref), (mixed_hbm, mixed_ref), (rows_hbm, rows_ref)))]
    start(loads)
    clear_rows(zero_s)

    def z_copy(c):
        return pltpu.make_async_copy(zero_s, dt_out.at[0, pl.ds(c * z_rows, z_rows)], z_sem)

    def z_start(c, carry):
        z_copy(c).start(priority=1)
        return carry

    def z_wait(c, carry):
        z_copy(c).wait()
        return carry

    lax.fori_loop(0, z_chunks, z_start, 0)
    wait(loads[:2])

    def product(i, carry):
        step = 64
        mixed = mixed_ref[pl.ds(pl.multiple_of(i * step, step), step), :].astype(F32)
        for h in range(2):
            at = pl.ds(i * (step // 8), step // 8)
            prod[at, h] = gate_ref[at, h] * mixed[:, h * 128:(h + 1) * 128].reshape(step // 8, 8, 128)
        return carry

    lax.fori_loop(0, n_slots // 64, product, 0, unroll=4)

    def move(buf, spot, group, n):
        return pltpu.make_async_copy(groups.at[buf, :, pl.ds(spot, n)], dt_out.at[pl.ds(1, n_back), pl.ds(group, n)], sems.at[buf])

    def move_late(spot, group, n):
        return pltpu.make_async_copy(late.at[pl.ds(spot, n)], dt_out.at[0, pl.ds(group, n)], sems.at[2])

    def each(n, k, body):
        def trip(t, carry):
            for i in range(k):
                body(t * k + i)
            return carry

        def one(i, carry):
            body(i)
            return carry

        full = n // k
        lax.fori_loop(0, full, trip, 0)
        lax.fori_loop(full * k, n, one, 0)

    def settle(n, copies):
        def drain_bulk(j, carry):
            copies(bulk).wait()
            return carry

        def drain(j, carry):
            copies(1).wait()
            return carry

        lax.fori_loop(0, n // bulk, drain_bulk, 0)
        lax.fori_loop(0, lax.rem(n, bulk), drain, 0)

    blank = jnp.zeros(groups.shape[3:], F32)
    accs = tuple(jnp.zeros((2, 128), F32) for _ in range(1 + n_back))
    for w in range(n_win):
        buf, base = w % 2, w * window
        if w >= 2:
            settle(meta_ref[w - 1], lambda n, buf=buf: move(buf, 0, 0, n))
        left = jnp.clip(count - base, 0, window)
        trips = (left + (unroll - 1)) // unroll
        n_out = meta_ref[1 + w]

        def clear(u, buf=buf, base=base):
            late[base + u] = blank
            for l in range(n_back):
                groups[buf, l, u] = blank

        each(jnp.where(left > 0, jnp.minimum(n_out + 1, window), 0), 4, clear)
        if w == 0:
            wait(loads[2:])
        else:
            @pl.when(meta_ref[1 + 2 * n_win + w] > 0)
            def _(w=w, buf=buf, base=base):
                last = meta_ref[n_win + w]
                late[base] = late[base - window + last]
                for l in range(n_back):
                    groups[buf, l, 0] = groups[1 - buf, l, last]

        sums = [late.at[pl.ds(base, window)].reshape(window * 16, 128)] + [groups.at[buf, l].reshape(window * 16, 128) for l in range(n_back)]
        rows = [prod.reshape(n_slots * 2, 128)] + [rows_ref.at[l] for l in range(n_back)]

        def add(t, accs, base=base, sums=sums, rows=rows):
            for k in range(unroll):
                j = base + t * unroll + k
                word = read_ref[j]
                at = jnp.bitwise_and(word, n_slots * 2 - 1)
                same = word < 0
                to = write_ref[j]
                spots[base + jnp.right_shift(to, 4)] = group_ref[j]
                accs = tuple(jnp.where(same, acc, 0.0) + src[pl.ds(at, 2, stride=8), :] for acc, src in zip(accs, rows))
                for acc, dst in zip(accs, sums):
                    dst[pl.ds(to, 2, stride=8), :] = acc
            return accs

        accs = lax.fori_loop(0, trips, add, accs)
        each(n_out, 4, lambda u, buf=buf, base=base: move(buf, u, spots[base + u], 1).start())
    lax.fori_loop(0, z_chunks, z_wait, 0)
    for w in range(n_win):
        base = w * window
        each(meta_ref[1 + w], 4, lambda u, base=base: move_late(base + u, spots[base + u], 1).start())
    for w in range(n_win):
        if w >= n_win - 2:
            settle(meta_ref[1 + w], lambda n, w=w: move(w % 2, 0, 0, n))
        settle(meta_ref[1 + w], lambda n: move_late(0, 0, n))


def solution(mesh):
    n_emb, n_dp = mesh.shape['emb'], mesh.shape['dp']
    n_dev = n_emb * n_dp
    tok_spec = P(('dp', 'emb'))
    act_spec = P(('dp', 'emb'), None)
    table_spec = P(None, 'emb', None)
    full_spec = P(None, None, None)
    hbm = pl.BlockSpec(memory_space=pl.ANY)
    vm = pl.BlockSpec(memory_space=pltpu.VMEM)
    sm = pl.BlockSpec(memory_space=pltpu.SMEM)
    big = jnp.iinfo(jnp.int32).max

    def params(n_grid, **kw):
        return pltpu.CompilerParams(vmem_limit_bytes=VMEM_BYTES, dimension_semantics=('arbitrary',) * n_grid if n_grid else None, **kw)

    def device_body(tok_ids, resid_in, cot_out, tables, w_up, w_down, w_gate, w_proj):
        n_layers, range_rows, e_dim = tables.shape
        tok = tok_ids.shape[0]
        dim, ffn = w_up.shape[1:]
        n_slots, n_serve = n_dev * CAP, n_emb * CAP
        my_emb, my_dp = lax.axis_index('emb'), lax.axis_index('dp')

        lanes = 128
        per_dot, dots = 32, 2
        dma = pltpu.SemaphoreType.DMA
        _, recv_loc, counts, pick, slot_row, slot_col = pl.pallas_call(
            functools.partial(plan_kernel, (n_dp, n_emb, CAP, range_rows, per_dot)),
            out_shape=[jax.ShapeDtypeStruct(shape, I32) for shape in (
                (n_dev, tok // lanes, lanes), (n_dev, CAP), (n_dev, lanes), (n_serve, 1), (1, tok), (tok, 1))],
            in_specs=[vm], out_specs=[vm] * 6,
            scratch_shapes=[pltpu.VMEM((n_dev, tok), F32), dma((n_dev - 1,)), dma((n_dev - 1,))],
            compiler_params=pltpu.CompilerParams(collective_id=0, has_side_effects=True),
            name='plan',
        )(tok_ids.reshape(tok // lanes, lanes))
        c_iota = jnp.arange(CAP, dtype=I32)
        valid = c_iota[None, :] < counts[:, :1]
        slot_bits = (n_slots - 1).bit_length()
        slot_ids = jnp.arange(n_slots, dtype=I32).reshape(n_dev, CAP)
        keys = jnp.where(valid, recv_loc * (1 << slot_bits) + slot_ids, big)
        window, sub = 256, 8
        n_win = n_slots // window
        skeys = lax.sort(keys.reshape(-1))
        total = jnp.sum(counts[:, 0])
        live = jnp.arange(n_slots, dtype=I32) < total
        slot = jnp.bitwise_and(skeys, (1 << slot_bits) - 1)
        row = jnp.right_shift(skeys, slot_bits)
        group = jnp.right_shift(row, 3)
        same_row = jnp.concatenate([jnp.zeros((1,), jnp.bool_), row[1:] == row[:-1]])
        edge = group[1:] != group[:-1]
        one = jnp.ones((1,), jnp.bool_)
        fresh = jnp.concatenate([one, edge])
        last = jnp.concatenate([edge, one]) & live
        place = jnp.cumsum(fresh.astype(I32)).reshape(-1, window)
        place = place - place[:, :1]
        read_word = jnp.right_shift(slot, 3) * 16 + jnp.bitwise_and(slot, 7) + jnp.where(same_row, jnp.int32(-(1 << 31)), 0)
        write_word = place.reshape(-1) * 16 + jnp.bitwise_and(row, 7)
        group_word = jnp.where(live, group, 0)
        goes_on = jnp.logical_not(fresh) & live
        meta = jnp.concatenate([total.reshape(1), jnp.sum(last.reshape(-1, window).astype(I32), axis=1), place[:, -1],
                                goes_on.reshape(-1, window)[:, 0].astype(I32)])

        tab_shape = (n_layers, range_rows // 8, e_dim // 128, 8, 128)
        z_rows = 167
        z_chunks = tab_shape[1] // z_rows
        z_first = z_chunks // 2
        served, dtab = pl.pallas_call(
            functools.partial(gather_kernel, (n_layers, n_emb, CAP, per_dot, dots, z_first)),
            out_shape=[jax.ShapeDtypeStruct((n_layers, n_serve, e_dim), BF), jax.ShapeDtypeStruct(tab_shape, F32)],
            in_specs=[sm, sm, vm, hbm],
            out_specs=[vm, hbm],
            scratch_shapes=[pltpu.VMEM((n_layers, n_serve * 8, e_dim), BF), pltpu.VMEM((z_rows,) + tab_shape[2:], F32), dma((n_emb,)), dma],
            compiler_params=params(0),
            name='table_rows',
        )(recv_loc, counts, pick, tables)

        fb = 1024
        n_blk = ffn // fb
        cw, nw, slab = 512, 512, 16
        n_back = n_layers - 1
        z_pair = 2 * (n_back * z_chunks - z_first) // (n_back * n_blk)
        assert z_chunks * z_rows == tab_shape[1] and z_pair * n_back * n_blk == 2 * (n_back * z_chunks - z_first)
        matmul_flops = 4 * tok * dim * ffn
        w_bufs = [pltpu.VMEM((2, dim, fb), BF), pltpu.VMEM((2, fb, dim), BF), pltpu.VMEM((dim, e_dim), BF), pltpu.VMEM((e_dim, dim), BF)]
        x1, gate0, fetched = pl.pallas_call(
            functools.partial(first_kernel, (n_dp, n_emb, CAP, n_blk, cw, nw, slab)),
            out_shape=[
                jax.ShapeDtypeStruct((tok, dim), BF),
                jax.ShapeDtypeStruct((1, tok, e_dim), F32),
                jax.ShapeDtypeStruct((n_layers, tok, e_dim), BF),
            ],
            in_specs=[hbm, vm, hbm, hbm, hbm, hbm, hbm],
            out_specs=[vm, vm, vm],
            scratch_shapes=[
                pltpu.VMEM((tok, dim), BF), pltpu.VMEM((tok, dim), F32), pltpu.VMEM((tok, fb), BF), pltpu.VMEM((tok, fb), F32),
                pltpu.VMEM((n_layers, n_serve, e_dim), BF), *w_bufs, dma((3,)), dma((2, 2)), dma, dma((n_emb - 1,)), dma((n_emb - 1,)),
            ],
            compiler_params=params(0, collective_id=1, has_side_effects=True),
            cost_estimate=pl.CostEstimate(flops=matmul_flops, bytes_accessed=100 << 20, transcendentals=0),
            name='first_layer',
        )(resid_in, slot_col, served, w_gate, w_proj, w_up, w_down)

        out, saved, ups, gates, rows, dgp, dtab = pl.pallas_call(
            functools.partial(forward_kernel, (n_back, n_blk, cw, nw, slab, z_pair, z_chunks, z_first)),
            out_shape=[
                jax.ShapeDtypeStruct((tok, dim), BF),
                jax.ShapeDtypeStruct((n_back - 1, tok, dim), BF),
                jax.ShapeDtypeStruct((n_back, tok, ffn), F32),
                jax.ShapeDtypeStruct((n_back, tok, e_dim), F32),
                jax.ShapeDtypeStruct((tok, e_dim), F32),
                jax.ShapeDtypeStruct((tok, e_dim), BF),
                jax.ShapeDtypeStruct(tab_shape, F32),
            ],
            in_specs=[hbm, hbm, vm, hbm, hbm, hbm, hbm, hbm],
            out_specs=[hbm, hbm, hbm, vm, vm, vm, hbm],
            input_output_aliases={7: 6},
            scratch_shapes=[
                pltpu.VMEM((tok, dim), BF), pltpu.VMEM((tok, dim), BF), pltpu.VMEM((tok, dim), F32), pltpu.VMEM((tok, fb), BF),
                pltpu.VMEM((2, tok, fb), F32), pltpu.VMEM((z_rows,) + tab_shape[2:], F32), *w_bufs,
                dma((3,)), dma((2, 2)), dma((2,)), dma, dma((z_pair - z_pair // 2,)),
            ],
            compiler_params=params(0),
            cost_estimate=pl.CostEstimate(flops=n_back * matmul_flops, bytes_accessed=400 << 20, transcendentals=0),
            name='forward',
        )(x1, cot_out, fetched, w_gate, w_proj, w_up, w_down, dtab)

        got, got_gate, slots0 = pl.pallas_call(
            functools.partial(backward_kernel, (n_back, n_blk, n_dp, n_emb, CAP, cw, nw, slab)),
            out_shape=[jax.ShapeDtypeStruct((n_back, n_slots // 8, e_dim // 128, 8, 128), F32), jax.ShapeDtypeStruct((n_slots // 8, e_dim // 128, 8, 128), F32),
                       jax.ShapeDtypeStruct((n_dp, n_serve, e_dim), BF)],
            in_specs=[hbm, hbm, hbm, vm, vm, vm, vm, vm, vm, hbm, hbm, hbm, hbm, hbm],
            out_specs=[hbm, hbm, vm],
            scratch_shapes=[
                pltpu.VMEM((tok, dim), BF), pltpu.VMEM((tok, dim), BF), pltpu.VMEM((tok, dim), F32), pltpu.VMEM((tok, fb), BF), pltpu.VMEM((tok, fb), BF),
                pltpu.VMEM((tok, dim), BF), pltpu.VMEM((n_serve // 8, e_dim // 128, 8, 128), F32), pltpu.VMEM((n_serve // 8, e_dim // 128, 8, 128), F32),
                pltpu.VMEM((tok, e_dim), F32), pltpu.VMEM((tok, e_dim), BF), pltpu.VMEM((2, tok, fb), F32), *w_bufs,
                dma((4,)), dma((2, 2)), dma((2,)), dma((2, n_dev - 1)), dma((2,)), dma((n_back + 1, n_dev - 1)),
            ],
            compiler_params=params(0, collective_id=2, has_side_effects=True),
            cost_estimate=pl.CostEstimate(flops=n_back * matmul_flops, bytes_accessed=400 << 20, transcendentals=0),
            name='backward',
        )(cot_out, x1, saved, rows, dgp, slot_row, gate0, gates, fetched, ups, w_up, w_down, w_gate, w_proj)

        mixed0 = lax.all_to_all(slots0.reshape(n_dev, CAP, e_dim), MESH_AXES, 0, 0, tiled=True).reshape(n_slots, e_dim)
        dtab = pl.pallas_call(
            functools.partial(scatter_kernel, (8, window, 32, z_chunks)),
            out_shape=jax.ShapeDtypeStruct(dtab.shape, F32),
            in_specs=[sm, sm, sm, sm, hbm, hbm, hbm, hbm],
            out_specs=hbm,
            input_output_aliases={7: 0},
            scratch_shapes=[pltpu.VMEM((n_back, n_slots * 2, 128), F32), pltpu.VMEM((n_slots // 8,) + tab_shape[2:], F32),
                            pltpu.VMEM((n_slots, e_dim), BF), pltpu.VMEM((n_slots,) + tab_shape[2:], F32),
                            pltpu.VMEM((2, n_back, window) + tab_shape[2:], F32), pltpu.VMEM((n_slots // 8,) + tab_shape[2:], F32),
                            pltpu.VMEM((z_rows,) + tab_shape[2:], F32), pltpu.SMEM((n_slots,), I32), dma((3,)), dma((3,)), dma],
            compiler_params=params(0),
            name='scatter',
        )(read_word, write_word, group_word, meta, got.reshape(n_back, n_slots * 2, 128), got_gate, mixed0, dtab)
        dtab = dtab.transpose(0, 1, 3, 2, 4).reshape(n_layers, range_rows, e_dim)
        return out, dtab

    return jax.shard_map(device_body, mesh=mesh, in_specs=(tok_spec, act_spec, act_spec, table_spec, full_spec, full_spec, full_spec, full_spec), out_specs=(act_spec, table_spec), check_vma=False)
```

```python
import functools

import jax
import jax.numpy as jnp
from jax import lax
from jax.experimental import pallas as pl
from jax.experimental.pallas import tpu as pltpu
from jax.sharding import PartitionSpec as P

NORM_EPS = 1e-6
BF = jnp.bfloat16
F32 = jnp.float32
I32 = jnp.int32
VMEM_BYTES = 67043328
GELU_C = 0.7978845608028654
GELU_A = 0.044715

MESH_AXES = ('dp', 'emb')
CAP = 256


def gelu(x):
    return 0.5 * x * (1.0 + jnp.tanh(GELU_C * (x + GELU_A * (x * x * x))))


def gelu_slope(x):
    sq = x * x
    th = jnp.tanh(GELU_C * (x + GELU_A * (x * sq)))
    return 0.5 * (1.0 + th) + (0.5 * GELU_C) * x * (1.0 - th * th) * (1.0 + (3 * GELU_A) * sq)


def dot(a, b):
    return jnp.dot(a, b, preferred_element_type=F32)


def dot_t(a, b):
    return lax.dot_general(a, b, (((1,), (1,)), ((), ())), preferred_element_type=F32)


def row_loop(rows, slab, unroll=2):
    def run(body):
        def step(i, carry):
            body(pl.ds(pl.multiple_of(i * slab, slab), slab))
            return carry

        lax.fori_loop(0, rows // slab, step, 0, unroll=unroll)

    return run


def peer_of(n_emb, index):
    dp = index // n_emb
    return {'dp': dp, 'emb': index - dp * n_emb}


def remote(src, dst, send_sem, recv_sem, device):
    return pltpu.make_async_remote_copy(src_ref=src, dst_ref=dst, send_sem=send_sem, recv_sem=recv_sem,
                                        device_id=device, device_id_type=pl.DeviceIdType.MESH)


def meet(devices):
    barrier = pltpu.get_barrier_semaphore()
    for device in devices:
        pl.semaphore_signal(barrier, inc=1, device_id=device, device_id_type=pl.DeviceIdType.MESH)
    pl.semaphore_wait(barrier, len(devices))


def plan_kernel(cfg, in_ref, ids_ref, recv_ref, counts_ref, pick_ref, slot_row_ref, slot_col_ref, rank_s, send_sem, recv_sem):
    n_dp, n_emb, cap, range_rows, per_dot = cfg
    n_dev = n_dp * n_emb
    my_dp, my_emb = lax.axis_index('dp'), lax.axis_index('emb')
    me = my_dp * n_emb + my_emb
    n_sub, lanes = in_ref.shape
    tok = n_sub * lanes
    peers = [peer_of(n_emb, lax.rem(me + k, n_dev)) for k in range(1, n_dev)]
    meet(peers)
    copies = [remote(in_ref, ids_ref.at[me], send_sem.at[k], recv_sem.at[k], peer) for k, peer in enumerate(peers)]
    start(copies)
    ids_ref[me] = in_ref[...]

    def line(ref):
        return jnp.concatenate([ref[..., j, :] for j in range(n_sub)], axis=-1)

    def ones(cond):
        return jnp.where(cond, 1.0, 0.0)

    def digits(x):
        return jnp.concatenate([jnp.right_shift(x, 8), jnp.bitwise_and(x, 255)], axis=0).astype(F32).astype(BF)

    square = (tok, tok)
    down, right = lax.broadcasted_iota(I32, square, 0), lax.broadcasted_iota(I32, square, 1)
    earlier = ones(down < right).astype(BF)
    own = jnp.broadcast_to(jnp.concatenate([in_ref[j:j + 1, :] for j in range(n_sub)], axis=-1), (8, tok))
    owner = sum(jnp.where(own >= e * range_rows, 1, 0) for e in range(1, n_emb))
    is_owner = owner == lax.broadcasted_iota(I32, (8, tok), 0)
    own_rank = dot(ones(is_owner).astype(BF), earlier).astype(I32)
    slot_row = jnp.sum(jnp.where(is_owner, own_rank + owner * cap, 0).astype(F32), axis=0, keepdims=True).astype(I32)
    slot_row_ref[...] = slot_row
    turned = dot_t(ones(down == right).astype(BF), digits(jnp.broadcast_to(slot_row, (8, tok))))
    slot_col_ref[...] = (turned[:, 0:1] * 256.0 + turned[:, 8:9]).astype(I32)

    wait(copies)
    ids8 = line(ids_ref)
    low = my_emb * range_rows
    mine = jnp.logical_and(ids8 >= low, ids8 < low + range_rows)
    mine_f = ones(mine)
    rank_s[...] = jnp.where(mine, dot(mine_f.astype(BF), earlier), -1.0)
    counts = jnp.sum(mine_f, axis=1, keepdims=True).astype(I32)
    counts_ref[...] = jnp.broadcast_to(counts, counts_ref.shape)
    loc = digits(jnp.where(mine, ids8 - low, 0))
    c_iota = lax.broadcasted_iota(I32, (cap, tok), 0).astype(F32)
    dev_iota = lax.broadcasted_iota(I32, (n_dev, cap), 0)
    recv = jnp.zeros((n_dev, cap), F32)
    for d in range(n_dev):
        found = dot_t(loc, ones(rank_s[d:d + 1, :] == c_iota).astype(BF))
        recv = jnp.where(dev_iota == d, found[:n_dev] * 256.0 + found[n_dev:], recv)
    slot = dev_iota * cap + lax.broadcasted_iota(I32, (n_dev, cap), 1)
    recv_ref[...] = jnp.where(slot - dev_iota * cap < counts, recv.astype(I32), slot * 8)
    lane16 = lax.broadcasted_iota(I32, (cap, 2 * n_dev), 1)
    row1 = lax.broadcasted_iota(I32, (cap, 1), 0)
    for e in range(n_emb):
        d = my_dp * n_emb + e
        found = dot_t(ones(rank_s[pl.ds(d, 1), :] == c_iota).astype(BF), loc)
        low8 = jnp.sum(jnp.where(lane16 == n_dev + d, found, 0.0), axis=1, keepdims=True).astype(I32)
        pick_ref[e * cap:(e + 1) * cap, :] = jnp.bitwise_and(low8, 7) + 8 * jnp.bitwise_and(row1, per_dot - 1)


def gather_kernel(cfg, loc_ref, counts_ref, recv_ref, tally_ref, pick_ref, tables_hbm,
                  out_ref, dtab_hbm, read_ref, write_ref, group_ref, meta_ref, buf, zero_s, sems, z_sem):
    n_layers, n_dest, cap, per_dot, group, z_chunks, slot_bits = cfg
    trip = per_dot * group
    z_rows = zero_s.shape[0]
    first = lax.axis_index('dp') * n_dest
    n_trips = [(counts_ref[first + d, 0] + (trip - 1)) // trip for d in range(n_dest)]

    def row_copy(d, c):
        base = pl.multiple_of(jnp.left_shift(jnp.right_shift(loc_ref[first + d, c], 3), 3), 8)
        at = pl.multiple_of(d * cap * 8 + c * 8, 8)
        return pltpu.make_async_copy(tables_hbm.at[:, pl.ds(base, 8), :], buf.at[:, pl.ds(at, 8), :], sems.at[d])

    def z_copy(c):
        return pltpu.make_async_copy(zero_s, dtab_hbm.at[1, pl.ds(c * z_rows, z_rows)], z_sem)

    for d in range(n_dest):
        def issue(i, carry, d=d):
            for k in range(8):
                row_copy(d, i * 8 + k).start()
            return carry

        lax.fori_loop(0, n_trips[d] * (trip // 8), issue, 0)

    clear_rows(zero_s)

    def z_start(c, carry):
        z_copy(c).start(priority=1)
        return carry

    lax.fori_loop(0, z_chunks, z_start, 0)
    order_rows(recv_ref, tally_ref, slot_bits, read_ref, write_ref, group_ref, meta_ref)
    for d in range(n_dest):
        def drain(i, carry, d=d):
            part = buf.at[:, pl.ds(pl.multiple_of((d * cap + i * trip) * 8, 8), trip * 8), :]
            pltpu.make_async_copy(part, part, sems.at[d]).wait()
            return carry

        lax.fori_loop(0, n_trips[d], drain, 0)

        def pick(i, carry, d=d):
            for k in range(group):
                s0 = pl.multiple_of(d * cap + i * trip + k * per_dot, per_dot)
                want = pick_ref[pl.ds(s0, per_dot), :]
                sel = (lax.broadcasted_iota(I32, (per_dot, per_dot * 8), 1) == want).astype(BF)
                for l in range(n_layers):
                    rows = buf[l, pl.ds(pl.multiple_of(s0 * 8, 8), per_dot * 8), :]
                    out_ref[l, pl.ds(s0, per_dot), :] = dot(sel, rows).astype(BF)
            return carry

        lax.fori_loop(0, n_trips[d], pick, 0)

        def blank(i, carry, d=d):
            s0 = pl.multiple_of(d * cap + i * trip, trip)
            for l in range(n_layers):
                out_ref[l, pl.ds(s0, trip), :] = jnp.zeros((trip, out_ref.shape[2]), BF)
            return carry

        lax.fori_loop(n_trips[d], cap // trip, blank, 0)

    def z_wait(c, carry):
        z_copy(c).wait()
        return carry

    lax.fori_loop(0, z_chunks, z_wait, 0)


def clear_rows(ref):
    def clear(i, carry):
        ref[i] = jnp.zeros(ref.shape[1:], F32)
        return carry

    lax.fori_loop(0, ref.shape[0], clear, 0)


def weight_copies(wu_hbm, wd_hbm, wu_s, wd_s, sems):
    fb = wu_s.shape[2]

    def copies(layer, blk, slot):
        at = pl.multiple_of(blk * fb, fb)
        return (pltpu.make_async_copy(wu_hbm.at[layer, :, pl.ds(at, fb)], wu_s.at[slot], sems.at[0, slot]),
                pltpu.make_async_copy(wd_hbm.at[layer, pl.ds(at, fb), :], wd_s.at[slot], sems.at[1, slot]))

    return copies


def start(copies):
    for copy in copies:
        copy.start()


def wait(copies):
    for copy in copies:
        copy.wait()


def mlp_block(cfg, u_s, h_s, acc_s, wu_ref, wd_ref, up_ref, second=None):
    cw, nw = cfg
    gw = 128
    n_c = wu_ref.shape[1] // cw

    def act(c):
        for g in range(cw // gw):
            gs = slice(c * cw + g * gw, c * cw + (g + 1) * gw)
            h_s[:, gs] = gelu(up_ref[:, gs]).astype(BF)

    for c in range(n_c):
        cs = slice(c * cw, (c + 1) * cw)
        up_ref[:, cs] = dot(u_s[...], wu_ref[:, cs])
        if c > 0:
            act(c - 1)
    if second is not None:
        second.wait()
    for c in range(n_c):
        cs = slice(c * cw, (c + 1) * cw)
        for n in range(acc_s.shape[1] // nw):
            ns = slice(n * nw, (n + 1) * nw)
            acc_s[:, ns] += dot(h_s[:, cs], wd_ref[cs, ns])
        if c == 0:
            act(n_c - 1)


def norm_rows(x, sl, u_s, acc_s):
    scale = lax.rsqrt(jnp.mean(x * x, axis=-1, keepdims=True) + NORM_EPS)
    u_s[sl, :] = (x * scale).astype(BF)
    acc_s[sl, :] = x


def add_proj(nw, acc_s, mixed, wp_ref):
    for n in range(acc_s.shape[1] // nw):
        ns = slice(n * nw, (n + 1) * nw)
        acc_s[:, ns] += dot(mixed, wp_ref[:, ns])


def first_kernel(cfg, x_hbm, slot_ref, served_hbm, wg_hbm, wp_hbm, wu_hbm, wd_hbm,
                 x_out_ref, gate_ref, fet_ref,
                 u_s, acc_s, h_s, up_s, ret_s, wu_s, wd_s, wg_s, wp_s, in_sem, w_sem, self_sem, send_sem, recv_sem):
    n_dp, n_emb, cap, n_blk, cw, nw, slab = cfg
    tok, dim = u_s.shape
    my_emb = lax.axis_index('emb')
    my_dp = lax.axis_index('dp')
    here = ret_s.at[:, pl.ds(pl.multiple_of(my_emb * cap, cap), cap), :]
    own = pltpu.make_async_copy(served_hbm.at[:, pl.ds(pl.multiple_of(my_emb * cap, cap), cap), :], here, self_sem)
    peers = [lax.rem(my_emb + k, n_emb) for k in range(1, n_emb)]
    copies = [remote(served_hbm.at[:, pl.ds(pl.multiple_of(p * cap, cap), cap), :], here,
                     send_sem.at[k], recv_sem.at[k], {'dp': my_dp, 'emb': p}) for k, p in enumerate(peers)]
    weights = weight_copies(wu_hbm, wd_hbm, wu_s, wd_s, w_sem)
    first = [pltpu.make_async_copy(x_hbm, x_out_ref, in_sem.at[0]),
             pltpu.make_async_copy(wg_hbm.at[0], wg_s, in_sem.at[1]),
             pltpu.make_async_copy(wp_hbm.at[0], wp_s, in_sem.at[2])]
    start(first[:2])
    start(weights(0, 0, 0))
    start(first[2:])
    meet([{'dp': my_dp, 'emb': p} for p in peers])
    own.start()
    start(copies)
    first[0].wait()
    row_loop(tok, slab)(lambda sl: norm_rows(x_out_ref[sl, :].astype(F32), sl, u_s, acc_s))
    first[1].wait()
    gate_ref[0] = dot(u_s[...], wg_s[...])

    def block(f, carry):
        slot = lax.rem(f, 2)

        @pl.when(f + 1 < n_blk)
        def _():
            start(weights(0, f + 1, 1 - slot))

        up_w, down_w = weights(0, f, slot)
        up_w.wait()
        mlp_block((cw, nw), u_s, h_s, acc_s, wu_s.at[slot], wd_s.at[slot], up_s, down_w)
        return carry

    lax.fori_loop(0, n_blk, block, 0)
    own.wait()
    wait(copies)
    first[2].wait()
    sel = (lax.broadcasted_iota(I32, (tok, n_emb * cap), 1) == slot_ref[...]).astype(BF)
    for l in range(fet_ref.shape[0]):
        fet_ref[l] = dot(sel, ret_s[l]).astype(BF)
    add_proj(nw, acc_s, (gelu(gate_ref[0]) * fet_ref[0].astype(F32)).astype(BF), wp_s)

    def finish(sl):
        x_out_ref[sl, :] = acc_s[sl, :].astype(BF)

    row_loop(tok, slab)(finish)


def forward_kernel(cfg, x_hbm, cot_hbm, fet_ref, wg_hbm, wp_hbm, wu_hbm, wd_hbm, dt_in,
                   out_hbm, saved_hbm, ups_hbm, gate_ref, rows_ref, dgp_ref, dtab_hbm,
                   x_s, u_s, acc_s, h_s, up_s, zero_s, wu_s, wd_s, wg_s, wp_s, in_sem, w_sem, up_sem, out_sem, z_sem):
    n_layers, n_blk, cw, nw, slab, z_pair, z_chunks, z_first = cfg
    tok, dim = x_s.shape
    fb = wu_s.shape[2]
    z_rows = zero_s.shape[0]
    n_steps = n_layers * n_blk
    weights = weight_copies(wu_hbm, wd_hbm, wu_s, wd_s, w_sem)

    def z_copies(step, js):
        found = []
        for j in js:
            c = z_first + jnp.right_shift(step, 1) * z_pair + jnp.bitwise_and(step, 1) * (z_pair // 2) + j
            zl = c // z_chunks
            found.append(pltpu.make_async_copy(zero_s, dtab_hbm.at[zl + 1, pl.ds((c - zl * z_chunks) * z_rows, z_rows)], z_sem.at[j]))
        return found

    few, more = range(z_pair // 2), range(z_pair // 2, z_pair - z_pair // 2)

    def up_copy(layer, blk, slot):
        return pltpu.make_async_copy(up_s.at[slot], ups_hbm.at[layer, :, pl.ds(pl.multiple_of(blk * fb, fb), fb)], up_sem.at[slot])

    def gate_copy(layer):
        return pltpu.make_async_copy(wg_hbm.at[layer + 1], wg_s, in_sem.at[1])

    def proj_copy(layer):
        return pltpu.make_async_copy(wp_hbm.at[layer + 1], wp_s, in_sem.at[2])

    fetch = pltpu.make_async_copy(x_hbm, x_s, in_sem.at[0])
    fetch.start()
    gate_copy(0).start()
    start(weights(1, 0, 0))
    proj_copy(0).start()
    clear_rows(zero_s)
    fetch.wait()
    row_loop(tok, slab)(lambda sl: norm_rows(x_s[sl, :].astype(F32), sl, u_s, acc_s))

    def one_layer(layer, carry):
        gate_copy(layer).wait()
        gate_ref[layer] = dot(u_s[...], wg_s[...])

        @pl.when(layer + 1 < n_layers)
        def _():
            gate_copy(layer + 1).start()

        def block(f, carry):
            step = layer * n_blk + f
            slot = lax.rem(step, 2)

            @pl.when(step + 1 < n_steps)
            def _():
                nxt = step + 1
                start(weights(1 + nxt // n_blk, lax.rem(nxt, n_blk), 1 - slot))

            odd = jnp.bitwise_and(step, 1) == 1

            @pl.when(step > 0)
            def _():
                wait(z_copies(step - 1, few))

            @pl.when((step > 0) & jnp.logical_not(odd))
            def _():
                wait(z_copies(step - 1, more))

            for copy in z_copies(step, few):
                copy.start(priority=1)

            @pl.when(odd)
            def _():
                for copy in z_copies(step, more):
                    copy.start(priority=1)

            @pl.when(step > 1)
            def _():
                up_copy(layer, f, slot).wait()

            wait(weights(1 + layer, f, slot))
            mlp_block((cw, nw), u_s, h_s, acc_s, wu_s.at[slot], wd_s.at[slot], up_s.at[slot])
            up_copy(layer, f, slot).start()
            return carry

        lax.fori_loop(0, n_blk, block, 0)
        proj_copy(layer).wait()
        add_proj(nw, acc_s, (gelu(gate_ref[layer]) * fet_ref[layer + 1].astype(F32)).astype(BF), wp_s)

        @pl.when(layer > 0)
        def _():
            pltpu.make_async_copy(x_s, saved_hbm.at[layer - 1], out_sem).wait()

        def next_rows(sl):
            x_new = acc_s[sl, :].astype(BF)
            x_s[sl, :] = x_new
            norm_rows(x_new.astype(F32), sl, u_s, acc_s)

        row_loop(tok, slab)(next_rows)

        @pl.when(layer < n_layers - 1)
        def _():
            pltpu.make_async_copy(x_s, saved_hbm.at[layer], out_sem).start()
            proj_copy(layer + 1).start()

        return carry

    lax.fori_loop(0, n_layers, one_layer, 0)
    put = pltpu.make_async_copy(x_s, out_hbm, out_sem)
    put.start()
    get = pltpu.make_async_copy(cot_hbm, u_s, in_sem.at[0])
    get.start()
    wait(z_copies(n_steps - 1, few))
    if n_steps % 2 == 0:
        wait(z_copies(n_steps - 1, more))
    up_copy(0, 0, 0).wait()
    up_copy(0, 0, 1).wait()
    get.wait()
    d_mixed = dot_t(u_s[...], wp_s[...]).astype(BF).astype(F32)
    gate_grads(gate_ref[n_layers - 1], fet_ref[n_layers], d_mixed, rows_ref, dgp_ref)
    put.wait()


def gate_grads(gate_pre, fetched, d_mixed, rows_ref, dgp_ref):
    rows_ref[...] = gelu(gate_pre) * d_mixed
    dgp_ref[...] = (d_mixed * fetched.astype(F32) * gelu_slope(gate_pre)).astype(BF)


def to_slots(rows, slot_ref, slots_s):
    hi = rows.astype(BF)
    rest = rows - hi.astype(F32)
    mid = rest.astype(BF)
    low = (rest - mid.astype(F32)).astype(BF)
    n = slots_s.shape[0] * slots_s.shape[2]
    sel = slot_pick(n, slot_ref)
    slots = (dot(sel, hi) + dot(sel, mid)) + dot(sel, low)
    for h in range(slots_s.shape[1]):
        slots_s[:, h] = slots[:, h * 128:(h + 1) * 128].reshape(n // 8, 8, 128)


def slot_pick(n, slot_ref):
    return (lax.broadcasted_iota(I32, (n, slot_ref.shape[1]), 0) == slot_ref[...]).astype(BF)


def backward_kernel(cfg, cot_hbm, x1_hbm, saved_hbm, rows_in_ref, dgp_in_ref, slot_ref, gate0_ref, gate_ref, fet_ref,
                    ups_hbm, wu_hbm, wd_hbm, wg_hbm, wp_hbm,
                    got_hbm, gate_hbm, mixed_hbm,
                    cot_s, x_s, acc_s, dup_s, dh_s, dng_s, slots_s, gslots_s, dslots_s, rows_s, dgp_s, up_s, wu_s, wd_s, wg_s, wp_s,
                    in_sem, w_sem, up_sem, send_sem, self_sem, recv_sem):
    n_layers, n_blk, n_dp, n_emb, cap, cw, nw, slab = cfg
    tok, dim = cot_s.shape
    fb = wu_s.shape[2]
    gw = 128
    n_dev = n_dp * n_emb
    n_steps = n_layers * n_blk
    my_emb = lax.axis_index('emb')
    me = lax.axis_index('dp') * n_emb + my_emb
    peers = [peer_of(n_emb, lax.rem(me + k, n_dev)) for k in range(1, n_dev)]
    weights = weight_copies(wu_hbm, wd_hbm, wu_s, wd_s, w_sem)

    def part(ref, emb):
        return ref.at[pl.ds(emb * (cap // 8), cap // 8)]

    def sends(ref, there, which, got):
        return [pltpu.make_async_copy(part(ref, my_emb), there, self_sem.at[which])] + [
            remote(part(ref, peer['emb']), there, send_sem.at[which, k], recv_sem.at[got, k], peer) for k, peer in enumerate(peers)]

    def row_sends(i):
        return sends(slots_s, part(got_hbm.at[n_layers - 1 - i], me), 0, i)

    gate_sends = sends(gslots_s, part(gate_hbm, me), 1, n_layers)

    def flat(ref, dev):
        return ref.at[pl.ds(pl.multiple_of(dev * cap, cap), cap), :]

    mixed_sends = [pltpu.make_async_copy(flat(dslots_s, my_emb), flat(mixed_hbm, me), self_sem.at[2])] + [
        remote(flat(dslots_s, peer['emb']), flat(mixed_hbm, me), send_sem.at[2, k], recv_sem.at[n_layers + 1, k], peer)
        for k, peer in enumerate(peers)]

    def up_copy(step, slot):
        i = step // n_blk
        blk = step - i * n_blk
        return pltpu.make_async_copy(ups_hbm.at[n_layers - 1 - i, :, pl.ds(pl.multiple_of(blk * fb, fb), fb)], up_s.at[slot], up_sem.at[slot])

    def load(step, slot):
        i = step // n_blk
        return weights(n_layers - i, step - i * n_blk, slot) + (up_copy(step, slot),)

    def gate_copy(i):
        return pltpu.make_async_copy(wg_hbm.at[n_layers - i], wg_s, in_sem.at[1])

    def proj_copy(i):
        return pltpu.make_async_copy(wp_hbm.at[n_layers - 1 - i], wp_s, in_sem.at[2])

    def x_copy(i):
        return pltpu.make_async_copy(saved_hbm.at[n_layers - 2 - i], x_s, in_sem.at[3])

    fetch = pltpu.make_async_copy(cot_hbm, cot_s, in_sem.at[0])
    gate_copy(0).start()
    fetch.start()
    start(load(0, 0))
    proj_copy(0).start()
    rows_s[...] = rows_in_ref[...]
    dgp_s[...] = dgp_in_ref[...]

    def clear(sl):
        acc_s[sl, :] = jnp.zeros((slab, dim), F32)

    row_loop(tok, slab)(clear)
    meet(peers)
    to_slots(gelu(gate0_ref[0]), slot_ref, gslots_s)

    def one_layer(i, carry):
        @pl.when(i < n_layers - 1)
        def _():
            x_copy(i).start()

        @pl.when(i == n_layers - 1)
        def _():
            pltpu.make_async_copy(x1_hbm, x_s, in_sem.at[3]).start()

        gate_copy(i).wait()
        to_slots(rows_s[...], slot_ref, slots_s)
        for n in range(dim // nw):
            ns = slice(n * nw, (n + 1) * nw)
            dng_s[:, ns] = dot_t(dgp_s[...], wg_s[ns, :]).astype(BF)
        start(row_sends(i))

        @pl.when(i < n_layers - 1)
        def _():
            gate_copy(i + 1).start()

        @pl.when(i == 0)
        def _():
            start(gate_sends)
            fetch.wait()

        def block(f, carry):
            step = i * n_blk + f
            slot = lax.rem(step, 2)

            @pl.when(step + 1 < n_steps)
            def _():
                start(load(step + 1, 1 - slot))

            wait(load(step, slot))
            wu_ref, wd_ref, up_ref = wu_s.at[slot], wd_s.at[slot], up_s.at[slot]

            def act(c):
                for g in range(cw // gw):
                    gs = slice(c * cw + g * gw, c * cw + (g + 1) * gw)
                    dup_s[:, gs] = (dh_s[:, gs].astype(F32) * gelu_slope(up_ref[:, gs])).astype(BF)

            n_c = fb // cw
            for c in range(n_c):
                cs = slice(c * cw, (c + 1) * cw)
                dh_s[:, cs] = dot_t(cot_s[...], wd_ref[cs, :]).astype(BF)
                if c > 0:
                    act(c - 1)
            for c in range(n_c):
                cs = slice(c * cw, (c + 1) * cw)
                for n in range(dim // nw):
                    ns = slice(n * nw, (n + 1) * nw)
                    acc_s[:, ns] += dot_t(dup_s[:, cs], wu_ref[ns, cs])
                if c == 0:
                    act(n_c - 1)
            return carry

        lax.fori_loop(0, n_blk, block, 0)
        pltpu.make_async_copy(x1_hbm, x_s, in_sem.at[3]).wait()

        def rows_back(sl):
            x = x_s[sl, :].astype(F32)
            scale = lax.rsqrt(jnp.mean(x * x, axis=-1, keepdims=True) + NORM_EPS)
            d_n = (acc_s[sl, :].astype(BF) + dng_s[sl, :]).astype(F32)
            acc_s[sl, :] = jnp.zeros((slab, dim), F32)
            proj = jnp.mean(d_n * x, axis=-1, keepdims=True)
            d_x = d_n * scale - x * (proj * (scale * scale * scale))
            cot_s[sl, :] = (cot_s[sl, :].astype(F32) + d_x).astype(BF)

        row_loop(tok, slab)(rows_back)
        proj_copy(i).wait()
        d_mixed = dot_t(cot_s[...], wp_s[...]).astype(BF)

        @pl.when(i == n_layers - 1)
        def _():
            dslots_s[...] = dot(slot_pick(n_emb * cap, slot_ref), d_mixed).astype(BF)

        wait(row_sends(i))

        @pl.when(i < n_layers - 1)
        def _():
            proj_copy(i + 1).start()
            gate_grads(gate_ref[jnp.maximum(n_layers - 2 - i, 0)], fet_ref[n_layers - 1 - i], d_mixed.astype(F32), rows_s, dgp_s)

        return carry

    lax.fori_loop(0, n_layers, one_layer, 0)
    start(mixed_sends)
    wait(gate_sends)
    wait(mixed_sends)


def order_rows(recv_ref, counts_ref, slot_bits, read_ref, write_ref, group_ref, meta_ref):
    n_dev, cap = recv_ref.shape
    shape = (n_dev, cap)
    square = (cap, cap)
    dev, lane = lax.broadcasted_iota(I32, shape, 0), lax.broadcasted_iota(I32, shape, 1)
    down, right = lax.broadcasted_iota(I32, square, 0), lax.broadcasted_iota(I32, square, 1)
    counts = counts_ref[:, 0:1]
    key = jnp.where(lane < counts, jnp.left_shift(recv_ref[...], slot_bits), 1 << 30) + dev * cap + lane

    def ones(cond):
        return jnp.where(cond, 1.0, 0.0)

    def digit(k):
        return jnp.bitwise_and(jnp.right_shift(key, 8 * k), 255).astype(F32).astype(BF)

    digits = [digit(k) for k in range(4)]
    same = ones(down == right).astype(BF)
    turned = sum(jnp.left_shift(dot_t(same, d).astype(I32), 8 * k) for k, d in enumerate(digits))
    rows = jnp.concatenate([d[None] for d in digits], axis=0)
    found = [jnp.zeros((8, cap), F32) for _ in range(n_dev)]
    for d in range(n_dev):
        column = turned[:, d:d + 1]
        smaller = sum(ones(key[e:e + 1, :] < column) for e in range(n_dev))
        rank = jnp.sum(smaller, axis=1, keepdims=True)
        mine = jnp.concatenate([rows[k, d:d + 1, :] for k in range(4)] * 2, axis=0)
        for w in range(n_dev):
            found[w] = found[w] + dot(mine, ones(rank - (w * cap) == right.astype(F32)).astype(BF))
    merged = [sum(jnp.left_shift(f[k:k + 1].astype(I32), 8 * k) for k in range(4)) for f in found]
    ordered = jnp.concatenate(merged, axis=0)

    before = pltpu.roll(ordered, 1, 1)
    before = jnp.where(lane == 0, pltpu.roll(before, 1, 0), before)
    after = pltpu.roll(ordered, cap - 1, 1)
    after = jnp.where(lane == cap - 1, pltpu.roll(after, n_dev - 1, 0), after)
    total = jnp.sum(counts_ref[...].astype(F32), axis=0, keepdims=True).astype(I32)
    place_in = dev * cap + lane
    live = place_in < total[:, 0:1]
    slot = jnp.bitwise_and(ordered, (1 << slot_bits) - 1)
    row = jnp.right_shift(ordered, slot_bits)
    group = jnp.right_shift(ordered, slot_bits + 3)
    begin, end = place_in == 0, place_in == n_dev * cap - 1
    same_row = jnp.logical_and(row == jnp.right_shift(before, slot_bits), jnp.logical_not(begin))
    fresh = jnp.logical_or(group != jnp.right_shift(before, slot_bits + 3), begin)
    last = jnp.logical_and(jnp.logical_or(group != jnp.right_shift(after, slot_bits + 3), end), live)
    place = dot(ones(fresh).astype(BF), ones(down <= right).astype(BF)).astype(I32)
    place = place - place[:, 0:1]
    read_ref[...] = jnp.right_shift(slot, 3) * 16 + jnp.bitwise_and(slot, 7) + jnp.where(same_row, -(1 << 31), 0)
    write_ref[...] = place * 16 + jnp.bitwise_and(row, 7)
    group_ref[...] = jnp.where(live, group, 0)
    n_out = jnp.sum(ones(last), axis=1, keepdims=True).astype(I32)
    goes_on = jnp.where(jnp.logical_and(jnp.logical_not(fresh), live), 1, 0)[:, 0:1]
    meta_lane = lax.broadcasted_iota(I32, meta_ref.shape, 1)
    meta = jnp.where(meta_lane == 0, n_out, jnp.where(meta_lane == 1, place[:, cap - 1:cap], goes_on))
    meta_ref[...] = jnp.where(meta_lane == 3, total, meta)


def scatter_kernel(cfg, read_ref, write_ref, group_ref, meta_ref, rows_hbm, gate_hbm, mixed_hbm, dt_in, dt_out,
                   rows_ref, gate_ref, mixed_ref, groups, prod, zero_s, spots, sems, in_sem, z_sem):
    unroll, bulk, z_chunks = cfg
    n_layers, window = groups.shape[1:3]
    n_slots = mixed_ref.shape[0]
    n_win = n_slots // window
    z_rows = zero_s.shape[0]
    count = meta_ref[0, 3]
    loads = [pltpu.make_async_copy(src, dst, in_sem.at[k]) for k, (src, dst) in enumerate(
        ((gate_hbm, gate_ref), (mixed_hbm, mixed_ref), (rows_hbm, rows_ref)))]
    start(loads)
    clear_rows(zero_s)

    def z_copy(c):
        return pltpu.make_async_copy(zero_s, dt_out.at[0, pl.ds(c * z_rows, z_rows)], z_sem.at[c])

    def z_start(c, carry):
        z_copy(c).start()
        return carry

    def z_wait(c, carry):
        z_copy(c).wait()
        return carry

    lax.fori_loop(0, z_chunks, z_start, 0)
    wait(loads[:2])

    def product(i, carry):
        step = 64
        mixed = mixed_ref[pl.ds(pl.multiple_of(i * step, step), step), :].astype(F32)
        for h in range(2):
            at = pl.ds(i * (step // 8), step // 8)
            prod[at, h] = gate_ref[at, h] * mixed[:, h * 128:(h + 1) * 128].reshape(step // 8, 8, 128)
        return carry

    lax.fori_loop(0, n_slots // 64, product, 0, unroll=4)

    def move(buf, spot, group, n):
        return pltpu.make_async_copy(groups.at[buf, :, pl.ds(spot, n)], dt_out.at[:, pl.ds(group, n)], sems.at[buf])

    def each(n, k, body):
        def trip(t, carry):
            for i in range(k):
                body(t * k + i)
            return carry

        def one(i, carry):
            body(i)
            return carry

        full = n // k
        lax.fori_loop(0, full, trip, 0)
        lax.fori_loop(full * k, n, one, 0)

    def settle(w):
        n = meta_ref[w, 0]

        def drain_bulk(j, carry):
            move(w % 2, 0, 0, bulk).wait()
            return carry

        def drain(j, carry):
            move(w % 2, 0, 0, 1).wait()
            return carry

        lax.fori_loop(0, n // bulk, drain_bulk, 0)
        lax.fori_loop(0, lax.rem(n, bulk), drain, 0)

    blank = jnp.zeros(groups.shape[3:], F32)
    accs = tuple(jnp.zeros((2, 128), F32) for _ in range(n_layers))
    z_done = jnp.int32(0)
    for w in range(n_win):
        buf = w % 2
        if w >= 2:
            settle(w - 2)
        left = jnp.clip(count - w * window, 0, window)
        trips = (left + (unroll - 1)) // unroll
        n_out = meta_ref[w, 0]

        def clear(u, buf=buf):
            for l in range(n_layers):
                groups[buf, l, u] = blank

        each(jnp.where(left > 0, jnp.minimum(n_out + 1, window), 0), 4, clear)
        if w == 0:
            wait(loads[2:])
        else:
            @pl.when(meta_ref[w, 2] > 0)
            def _(w=w, buf=buf):
                for l in range(n_layers):
                    groups[buf, l, 0] = groups[1 - buf, l, meta_ref[w - 1, 1]]

        sums = [groups.at[buf, l].reshape(window * 16, 128) for l in range(n_layers)]
        rows = [prod.reshape(n_slots * 2, 128)] + [rows_ref.at[l] for l in range(n_layers - 1)]

        def add(t, accs, w=w, sums=sums, rows=rows):
            for k in range(unroll):
                j = t * unroll + k
                word = read_ref[w, j]
                at = jnp.bitwise_and(word, n_slots * 2 - 1)
                same = word < 0
                to = write_ref[w, j]
                spots[jnp.right_shift(to, 4)] = group_ref[w, j]
                accs = tuple(jnp.where(same, acc, 0.0) + src[pl.ds(at, 2, stride=8), :] for acc, src in zip(accs, rows))
                for acc, dst in zip(accs, sums):
                    dst[pl.ds(to, 2, stride=8), :] = acc
            return accs

        accs = lax.fori_loop(0, trips, add, accs)
        need = jnp.where(n_out > 0, spots[jnp.maximum(n_out - 1, 0)] // z_rows + 1, z_done)
        need = jnp.maximum(need, z_done)
        lax.fori_loop(z_done, need, z_wait, 0)
        z_done = need
        each(n_out, 4, lambda u, buf=buf: move(buf, u, spots[u], 1).start())
    lax.fori_loop(z_done, z_chunks, z_wait, 0)
    for w in range(max(n_win - 2, 0), n_win):
        settle(w)


def solution(mesh):
    n_emb, n_dp = mesh.shape['emb'], mesh.shape['dp']
    n_dev = n_emb * n_dp
    tok_spec = P(('dp', 'emb'))
    act_spec = P(('dp', 'emb'), None)
    table_spec = P(None, 'emb', None)
    full_spec = P(None, None, None)
    hbm = pl.BlockSpec(memory_space=pl.ANY)
    vm = pl.BlockSpec(memory_space=pltpu.VMEM)
    sm = pl.BlockSpec(memory_space=pltpu.SMEM)
    big = jnp.iinfo(jnp.int32).max

    def params(n_grid, **kw):
        return pltpu.CompilerParams(vmem_limit_bytes=VMEM_BYTES, dimension_semantics=('arbitrary',) * n_grid if n_grid else None, **kw)

    def device_body(tok_ids, resid_in, cot_out, tables, w_up, w_down, w_gate, w_proj):
        n_layers, range_rows, e_dim = tables.shape
        tok = tok_ids.shape[0]
        dim, ffn = w_up.shape[1:]
        n_slots, n_serve = n_dev * CAP, n_emb * CAP
        my_emb, my_dp = lax.axis_index('emb'), lax.axis_index('dp')

        lanes = 128
        per_dot, dots = 32, 2
        dma = pltpu.SemaphoreType.DMA
        _, recv_loc, counts, pick, slot_row, slot_col = pl.pallas_call(
            functools.partial(plan_kernel, (n_dp, n_emb, CAP, range_rows, per_dot)),
            out_shape=[jax.ShapeDtypeStruct(shape, I32) for shape in (
                (n_dev, tok // lanes, lanes), (n_dev, CAP), (n_dev, lanes), (n_serve, 1), (1, tok), (tok, 1))],
            in_specs=[vm], out_specs=[vm] * 6,
            scratch_shapes=[pltpu.VMEM((n_dev, tok), F32), dma((n_dev - 1,)), dma((n_dev - 1,))],
            compiler_params=pltpu.CompilerParams(collective_id=0, has_side_effects=True),
            name='plan',
        )(tok_ids.reshape(tok // lanes, lanes))
        slot_bits = (n_slots - 1).bit_length()
        tab_shape = (n_layers, range_rows // 8, e_dim // 128, 8, 128)
        z_rows = 167
        z_chunks = tab_shape[1] // z_rows
        z_first = z_chunks // 2
        words = [jax.ShapeDtypeStruct((n_dev, CAP), I32)] * 3 + [jax.ShapeDtypeStruct((n_dev, lanes), I32)]
        served, dtab, read_word, write_word, group_word, meta = pl.pallas_call(
            functools.partial(gather_kernel, (n_layers, n_emb, CAP, per_dot, dots, z_first, slot_bits)),
            out_shape=[jax.ShapeDtypeStruct((n_layers, n_serve, e_dim), BF), jax.ShapeDtypeStruct(tab_shape, F32)] + words,
            in_specs=[sm, sm, vm, vm, vm, hbm],
            out_specs=[vm, hbm, vm, vm, vm, vm],
            scratch_shapes=[pltpu.VMEM((n_layers, n_serve * 8, e_dim), BF), pltpu.VMEM((z_rows,) + tab_shape[2:], F32), dma((n_emb,)), dma],
            compiler_params=params(0),
            name='table_rows',
        )(recv_loc, counts, recv_loc, counts, pick, tables)

        fb = 1024
        n_blk = ffn // fb
        cw, nw, slab = 512, 512, 16
        n_back = n_layers - 1
        z_pair = 2 * (n_back * z_chunks - z_first) // (n_back * n_blk)
        assert z_chunks * z_rows == tab_shape[1] and z_pair * n_back * n_blk == 2 * (n_back * z_chunks - z_first)
        matmul_flops = 4 * tok * dim * ffn
        w_bufs = [pltpu.VMEM((2, dim, fb), BF), pltpu.VMEM((2, fb, dim), BF), pltpu.VMEM((dim, e_dim), BF), pltpu.VMEM((e_dim, dim), BF)]
        x1, gate0, fetched = pl.pallas_call(
            functools.partial(first_kernel, (n_dp, n_emb, CAP, n_blk, cw, nw, slab)),
            out_shape=[
                jax.ShapeDtypeStruct((tok, dim), BF),
                jax.ShapeDtypeStruct((1, tok, e_dim), F32),
                jax.ShapeDtypeStruct((n_layers, tok, e_dim), BF),
            ],
            in_specs=[hbm, vm, hbm, hbm, hbm, hbm, hbm],
            out_specs=[vm, vm, vm],
            scratch_shapes=[
                pltpu.VMEM((tok, dim), BF), pltpu.VMEM((tok, dim), F32), pltpu.VMEM((tok, fb), BF), pltpu.VMEM((tok, fb), F32),
                pltpu.VMEM((n_layers, n_serve, e_dim), BF), *w_bufs, dma((3,)), dma((2, 2)), dma, dma((n_emb - 1,)), dma((n_emb - 1,)),
            ],
            compiler_params=params(0, collective_id=1, has_side_effects=True),
            cost_estimate=pl.CostEstimate(flops=matmul_flops, bytes_accessed=100 << 20, transcendentals=0),
            name='first_layer',
        )(resid_in, slot_col, served, w_gate, w_proj, w_up, w_down)

        out, saved, ups, gates, rows, dgp, dtab = pl.pallas_call(
            functools.partial(forward_kernel, (n_back, n_blk, cw, nw, slab, z_pair, z_chunks, z_first)),
            out_shape=[
                jax.ShapeDtypeStruct((tok, dim), BF),
                jax.ShapeDtypeStruct((n_back - 1, tok, dim), BF),
                jax.ShapeDtypeStruct((n_back, tok, ffn), F32),
                jax.ShapeDtypeStruct((n_back, tok, e_dim), F32),
                jax.ShapeDtypeStruct((tok, e_dim), F32),
                jax.ShapeDtypeStruct((tok, e_dim), BF),
                jax.ShapeDtypeStruct(tab_shape, F32),
            ],
            in_specs=[hbm, hbm, vm, hbm, hbm, hbm, hbm, hbm],
            out_specs=[hbm, hbm, hbm, vm, vm, vm, hbm],
            input_output_aliases={7: 6},
            scratch_shapes=[
                pltpu.VMEM((tok, dim), BF), pltpu.VMEM((tok, dim), BF), pltpu.VMEM((tok, dim), F32), pltpu.VMEM((tok, fb), BF),
                pltpu.VMEM((2, tok, fb), F32), pltpu.VMEM((z_rows,) + tab_shape[2:], F32), *w_bufs,
                dma((3,)), dma((2, 2)), dma((2,)), dma, dma((z_pair - z_pair // 2,)),
            ],
            compiler_params=params(0),
            cost_estimate=pl.CostEstimate(flops=n_back * matmul_flops, bytes_accessed=400 << 20, transcendentals=0),
            name='forward',
        )(x1, cot_out, fetched, w_gate, w_proj, w_up, w_down, dtab)

        got, got_gate, mixed0 = pl.pallas_call(
            functools.partial(backward_kernel, (n_back, n_blk, n_dp, n_emb, CAP, cw, nw, slab)),
            out_shape=[jax.ShapeDtypeStruct((n_back, n_slots // 8, e_dim // 128, 8, 128), F32), jax.ShapeDtypeStruct((n_slots // 8, e_dim // 128, 8, 128), F32),
                       jax.ShapeDtypeStruct((n_slots, e_dim), BF)],
            in_specs=[hbm, hbm, hbm, vm, vm, vm, vm, vm, vm, hbm, hbm, hbm, hbm, hbm],
            out_specs=[hbm, hbm, hbm],
            scratch_shapes=[
                pltpu.VMEM((tok, dim), BF), pltpu.VMEM((tok, dim), BF), pltpu.VMEM((tok, dim), F32), pltpu.VMEM((tok, fb), BF), pltpu.VMEM((tok, fb), BF),
                pltpu.VMEM((tok, dim), BF), pltpu.VMEM((n_serve // 8, e_dim // 128, 8, 128), F32), pltpu.VMEM((n_serve // 8, e_dim // 128, 8, 128), F32),
                pltpu.VMEM((n_serve, e_dim), BF), pltpu.VMEM((tok, e_dim), F32), pltpu.VMEM((tok, e_dim), BF), pltpu.VMEM((2, tok, fb), F32), *w_bufs,
                dma((4,)), dma((2, 2)), dma((2,)), dma((3, n_dev - 1)), dma((3,)), dma((n_back + 2, n_dev - 1)),
            ],
            compiler_params=params(0, collective_id=2, has_side_effects=True),
            cost_estimate=pl.CostEstimate(flops=n_back * matmul_flops, bytes_accessed=400 << 20, transcendentals=0),
            name='backward',
        )(cot_out, x1, saved, rows, dgp, slot_row, gate0, gates, fetched, ups, w_up, w_down, w_gate, w_proj)

        dtab = pl.pallas_call(
            functools.partial(scatter_kernel, (8, 32, z_chunks)),
            out_shape=jax.ShapeDtypeStruct(dtab.shape, F32),
            in_specs=[sm, sm, sm, sm, hbm, hbm, hbm, hbm],
            out_specs=hbm,
            input_output_aliases={7: 0},
            scratch_shapes=[pltpu.VMEM((n_back, n_slots * 2, 128), F32), pltpu.VMEM((n_slots // 8,) + tab_shape[2:], F32),
                            pltpu.VMEM((n_slots, e_dim), BF), pltpu.VMEM((2, n_layers, CAP) + tab_shape[2:], F32),
                            pltpu.VMEM((n_slots // 8,) + tab_shape[2:], F32), pltpu.VMEM((z_rows,) + tab_shape[2:], F32),
                            pltpu.SMEM((CAP,), I32), dma((2,)), dma((3,)), dma((z_chunks,))],
            compiler_params=params(0),
            name='scatter',
        )(read_word, write_word, group_word, meta, got.reshape(n_back, n_slots * 2, 128), got_gate, mixed0, dtab)
        dtab = dtab.transpose(0, 1, 3, 2, 4).reshape(n_layers, range_rows, e_dim)
        return out, dtab

    return jax.shard_map(device_body, mesh=mesh, in_specs=(tok_spec, act_spec, act_spec, table_spec, full_spec, full_spec, full_spec, full_spec), out_specs=(act_spec, table_spec), check_vma=False)
```

```python
import functools

import jax
import jax.numpy as jnp
from jax import lax
from jax.experimental import pallas as pl
from jax.experimental.pallas import tpu as pltpu
from jax.sharding import PartitionSpec as P

NORM_EPS = 1e-6
BF = jnp.bfloat16
F32 = jnp.float32
I32 = jnp.int32
VMEM_BYTES = 67043328
GELU_C = 0.7978845608028654
GELU_A = 0.044715

MESH_AXES = ('dp', 'emb')
CAP = 256


def gelu(x):
    return 0.5 * x * (1.0 + jnp.tanh(GELU_C * (x + GELU_A * (x * x * x))))


def gelu_slope(x):
    sq = x * x
    th = jnp.tanh(GELU_C * (x + GELU_A * (x * sq)))
    return 0.5 * (1.0 + th) + (0.5 * GELU_C) * x * (1.0 - th * th) * (1.0 + (3 * GELU_A) * sq)


def dot(a, b):
    return jnp.dot(a, b, preferred_element_type=F32)


def dot_t(a, b):
    return lax.dot_general(a, b, (((1,), (1,)), ((), ())), preferred_element_type=F32)


def row_loop(rows, slab, unroll=1):
    def run(body):
        def step(i, carry):
            body(pl.ds(pl.multiple_of(i * slab, slab), slab))
            return carry

        lax.fori_loop(0, rows // slab, step, 0, unroll=unroll)

    return run


def peer_of(n_emb, index):
    dp = index // n_emb
    return {'dp': dp, 'emb': index - dp * n_emb}


def remote(src, dst, send_sem, recv_sem, device):
    return pltpu.make_async_remote_copy(src_ref=src, dst_ref=dst, send_sem=send_sem, recv_sem=recv_sem,
                                        device_id=device, device_id_type=pl.DeviceIdType.MESH)


def meet(devices):
    barrier = pltpu.get_barrier_semaphore()
    for device in devices:
        pl.semaphore_signal(barrier, inc=1, device_id=device, device_id_type=pl.DeviceIdType.MESH)
    pl.semaphore_wait(barrier, len(devices))


def plan_kernel(cfg, in_ref, ids_ref, recv_ref, counts_ref, pick_ref, slot_row_ref, slot_col_ref, rank_s, send_sem, recv_sem):
    n_dp, n_emb, cap, range_rows, per_dot = cfg
    n_dev = n_dp * n_emb
    my_dp, my_emb = lax.axis_index('dp'), lax.axis_index('emb')
    me = my_dp * n_emb + my_emb
    n_sub, lanes = in_ref.shape
    tok = n_sub * lanes
    peers = [peer_of(n_emb, lax.rem(me + k, n_dev)) for k in range(1, n_dev)]
    meet(peers)
    copies = [remote(in_ref, ids_ref.at[me], send_sem.at[k], recv_sem.at[k], peer) for k, peer in enumerate(peers)]
    start(copies)
    ids_ref[me] = in_ref[...]

    def line(ref):
        return jnp.concatenate([ref[..., j, :] for j in range(n_sub)], axis=-1)

    def ones(cond):
        return jnp.where(cond, 1.0, 0.0)

    def digits(x):
        return jnp.concatenate([jnp.right_shift(x, 8), jnp.bitwise_and(x, 255)], axis=0).astype(F32).astype(BF)

    square = (tok, tok)
    down, right = lax.broadcasted_iota(I32, square, 0), lax.broadcasted_iota(I32, square, 1)
    earlier = ones(down < right).astype(BF)
    own = jnp.broadcast_to(jnp.concatenate([in_ref[j:j + 1, :] for j in range(n_sub)], axis=-1), (8, tok))
    owner = sum(jnp.where(own >= e * range_rows, 1, 0) for e in range(1, n_emb))
    is_owner = owner == lax.broadcasted_iota(I32, (8, tok), 0)
    own_rank = dot(ones(is_owner).astype(BF), earlier).astype(I32)
    slot_row = jnp.sum(jnp.where(is_owner, own_rank + owner * cap, 0).astype(F32), axis=0, keepdims=True).astype(I32)
    slot_row_ref[...] = slot_row
    turned = dot_t(ones(down == right).astype(BF), digits(jnp.broadcast_to(slot_row, (8, tok))))
    slot_col_ref[...] = (turned[:, 0:1] * 256.0 + turned[:, 8:9]).astype(I32)

    wait(copies)
    ids8 = line(ids_ref)
    low = my_emb * range_rows
    mine = jnp.logical_and(ids8 >= low, ids8 < low + range_rows)
    mine_f = ones(mine)
    rank_s[...] = jnp.where(mine, dot(mine_f.astype(BF), earlier), -1.0)
    counts = jnp.sum(mine_f, axis=1, keepdims=True).astype(I32)
    counts_ref[...] = jnp.broadcast_to(counts, counts_ref.shape)
    loc = digits(jnp.where(mine, ids8 - low, 0))
    c_iota = lax.broadcasted_iota(I32, (cap, tok), 0).astype(F32)
    dev_iota = lax.broadcasted_iota(I32, (n_dev, cap), 0)
    recv = jnp.zeros((n_dev, cap), F32)
    for d in range(n_dev):
        found = dot_t(loc, ones(rank_s[d:d + 1, :] == c_iota).astype(BF))
        recv = jnp.where(dev_iota == d, found[:n_dev] * 256.0 + found[n_dev:], recv)
    slot = dev_iota * cap + lax.broadcasted_iota(I32, (n_dev, cap), 1)
    recv_ref[...] = jnp.where(slot - dev_iota * cap < counts, recv.astype(I32), slot * 8)
    lane16 = lax.broadcasted_iota(I32, (cap, 2 * n_dev), 1)
    row1 = lax.broadcasted_iota(I32, (cap, 1), 0)
    for e in range(n_emb):
        d = my_dp * n_emb + e
        found = dot_t(ones(rank_s[pl.ds(d, 1), :] == c_iota).astype(BF), loc)
        low8 = jnp.sum(jnp.where(lane16 == n_dev + d, found, 0.0), axis=1, keepdims=True).astype(I32)
        pick_ref[e * cap:(e + 1) * cap, :] = jnp.bitwise_and(low8, 7) + 8 * jnp.bitwise_and(row1, per_dot - 1)


def gather_kernel(cfg, loc_ref, counts_ref, recv_ref, tally_ref, pick_ref, tables_hbm,
                  out_ref, dtab_hbm, read_ref, write_ref, group_ref, meta_ref, buf, zero_s, sems, z_sem):
    n_layers, n_dest, cap, per_dot, group, z_chunks, slot_bits = cfg
    trip = per_dot * group
    z_rows = zero_s.shape[0]
    first = lax.axis_index('dp') * n_dest
    n_trips = [(counts_ref[first + d, 0] + (trip - 1)) // trip for d in range(n_dest)]

    def row_copy(d, c):
        base = pl.multiple_of(jnp.left_shift(jnp.right_shift(loc_ref[first + d, c], 3), 3), 8)
        at = pl.multiple_of(d * cap * 8 + c * 8, 8)
        return pltpu.make_async_copy(tables_hbm.at[:, pl.ds(base, 8), :], buf.at[:, pl.ds(at, 8), :], sems.at[d])

    def z_copy(c):
        return pltpu.make_async_copy(zero_s, dtab_hbm.at[0, pl.ds(c * z_rows, z_rows)], z_sem)

    for d in range(n_dest):
        def issue(i, carry, d=d):
            for k in range(8):
                row_copy(d, i * 8 + k).start()
            return carry

        lax.fori_loop(0, n_trips[d] * (trip // 8), issue, 0)

    clear_rows(zero_s)

    def z_start(c, carry):
        z_copy(c).start(priority=1)
        return carry

    lax.fori_loop(0, z_chunks, z_start, 0)
    order_rows(recv_ref, tally_ref, slot_bits, read_ref, write_ref, group_ref, meta_ref)
    for d in range(n_dest):
        def drain(i, carry, d=d):
            part = buf.at[:, pl.ds(pl.multiple_of((d * cap + i * trip) * 8, 8), trip * 8), :]
            pltpu.make_async_copy(part, part, sems.at[d]).wait()
            return carry

        lax.fori_loop(0, n_trips[d], drain, 0)

        def pick(i, carry, d=d):
            for k in range(group):
                s0 = pl.multiple_of(d * cap + i * trip + k * per_dot, per_dot)
                want = pick_ref[pl.ds(s0, per_dot), :]
                sel = (lax.broadcasted_iota(I32, (per_dot, per_dot * 8), 1) == want).astype(BF)
                for l in range(n_layers):
                    rows = buf[l, pl.ds(pl.multiple_of(s0 * 8, 8), per_dot * 8), :]
                    out_ref[l, pl.ds(s0, per_dot), :] = dot(sel, rows).astype(BF)
            return carry

        lax.fori_loop(0, n_trips[d], pick, 0)

        def blank(i, carry, d=d):
            s0 = pl.multiple_of(d * cap + i * trip, trip)
            for l in range(n_layers):
                out_ref[l, pl.ds(s0, trip), :] = jnp.zeros((trip, out_ref.shape[2]), BF)
            return carry

        lax.fori_loop(n_trips[d], cap // trip, blank, 0)

    def z_wait(c, carry):
        z_copy(c).wait()
        return carry

    lax.fori_loop(0, z_chunks, z_wait, 0)


def clear_rows(ref):
    def clear(i, carry):
        ref[i] = jnp.zeros(ref.shape[1:], F32)
        return carry

    lax.fori_loop(0, ref.shape[0], clear, 0)


def weight_copies(wu_hbm, wd_hbm, wu_s, wd_s, sems):
    fb = wu_s.shape[2]

    def copies(layer, blk, slot):
        at = pl.multiple_of(blk * fb, fb)
        return (pltpu.make_async_copy(wu_hbm.at[layer, :, pl.ds(at, fb)], wu_s.at[slot], sems.at[0, slot]),
                pltpu.make_async_copy(wd_hbm.at[layer, pl.ds(at, fb), :], wd_s.at[slot], sems.at[1, slot]))

    return copies


def start(copies):
    for copy in copies:
        copy.start()


def wait(copies):
    for copy in copies:
        copy.wait()


def mlp_block(cfg, u_s, h_s, acc_s, wu_ref, wd_ref, up_ref, second=None):
    cw, nw = cfg
    gw = 128
    n_c = wu_ref.shape[1] // cw

    def act(c):
        for g in range(cw // gw):
            gs = slice(c * cw + g * gw, c * cw + (g + 1) * gw)
            h_s[:, gs] = gelu(up_ref[:, gs]).astype(BF)

    for c in range(n_c):
        cs = slice(c * cw, (c + 1) * cw)
        up_ref[:, cs] = dot(u_s[...], wu_ref[:, cs])
        if c > 0:
            act(c - 1)
    if second is not None:
        second.wait()
    for c in range(n_c):
        cs = slice(c * cw, (c + 1) * cw)
        for n in range(acc_s.shape[1] // nw):
            ns = slice(n * nw, (n + 1) * nw)
            acc_s[:, ns] += dot(h_s[:, cs], wd_ref[cs, ns])
        if c == 0:
            act(n_c - 1)


def norm_rows(x, sl, u_s, acc_s, scale_ref=None):
    scale = lax.rsqrt(jnp.mean(x * x, axis=-1, keepdims=True) + NORM_EPS)
    u_s[sl, :] = (x * scale).astype(BF)
    acc_s[sl, :] = x
    if scale_ref is not None:
        scale_ref[sl, :] = jnp.broadcast_to(scale, (scale.shape[0], scale_ref.shape[1]))


def add_proj(nw, acc_s, mixed, wp_ref):
    for n in range(acc_s.shape[1] // nw):
        ns = slice(n * nw, (n + 1) * nw)
        acc_s[:, ns] += dot(mixed, wp_ref[:, ns])


def first_kernel(cfg, x_hbm, slot_ref, served_hbm, wg_hbm, wp_hbm, wu_hbm, wd_hbm,
                 x_out_ref, gate_ref, fet_ref,
                 u_s, acc_s, h_s, up_s, ret_s, wu_s, wd_s, wg_s, wp_s, in_sem, w_sem, self_sem, send_sem, recv_sem):
    n_dp, n_emb, cap, n_blk, cw, nw, slab = cfg
    tok, dim = u_s.shape
    my_emb = lax.axis_index('emb')
    my_dp = lax.axis_index('dp')
    here = ret_s.at[:, pl.ds(pl.multiple_of(my_emb * cap, cap), cap), :]
    own = pltpu.make_async_copy(served_hbm.at[:, pl.ds(pl.multiple_of(my_emb * cap, cap), cap), :], here, self_sem)
    peers = [lax.rem(my_emb + k, n_emb) for k in range(1, n_emb)]
    copies = [remote(served_hbm.at[:, pl.ds(pl.multiple_of(p * cap, cap), cap), :], here,
                     send_sem.at[k], recv_sem.at[k], {'dp': my_dp, 'emb': p}) for k, p in enumerate(peers)]
    weights = weight_copies(wu_hbm, wd_hbm, wu_s, wd_s, w_sem)
    first = [pltpu.make_async_copy(x_hbm, x_out_ref, in_sem.at[0]),
             pltpu.make_async_copy(wg_hbm.at[0], wg_s, in_sem.at[1]),
             pltpu.make_async_copy(wp_hbm.at[0], wp_s, in_sem.at[2])]
    start(first[:2])
    start(weights(0, 0, 0))
    start(first[2:])
    meet([{'dp': my_dp, 'emb': p} for p in peers])
    own.start()
    start(copies)
    first[0].wait()
    row_loop(tok, slab)(lambda sl: norm_rows(x_out_ref[sl, :].astype(F32), sl, u_s, acc_s))
    first[1].wait()
    gate_ref[0] = dot(u_s[...], wg_s[...])

    def block(f, carry):
        slot = lax.rem(f, 2)

        @pl.when(f + 1 < n_blk)
        def _():
            start(weights(0, f + 1, 1 - slot))

        up_w, down_w = weights(0, f, slot)
        up_w.wait()
        mlp_block((cw, nw), u_s, h_s, acc_s, wu_s.at[slot], wd_s.at[slot], up_s, down_w)
        return carry

    lax.fori_loop(0, n_blk, block, 0)
    own.wait()
    wait(copies)
    first[2].wait()
    sel = (lax.broadcasted_iota(I32, (tok, n_emb * cap), 1) == slot_ref[...]).astype(BF)
    for l in range(fet_ref.shape[0]):
        fet_ref[l] = dot(sel, ret_s[l]).astype(BF)
    add_proj(nw, acc_s, (gelu(gate_ref[0]) * fet_ref[0].astype(F32)).astype(BF), wp_s)

    def finish(sl):
        x_out_ref[sl, :] = acc_s[sl, :].astype(BF)

    row_loop(tok, slab)(finish)


def forward_kernel(cfg, x_hbm, cot_hbm, fet_ref, wg_hbm, wp_hbm, wu_hbm, wd_hbm, dt_in,
                   out_hbm, saved_hbm, ups_hbm, gate_ref, rows_ref, dgp_ref, dtab_hbm, scale_ref,
                   x_s, u_s, acc_s, h_s, up_s, zero_s, wu_s, wd_s, wg_s, wp_s, in_sem, w_sem, up_sem, out_sem, z_sem):
    n_layers, n_blk, cw, nw, slab, z_per, z_chunks = cfg
    tok, dim = x_s.shape
    fb = wu_s.shape[2]
    z_rows = zero_s.shape[0]
    n_steps = n_layers * n_blk
    weights = weight_copies(wu_hbm, wd_hbm, wu_s, wd_s, w_sem)

    def z_copies(step):
        found = []
        for j in range(z_per):
            c = step * z_per + j
            zl = c // z_chunks
            found.append(pltpu.make_async_copy(zero_s, dtab_hbm.at[zl + 1, pl.ds((c - zl * z_chunks) * z_rows, z_rows)], z_sem.at[j]))
        return found

    def up_copy(layer, blk, slot):
        return pltpu.make_async_copy(up_s.at[slot], ups_hbm.at[layer, :, pl.ds(pl.multiple_of(blk * fb, fb), fb)], up_sem.at[slot])

    def gate_copy(layer):
        return pltpu.make_async_copy(wg_hbm.at[layer + 1], wg_s, in_sem.at[1])

    def proj_copy(layer):
        return pltpu.make_async_copy(wp_hbm.at[layer + 1], wp_s, in_sem.at[2])

    fetch = pltpu.make_async_copy(x_hbm, x_s, in_sem.at[0])
    fetch.start()
    gate_copy(0).start()
    start(weights(1, 0, 0))
    proj_copy(0).start()
    clear_rows(zero_s)
    fetch.wait()
    row_loop(tok, slab)(lambda sl: norm_rows(x_s[sl, :].astype(F32), sl, u_s, acc_s, scale_ref.at[0]))

    def one_layer(layer, carry):
        gate_copy(layer).wait()
        gate_ref[layer] = dot(u_s[...], wg_s[...])

        @pl.when(layer + 1 < n_layers)
        def _():
            gate_copy(layer + 1).start()

        def block(f, carry):
            step = layer * n_blk + f
            slot = lax.rem(step, 2)

            @pl.when(step + 1 < n_steps)
            def _():
                nxt = step + 1
                start(weights(1 + nxt // n_blk, lax.rem(nxt, n_blk), 1 - slot))

            @pl.when(step > 0)
            def _():
                wait(z_copies(step - 1))

            for copy in z_copies(step):
                copy.start(priority=1)

            @pl.when(step > 1)
            def _():
                up_copy(layer, f, slot).wait()

            wait(weights(1 + layer, f, slot))
            mlp_block((cw, nw), u_s, h_s, acc_s, wu_s.at[slot], wd_s.at[slot], up_s.at[slot])
            up_copy(layer, f, slot).start()
            return carry

        lax.fori_loop(0, n_blk, block, 0)
        proj_copy(layer).wait()
        add_proj(nw, acc_s, (gelu(gate_ref[layer]) * fet_ref[layer + 1].astype(F32)).astype(BF), wp_s)

        @pl.when(layer > 0)
        def _():
            pltpu.make_async_copy(x_s, saved_hbm.at[layer - 1], out_sem).wait()

        def next_rows(sl):
            x_new = acc_s[sl, :].astype(BF)
            x_s[sl, :] = x_new
            norm_rows(x_new.astype(F32), sl, u_s, acc_s, scale_ref.at[jnp.minimum(layer + 1, n_layers - 1)])

        def last_rows(sl):
            x_s[sl, :] = acc_s[sl, :].astype(BF)

        @pl.when(layer < n_layers - 1)
        def _():
            row_loop(tok, slab)(next_rows)

        @pl.when(layer == n_layers - 1)
        def _():
            row_loop(tok, slab)(last_rows)

        @pl.when(layer < n_layers - 1)
        def _():
            pltpu.make_async_copy(x_s, saved_hbm.at[layer], out_sem).start()
            proj_copy(layer + 1).start()

        return carry

    lax.fori_loop(0, n_layers, one_layer, 0)
    put = pltpu.make_async_copy(x_s, out_hbm, out_sem)
    put.start()
    get = pltpu.make_async_copy(cot_hbm, u_s, in_sem.at[0])
    get.start()
    wait(z_copies(n_steps - 1))
    up_copy(0, 0, 0).wait()
    up_copy(0, 0, 1).wait()
    get.wait()
    d_mixed = dot_t(u_s[...], wp_s[...]).astype(BF).astype(F32)
    gate_grads(gate_ref[n_layers - 1], fet_ref[n_layers], d_mixed, rows_ref, dgp_ref)
    put.wait()


def gate_grads(gate_pre, fetched, d_mixed, rows_ref, dgp_ref):
    rows_ref[...] = gelu(gate_pre) * d_mixed
    dgp_ref[...] = (d_mixed * fetched.astype(F32) * gelu_slope(gate_pre)).astype(BF)


def to_slots(rows, slot_ref, slots_s):
    hi = rows.astype(BF)
    rest = rows - hi.astype(F32)
    mid = rest.astype(BF)
    low = (rest - mid.astype(F32)).astype(BF)
    n = slots_s.shape[0] * slots_s.shape[2]
    sel = slot_pick(n, slot_ref)
    slots = (dot(sel, hi) + dot(sel, mid)) + dot(sel, low)
    for h in range(slots_s.shape[1]):
        slots_s[:, h] = slots[:, h * 128:(h + 1) * 128].reshape(n // 8, 8, 128)


def slot_pick(n, slot_ref):
    return (lax.broadcasted_iota(I32, (n, slot_ref.shape[1]), 0) == slot_ref[...]).astype(BF)


def backward_kernel(cfg, cot_hbm, x1_hbm, saved_hbm, rows_in_ref, dgp_in_ref, slot_ref, gate0_ref, gate_ref, fet_ref, scale_ref,
                    ups_hbm, wu_hbm, wd_hbm, wg_hbm, wp_hbm,
                    got_hbm, gate_hbm, mixed_hbm,
                    cot_s, x_s, acc_s, dup_s, dh_s, dng_s, slots_s, gslots_s, dslots_s, rows_s, dgp_s, up_s, wu_s, wd_s, wg_s, wp_s,
                    in_sem, w_sem, up_sem, send_sem, self_sem, recv_sem):
    n_layers, n_blk, n_dp, n_emb, cap, cw, nw, slab = cfg
    tok, dim = cot_s.shape
    fb = wu_s.shape[2]
    gw = 128
    n_dev = n_dp * n_emb
    n_steps = n_layers * n_blk
    my_emb = lax.axis_index('emb')
    me = lax.axis_index('dp') * n_emb + my_emb
    peers = [peer_of(n_emb, lax.rem(me + k, n_dev)) for k in range(1, n_dev)]
    weights = weight_copies(wu_hbm, wd_hbm, wu_s, wd_s, w_sem)

    def part(ref, emb):
        return ref.at[pl.ds(emb * (cap // 8), cap // 8)]

    def sends(ref, there, which, got):
        return [pltpu.make_async_copy(part(ref, my_emb), there, self_sem.at[which])] + [
            remote(part(ref, peer['emb']), there, send_sem.at[which, k], recv_sem.at[got, k], peer) for k, peer in enumerate(peers)]

    def row_sends(i):
        return sends(slots_s, part(got_hbm.at[n_layers - 1 - i], me), 0, i)

    gate_sends = sends(gslots_s, part(gate_hbm, me), 1, n_layers)

    def flat(ref, dev):
        return ref.at[pl.ds(pl.multiple_of(dev * cap, cap), cap), :]

    mixed_sends = [pltpu.make_async_copy(flat(dslots_s, my_emb), flat(mixed_hbm, me), self_sem.at[2])] + [
        remote(flat(dslots_s, peer['emb']), flat(mixed_hbm, me), send_sem.at[2, k], recv_sem.at[n_layers + 1, k], peer)
        for k, peer in enumerate(peers)]

    def up_copy(step, slot):
        i = step // n_blk
        blk = step - i * n_blk
        return pltpu.make_async_copy(ups_hbm.at[n_layers - 1 - i, :, pl.ds(pl.multiple_of(blk * fb, fb), fb)], up_s.at[slot], up_sem.at[slot])

    def load(step, slot):
        i = step // n_blk
        return weights(n_layers - i, step - i * n_blk, slot) + (up_copy(step, slot),)

    def gate_copy(i):
        return pltpu.make_async_copy(wg_hbm.at[n_layers - i], wg_s, in_sem.at[1])

    def proj_copy(i):
        return pltpu.make_async_copy(wp_hbm.at[n_layers - 1 - i], wp_s, in_sem.at[2])

    def x_copy(i):
        return pltpu.make_async_copy(saved_hbm.at[n_layers - 2 - i], x_s, in_sem.at[3])

    fetch = pltpu.make_async_copy(cot_hbm, cot_s, in_sem.at[0])
    gate_copy(0).start()
    fetch.start()
    start(load(0, 0))
    proj_copy(0).start()
    rows_s[...] = rows_in_ref[...]
    dgp_s[...] = dgp_in_ref[...]

    def clear(sl):
        acc_s[sl, :] = jnp.zeros((slab, dim), F32)

    row_loop(tok, slab)(clear)
    meet(peers)
    to_slots(gelu(gate0_ref[0]), slot_ref, gslots_s)

    def one_layer(i, carry):
        @pl.when(i < n_layers - 1)
        def _():
            x_copy(i).start()

        @pl.when(i == n_layers - 1)
        def _():
            pltpu.make_async_copy(x1_hbm, x_s, in_sem.at[3]).start()

        gate_copy(i).wait()
        to_slots(rows_s[...], slot_ref, slots_s)
        for n in range(dim // nw):
            ns = slice(n * nw, (n + 1) * nw)
            dng_s[:, ns] = dot_t(dgp_s[...], wg_s[ns, :]).astype(BF)
        start(row_sends(i))

        @pl.when(i < n_layers - 1)
        def _():
            gate_copy(i + 1).start()

        @pl.when(i == 0)
        def _():
            start(gate_sends)
            fetch.wait()

        def block(f, carry):
            step = i * n_blk + f
            slot = lax.rem(step, 2)

            @pl.when(step + 1 < n_steps)
            def _():
                start(load(step + 1, 1 - slot))

            wait(load(step, slot))
            wu_ref, wd_ref, up_ref = wu_s.at[slot], wd_s.at[slot], up_s.at[slot]

            def act(c):
                for g in range(cw // gw):
                    gs = slice(c * cw + g * gw, c * cw + (g + 1) * gw)
                    dup_s[:, gs] = (dh_s[:, gs].astype(F32) * gelu_slope(up_ref[:, gs])).astype(BF)

            n_c = fb // cw
            for c in range(n_c):
                cs = slice(c * cw, (c + 1) * cw)
                dh_s[:, cs] = dot_t(cot_s[...], wd_ref[cs, :]).astype(BF)
                if c > 0:
                    act(c - 1)
            for c in range(n_c):
                cs = slice(c * cw, (c + 1) * cw)
                for n in range(dim // nw):
                    ns = slice(n * nw, (n + 1) * nw)
                    acc_s[:, ns] += dot_t(dup_s[:, cs], wu_ref[ns, cs])
                if c == 0:
                    act(n_c - 1)
            return carry

        lax.fori_loop(0, n_blk, block, 0)
        pltpu.make_async_copy(x1_hbm, x_s, in_sem.at[3]).wait()

        def rows_back(sl):
            x = x_s[sl, :].astype(F32)
            scale = scale_ref[n_layers - 1 - i, sl, 0:1]
            d_n = (acc_s[sl, :].astype(BF) + dng_s[sl, :]).astype(F32)
            acc_s[sl, :] = jnp.zeros((slab, dim), F32)
            proj = jnp.mean(d_n * x, axis=-1, keepdims=True)
            d_x = d_n * scale - x * (proj * (scale * scale * scale))
            cot_s[sl, :] = (cot_s[sl, :].astype(F32) + d_x).astype(BF)

        row_loop(tok, slab)(rows_back)
        proj_copy(i).wait()
        d_mixed = dot_t(cot_s[...], wp_s[...]).astype(BF)

        @pl.when(i == n_layers - 1)
        def _():
            dslots_s[...] = dot(slot_pick(n_emb * cap, slot_ref), d_mixed).astype(BF)

        wait(row_sends(i))

        @pl.when(i < n_layers - 1)
        def _():
            proj_copy(i + 1).start()
            gate_grads(gate_ref[jnp.maximum(n_layers - 2 - i, 0)], fet_ref[n_layers - 1 - i], d_mixed.astype(F32), rows_s, dgp_s)

        return carry

    lax.fori_loop(0, n_layers, one_layer, 0)
    start(mixed_sends)
    wait(gate_sends)
    wait(mixed_sends)


def order_rows(recv_ref, counts_ref, slot_bits, read_ref, write_ref, group_ref, meta_ref):
    n_dev, cap = recv_ref.shape
    shape = (n_dev, cap)
    square = (cap, cap)
    dev, lane = lax.broadcasted_iota(I32, shape, 0), lax.broadcasted_iota(I32, shape, 1)
    down, right = lax.broadcasted_iota(I32, square, 0), lax.broadcasted_iota(I32, square, 1)
    counts = counts_ref[:, 0:1]
    key = jnp.where(lane < counts, jnp.left_shift(recv_ref[...], slot_bits), 1 << 30) + dev * cap + lane

    def ones(cond):
        return jnp.where(cond, 1.0, 0.0)

    def digit(k):
        return jnp.bitwise_and(jnp.right_shift(key, 8 * k), 255).astype(F32).astype(BF)

    digits = [digit(k) for k in range(4)]
    same = ones(down == right).astype(BF)
    turned = sum(jnp.left_shift(dot_t(same, d).astype(I32), 8 * k) for k, d in enumerate(digits))
    rows = jnp.concatenate([d[None] for d in digits], axis=0)
    found = [jnp.zeros((8, cap), F32) for _ in range(n_dev)]
    for d in range(n_dev):
        column = turned[:, d:d + 1]
        smaller = sum(ones(key[e:e + 1, :] < column) for e in range(n_dev))
        rank = jnp.sum(smaller, axis=1, keepdims=True)
        mine = jnp.concatenate([rows[k, d:d + 1, :] for k in range(4)] * 2, axis=0)
        for w in range(n_dev):
            found[w] = found[w] + dot(mine, ones(rank - (w * cap) == right.astype(F32)).astype(BF))
    merged = [sum(jnp.left_shift(f[k:k + 1].astype(I32), 8 * k) for k in range(4)) for f in found]
    ordered = jnp.concatenate(merged, axis=0)

    before = pltpu.roll(ordered, 1, 1)
    before = jnp.where(lane == 0, pltpu.roll(before, 1, 0), before)
    after = pltpu.roll(ordered, cap - 1, 1)
    after = jnp.where(lane == cap - 1, pltpu.roll(after, n_dev - 1, 0), after)
    total = jnp.sum(counts_ref[...].astype(F32), axis=0, keepdims=True).astype(I32)
    place_in = dev * cap + lane
    live = place_in < total[:, 0:1]
    slot = jnp.bitwise_and(ordered, (1 << slot_bits) - 1)
    row = jnp.right_shift(ordered, slot_bits)
    group = jnp.right_shift(ordered, slot_bits + 3)
    begin, end = place_in == 0, place_in == n_dev * cap - 1
    same_row = jnp.logical_and(row == jnp.right_shift(before, slot_bits), jnp.logical_not(begin))
    fresh = jnp.logical_or(group != jnp.right_shift(before, slot_bits + 3), begin)
    last = jnp.logical_and(jnp.logical_or(group != jnp.right_shift(after, slot_bits + 3), end), live)
    place = dot(ones(fresh).astype(BF), ones(down <= right).astype(BF)).astype(I32)
    place = place - place[:, 0:1]
    read_ref[...] = jnp.right_shift(slot, 3) * 16 + jnp.bitwise_and(slot, 7) + jnp.where(same_row, -(1 << 31), 0)
    write_ref[...] = place * 16 + jnp.bitwise_and(row, 7)
    group_ref[...] = jnp.where(live, group, 0)
    n_out = jnp.sum(ones(last), axis=1, keepdims=True).astype(I32)
    goes_on = jnp.where(jnp.logical_and(jnp.logical_not(fresh), live), 1, 0)[:, 0:1]
    meta_lane = lax.broadcasted_iota(I32, meta_ref.shape, 1)
    meta = jnp.where(meta_lane == 0, n_out, jnp.where(meta_lane == 1, place[:, cap - 1:cap], goes_on))
    meta_ref[...] = jnp.where(meta_lane == 3, total, meta)


def scatter_kernel(cfg, read_ref, write_ref, group_ref, meta_ref, rows_hbm, gate_hbm, mixed_hbm, dt_in, dt_out,
                   rows_ref, gate_ref, mixed_ref, groups, prod, zero_s, spots, sems, in_sem, z_sem):
    unroll, bulk, z_first, z_chunks = cfg
    n_layers, window = groups.shape[1:3]
    n_slots = mixed_ref.shape[0]
    n_win = n_slots // window
    z_rows = zero_s.shape[0]
    count = meta_ref[0, 3]
    loads = [pltpu.make_async_copy(src, dst, in_sem.at[k]) for k, (src, dst) in enumerate(
        ((gate_hbm, gate_ref), (mixed_hbm, mixed_ref), (rows_hbm, rows_ref)))]
    start(loads)
    clear_rows(zero_s)

    def z_copy(c):
        return pltpu.make_async_copy(zero_s, dt_out.at[0, pl.ds(c * z_rows, z_rows)], z_sem.at[c])

    def z_start(c, carry):
        z_copy(c).start()
        return carry

    def z_wait(c, carry):
        z_copy(c).wait()
        return carry

    lax.fori_loop(z_first, z_chunks, z_start, 0)
    wait(loads[:2])

    def product(i, carry):
        step = 64
        mixed = mixed_ref[pl.ds(pl.multiple_of(i * step, step), step), :].astype(F32)
        for h in range(2):
            at = pl.ds(i * (step // 8), step // 8)
            prod[at, h] = gate_ref[at, h] * mixed[:, h * 128:(h + 1) * 128].reshape(step // 8, 8, 128)
        return carry

    lax.fori_loop(0, n_slots // 64, product, 0, unroll=4)

    def move(buf, spot, group, n):
        return pltpu.make_async_copy(groups.at[buf, :, pl.ds(spot, n)], dt_out.at[:, pl.ds(group, n)], sems.at[buf])

    def each(n, k, body):
        def trip(t, carry):
            for i in range(k):
                body(t * k + i)
            return carry

        def one(i, carry):
            body(i)
            return carry

        full = n // k
        lax.fori_loop(0, full, trip, 0)
        lax.fori_loop(full * k, n, one, 0)

    def settle(w):
        n = meta_ref[w, 0]

        def drain_bulk(j, carry):
            move(w % 2, 0, 0, bulk).wait()
            return carry

        def drain(j, carry):
            move(w % 2, 0, 0, 1).wait()
            return carry

        lax.fori_loop(0, n // bulk, drain_bulk, 0)
        lax.fori_loop(0, lax.rem(n, bulk), drain, 0)

    blank = jnp.zeros(groups.shape[3:], F32)
    accs = tuple(jnp.zeros((2, 128), F32) for _ in range(n_layers))
    z_done = jnp.int32(z_first)
    for w in range(n_win):
        buf = w % 2
        if w >= 2:
            settle(w - 2)
        left = jnp.clip(count - w * window, 0, window)
        trips = (left + (unroll - 1)) // unroll
        n_out = meta_ref[w, 0]

        def clear(u, buf=buf):
            for l in range(n_layers):
                groups[buf, l, u] = blank

        each(jnp.where(left > 0, jnp.minimum(n_out + 1, window), 0), 4, clear)
        if w == 0:
            wait(loads[2:])
        else:
            @pl.when(meta_ref[w, 2] > 0)
            def _(w=w, buf=buf):
                for l in range(n_layers):
                    groups[buf, l, 0] = groups[1 - buf, l, meta_ref[w - 1, 1]]

        sums = [groups.at[buf, l].reshape(window * 16, 128) for l in range(n_layers)]
        rows = [prod.reshape(n_slots * 2, 128)] + [rows_ref.at[l] for l in range(n_layers - 1)]

        def add(t, accs, w=w, sums=sums, rows=rows):
            for k in range(unroll):
                j = t * unroll + k
                word = read_ref[w, j]
                at = jnp.bitwise_and(word, n_slots * 2 - 1)
                same = word < 0
                to = write_ref[w, j]
                spots[jnp.right_shift(to, 4)] = group_ref[w, j]
                accs = tuple(jnp.where(same, acc, 0.0) + src[pl.ds(at, 2, stride=8), :] for acc, src in zip(accs, rows))
                for acc, dst in zip(accs, sums):
                    dst[pl.ds(to, 2, stride=8), :] = acc
            return accs

        accs = lax.fori_loop(0, trips, add, accs)
        need = jnp.where(n_out > 0, spots[jnp.maximum(n_out - 1, 0)] // z_rows + 1, z_done)
        need = jnp.maximum(need, z_done)
        lax.fori_loop(z_done, need, z_wait, 0)
        z_done = need
        each(n_out, 4, lambda u, buf=buf: move(buf, u, spots[u], 1).start())
    lax.fori_loop(z_done, z_chunks, z_wait, 0)
    for w in range(max(n_win - 2, 0), n_win):
        settle(w)


def solution(mesh):
    n_emb, n_dp = mesh.shape['emb'], mesh.shape['dp']
    n_dev = n_emb * n_dp
    tok_spec = P(('dp', 'emb'))
    act_spec = P(('dp', 'emb'), None)
    table_spec = P(None, 'emb', None)
    full_spec = P(None, None, None)
    hbm = pl.BlockSpec(memory_space=pl.ANY)
    vm = pl.BlockSpec(memory_space=pltpu.VMEM)
    sm = pl.BlockSpec(memory_space=pltpu.SMEM)
    big = jnp.iinfo(jnp.int32).max

    def params(n_grid, **kw):
        return pltpu.CompilerParams(vmem_limit_bytes=VMEM_BYTES, dimension_semantics=('arbitrary',) * n_grid if n_grid else None, **kw)

    def device_body(tok_ids, resid_in, cot_out, tables, w_up, w_down, w_gate, w_proj):
        n_layers, range_rows, e_dim = tables.shape
        tok = tok_ids.shape[0]
        dim, ffn = w_up.shape[1:]
        n_slots, n_serve = n_dev * CAP, n_emb * CAP
        my_emb, my_dp = lax.axis_index('emb'), lax.axis_index('dp')

        lanes = 128
        per_dot, dots = 32, 2
        dma = pltpu.SemaphoreType.DMA
        _, recv_loc, counts, pick, slot_row, slot_col = pl.pallas_call(
            functools.partial(plan_kernel, (n_dp, n_emb, CAP, range_rows, per_dot)),
            out_shape=[jax.ShapeDtypeStruct(shape, I32) for shape in (
                (n_dev, tok // lanes, lanes), (n_dev, CAP), (n_dev, lanes), (n_serve, 1), (1, tok), (tok, 1))],
            in_specs=[vm], out_specs=[vm] * 6,
            scratch_shapes=[pltpu.VMEM((n_dev, tok), F32), dma((n_dev - 1,)), dma((n_dev - 1,))],
            compiler_params=pltpu.CompilerParams(collective_id=0, has_side_effects=True),
            name='plan',
        )(tok_ids.reshape(tok // lanes, lanes))
        slot_bits = (n_slots - 1).bit_length()
        tab_shape = (n_layers, range_rows // 8, e_dim // 128, 8, 128)
        z_rows = 167
        z_chunks = tab_shape[1] // z_rows
        z_first = 2 * z_chunks // 3
        words = [jax.ShapeDtypeStruct((n_dev, CAP), I32)] * 3 + [jax.ShapeDtypeStruct((n_dev, lanes), I32)]
        served, dtab, read_word, write_word, group_word, meta = pl.pallas_call(
            functools.partial(gather_kernel, (n_layers, n_emb, CAP, per_dot, dots, z_first, slot_bits)),
            out_shape=[jax.ShapeDtypeStruct((n_layers, n_serve, e_dim), BF), jax.ShapeDtypeStruct(tab_shape, F32)] + words,
            in_specs=[sm, sm, vm, vm, vm, hbm],
            out_specs=[vm, hbm, vm, vm, vm, vm],
            scratch_shapes=[pltpu.VMEM((n_layers, n_serve * 8, e_dim), BF), pltpu.VMEM((z_rows,) + tab_shape[2:], F32), dma((n_emb,)), dma],
            compiler_params=params(0),
            name='table_rows',
        )(recv_loc, counts, recv_loc, counts, pick, tables)

        fb = 1024
        n_blk = ffn // fb
        cw, nw, slab = 512, 512, 32
        n_back = n_layers - 1
        z_per = z_chunks // n_blk
        assert z_chunks * z_rows == tab_shape[1] and z_per * n_blk == z_chunks
        matmul_flops = 4 * tok * dim * ffn
        w_bufs = [pltpu.VMEM((2, dim, fb), BF), pltpu.VMEM((2, fb, dim), BF), pltpu.VMEM((dim, e_dim), BF), pltpu.VMEM((e_dim, dim), BF)]
        x1, gate0, fetched = pl.pallas_call(
            functools.partial(first_kernel, (n_dp, n_emb, CAP, n_blk, cw, nw, slab)),
            out_shape=[
                jax.ShapeDtypeStruct((tok, dim), BF),
                jax.ShapeDtypeStruct((1, tok, e_dim), F32),
                jax.ShapeDtypeStruct((n_layers, tok, e_dim), BF),
            ],
            in_specs=[hbm, vm, hbm, hbm, hbm, hbm, hbm],
            out_specs=[vm, vm, vm],
            scratch_shapes=[
                pltpu.VMEM((tok, dim), BF), pltpu.VMEM((tok, dim), F32), pltpu.VMEM((tok, fb), BF), pltpu.VMEM((tok, fb), F32),
                pltpu.VMEM((n_layers, n_serve, e_dim), BF), *w_bufs, dma((3,)), dma((2, 2)), dma, dma((n_emb - 1,)), dma((n_emb - 1,)),
            ],
            compiler_params=params(0, collective_id=1, has_side_effects=True),
            cost_estimate=pl.CostEstimate(flops=matmul_flops, bytes_accessed=100 << 20, transcendentals=0),
            name='first_layer',
        )(resid_in, slot_col, served, w_gate, w_proj, w_up, w_down)

        out, saved, ups, gates, rows, dgp, dtab, scales = pl.pallas_call(
            functools.partial(forward_kernel, (n_back, n_blk, cw, nw, slab, z_per, z_chunks)),
            out_shape=[
                jax.ShapeDtypeStruct((tok, dim), BF),
                jax.ShapeDtypeStruct((n_back - 1, tok, dim), BF),
                jax.ShapeDtypeStruct((n_back, tok, ffn), F32),
                jax.ShapeDtypeStruct((n_back, tok, e_dim), F32),
                jax.ShapeDtypeStruct((tok, e_dim), F32),
                jax.ShapeDtypeStruct((tok, e_dim), BF),
                jax.ShapeDtypeStruct(tab_shape, F32),
                jax.ShapeDtypeStruct((n_back, tok, lanes), F32),
            ],
            in_specs=[hbm, hbm, vm, hbm, hbm, hbm, hbm, hbm],
            out_specs=[hbm, hbm, hbm, vm, vm, vm, hbm, vm],
            input_output_aliases={7: 6},
            scratch_shapes=[
                pltpu.VMEM((tok, dim), BF), pltpu.VMEM((tok, dim), BF), pltpu.VMEM((tok, dim), F32), pltpu.VMEM((tok, fb), BF),
                pltpu.VMEM((2, tok, fb), F32), pltpu.VMEM((z_rows,) + tab_shape[2:], F32), *w_bufs,
                dma((3,)), dma((2, 2)), dma((2,)), dma, dma((z_per,)),
            ],
            compiler_params=params(0),
            cost_estimate=pl.CostEstimate(flops=n_back * matmul_flops, bytes_accessed=400 << 20, transcendentals=0),
            name='forward',
        )(x1, cot_out, fetched, w_gate, w_proj, w_up, w_down, dtab)

        got, got_gate, mixed0 = pl.pallas_call(
            functools.partial(backward_kernel, (n_back, n_blk, n_dp, n_emb, CAP, cw, nw, slab)),
            out_shape=[jax.ShapeDtypeStruct((n_back, n_slots // 8, e_dim // 128, 8, 128), F32), jax.ShapeDtypeStruct((n_slots // 8, e_dim // 128, 8, 128), F32),
                       jax.ShapeDtypeStruct((n_slots, e_dim), BF)],
            in_specs=[hbm, hbm, hbm, vm, vm, vm, vm, vm, vm, vm, hbm, hbm, hbm, hbm, hbm],
            out_specs=[hbm, hbm, hbm],
            scratch_shapes=[
                pltpu.VMEM((tok, dim), BF), pltpu.VMEM((tok, dim), BF), pltpu.VMEM((tok, dim), F32), pltpu.VMEM((tok, fb), BF), pltpu.VMEM((tok, fb), BF),
                pltpu.VMEM((tok, dim), BF), pltpu.VMEM((n_serve // 8, e_dim // 128, 8, 128), F32), pltpu.VMEM((n_serve // 8, e_dim // 128, 8, 128), F32),
                pltpu.VMEM((n_serve, e_dim), BF), pltpu.VMEM((tok, e_dim), F32), pltpu.VMEM((tok, e_dim), BF), pltpu.VMEM((2, tok, fb), F32), *w_bufs,
                dma((4,)), dma((2, 2)), dma((2,)), dma((3, n_dev - 1)), dma((3,)), dma((n_back + 2, n_dev - 1)),
            ],
            compiler_params=params(0, collective_id=2, has_side_effects=True),
            cost_estimate=pl.CostEstimate(flops=n_back * matmul_flops, bytes_accessed=400 << 20, transcendentals=0),
            name='backward',
        )(cot_out, x1, saved, rows, dgp, slot_row, gate0, gates, fetched, scales, ups, w_up, w_down, w_gate, w_proj)

        dtab = pl.pallas_call(
            functools.partial(scatter_kernel, (8, 32, z_first, z_chunks)),
            out_shape=jax.ShapeDtypeStruct(dtab.shape, F32),
            in_specs=[sm, sm, sm, sm, hbm, hbm, hbm, hbm],
            out_specs=hbm,
            input_output_aliases={7: 0},
            scratch_shapes=[pltpu.VMEM((n_back, n_slots * 2, 128), F32), pltpu.VMEM((n_slots // 8,) + tab_shape[2:], F32),
                            pltpu.VMEM((n_slots, e_dim), BF), pltpu.VMEM((2, n_layers, CAP) + tab_shape[2:], F32),
                            pltpu.VMEM((n_slots // 8,) + tab_shape[2:], F32), pltpu.VMEM((z_rows,) + tab_shape[2:], F32),
                            pltpu.SMEM((CAP,), I32), dma((2,)), dma((3,)), dma((z_chunks,))],
            compiler_params=params(0),
            name='scatter',
        )(read_word, write_word, group_word, meta, got.reshape(n_back, n_slots * 2, 128), got_gate, mixed0, dtab)
        dtab = dtab.transpose(0, 1, 3, 2, 4).reshape(n_layers, range_rows, e_dim)
        return out, dtab

    return jax.shard_map(device_body, mesh=mesh, in_specs=(tok_spec, act_spec, act_spec, table_spec, full_spec, full_spec, full_spec, full_spec), out_specs=(act_spec, table_spec), check_vma=False)
```

```python
import functools

import jax
import jax.numpy as jnp
from jax import lax
from jax.experimental import pallas as pl
from jax.experimental.pallas import tpu as pltpu
from jax.sharding import PartitionSpec as P

NORM_EPS = 1e-6
BF = jnp.bfloat16
F32 = jnp.float32
I32 = jnp.int32
VMEM_BYTES = 67043328
GELU_C = 0.7978845608028654
GELU_A = 0.044715

MESH_AXES = ('dp', 'emb')
CAP = 256


def gelu(x):
    return 0.5 * x * (1.0 + jnp.tanh(GELU_C * (x + GELU_A * (x * x * x))))


def gelu_slope(x):
    sq = x * x
    th = jnp.tanh(GELU_C * (x + GELU_A * (x * sq)))
    return 0.5 * (1.0 + th) + (0.5 * GELU_C) * x * (1.0 - th * th) * (1.0 + (3 * GELU_A) * sq)


def dot(a, b):
    return jnp.dot(a, b, preferred_element_type=F32)


def dot_t(a, b):
    return lax.dot_general(a, b, (((1,), (1,)), ((), ())), preferred_element_type=F32)


def row_loop(rows, slab, unroll=1):
    def run(body):
        def step(i, carry):
            body(pl.ds(pl.multiple_of(i * slab, slab), slab))
            return carry

        lax.fori_loop(0, rows // slab, step, 0, unroll=unroll)

    return run


def peer_of(n_emb, index):
    dp = index // n_emb
    return {'dp': dp, 'emb': index - dp * n_emb}


def remote(src, dst, send_sem, recv_sem, device):
    return pltpu.make_async_remote_copy(src_ref=src, dst_ref=dst, send_sem=send_sem, recv_sem=recv_sem,
                                        device_id=device, device_id_type=pl.DeviceIdType.MESH)


def meet(devices):
    barrier = pltpu.get_barrier_semaphore()
    for device in devices:
        pl.semaphore_signal(barrier, inc=1, device_id=device, device_id_type=pl.DeviceIdType.MESH)
    pl.semaphore_wait(barrier, len(devices))


def plan_kernel(cfg, in_ref, ids_ref, recv_ref, counts_ref, pick_ref, slot_row_ref, slot_col_ref, rank_s, send_sem, recv_sem):
    n_dp, n_emb, cap, range_rows, per_dot = cfg
    n_dev = n_dp * n_emb
    my_dp, my_emb = lax.axis_index('dp'), lax.axis_index('emb')
    me = my_dp * n_emb + my_emb
    n_sub, lanes = in_ref.shape
    tok = n_sub * lanes
    peers = [peer_of(n_emb, lax.rem(me + k, n_dev)) for k in range(1, n_dev)]
    meet(peers)
    copies = [remote(in_ref, ids_ref.at[me], send_sem.at[k], recv_sem.at[k], peer) for k, peer in enumerate(peers)]
    start(copies)
    ids_ref[me] = in_ref[...]

    def line(ref):
        return jnp.concatenate([ref[..., j, :] for j in range(n_sub)], axis=-1)

    def ones(cond):
        return jnp.where(cond, 1.0, 0.0)

    def digits(x):
        return jnp.concatenate([jnp.right_shift(x, 8), jnp.bitwise_and(x, 255)], axis=0).astype(F32).astype(BF)

    square = (tok, tok)
    down, right = lax.broadcasted_iota(I32, square, 0), lax.broadcasted_iota(I32, square, 1)
    earlier = ones(down < right).astype(BF)
    own = jnp.broadcast_to(jnp.concatenate([in_ref[j:j + 1, :] for j in range(n_sub)], axis=-1), (8, tok))
    owner = sum(jnp.where(own >= e * range_rows, 1, 0) for e in range(1, n_emb))
    is_owner = owner == lax.broadcasted_iota(I32, (8, tok), 0)
    own_rank = dot(ones(is_owner).astype(BF), earlier).astype(I32)
    slot_row = jnp.sum(jnp.where(is_owner, own_rank + owner * cap, 0).astype(F32), axis=0, keepdims=True).astype(I32)
    slot_row_ref[...] = slot_row
    turned = dot_t(ones(down == right).astype(BF), digits(jnp.broadcast_to(slot_row, (8, tok))))
    slot_col_ref[...] = (turned[:, 0:1] * 256.0 + turned[:, 8:9]).astype(I32)

    wait(copies)
    ids8 = line(ids_ref)
    low = my_emb * range_rows
    mine = jnp.logical_and(ids8 >= low, ids8 < low + range_rows)
    mine_f = ones(mine)
    rank_s[...] = jnp.where(mine, dot(mine_f.astype(BF), earlier), -1.0)
    counts = jnp.sum(mine_f, axis=1, keepdims=True).astype(I32)
    counts_ref[...] = jnp.broadcast_to(counts, counts_ref.shape)
    loc = digits(jnp.where(mine, ids8 - low, 0))
    c_iota = lax.broadcasted_iota(I32, (cap, tok), 0).astype(F32)
    dev_iota = lax.broadcasted_iota(I32, (n_dev, cap), 0)
    recv = jnp.zeros((n_dev, cap), F32)
    for d in range(n_dev):
        found = dot_t(loc, ones(rank_s[d:d + 1, :] == c_iota).astype(BF))
        recv = jnp.where(dev_iota == d, found[:n_dev] * 256.0 + found[n_dev:], recv)
    slot = dev_iota * cap + lax.broadcasted_iota(I32, (n_dev, cap), 1)
    recv_ref[...] = jnp.where(slot - dev_iota * cap < counts, recv.astype(I32), slot * 8)
    lane16 = lax.broadcasted_iota(I32, (cap, 2 * n_dev), 1)
    row1 = lax.broadcasted_iota(I32, (cap, 1), 0)
    for e in range(n_emb):
        d = my_dp * n_emb + e
        found = dot_t(ones(rank_s[pl.ds(d, 1), :] == c_iota).astype(BF), loc)
        low8 = jnp.sum(jnp.where(lane16 == n_dev + d, found, 0.0), axis=1, keepdims=True).astype(I32)
        pick_ref[e * cap:(e + 1) * cap, :] = jnp.bitwise_and(low8, 7) + 8 * jnp.bitwise_and(row1, per_dot - 1)


def gather_kernel(cfg, loc_ref, counts_ref, recv_ref, tally_ref, pick_ref, tables_hbm,
                  out_ref, dtab_hbm, read_ref, write_ref, group_ref, meta_ref, buf, zero_s, sems, z_sem):
    n_layers, n_dest, cap, per_dot, group, z_chunks, slot_bits = cfg
    trip = per_dot * group
    z_rows = zero_s.shape[0]
    first = lax.axis_index('dp') * n_dest
    n_trips = [(counts_ref[first + d, 0] + (trip - 1)) // trip for d in range(n_dest)]

    def row_copy(d, c):
        base = pl.multiple_of(jnp.left_shift(jnp.right_shift(loc_ref[first + d, c], 3), 3), 8)
        at = pl.multiple_of(d * cap * 8 + c * 8, 8)
        return pltpu.make_async_copy(tables_hbm.at[:, pl.ds(base, 8), :], buf.at[:, pl.ds(at, 8), :], sems.at[d])

    def z_copy(c):
        return pltpu.make_async_copy(zero_s, dtab_hbm.at[0, pl.ds(c * z_rows, z_rows)], z_sem)

    for d in range(n_dest):
        def issue(i, carry, d=d):
            for k in range(8):
                row_copy(d, i * 8 + k).start()
            return carry

        lax.fori_loop(0, n_trips[d] * (trip // 8), issue, 0)

    clear_rows(zero_s)

    def z_start(c, carry):
        z_copy(c).start(priority=1)
        return carry

    lax.fori_loop(0, z_chunks, z_start, 0)
    order_rows(recv_ref, tally_ref, slot_bits, read_ref, write_ref, group_ref, meta_ref)
    for d in range(n_dest):
        def drain(i, carry, d=d):
            part = buf.at[:, pl.ds(pl.multiple_of((d * cap + i * trip) * 8, 8), trip * 8), :]
            pltpu.make_async_copy(part, part, sems.at[d]).wait()
            return carry

        lax.fori_loop(0, n_trips[d], drain, 0)

        def pick(i, carry, d=d):
            for k in range(group):
                s0 = pl.multiple_of(d * cap + i * trip + k * per_dot, per_dot)
                want = pick_ref[pl.ds(s0, per_dot), :]
                sel = (lax.broadcasted_iota(I32, (per_dot, per_dot * 8), 1) == want).astype(BF)
                for l in range(n_layers):
                    rows = buf[l, pl.ds(pl.multiple_of(s0 * 8, 8), per_dot * 8), :]
                    out_ref[l, pl.ds(s0, per_dot), :] = dot(sel, rows).astype(BF)
            return carry

        lax.fori_loop(0, n_trips[d], pick, 0)

        def blank(i, carry, d=d):
            s0 = pl.multiple_of(d * cap + i * trip, trip)
            for l in range(n_layers):
                out_ref[l, pl.ds(s0, trip), :] = jnp.zeros((trip, out_ref.shape[2]), BF)
            return carry

        lax.fori_loop(n_trips[d], cap // trip, blank, 0)

    def z_wait(c, carry):
        z_copy(c).wait()
        return carry

    lax.fori_loop(0, z_chunks, z_wait, 0)


def clear_rows(ref):
    def clear(i, carry):
        ref[i] = jnp.zeros(ref.shape[1:], F32)
        return carry

    lax.fori_loop(0, ref.shape[0], clear, 0)


def weight_copies(wu_hbm, wd_hbm, wu_s, wd_s, sems):
    fb = wu_s.shape[2]

    def copies(layer, blk, slot):
        at = pl.multiple_of(blk * fb, fb)
        return (pltpu.make_async_copy(wu_hbm.at[layer, :, pl.ds(at, fb)], wu_s.at[slot], sems.at[0, slot]),
                pltpu.make_async_copy(wd_hbm.at[layer, pl.ds(at, fb), :], wd_s.at[slot], sems.at[1, slot]))

    return copies


def start(copies):
    for copy in copies:
        copy.start()


def wait(copies):
    for copy in copies:
        copy.wait()


def mlp_block(cfg, u_s, h_s, acc_s, wu_ref, wd_ref, up_ref, second=None):
    cw, nw = cfg
    gw = 128
    n_c = wu_ref.shape[1] // cw

    def act(c):
        for g in range(cw // gw):
            gs = slice(c * cw + g * gw, c * cw + (g + 1) * gw)
            h_s[:, gs] = gelu(up_ref[:, gs]).astype(BF)

    for c in range(n_c):
        cs = slice(c * cw, (c + 1) * cw)
        up_ref[:, cs] = dot(u_s[...], wu_ref[:, cs])
        if c > 0:
            act(c - 1)
    if second is not None:
        second.wait()
    for c in range(n_c):
        cs = slice(c * cw, (c + 1) * cw)
        for n in range(acc_s.shape[1] // nw):
            ns = slice(n * nw, (n + 1) * nw)
            acc_s[:, ns] += dot(h_s[:, cs], wd_ref[cs, ns])
        if c == 0:
            act(n_c - 1)


def norm_rows(x, sl, u_s, acc_s, scale_ref=None):
    scale = lax.rsqrt(jnp.mean(x * x, axis=-1, keepdims=True) + NORM_EPS)
    u_s[sl, :] = (x * scale).astype(BF)
    acc_s[sl, :] = x
    if scale_ref is not None:
        scale_ref[sl, :] = jnp.broadcast_to(scale, (scale.shape[0], scale_ref.shape[1]))


def add_proj(nw, acc_s, mixed, wp_ref):
    for n in range(acc_s.shape[1] // nw):
        ns = slice(n * nw, (n + 1) * nw)
        acc_s[:, ns] += dot(mixed, wp_ref[:, ns])


def first_kernel(cfg, x_hbm, slot_hbm, served_hbm, wg_hbm, wp_hbm, wu_hbm, wd_hbm,
                 x_out_hbm, gate_hbm, fet_hbm,
                 x_s, slot_s, gate_s, fet_s, u_s, acc_s, h_s, up_s, ret_s, wu_s, wd_s, wg_s, wp_s,
                 in_sem, out_sem, w_sem, self_sem, send_sem, recv_sem):
    n_dp, n_emb, cap, n_blk, cw, nw, slab = cfg
    tok, dim = u_s.shape
    my_emb = lax.axis_index('emb')
    my_dp = lax.axis_index('dp')
    here = ret_s.at[:, pl.ds(pl.multiple_of(my_emb * cap, cap), cap), :]
    own = pltpu.make_async_copy(served_hbm.at[:, pl.ds(pl.multiple_of(my_emb * cap, cap), cap), :], here, self_sem)
    peers = [lax.rem(my_emb + k, n_emb) for k in range(1, n_emb)]
    copies = [remote(served_hbm.at[:, pl.ds(pl.multiple_of(p * cap, cap), cap), :], here,
                     send_sem.at[k], recv_sem.at[k], {'dp': my_dp, 'emb': p}) for k, p in enumerate(peers)]
    weights = weight_copies(wu_hbm, wd_hbm, wu_s, wd_s, w_sem)
    first = [pltpu.make_async_copy(x_hbm, x_s, in_sem.at[0]),
             pltpu.make_async_copy(wg_hbm.at[0], wg_s, in_sem.at[1]),
             pltpu.make_async_copy(wp_hbm.at[0], wp_s, in_sem.at[2]),
             pltpu.make_async_copy(slot_hbm, slot_s, in_sem.at[3])]
    start(first[:2])
    start(weights(0, 0, 0))
    start(first[2:])
    meet([{'dp': my_dp, 'emb': p} for p in peers])
    own.start()
    start(copies)
    first[0].wait()
    row_loop(tok, slab)(lambda sl: norm_rows(x_s[sl, :].astype(F32), sl, u_s, acc_s))
    first[1].wait()
    gate_s[0] = dot(u_s[...], wg_s[...])
    gate_out = pltpu.make_async_copy(gate_s, gate_hbm, out_sem.at[0])
    gate_out.start()

    def block(f, carry):
        slot = lax.rem(f, 2)

        @pl.when(f + 1 < n_blk)
        def _():
            start(weights(0, f + 1, 1 - slot))

        up_w, down_w = weights(0, f, slot)
        up_w.wait()
        mlp_block((cw, nw), u_s, h_s, acc_s, wu_s.at[slot], wd_s.at[slot], up_s, down_w)
        return carry

    lax.fori_loop(0, n_blk, block, 0)
    own.wait()
    wait(copies)
    wait(first[2:])
    sel = (lax.broadcasted_iota(I32, (tok, n_emb * cap), 1) == slot_s[...]).astype(BF)
    for l in range(fet_s.shape[0]):
        fet_s[l] = dot(sel, ret_s[l]).astype(BF)
    add_proj(nw, acc_s, (gelu(gate_s[0]) * fet_s[0].astype(F32)).astype(BF), wp_s)
    fet_out = pltpu.make_async_copy(fet_s, fet_hbm, out_sem.at[1])
    fet_out.start()
    outs = []
    for half in range(2):
        rows = pl.ds(half * (tok // 2), tok // 2)

        def finish(sl, half=half):
            sl = pl.ds(sl.start + half * (tok // 2), slab)
            x_s[sl, :] = acc_s[sl, :].astype(BF)

        row_loop(tok // 2, slab)(finish)
        outs.append(pltpu.make_async_copy(x_s.at[rows], x_out_hbm.at[rows], out_sem.at[2 + half]))
        outs[-1].start()
    gate_out.wait()
    fet_out.wait()
    wait(outs)


def forward_kernel(cfg, x_hbm, cot_hbm, fet_hbm, wg_hbm, wp_hbm, wu_hbm, wd_hbm, dt_in,
                   out_hbm, saved_hbm, ups_hbm, gate_hbm, rows_hbm, dgp_hbm, dtab_hbm, scale_hbm,
                   x_s, u_s, acc_s, h_s, up_s, zero_s, fet_ref, gate_ref, rows_ref, dgp_ref, scale_ref, wu_s, wd_s, wg_s, wp_s,
                   in_sem, w_sem, up_sem, out_sem, z_sem):
    n_layers, n_blk, cw, nw, slab, z_per, z_chunks = cfg
    tok, dim = x_s.shape
    fb = wu_s.shape[2]
    z_rows = zero_s.shape[0]
    n_steps = n_layers * n_blk
    weights = weight_copies(wu_hbm, wd_hbm, wu_s, wd_s, w_sem)

    def z_copies(step):
        found = []
        for j in range(z_per):
            c = step * z_per + j
            zl = c // z_chunks
            found.append(pltpu.make_async_copy(zero_s, dtab_hbm.at[zl + 1, pl.ds((c - zl * z_chunks) * z_rows, z_rows)], z_sem.at[j]))
        return found

    def up_copy(layer, blk, slot):
        return pltpu.make_async_copy(up_s.at[slot], ups_hbm.at[layer, :, pl.ds(pl.multiple_of(blk * fb, fb), fb)], up_sem.at[slot])

    def gate_copy(layer):
        return pltpu.make_async_copy(wg_hbm.at[layer + 1], wg_s, in_sem.at[1])

    def proj_copy(layer):
        return pltpu.make_async_copy(wp_hbm.at[layer + 1], wp_s, in_sem.at[2])

    fetch = pltpu.make_async_copy(x_hbm, x_s, in_sem.at[0])
    fetch.start()
    gate_copy(0).start()
    start(weights(1, 0, 0))
    proj_copy(0).start()
    get_fet = pltpu.make_async_copy(fet_hbm, fet_ref, in_sem.at[3])
    get_fet.start()
    put_scales = pltpu.make_async_copy(scale_ref, scale_hbm, out_sem.at[1])

    def put_gate(layer):
        return pltpu.make_async_copy(gate_ref.at[layer], gate_hbm.at[layer], out_sem.at[2])

    clear_rows(zero_s)
    fetch.wait()
    row_loop(tok, slab)(lambda sl: norm_rows(x_s[sl, :].astype(F32), sl, u_s, acc_s, scale_ref.at[0]))

    def one_layer(layer, carry):
        gate_copy(layer).wait()
        gate_ref[layer] = dot(u_s[...], wg_s[...])
        put_gate(layer).start()

        @pl.when(layer == n_layers - 1)
        def _():
            put_scales.start()

        @pl.when(layer + 1 < n_layers)
        def _():
            gate_copy(layer + 1).start()

        def block(f, carry):
            step = layer * n_blk + f
            slot = lax.rem(step, 2)

            @pl.when(step + 1 < n_steps)
            def _():
                nxt = step + 1
                start(weights(1 + nxt // n_blk, lax.rem(nxt, n_blk), 1 - slot))

            @pl.when(step > 0)
            def _():
                wait(z_copies(step - 1))

            for copy in z_copies(step):
                copy.start(priority=1)

            @pl.when(step > 1)
            def _():
                up_copy(layer, f, slot).wait()

            wait(weights(1 + layer, f, slot))
            mlp_block((cw, nw), u_s, h_s, acc_s, wu_s.at[slot], wd_s.at[slot], up_s.at[slot])
            up_copy(layer, f, slot).start()
            return carry

        lax.fori_loop(0, n_blk, block, 0)
        proj_copy(layer).wait()
        put_gate(layer).wait()

        @pl.when(layer == 0)
        def _():
            get_fet.wait()

        add_proj(nw, acc_s, (gelu(gate_ref[layer]) * fet_ref[layer + 1].astype(F32)).astype(BF), wp_s)

        @pl.when(layer > 0)
        def _():
            pltpu.make_async_copy(x_s, saved_hbm.at[layer - 1], out_sem.at[0]).wait()

        def next_rows(sl):
            x_new = acc_s[sl, :].astype(BF)
            x_s[sl, :] = x_new
            norm_rows(x_new.astype(F32), sl, u_s, acc_s, scale_ref.at[jnp.minimum(layer + 1, n_layers - 1)])

        def last_rows(sl):
            x_s[sl, :] = acc_s[sl, :].astype(BF)

        @pl.when(layer < n_layers - 1)
        def _():
            row_loop(tok, slab)(next_rows)

        @pl.when(layer == n_layers - 1)
        def _():
            row_loop(tok, slab)(last_rows)

        @pl.when(layer < n_layers - 1)
        def _():
            pltpu.make_async_copy(x_s, saved_hbm.at[layer], out_sem.at[0]).start()
            proj_copy(layer + 1).start()

        return carry

    lax.fori_loop(0, n_layers, one_layer, 0)
    put = pltpu.make_async_copy(x_s, out_hbm, out_sem.at[0])
    put.start()
    get = pltpu.make_async_copy(cot_hbm, u_s, in_sem.at[0])
    get.start()
    wait(z_copies(n_steps - 1))
    up_copy(0, 0, 0).wait()
    up_copy(0, 0, 1).wait()
    get.wait()
    d_mixed = dot_t(u_s[...], wp_s[...]).astype(BF).astype(F32)
    gate_grads(gate_ref[n_layers - 1], fet_ref[n_layers], d_mixed, rows_ref, dgp_ref)
    small = [pltpu.make_async_copy(rows_ref, rows_hbm, out_sem.at[2]), pltpu.make_async_copy(dgp_ref, dgp_hbm, out_sem.at[3])]
    start(small)
    put_scales.wait()
    put.wait()
    wait(small)


def gate_grads(gate_pre, fetched, d_mixed, rows_ref, dgp_ref):
    rows_ref[...] = gelu(gate_pre) * d_mixed
    dgp_ref[...] = (d_mixed * fetched.astype(F32) * gelu_slope(gate_pre)).astype(BF)


def to_slots(rows, slot_ref, slots_s):
    hi = rows.astype(BF)
    rest = rows - hi.astype(F32)
    mid = rest.astype(BF)
    low = (rest - mid.astype(F32)).astype(BF)
    n = slots_s.shape[0] * slots_s.shape[2]
    sel = slot_pick(n, slot_ref)
    slots = (dot(sel, hi) + dot(sel, mid)) + dot(sel, low)
    for h in range(slots_s.shape[1]):
        slots_s[:, h] = slots[:, h * 128:(h + 1) * 128].reshape(n // 8, 8, 128)


def slot_pick(n, slot_ref):
    return (lax.broadcasted_iota(I32, (n, slot_ref.shape[1]), 0) == slot_ref[...]).astype(BF)


def backward_kernel(cfg, cot_hbm, x1_hbm, saved_hbm, rows_hbm, dgp_hbm, slot_hbm, gate0_hbm, gates_hbm, fet_hbm, scale_hbm,
                    ups_hbm, wu_hbm, wd_hbm, wg_hbm, wp_hbm,
                    got_hbm, gate_hbm, mixed_hbm,
                    cot_s, x_s, acc_s, dup_s, dh_s, dng_s, slots_s, gslots_s, dslots_s, rows_s, dgp_s, slot_ref, gate0_ref, gate_ref, fet_ref, scale_ref, up_s, wu_s, wd_s, wg_s, wp_s,
                    in_sem, w_sem, up_sem, send_sem, self_sem, recv_sem):
    n_layers, n_blk, n_dp, n_emb, cap, cw, nw, slab = cfg
    tok, dim = cot_s.shape
    fb = wu_s.shape[2]
    gw = 128
    n_dev = n_dp * n_emb
    n_steps = n_layers * n_blk
    my_emb = lax.axis_index('emb')
    me = lax.axis_index('dp') * n_emb + my_emb
    peers = [peer_of(n_emb, lax.rem(me + k, n_dev)) for k in range(1, n_dev)]
    weights = weight_copies(wu_hbm, wd_hbm, wu_s, wd_s, w_sem)

    def part(ref, emb):
        return ref.at[pl.ds(emb * (cap // 8), cap // 8)]

    def sends(ref, there, which, got):
        return [pltpu.make_async_copy(part(ref, my_emb), there, self_sem.at[which])] + [
            remote(part(ref, peer['emb']), there, send_sem.at[which, k], recv_sem.at[got, k], peer) for k, peer in enumerate(peers)]

    def row_sends(i):
        return sends(slots_s, part(got_hbm.at[n_layers - 1 - i], me), 0, i)

    gate_sends = sends(gslots_s, part(gate_hbm, me), 1, n_layers)

    def flat(ref, dev):
        return ref.at[pl.ds(pl.multiple_of(dev * cap, cap), cap), :]

    mixed_sends = [pltpu.make_async_copy(flat(dslots_s, my_emb), flat(mixed_hbm, me), self_sem.at[2])] + [
        remote(flat(dslots_s, peer['emb']), flat(mixed_hbm, me), send_sem.at[2, k], recv_sem.at[n_layers + 1, k], peer)
        for k, peer in enumerate(peers)]

    def up_copy(step, slot):
        i = step // n_blk
        blk = step - i * n_blk
        return pltpu.make_async_copy(ups_hbm.at[n_layers - 1 - i, :, pl.ds(pl.multiple_of(blk * fb, fb), fb)], up_s.at[slot], up_sem.at[slot])

    def load(step, slot):
        i = step // n_blk
        return weights(n_layers - i, step - i * n_blk, slot) + (up_copy(step, slot),)

    def gate_copy(i):
        return pltpu.make_async_copy(wg_hbm.at[n_layers - i], wg_s, in_sem.at[1])

    def proj_copy(i):
        return pltpu.make_async_copy(wp_hbm.at[n_layers - 1 - i], wp_s, in_sem.at[2])

    def x_copy(i):
        return pltpu.make_async_copy(saved_hbm.at[n_layers - 2 - i], x_s, in_sem.at[3])

    fetch = pltpu.make_async_copy(cot_hbm, cot_s, in_sem.at[0])
    soon = [pltpu.make_async_copy(src, dst, in_sem.at[4 + k]) for k, (src, dst) in enumerate(
        ((gate0_hbm, gate0_ref), (slot_hbm, slot_ref), (rows_hbm, rows_s), (dgp_hbm, dgp_s)))]
    later = [pltpu.make_async_copy(src, dst, in_sem.at[8 + k]) for k, (src, dst) in enumerate(
        ((gates_hbm, gate_ref), (fet_hbm, fet_ref), (scale_hbm, scale_ref)))]
    start(soon)
    gate_copy(0).start()
    fetch.start()
    start(load(0, 0))
    proj_copy(0).start()
    start(later)

    def clear(sl):
        acc_s[sl, :] = jnp.zeros((slab, dim), F32)

    row_loop(tok, slab)(clear)
    meet(peers)
    wait(soon)
    to_slots(gelu(gate0_ref[0]), slot_ref, gslots_s)

    def one_layer(i, carry):
        @pl.when(i < n_layers - 1)
        def _():
            x_copy(i).start()

        @pl.when(i == n_layers - 1)
        def _():
            pltpu.make_async_copy(x1_hbm, x_s, in_sem.at[3]).start()

        gate_copy(i).wait()
        to_slots(rows_s[...], slot_ref, slots_s)
        for n in range(dim // nw):
            ns = slice(n * nw, (n + 1) * nw)
            dng_s[:, ns] = dot_t(dgp_s[...], wg_s[ns, :]).astype(BF)
        start(row_sends(i))

        @pl.when(i < n_layers - 1)
        def _():
            gate_copy(i + 1).start()

        @pl.when(i == 0)
        def _():
            start(gate_sends)
            fetch.wait()

        def block(f, carry):
            step = i * n_blk + f
            slot = lax.rem(step, 2)

            @pl.when(step + 1 < n_steps)
            def _():
                start(load(step + 1, 1 - slot))

            wait(load(step, slot))
            wu_ref, wd_ref, up_ref = wu_s.at[slot], wd_s.at[slot], up_s.at[slot]

            def act(c):
                for g in range(cw // gw):
                    gs = slice(c * cw + g * gw, c * cw + (g + 1) * gw)
                    dup_s[:, gs] = (dh_s[:, gs].astype(F32) * gelu_slope(up_ref[:, gs])).astype(BF)

            n_c = fb // cw
            for c in range(n_c):
                cs = slice(c * cw, (c + 1) * cw)
                dh_s[:, cs] = dot_t(cot_s[...], wd_ref[cs, :]).astype(BF)
                if c > 0:
                    act(c - 1)
            for c in range(n_c):
                cs = slice(c * cw, (c + 1) * cw)
                for n in range(dim // nw):
                    ns = slice(n * nw, (n + 1) * nw)
                    acc_s[:, ns] += dot_t(dup_s[:, cs], wu_ref[ns, cs])
                if c == 0:
                    act(n_c - 1)
            return carry

        lax.fori_loop(0, n_blk, block, 0)
        pltpu.make_async_copy(x1_hbm, x_s, in_sem.at[3]).wait()

        @pl.when(i == 0)
        def _():
            wait(later)


        def rows_back(sl):
            x = x_s[sl, :].astype(F32)
            scale = scale_ref[n_layers - 1 - i, sl, 0:1]
            d_n = (acc_s[sl, :].astype(BF) + dng_s[sl, :]).astype(F32)
            acc_s[sl, :] = jnp.zeros((slab, dim), F32)
            proj = jnp.mean(d_n * x, axis=-1, keepdims=True)
            d_x = d_n * scale - x * (proj * (scale * scale * scale))
            cot_s[sl, :] = (cot_s[sl, :].astype(F32) + d_x).astype(BF)

        row_loop(tok, slab)(rows_back)
        proj_copy(i).wait()
        d_mixed = dot_t(cot_s[...], wp_s[...]).astype(BF)

        @pl.when(i == n_layers - 1)
        def _():
            dslots_s[...] = dot(slot_pick(n_emb * cap, slot_ref), d_mixed).astype(BF)

        wait(row_sends(i))

        @pl.when(i < n_layers - 1)
        def _():
            proj_copy(i + 1).start()
            gate_grads(gate_ref[jnp.maximum(n_layers - 2 - i, 0)], fet_ref[n_layers - 1 - i], d_mixed.astype(F32), rows_s, dgp_s)

        return carry

    lax.fori_loop(0, n_layers, one_layer, 0)
    start(mixed_sends)
    wait(gate_sends)
    wait(mixed_sends)


def order_rows(recv_ref, counts_ref, slot_bits, read_ref, write_ref, group_ref, meta_ref):
    n_dev, cap = recv_ref.shape
    shape = (n_dev, cap)
    square = (cap, cap)
    dev, lane = lax.broadcasted_iota(I32, shape, 0), lax.broadcasted_iota(I32, shape, 1)
    down, right = lax.broadcasted_iota(I32, square, 0), lax.broadcasted_iota(I32, square, 1)
    counts = counts_ref[:, 0:1]
    key = jnp.where(lane < counts, jnp.left_shift(recv_ref[...], slot_bits), 1 << 30) + dev * cap + lane

    def ones(cond):
        return jnp.where(cond, 1.0, 0.0)

    def digit(k):
        return jnp.bitwise_and(jnp.right_shift(key, 8 * k), 255).astype(F32).astype(BF)

    digits = [digit(k) for k in range(4)]
    same = ones(down == right).astype(BF)
    turned = sum(jnp.left_shift(dot_t(same, d).astype(I32), 8 * k) for k, d in enumerate(digits))
    rows = jnp.concatenate([d[None] for d in digits], axis=0)
    found = [jnp.zeros((8, cap), F32) for _ in range(n_dev)]
    for d in range(n_dev):
        column = turned[:, d:d + 1]
        smaller = sum(ones(key[e:e + 1, :] < column) for e in range(n_dev))
        rank = jnp.sum(smaller, axis=1, keepdims=True)
        mine = jnp.concatenate([rows[k, d:d + 1, :] for k in range(4)] * 2, axis=0)
        for w in range(n_dev):
            found[w] = found[w] + dot(mine, ones(rank - (w * cap) == right.astype(F32)).astype(BF))
    merged = [sum(jnp.left_shift(f[k:k + 1].astype(I32), 8 * k) for k in range(4)) for f in found]
    ordered = jnp.concatenate(merged, axis=0)

    before = pltpu.roll(ordered, 1, 1)
    before = jnp.where(lane == 0, pltpu.roll(before, 1, 0), before)
    after = pltpu.roll(ordered, cap - 1, 1)
    after = jnp.where(lane == cap - 1, pltpu.roll(after, n_dev - 1, 0), after)
    total = jnp.sum(counts_ref[...].astype(F32), axis=0, keepdims=True).astype(I32)
    place_in = dev * cap + lane
    live = place_in < total[:, 0:1]
    slot = jnp.bitwise_and(ordered, (1 << slot_bits) - 1)
    row = jnp.right_shift(ordered, slot_bits)
    group = jnp.right_shift(ordered, slot_bits + 3)
    begin, end = place_in == 0, place_in == n_dev * cap - 1
    same_row = jnp.logical_and(row == jnp.right_shift(before, slot_bits), jnp.logical_not(begin))
    fresh = jnp.logical_or(group != jnp.right_shift(before, slot_bits + 3), begin)
    last = jnp.logical_and(jnp.logical_or(group != jnp.right_shift(after, slot_bits + 3), end), live)
    place = dot(ones(fresh).astype(BF), ones(down <= right).astype(BF)).astype(I32)
    place = place - place[:, 0:1]
    read_ref[...] = jnp.right_shift(slot, 3) * 16 + jnp.bitwise_and(slot, 7) + jnp.where(same_row, -(1 << 31), 0)
    write_ref[...] = place * 16 + jnp.bitwise_and(row, 7)
    group_ref[...] = jnp.where(live, group, 0)
    n_out = jnp.sum(ones(last), axis=1, keepdims=True).astype(I32)
    goes_on = jnp.where(jnp.logical_and(jnp.logical_not(fresh), live), 1, 0)[:, 0:1]
    meta_lane = lax.broadcasted_iota(I32, meta_ref.shape, 1)
    meta = jnp.where(meta_lane == 0, n_out, jnp.where(meta_lane == 1, place[:, cap - 1:cap], goes_on))
    meta_ref[...] = jnp.where(meta_lane == 3, total, meta)


def scatter_kernel(cfg, read_ref, write_ref, group_ref, meta_ref, rows_hbm, gate_hbm, mixed_hbm, dt_in, dt_out,
                   rows_ref, gate_ref, mixed_ref, groups, prod, zero_s, spots, sems, in_sem, z_sem):
    unroll, bulk, z_first, z_chunks = cfg
    n_layers, window = groups.shape[1:3]
    n_slots = mixed_ref.shape[0]
    n_win = n_slots // window
    z_rows = zero_s.shape[0]
    count = meta_ref[0, 3]
    loads = [pltpu.make_async_copy(src, dst, in_sem.at[k]) for k, (src, dst) in enumerate(
        ((gate_hbm, gate_ref), (mixed_hbm, mixed_ref), (rows_hbm, rows_ref)))]
    start(loads)
    clear_rows(zero_s)

    def z_copy(c):
        return pltpu.make_async_copy(zero_s, dt_out.at[0, pl.ds(c * z_rows, z_rows)], z_sem.at[c])

    def z_start(c, carry):
        z_copy(c).start()
        return carry

    def z_wait(c, carry):
        z_copy(c).wait()
        return carry

    lax.fori_loop(z_first, z_chunks, z_start, 0)
    wait(loads[:2])

    def product(i, carry):
        step = 64
        mixed = mixed_ref[pl.ds(pl.multiple_of(i * step, step), step), :].astype(F32)
        for h in range(2):
            at = pl.ds(i * (step // 8), step // 8)
            prod[at, h] = gate_ref[at, h] * mixed[:, h * 128:(h + 1) * 128].reshape(step // 8, 8, 128)
        return carry

    lax.fori_loop(0, n_slots // 64, product, 0, unroll=4)

    def move(buf, spot, group, n):
        return pltpu.make_async_copy(groups.at[buf, :, pl.ds(spot, n)], dt_out.at[:, pl.ds(group, n)], sems.at[buf])

    def each(n, k, body):
        def trip(t, carry):
            for i in range(k):
                body(t * k + i)
            return carry

        def one(i, carry):
            body(i)
            return carry

        full = n // k
        lax.fori_loop(0, full, trip, 0)
        lax.fori_loop(full * k, n, one, 0)

    def settle(w):
        n = meta_ref[w, 0]

        def drain_bulk(j, carry):
            move(w % 2, 0, 0, bulk).wait()
            return carry

        def drain(j, carry):
            move(w % 2, 0, 0, 1).wait()
            return carry

        lax.fori_loop(0, n // bulk, drain_bulk, 0)
        lax.fori_loop(0, lax.rem(n, bulk), drain, 0)

    blank = jnp.zeros(groups.shape[3:], F32)
    accs = tuple(jnp.zeros((2, 128), F32) for _ in range(n_layers))
    z_done = jnp.int32(z_first)
    for w in range(n_win):
        buf = w % 2
        if w >= 2:
            settle(w - 2)
        left = jnp.clip(count - w * window, 0, window)
        trips = (left + (unroll - 1)) // unroll
        n_out = meta_ref[w, 0]

        def clear(u, buf=buf):
            for l in range(n_layers):
                groups[buf, l, u] = blank

        each(jnp.where(left > 0, jnp.minimum(n_out + 1, window), 0), 4, clear)
        if w == 0:
            wait(loads[2:])
        else:
            @pl.when(meta_ref[w, 2] > 0)
            def _(w=w, buf=buf):
                for l in range(n_layers):
                    groups[buf, l, 0] = groups[1 - buf, l, meta_ref[w - 1, 1]]

        sums = [groups.at[buf, l].reshape(window * 16, 128) for l in range(n_layers)]
        rows = [prod.reshape(n_slots * 2, 128)] + [rows_ref.at[l] for l in range(n_layers - 1)]

        def add(t, accs, w=w, sums=sums, rows=rows):
            for k in range(unroll):
                j = t * unroll + k
                word = read_ref[w, j]
                at = jnp.bitwise_and(word, n_slots * 2 - 1)
                same = word < 0
                to = write_ref[w, j]
                spots[jnp.right_shift(to, 4)] = group_ref[w, j]
                accs = tuple(jnp.where(same, acc, 0.0) + src[pl.ds(at, 2, stride=8), :] for acc, src in zip(accs, rows))
                for acc, dst in zip(accs, sums):
                    dst[pl.ds(to, 2, stride=8), :] = acc
            return accs

        accs = lax.fori_loop(0, trips, add, accs)
        need = jnp.where(n_out > 0, spots[jnp.maximum(n_out - 1, 0)] // z_rows + 1, z_done)
        need = jnp.maximum(need, z_done)
        lax.fori_loop(z_done, need, z_wait, 0)
        z_done = need
        each(n_out, 4, lambda u, buf=buf: move(buf, u, spots[u], 1).start())
    lax.fori_loop(z_done, z_chunks, z_wait, 0)
    for w in range(max(n_win - 2, 0), n_win):
        settle(w)


def solution(mesh):
    n_emb, n_dp = mesh.shape['emb'], mesh.shape['dp']
    n_dev = n_emb * n_dp
    tok_spec = P(('dp', 'emb'))
    act_spec = P(('dp', 'emb'), None)
    table_spec = P(None, 'emb', None)
    full_spec = P(None, None, None)
    hbm = pl.BlockSpec(memory_space=pl.ANY)
    vm = pl.BlockSpec(memory_space=pltpu.VMEM)
    sm = pl.BlockSpec(memory_space=pltpu.SMEM)
    big = jnp.iinfo(jnp.int32).max

    def params(n_grid, **kw):
        return pltpu.CompilerParams(vmem_limit_bytes=VMEM_BYTES, dimension_semantics=('arbitrary',) * n_grid if n_grid else None, **kw)

    def device_body(tok_ids, resid_in, cot_out, tables, w_up, w_down, w_gate, w_proj):
        n_layers, range_rows, e_dim = tables.shape
        tok = tok_ids.shape[0]
        dim, ffn = w_up.shape[1:]
        n_slots, n_serve = n_dev * CAP, n_emb * CAP
        my_emb, my_dp = lax.axis_index('emb'), lax.axis_index('dp')

        lanes = 128
        per_dot, dots = 32, 2
        dma = pltpu.SemaphoreType.DMA
        _, recv_loc, counts, pick, slot_row, slot_col = pl.pallas_call(
            functools.partial(plan_kernel, (n_dp, n_emb, CAP, range_rows, per_dot)),
            out_shape=[jax.ShapeDtypeStruct(shape, I32) for shape in (
                (n_dev, tok // lanes, lanes), (n_dev, CAP), (n_dev, lanes), (n_serve, 1), (1, tok), (tok, 1))],
            in_specs=[vm], out_specs=[vm] * 6,
            scratch_shapes=[pltpu.VMEM((n_dev, tok), F32), dma((n_dev - 1,)), dma((n_dev - 1,))],
            compiler_params=pltpu.CompilerParams(collective_id=0, has_side_effects=True),
            name='plan',
        )(tok_ids.reshape(tok // lanes, lanes))
        slot_bits = (n_slots - 1).bit_length()
        tab_shape = (n_layers, range_rows // 8, e_dim // 128, 8, 128)
        z_rows = 167
        z_chunks = tab_shape[1] // z_rows
        z_first = 2 * z_chunks // 3
        words = [jax.ShapeDtypeStruct((n_dev, CAP), I32)] * 3 + [jax.ShapeDtypeStruct((n_dev, lanes), I32)]
        served, dtab, read_word, write_word, group_word, meta = pl.pallas_call(
            functools.partial(gather_kernel, (n_layers, n_emb, CAP, per_dot, dots, z_first, slot_bits)),
            out_shape=[jax.ShapeDtypeStruct((n_layers, n_serve, e_dim), BF), jax.ShapeDtypeStruct(tab_shape, F32)] + words,
            in_specs=[sm, sm, vm, vm, vm, hbm],
            out_specs=[vm, hbm, vm, vm, vm, vm],
            scratch_shapes=[pltpu.VMEM((n_layers, n_serve * 8, e_dim), BF), pltpu.VMEM((z_rows,) + tab_shape[2:], F32), dma((n_emb,)), dma],
            compiler_params=params(0),
            name='table_rows',
        )(recv_loc, counts, recv_loc, counts, pick, tables)

        fb = 1024
        n_blk = ffn // fb
        cw, nw, slab = 512, 512, 32
        n_back = n_layers - 1
        z_per = z_chunks // n_blk
        assert z_chunks * z_rows == tab_shape[1] and z_per * n_blk == z_chunks
        matmul_flops = 4 * tok * dim * ffn
        w_bufs = [pltpu.VMEM((2, dim, fb), BF), pltpu.VMEM((2, fb, dim), BF), pltpu.VMEM((dim, e_dim), BF), pltpu.VMEM((e_dim, dim), BF)]
        x1, gate0, fetched = pl.pallas_call(
            functools.partial(first_kernel, (n_dp, n_emb, CAP, n_blk, cw, nw, slab)),
            out_shape=[
                jax.ShapeDtypeStruct((tok, dim), BF),
                jax.ShapeDtypeStruct((1, tok, e_dim), F32),
                jax.ShapeDtypeStruct((n_layers, tok, e_dim), BF),
            ],
            in_specs=[hbm] * 7,
            out_specs=[hbm] * 3,
            scratch_shapes=[
                pltpu.VMEM((tok, dim), BF), pltpu.VMEM((tok, 1), I32), pltpu.VMEM((1, tok, e_dim), F32), pltpu.VMEM((n_layers, tok, e_dim), BF),
                pltpu.VMEM((tok, dim), BF), pltpu.VMEM((tok, dim), F32), pltpu.VMEM((tok, fb), BF), pltpu.VMEM((tok, fb), F32),
                pltpu.VMEM((n_layers, n_serve, e_dim), BF), *w_bufs,
                dma((4,)), dma((4,)), dma((2, 2)), dma, dma((n_emb - 1,)), dma((n_emb - 1,)),
            ],
            compiler_params=params(0, collective_id=1, has_side_effects=True),
            cost_estimate=pl.CostEstimate(flops=matmul_flops, bytes_accessed=100 << 20, transcendentals=0),
            name='first_layer',
        )(resid_in, slot_col, served, w_gate, w_proj, w_up, w_down)

        out, saved, ups, gates, rows, dgp, dtab, scales = pl.pallas_call(
            functools.partial(forward_kernel, (n_back, n_blk, cw, nw, slab, z_per, z_chunks)),
            out_shape=[
                jax.ShapeDtypeStruct((tok, dim), BF),
                jax.ShapeDtypeStruct((n_back - 1, tok, dim), BF),
                jax.ShapeDtypeStruct((n_back, tok, ffn), F32),
                jax.ShapeDtypeStruct((n_back, tok, e_dim), F32),
                jax.ShapeDtypeStruct((tok, e_dim), F32),
                jax.ShapeDtypeStruct((tok, e_dim), BF),
                jax.ShapeDtypeStruct(tab_shape, F32),
                jax.ShapeDtypeStruct((n_back, tok, lanes), F32),
            ],
            in_specs=[hbm] * 8,
            out_specs=[hbm] * 8,
            input_output_aliases={7: 6},
            scratch_shapes=[
                pltpu.VMEM((tok, dim), BF), pltpu.VMEM((tok, dim), BF), pltpu.VMEM((tok, dim), F32), pltpu.VMEM((tok, fb), BF),
                pltpu.VMEM((2, tok, fb), F32), pltpu.VMEM((z_rows,) + tab_shape[2:], F32),
                pltpu.VMEM((n_layers, tok, e_dim), BF), pltpu.VMEM((n_back, tok, e_dim), F32), pltpu.VMEM((tok, e_dim), F32),
                pltpu.VMEM((tok, e_dim), BF), pltpu.VMEM((n_back, tok, lanes), F32), *w_bufs,
                dma((4,)), dma((2, 2)), dma((2,)), dma((4,)), dma((z_per,)),
            ],
            compiler_params=params(0),
            cost_estimate=pl.CostEstimate(flops=n_back * matmul_flops, bytes_accessed=400 << 20, transcendentals=0),
            name='forward',
        )(x1, cot_out, fetched, w_gate, w_proj, w_up, w_down, dtab)

        got, got_gate, mixed0 = pl.pallas_call(
            functools.partial(backward_kernel, (n_back, n_blk, n_dp, n_emb, CAP, cw, nw, slab)),
            out_shape=[jax.ShapeDtypeStruct((n_back, n_slots // 8, e_dim // 128, 8, 128), F32), jax.ShapeDtypeStruct((n_slots // 8, e_dim // 128, 8, 128), F32),
                       jax.ShapeDtypeStruct((n_slots, e_dim), BF)],
            in_specs=[hbm] * 15,
            out_specs=[hbm, hbm, hbm],
            scratch_shapes=[
                pltpu.VMEM((tok, dim), BF), pltpu.VMEM((tok, dim), BF), pltpu.VMEM((tok, dim), F32), pltpu.VMEM((tok, fb), BF), pltpu.VMEM((tok, fb), BF),
                pltpu.VMEM((tok, dim), BF), pltpu.VMEM((n_serve // 8, e_dim // 128, 8, 128), F32), pltpu.VMEM((n_serve // 8, e_dim // 128, 8, 128), F32),
                pltpu.VMEM((n_serve, e_dim), BF), pltpu.VMEM((tok, e_dim), F32), pltpu.VMEM((tok, e_dim), BF), pltpu.VMEM((1, tok), I32),
                pltpu.VMEM((1, tok, e_dim), F32), pltpu.VMEM((n_back, tok, e_dim), F32), pltpu.VMEM((n_layers, tok, e_dim), BF),
                pltpu.VMEM((n_back, tok, lanes), F32), pltpu.VMEM((2, tok, fb), F32), *w_bufs,
                dma((11,)), dma((2, 2)), dma((2,)), dma((3, n_dev - 1)), dma((3,)), dma((n_back + 2, n_dev - 1)),
            ],
            compiler_params=params(0, collective_id=2, has_side_effects=True),
            cost_estimate=pl.CostEstimate(flops=n_back * matmul_flops, bytes_accessed=400 << 20, transcendentals=0),
            name='backward',
        )(cot_out, x1, saved, rows, dgp, slot_row, gate0, gates, fetched, scales, ups, w_up, w_down, w_gate, w_proj)

        dtab = pl.pallas_call(
            functools.partial(scatter_kernel, (8, 32, z_first, z_chunks)),
            out_shape=jax.ShapeDtypeStruct(dtab.shape, F32),
            in_specs=[sm, sm, sm, sm, hbm, hbm, hbm, hbm],
            out_specs=hbm,
            input_output_aliases={7: 0},
            scratch_shapes=[pltpu.VMEM((n_back, n_slots * 2, 128), F32), pltpu.VMEM((n_slots // 8,) + tab_shape[2:], F32),
                            pltpu.VMEM((n_slots, e_dim), BF), pltpu.VMEM((2, n_layers, CAP) + tab_shape[2:], F32),
                            pltpu.VMEM((n_slots // 8,) + tab_shape[2:], F32), pltpu.VMEM((z_rows,) + tab_shape[2:], F32),
                            pltpu.SMEM((CAP,), I32), dma((2,)), dma((3,)), dma((z_chunks,))],
            compiler_params=params(0),
            name='scatter',
        )(read_word, write_word, group_word, meta, got.reshape(n_back, n_slots * 2, 128), got_gate, mixed0, dtab)
        dtab = dtab.transpose(0, 1, 3, 2, 4).reshape(n_layers, range_rows, e_dim)
        return out, dtab

    return jax.shard_map(device_body, mesh=mesh, in_specs=(tok_spec, act_spec, act_spec, table_spec, full_spec, full_spec, full_spec, full_spec), out_specs=(act_spec, table_spec), check_vma=False)
```

```python
import functools

import jax
import jax.numpy as jnp
from jax import lax
from jax.experimental import pallas as pl
from jax.experimental.pallas import tpu as pltpu
from jax.sharding import PartitionSpec as P

NORM_EPS = 1e-6
BF = jnp.bfloat16
F32 = jnp.float32
I32 = jnp.int32
VMEM_BYTES = 67043328
GELU_C = 0.7978845608028654
GELU_A = 0.044715

MESH_AXES = ('dp', 'emb')
CAP = 256


def gelu(x):
    return 0.5 * x * (1.0 + jnp.tanh(GELU_C * (x + GELU_A * (x * x * x))))


def gelu_slope(x):
    sq = x * x
    th = jnp.tanh(GELU_C * (x + GELU_A * (x * sq)))
    return 0.5 * (1.0 + th) + (0.5 * GELU_C) * x * (1.0 - th * th) * (1.0 + (3 * GELU_A) * sq)


def dot(a, b):
    return jnp.dot(a, b, preferred_element_type=F32)


def dot_t(a, b):
    return lax.dot_general(a, b, (((1,), (1,)), ((), ())), preferred_element_type=F32)


def row_loop(rows, slab, unroll=1):
    def run(body):
        def step(i, carry):
            body(pl.ds(pl.multiple_of(i * slab, slab), slab))
            return carry

        lax.fori_loop(0, rows // slab, step, 0, unroll=unroll)

    return run


def peer_of(n_emb, index):
    dp = index // n_emb
    return {'dp': dp, 'emb': index - dp * n_emb}


def remote(src, dst, send_sem, recv_sem, device):
    return pltpu.make_async_remote_copy(src_ref=src, dst_ref=dst, send_sem=send_sem, recv_sem=recv_sem,
                                        device_id=device, device_id_type=pl.DeviceIdType.MESH)


def meet(devices):
    barrier = pltpu.get_barrier_semaphore()
    for device in devices:
        pl.semaphore_signal(barrier, inc=1, device_id=device, device_id_type=pl.DeviceIdType.MESH)
    pl.semaphore_wait(barrier, len(devices))


def plan_kernel(cfg, in_ref, ids_ref, recv_ref, counts_ref, pick_ref, slot_row_ref, slot_col_ref, rank_s, send_sem, recv_sem):
    n_dp, n_emb, cap, range_rows, per_dot = cfg
    n_dev = n_dp * n_emb
    my_dp, my_emb = lax.axis_index('dp'), lax.axis_index('emb')
    me = my_dp * n_emb + my_emb
    n_sub, lanes = in_ref.shape
    tok = n_sub * lanes
    peers = [peer_of(n_emb, lax.rem(me + k, n_dev)) for k in range(1, n_dev)]
    meet(peers)
    copies = [remote(in_ref, ids_ref.at[me], send_sem.at[k], recv_sem.at[k], peer) for k, peer in enumerate(peers)]
    start(copies)
    ids_ref[me] = in_ref[...]

    def line(ref):
        return jnp.concatenate([ref[..., j, :] for j in range(n_sub)], axis=-1)

    def ones(cond):
        return jnp.where(cond, 1.0, 0.0)

    def digits(x):
        return jnp.concatenate([jnp.right_shift(x, 8), jnp.bitwise_and(x, 255)], axis=0).astype(F32).astype(BF)

    square = (tok, tok)
    down, right = lax.broadcasted_iota(I32, square, 0), lax.broadcasted_iota(I32, square, 1)
    earlier = ones(down < right).astype(BF)
    own = jnp.broadcast_to(jnp.concatenate([in_ref[j:j + 1, :] for j in range(n_sub)], axis=-1), (8, tok))
    owner = sum(jnp.where(own >= e * range_rows, 1, 0) for e in range(1, n_emb))
    is_owner = owner == lax.broadcasted_iota(I32, (8, tok), 0)
    own_rank = dot(ones(is_owner).astype(BF), earlier).astype(I32)
    slot_row = jnp.sum(jnp.where(is_owner, own_rank + owner * cap, 0).astype(F32), axis=0, keepdims=True).astype(I32)
    slot_row_ref[...] = slot_row
    turned = dot_t(ones(down == right).astype(BF), digits(jnp.broadcast_to(slot_row, (8, tok))))
    slot_col_ref[...] = (turned[:, 0:1] * 256.0 + turned[:, 8:9]).astype(I32)

    wait(copies)
    ids8 = line(ids_ref)
    low = my_emb * range_rows
    mine = jnp.logical_and(ids8 >= low, ids8 < low + range_rows)
    mine_f = ones(mine)
    rank_s[...] = jnp.where(mine, dot(mine_f.astype(BF), earlier), -1.0)
    counts = jnp.sum(mine_f, axis=1, keepdims=True).astype(I32)
    counts_ref[...] = jnp.broadcast_to(counts, counts_ref.shape)
    loc = digits(jnp.where(mine, ids8 - low, 0))
    c_iota = lax.broadcasted_iota(I32, (cap, tok), 0).astype(F32)
    dev_iota = lax.broadcasted_iota(I32, (n_dev, cap), 0)
    recv = jnp.zeros((n_dev, cap), F32)
    for d in range(n_dev):
        found = dot_t(loc, ones(rank_s[d:d + 1, :] == c_iota).astype(BF))
        recv = jnp.where(dev_iota == d, found[:n_dev] * 256.0 + found[n_dev:], recv)
    slot = dev_iota * cap + lax.broadcasted_iota(I32, (n_dev, cap), 1)
    recv_ref[...] = jnp.where(slot - dev_iota * cap < counts, recv.astype(I32), slot * 8)
    lane16 = lax.broadcasted_iota(I32, (cap, 2 * n_dev), 1)
    row1 = lax.broadcasted_iota(I32, (cap, 1), 0)
    for e in range(n_emb):
        d = my_dp * n_emb + e
        found = dot_t(ones(rank_s[pl.ds(d, 1), :] == c_iota).astype(BF), loc)
        low8 = jnp.sum(jnp.where(lane16 == n_dev + d, found, 0.0), axis=1, keepdims=True).astype(I32)
        pick_ref[e * cap:(e + 1) * cap, :] = jnp.bitwise_and(low8, 7) + 8 * jnp.bitwise_and(row1, per_dot - 1)


def gather_kernel(cfg, loc_ref, counts_ref, recv_ref, tally_ref, pick_ref, tables_hbm,
                  out_ref, dtab_hbm, read_ref, write_ref, group_ref, meta_ref, buf, zero_s, sems, z_sem):
    n_layers, n_dest, cap, per_dot, group, z_chunks, slot_bits = cfg
    trip = per_dot * group
    z_rows = zero_s.shape[0]
    first = lax.axis_index('dp') * n_dest
    n_trips = [(counts_ref[first + d, 0] + (trip - 1)) // trip for d in range(n_dest)]

    def row_copy(d, c):
        base = pl.multiple_of(jnp.left_shift(jnp.right_shift(loc_ref[first + d, c], 3), 3), 8)
        at = pl.multiple_of(d * cap * 8 + c * 8, 8)
        return pltpu.make_async_copy(tables_hbm.at[:, pl.ds(base, 8), :], buf.at[:, pl.ds(at, 8), :], sems.at[d])

    def z_copy(c):
        return pltpu.make_async_copy(zero_s, dtab_hbm.at[0, pl.ds(c * z_rows, z_rows)], z_sem)

    for d in range(n_dest):
        def issue(i, carry, d=d):
            for k in range(8):
                row_copy(d, i * 8 + k).start()
            return carry

        lax.fori_loop(0, n_trips[d] * (trip // 8), issue, 0)

    clear_rows(zero_s)

    def z_start(c, carry):
        z_copy(c).start(priority=1)
        return carry

    lax.fori_loop(0, z_chunks, z_start, 0)
    order_rows(recv_ref, tally_ref, slot_bits, read_ref, write_ref, group_ref, meta_ref)
    for d in range(n_dest):
        def drain(i, carry, d=d):
            part = buf.at[:, pl.ds(pl.multiple_of((d * cap + i * trip) * 8, 8), trip * 8), :]
            pltpu.make_async_copy(part, part, sems.at[d]).wait()
            return carry

        lax.fori_loop(0, n_trips[d], drain, 0)

        def pick(i, carry, d=d):
            for k in range(group):
                s0 = pl.multiple_of(d * cap + i * trip + k * per_dot, per_dot)
                want = pick_ref[pl.ds(s0, per_dot), :]
                sel = (lax.broadcasted_iota(I32, (per_dot, per_dot * 8), 1) == want).astype(BF)
                for l in range(n_layers):
                    rows = buf[l, pl.ds(pl.multiple_of(s0 * 8, 8), per_dot * 8), :]
                    out_ref[l, pl.ds(s0, per_dot), :] = dot(sel, rows).astype(BF)
            return carry

        lax.fori_loop(0, n_trips[d], pick, 0)

        def blank(i, carry, d=d):
            s0 = pl.multiple_of(d * cap + i * trip, trip)
            for l in range(n_layers):
                out_ref[l, pl.ds(s0, trip), :] = jnp.zeros((trip, out_ref.shape[2]), BF)
            return carry

        lax.fori_loop(n_trips[d], cap // trip, blank, 0)

    def z_wait(c, carry):
        z_copy(c).wait()
        return carry

    lax.fori_loop(0, z_chunks, z_wait, 0)


def clear_rows(ref):
    def clear(i, carry):
        ref[i] = jnp.zeros(ref.shape[1:], F32)
        return carry

    lax.fori_loop(0, ref.shape[0], clear, 0)


def weight_copies(wu_hbm, wd_hbm, wu_s, wd_s, sems):
    fb = wu_s.shape[2]

    def copies(layer, blk, slot):
        at = pl.multiple_of(blk * fb, fb)
        return (pltpu.make_async_copy(wu_hbm.at[layer, :, pl.ds(at, fb)], wu_s.at[slot], sems.at[0, slot]),
                pltpu.make_async_copy(wd_hbm.at[layer, pl.ds(at, fb), :], wd_s.at[slot], sems.at[1, slot]))

    return copies


def start(copies):
    for copy in copies:
        copy.start()


def wait(copies):
    for copy in copies:
        copy.wait()


def mlp_block(cfg, u_s, h_s, acc_s, wu_ref, wd_ref, up_ref, second=None):
    cw, nw = cfg
    gw = 128
    n_c = wu_ref.shape[1] // cw

    def act(c):
        for g in range(cw // gw):
            gs = slice(c * cw + g * gw, c * cw + (g + 1) * gw)
            h_s[:, gs] = gelu(up_ref[:, gs]).astype(BF)

    for c in range(n_c):
        cs = slice(c * cw, (c + 1) * cw)
        up_ref[:, cs] = dot(u_s[...], wu_ref[:, cs])
        if c > 0:
            act(c - 1)
    if second is not None:
        second.wait()
    for c in range(n_c):
        cs = slice(c * cw, (c + 1) * cw)
        for n in range(acc_s.shape[1] // nw):
            ns = slice(n * nw, (n + 1) * nw)
            acc_s[:, ns] += dot(h_s[:, cs], wd_ref[cs, ns])
        if c == 0:
            act(n_c - 1)


def norm_rows(x, sl, u_s, acc_s, scale_ref=None):
    scale = lax.rsqrt(jnp.mean(x * x, axis=-1, keepdims=True) + NORM_EPS)
    u_s[sl, :] = (x * scale).astype(BF)
    acc_s[sl, :] = x
    if scale_ref is not None:
        scale_ref[sl, :] = jnp.broadcast_to(scale, (scale.shape[0], scale_ref.shape[1]))


def add_proj(nw, acc_s, mixed, wp_ref):
    for n in range(acc_s.shape[1] // nw):
        ns = slice(n * nw, (n + 1) * nw)
        acc_s[:, ns] += dot(mixed, wp_ref[:, ns])


def first_kernel(cfg, x_hbm, slot_hbm, served_hbm, wg_hbm, wp_hbm, wu_hbm, wd_hbm,
                 x_out_hbm, gate_hbm, fet_hbm,
                 x_s, slot_s, gate_s, fet_s, u_s, acc_s, h_s, up_s, ret_s, wu_s, wd_s, wg_s, wp_s,
                 in_sem, out_sem, w_sem, self_sem, send_sem, recv_sem):
    n_dp, n_emb, cap, n_blk, cw, nw, slab = cfg
    tok, dim = u_s.shape
    my_emb = lax.axis_index('emb')
    my_dp = lax.axis_index('dp')
    here = ret_s.at[:, pl.ds(pl.multiple_of(my_emb * cap, cap), cap), :]
    own = pltpu.make_async_copy(served_hbm.at[:, pl.ds(pl.multiple_of(my_emb * cap, cap), cap), :], here, self_sem)
    peers = [lax.rem(my_emb + k, n_emb) for k in range(1, n_emb)]
    copies = [remote(served_hbm.at[:, pl.ds(pl.multiple_of(p * cap, cap), cap), :], here,
                     send_sem.at[k], recv_sem.at[k], {'dp': my_dp, 'emb': p}) for k, p in enumerate(peers)]
    weights = weight_copies(wu_hbm, wd_hbm, wu_s, wd_s, w_sem)
    first = [pltpu.make_async_copy(x_hbm, x_s, in_sem.at[0]),
             pltpu.make_async_copy(wg_hbm.at[0], wg_s, in_sem.at[1]),
             pltpu.make_async_copy(wp_hbm.at[0], wp_s, in_sem.at[2]),
             pltpu.make_async_copy(slot_hbm, slot_s, in_sem.at[3])]
    start(first[:2])
    start(weights(0, 0, 0))
    start(first[2:])
    meet([{'dp': my_dp, 'emb': p} for p in peers])
    own.start()
    start(copies)
    first[0].wait()
    row_loop(tok, slab)(lambda sl: norm_rows(x_s[sl, :].astype(F32), sl, u_s, acc_s))
    first[1].wait()
    gate_s[0] = dot(u_s[...], wg_s[...])
    gate_out = pltpu.make_async_copy(gate_s, gate_hbm, out_sem.at[0])
    gate_out.start()

    def block(f, carry):
        slot = lax.rem(f, 2)

        @pl.when(f + 1 < n_blk)
        def _():
            start(weights(0, f + 1, 1 - slot))

        up_w, down_w = weights(0, f, slot)
        up_w.wait()
        mlp_block((cw, nw), u_s, h_s, acc_s, wu_s.at[slot], wd_s.at[slot], up_s, down_w)
        return carry

    lax.fori_loop(0, n_blk, block, 0)
    own.wait()
    wait(copies)
    wait(first[2:])
    sel = (lax.broadcasted_iota(I32, (tok, n_emb * cap), 1) == slot_s[...]).astype(BF)
    for l in range(fet_s.shape[0]):
        fet_s[l] = dot(sel, ret_s[l]).astype(BF)
    add_proj(nw, acc_s, (gelu(gate_s[0]) * fet_s[0].astype(F32)).astype(BF), wp_s)
    fet_out = pltpu.make_async_copy(fet_s, fet_hbm, out_sem.at[1])
    fet_out.start()
    outs = []
    for half in range(2):
        rows = pl.ds(half * (tok // 2), tok // 2)

        def finish(sl, half=half):
            sl = pl.ds(sl.start + half * (tok // 2), slab)
            x_s[sl, :] = acc_s[sl, :].astype(BF)

        row_loop(tok // 2, slab)(finish)
        outs.append(pltpu.make_async_copy(x_s.at[rows], x_out_hbm.at[rows], out_sem.at[2 + half]))
        outs[-1].start()
    gate_out.wait()
    fet_out.wait()
    wait(outs)


def forward_kernel(cfg, x_hbm, fet_hbm, wg_hbm, wp_hbm, wu_hbm, wd_hbm, dt_in,
                   out_hbm, saved_hbm, ups_hbm, gate_hbm, dtab_hbm, scale_hbm,
                   x_s, u_s, acc_s, h_s, up_s, zero_s, fet_ref, gate_ref, scale_ref, wu_s, wd_s, wg_s, wp_s,
                   in_sem, w_sem, up_sem, out_sem, z_sem):
    n_layers, n_blk, cw, nw, slab, z_per, z_chunks = cfg
    tok, dim = x_s.shape
    fb = wu_s.shape[2]
    z_rows = zero_s.shape[0]
    n_steps = n_layers * n_blk
    weights = weight_copies(wu_hbm, wd_hbm, wu_s, wd_s, w_sem)

    def z_copies(step):
        found = []
        for j in range(z_per):
            c = step * z_per + j
            zl = c // z_chunks
            found.append(pltpu.make_async_copy(zero_s, dtab_hbm.at[zl + 1, pl.ds((c - zl * z_chunks) * z_rows, z_rows)], z_sem.at[j]))
        return found

    def up_copy(layer, blk, slot):
        return pltpu.make_async_copy(up_s.at[slot], ups_hbm.at[layer, :, pl.ds(pl.multiple_of(blk * fb, fb), fb)], up_sem.at[slot])

    def gate_copy(layer):
        return pltpu.make_async_copy(wg_hbm.at[layer + 1], wg_s, in_sem.at[1])

    def proj_copy(layer):
        return pltpu.make_async_copy(wp_hbm.at[layer + 1], wp_s, in_sem.at[2])

    fetch = pltpu.make_async_copy(x_hbm, x_s, in_sem.at[0])
    fetch.start()
    gate_copy(0).start()
    start(weights(1, 0, 0))
    proj_copy(0).start()
    get_fet = pltpu.make_async_copy(fet_hbm, fet_ref, in_sem.at[3])
    get_fet.start()
    put_scales = pltpu.make_async_copy(scale_ref, scale_hbm, out_sem.at[1])

    def put_gate(layer):
        return pltpu.make_async_copy(gate_ref.at[layer], gate_hbm.at[layer], out_sem.at[2])

    clear_rows(zero_s)
    fetch.wait()
    row_loop(tok, slab)(lambda sl: norm_rows(x_s[sl, :].astype(F32), sl, u_s, acc_s, scale_ref.at[0]))

    def one_layer(layer, carry):
        gate_copy(layer).wait()
        gate_ref[layer] = dot(u_s[...], wg_s[...])
        put_gate(layer).start()

        @pl.when(layer == n_layers - 1)
        def _():
            put_scales.start()

        @pl.when(layer + 1 < n_layers)
        def _():
            gate_copy(layer + 1).start()

        def block(f, carry):
            step = layer * n_blk + f
            slot = lax.rem(step, 2)

            @pl.when(step + 1 < n_steps)
            def _():
                nxt = step + 1
                start(weights(1 + nxt // n_blk, lax.rem(nxt, n_blk), 1 - slot))

            @pl.when(step > 0)
            def _():
                wait(z_copies(step - 1))

            for copy in z_copies(step):
                copy.start(priority=1)

            @pl.when(step > 1)
            def _():
                up_copy(layer, f, slot).wait()

            wait(weights(1 + layer, f, slot))
            mlp_block((cw, nw), u_s, h_s, acc_s, wu_s.at[slot], wd_s.at[slot], up_s.at[slot])
            up_copy(layer, f, slot).start()
            return carry

        lax.fori_loop(0, n_blk, block, 0)
        proj_copy(layer).wait()
        put_gate(layer).wait()

        @pl.when(layer == 0)
        def _():
            get_fet.wait()

        add_proj(nw, acc_s, (gelu(gate_ref[layer]) * fet_ref[layer + 1].astype(F32)).astype(BF), wp_s)

        @pl.when(layer > 0)
        def _():
            pltpu.make_async_copy(x_s, saved_hbm.at[layer - 1], out_sem.at[0]).wait()

        def next_rows(sl):
            x_new = acc_s[sl, :].astype(BF)
            x_s[sl, :] = x_new
            norm_rows(x_new.astype(F32), sl, u_s, acc_s, scale_ref.at[jnp.minimum(layer + 1, n_layers - 1)])

        @pl.when(layer < n_layers - 1)
        def _():
            row_loop(tok, slab)(next_rows)

        @pl.when(layer < n_layers - 1)
        def _():
            pltpu.make_async_copy(x_s, saved_hbm.at[layer], out_sem.at[0]).start()
            proj_copy(layer + 1).start()

        return carry

    lax.fori_loop(0, n_layers, one_layer, 0)
    outs = []
    for half in range(2):
        rows = pl.ds(half * (tok // 2), tok // 2)

        def last_rows(sl, half=half):
            sl = pl.ds(sl.start + half * (tok // 2), slab)
            x_s[sl, :] = acc_s[sl, :].astype(BF)

        row_loop(tok // 2, slab)(last_rows)
        outs.append(pltpu.make_async_copy(x_s.at[rows], out_hbm.at[rows], out_sem.at[2 * half]))
        outs[-1].start()
    wait(z_copies(n_steps - 1))
    up_copy(0, 0, 0).wait()
    up_copy(0, 0, 1).wait()
    put_scales.wait()
    wait(outs)


def gate_grads(gate_pre, fetched, d_mixed, rows_ref, dgp_ref):
    rows_ref[...] = gelu(gate_pre) * d_mixed
    dgp_ref[...] = (d_mixed * fetched.astype(F32) * gelu_slope(gate_pre)).astype(BF)


def to_slots(rows, slot_ref, slots_s):
    hi = rows.astype(BF)
    rest = rows - hi.astype(F32)
    mid = rest.astype(BF)
    low = (rest - mid.astype(F32)).astype(BF)
    n = slots_s.shape[0] * slots_s.shape[2]
    sel = slot_pick(n, slot_ref)
    slots = (dot(sel, hi) + dot(sel, mid)) + dot(sel, low)
    for h in range(slots_s.shape[1]):
        slots_s[:, h] = slots[:, h * 128:(h + 1) * 128].reshape(n // 8, 8, 128)


def slot_pick(n, slot_ref):
    return (lax.broadcasted_iota(I32, (n, slot_ref.shape[1]), 0) == slot_ref[...]).astype(BF)


def backward_kernel(cfg, cot_hbm, x1_hbm, saved_hbm, slot_hbm, gate0_hbm, gates_hbm, fet_hbm, scale_hbm,
                    ups_hbm, wu_hbm, wd_hbm, wg_hbm, wp_hbm,
                    got_hbm, gate_hbm, mixed_hbm,
                    cot_s, x_s, acc_s, dup_s, dh_s, dng_s, slots_s, gslots_s, dslots_s, rows_s, dgp_s, slot_ref, gate0_ref, gate_ref, fet_ref, scale_ref, up_s, wu_s, wd_s, wg_s, wp_s,
                    in_sem, w_sem, up_sem, send_sem, self_sem, recv_sem):
    n_layers, n_blk, n_dp, n_emb, cap, cw, nw, slab = cfg
    tok, dim = cot_s.shape
    fb = wu_s.shape[2]
    gw = 128
    n_dev = n_dp * n_emb
    n_steps = n_layers * n_blk
    my_emb = lax.axis_index('emb')
    me = lax.axis_index('dp') * n_emb + my_emb
    peers = [peer_of(n_emb, lax.rem(me + k, n_dev)) for k in range(1, n_dev)]
    weights = weight_copies(wu_hbm, wd_hbm, wu_s, wd_s, w_sem)

    def part(ref, emb):
        return ref.at[pl.ds(emb * (cap // 8), cap // 8)]

    def sends(ref, there, which, got):
        return [pltpu.make_async_copy(part(ref, my_emb), there, self_sem.at[which])] + [
            remote(part(ref, peer['emb']), there, send_sem.at[which, k], recv_sem.at[got, k], peer) for k, peer in enumerate(peers)]

    def row_sends(i):
        return sends(slots_s, part(got_hbm.at[n_layers - 1 - i], me), 0, i)

    gate_sends = sends(gslots_s, part(gate_hbm, me), 1, n_layers)

    def flat(ref, dev):
        return ref.at[pl.ds(pl.multiple_of(dev * cap, cap), cap), :]

    mixed_sends = [pltpu.make_async_copy(flat(dslots_s, my_emb), flat(mixed_hbm, me), self_sem.at[2])] + [
        remote(flat(dslots_s, peer['emb']), flat(mixed_hbm, me), send_sem.at[2, k], recv_sem.at[n_layers + 1, k], peer)
        for k, peer in enumerate(peers)]

    def up_copy(step, slot):
        i = step // n_blk
        blk = step - i * n_blk
        return pltpu.make_async_copy(ups_hbm.at[n_layers - 1 - i, :, pl.ds(pl.multiple_of(blk * fb, fb), fb)], up_s.at[slot], up_sem.at[slot])

    def load(step, slot):
        i = step // n_blk
        return weights(n_layers - i, step - i * n_blk, slot) + (up_copy(step, slot),)

    def gate_copy(i):
        return pltpu.make_async_copy(wg_hbm.at[n_layers - i], wg_s, in_sem.at[1])

    def proj_copy(i):
        return pltpu.make_async_copy(wp_hbm.at[n_layers - 1 - i], wp_s, in_sem.at[2])

    def x_copy(i):
        return pltpu.make_async_copy(saved_hbm.at[n_layers - 2 - i], x_s, in_sem.at[3])

    fetch = pltpu.make_async_copy(cot_hbm, cot_s, in_sem.at[0])
    top = n_layers - 1
    soon = [pltpu.make_async_copy(src, dst, in_sem.at[4 + k]) for k, (src, dst) in enumerate(
        ((gate0_hbm, gate0_ref), (slot_hbm, slot_ref), (gates_hbm.at[top], gate_ref.at[top]), (fet_hbm.at[top + 1], fet_ref.at[top + 1])))]
    later = [pltpu.make_async_copy(src, dst, in_sem.at[8 + k]) for k, (src, dst) in enumerate(
        ((gates_hbm.at[pl.ds(0, top)], gate_ref.at[pl.ds(0, top)]), (fet_hbm.at[pl.ds(0, top + 1)], fet_ref.at[pl.ds(0, top + 1)]),
         (scale_hbm, scale_ref)))]
    start(soon[:2])
    fetch.start()
    proj_copy(-1).start()
    start(soon[2:])
    gate_copy(0).start()
    start(load(0, 0))
    start(later)

    def clear(sl):
        acc_s[sl, :] = jnp.zeros((slab, dim), F32)

    row_loop(tok, slab)(clear)
    meet(peers)
    wait(soon[:2])
    to_slots(gelu(gate0_ref[0]), slot_ref, gslots_s)
    fetch.wait()
    proj_copy(-1).wait()
    wait(soon[2:])
    gate_grads(gate_ref[n_layers - 1], fet_ref[n_layers], dot_t(cot_s[...], wp_s[...]).astype(BF).astype(F32), rows_s, dgp_s)
    proj_copy(0).start()

    def one_layer(i, carry):
        @pl.when(i < n_layers - 1)
        def _():
            x_copy(i).start()

        @pl.when(i == n_layers - 1)
        def _():
            pltpu.make_async_copy(x1_hbm, x_s, in_sem.at[3]).start()

        gate_copy(i).wait()
        to_slots(rows_s[...], slot_ref, slots_s)
        for n in range(dim // nw):
            ns = slice(n * nw, (n + 1) * nw)
            dng_s[:, ns] = dot_t(dgp_s[...], wg_s[ns, :]).astype(BF)
        start(row_sends(i))

        @pl.when(i < n_layers - 1)
        def _():
            gate_copy(i + 1).start()

        @pl.when(i == 0)
        def _():
            start(gate_sends)

        def block(f, carry):
            step = i * n_blk + f
            slot = lax.rem(step, 2)

            @pl.when(step + 1 < n_steps)
            def _():
                start(load(step + 1, 1 - slot))

            wait(load(step, slot))
            wu_ref, wd_ref, up_ref = wu_s.at[slot], wd_s.at[slot], up_s.at[slot]

            def act(c):
                for g in range(cw // gw):
                    gs = slice(c * cw + g * gw, c * cw + (g + 1) * gw)
                    dup_s[:, gs] = (dh_s[:, gs].astype(F32) * gelu_slope(up_ref[:, gs])).astype(BF)

            n_c = fb // cw
            for c in range(n_c):
                cs = slice(c * cw, (c + 1) * cw)
                dh_s[:, cs] = dot_t(cot_s[...], wd_ref[cs, :]).astype(BF)
                if c > 0:
                    act(c - 1)
            for c in range(n_c):
                cs = slice(c * cw, (c + 1) * cw)
                for n in range(dim // nw):
                    ns = slice(n * nw, (n + 1) * nw)
                    acc_s[:, ns] += dot_t(dup_s[:, cs], wu_ref[ns, cs])
                if c == 0:
                    act(n_c - 1)
            return carry

        lax.fori_loop(0, n_blk, block, 0)
        pltpu.make_async_copy(x1_hbm, x_s, in_sem.at[3]).wait()

        @pl.when(i == 0)
        def _():
            wait(later)


        def rows_back(sl):
            x = x_s[sl, :].astype(F32)
            scale = scale_ref[n_layers - 1 - i, sl, 0:1]
            d_n = (acc_s[sl, :].astype(BF) + dng_s[sl, :]).astype(F32)
            acc_s[sl, :] = jnp.zeros((slab, dim), F32)
            proj = jnp.mean(d_n * x, axis=-1, keepdims=True)
            d_x = d_n * scale - x * (proj * (scale * scale * scale))
            cot_s[sl, :] = (cot_s[sl, :].astype(F32) + d_x).astype(BF)

        row_loop(tok, slab)(rows_back)
        proj_copy(i).wait()
        d_mixed = dot_t(cot_s[...], wp_s[...]).astype(BF)

        @pl.when(i == n_layers - 1)
        def _():
            dslots_s[...] = dot(slot_pick(n_emb * cap, slot_ref), d_mixed).astype(BF)

        wait(row_sends(i))

        @pl.when(i < n_layers - 1)
        def _():
            proj_copy(i + 1).start()
            gate_grads(gate_ref[jnp.maximum(n_layers - 2 - i, 0)], fet_ref[n_layers - 1 - i], d_mixed.astype(F32), rows_s, dgp_s)

        return carry

    lax.fori_loop(0, n_layers, one_layer, 0)
    start(mixed_sends)
    wait(gate_sends)
    wait(mixed_sends)


def order_rows(recv_ref, counts_ref, slot_bits, read_ref, write_ref, group_ref, meta_ref):
    n_dev, cap = recv_ref.shape
    shape = (n_dev, cap)
    square = (cap, cap)
    dev, lane = lax.broadcasted_iota(I32, shape, 0), lax.broadcasted_iota(I32, shape, 1)
    down, right = lax.broadcasted_iota(I32, square, 0), lax.broadcasted_iota(I32, square, 1)
    counts = counts_ref[:, 0:1]
    key = jnp.where(lane < counts, jnp.left_shift(recv_ref[...], slot_bits), 1 << 30) + dev * cap + lane

    def ones(cond):
        return jnp.where(cond, 1.0, 0.0)

    def digit(k):
        return jnp.bitwise_and(jnp.right_shift(key, 8 * k), 255).astype(F32).astype(BF)

    digits = [digit(k) for k in range(4)]
    same = ones(down == right).astype(BF)
    turned = sum(jnp.left_shift(dot_t(same, d).astype(I32), 8 * k) for k, d in enumerate(digits))
    rows = jnp.concatenate([d[None] for d in digits], axis=0)
    found = [jnp.zeros((8, cap), F32) for _ in range(n_dev)]
    for d in range(n_dev):
        column = turned[:, d:d + 1]
        smaller = sum(ones(key[e:e + 1, :] < column) for e in range(n_dev))
        rank = jnp.sum(smaller, axis=1, keepdims=True)
        mine = jnp.concatenate([rows[k, d:d + 1, :] for k in range(4)] * 2, axis=0)
        for w in range(n_dev):
            found[w] = found[w] + dot(mine, ones(rank - (w * cap) == right.astype(F32)).astype(BF))
    merged = [sum(jnp.left_shift(f[k:k + 1].astype(I32), 8 * k) for k in range(4)) for f in found]
    ordered = jnp.concatenate(merged, axis=0)

    before = pltpu.roll(ordered, 1, 1)
    before = jnp.where(lane == 0, pltpu.roll(before, 1, 0), before)
    after = pltpu.roll(ordered, cap - 1, 1)
    after = jnp.where(lane == cap - 1, pltpu.roll(after, n_dev - 1, 0), after)
    total = jnp.sum(counts_ref[...].astype(F32), axis=0, keepdims=True).astype(I32)
    place_in = dev * cap + lane
    live = place_in < total[:, 0:1]
    slot = jnp.bitwise_and(ordered, (1 << slot_bits) - 1)
    row = jnp.right_shift(ordered, slot_bits)
    group = jnp.right_shift(ordered, slot_bits + 3)
    begin, end = place_in == 0, place_in == n_dev * cap - 1
    same_row = jnp.logical_and(row == jnp.right_shift(before, slot_bits), jnp.logical_not(begin))
    fresh = jnp.logical_or(group != jnp.right_shift(before, slot_bits + 3), begin)
    last = jnp.logical_and(jnp.logical_or(group != jnp.right_shift(after, slot_bits + 3), end), live)
    place = dot(ones(fresh).astype(BF), ones(down <= right).astype(BF)).astype(I32)
    place = place - place[:, 0:1]
    read_ref[...] = jnp.right_shift(slot, 3) * 16 + jnp.bitwise_and(slot, 7) + jnp.where(same_row, -(1 << 31), 0)
    write_ref[...] = place * 16 + jnp.bitwise_and(row, 7)
    group_ref[...] = jnp.where(live, group, 0)
    n_out = jnp.sum(ones(last), axis=1, keepdims=True).astype(I32)
    goes_on = jnp.where(jnp.logical_and(jnp.logical_not(fresh), live), 1, 0)[:, 0:1]
    meta_lane = lax.broadcasted_iota(I32, meta_ref.shape, 1)
    meta = jnp.where(meta_lane == 0, n_out, jnp.where(meta_lane == 1, place[:, cap - 1:cap], goes_on))
    meta_ref[...] = jnp.where(meta_lane == 3, total, meta)


def scatter_kernel(cfg, read_ref, write_ref, group_ref, meta_ref, rows_hbm, gate_hbm, mixed_hbm, dt_in, dt_out,
                   rows_ref, gate_ref, mixed_ref, groups, prod, spots, sems, in_sem):
    unroll, bulk = cfg
    n_layers, window = groups.shape[1:3]
    n_slots = mixed_ref.shape[0]
    n_win = n_slots // window
    count = meta_ref[0, 3]
    loads = [pltpu.make_async_copy(src, dst, in_sem.at[k]) for k, (src, dst) in enumerate(
        ((gate_hbm, gate_ref), (mixed_hbm, mixed_ref), (rows_hbm, rows_ref)))]
    start(loads)
    wait(loads[:2])

    def product(i, carry):
        step = 64
        mixed = mixed_ref[pl.ds(pl.multiple_of(i * step, step), step), :].astype(F32)
        for h in range(2):
            at = pl.ds(i * (step // 8), step // 8)
            prod[at, h] = gate_ref[at, h] * mixed[:, h * 128:(h + 1) * 128].reshape(step // 8, 8, 128)
        return carry

    lax.fori_loop(0, n_slots // 64, product, 0, unroll=4)

    def move(buf, spot, group, n):
        return pltpu.make_async_copy(groups.at[buf, :, pl.ds(spot, n)], dt_out.at[:, pl.ds(group, n)], sems.at[buf])

    def each(n, k, body):
        def trip(t, carry):
            for i in range(k):
                body(t * k + i)
            return carry

        def one(i, carry):
            body(i)
            return carry

        full = n // k
        lax.fori_loop(0, full, trip, 0)
        lax.fori_loop(full * k, n, one, 0)

    def settle(w):
        n = meta_ref[w, 0]

        def drain_bulk(j, carry):
            move(w % 2, 0, 0, bulk).wait()
            return carry

        def drain(j, carry):
            move(w % 2, 0, 0, 1).wait()
            return carry

        lax.fori_loop(0, n // bulk, drain_bulk, 0)
        lax.fori_loop(0, lax.rem(n, bulk), drain, 0)

    blank = jnp.zeros(groups.shape[3:], F32)
    accs = tuple(jnp.zeros((2, 128), F32) for _ in range(n_layers))
    for w in range(n_win):
        buf = w % 2
        if w >= 2:
            settle(w - 2)
        left = jnp.clip(count - w * window, 0, window)
        trips = (left + (unroll - 1)) // unroll
        n_out = meta_ref[w, 0]

        def clear(u, buf=buf):
            for l in range(n_layers):
                groups[buf, l, u] = blank

        each(jnp.where(left > 0, jnp.minimum(n_out + 1, window), 0), 4, clear)
        if w == 0:
            wait(loads[2:])
        else:
            @pl.when(meta_ref[w, 2] > 0)
            def _(w=w, buf=buf):
                for l in range(n_layers):
                    groups[buf, l, 0] = groups[1 - buf, l, meta_ref[w - 1, 1]]

        sums = [groups.at[buf, l].reshape(window * 16, 128) for l in range(n_layers)]
        rows = [prod.reshape(n_slots * 2, 128)] + [rows_ref.at[l] for l in range(n_layers - 1)]

        def add(t, accs, w=w, sums=sums, rows=rows):
            for k in range(unroll):
                j = t * unroll + k
                word = read_ref[w, j]
                at = jnp.bitwise_and(word, n_slots * 2 - 1)
                same = word < 0
                to = write_ref[w, j]
                spots[jnp.right_shift(to, 4)] = group_ref[w, j]
                accs = tuple(jnp.where(same, acc, 0.0) + src[pl.ds(at, 2, stride=8), :] for acc, src in zip(accs, rows))
                for acc, dst in zip(accs, sums):
                    dst[pl.ds(to, 2, stride=8), :] = acc
            return accs

        accs = lax.fori_loop(0, trips, add, accs)
        each(n_out, 8, lambda u, buf=buf: move(buf, u, spots[u], 1).start())
    for w in range(max(n_win - 2, 0), n_win):
        settle(w)


def solution(mesh):
    n_emb, n_dp = mesh.shape['emb'], mesh.shape['dp']
    n_dev = n_emb * n_dp
    tok_spec = P(('dp', 'emb'))
    act_spec = P(('dp', 'emb'), None)
    table_spec = P(None, 'emb', None)
    full_spec = P(None, None, None)
    hbm = pl.BlockSpec(memory_space=pl.ANY)
    vm = pl.BlockSpec(memory_space=pltpu.VMEM)
    sm = pl.BlockSpec(memory_space=pltpu.SMEM)
    big = jnp.iinfo(jnp.int32).max

    def params(n_grid, **kw):
        return pltpu.CompilerParams(vmem_limit_bytes=VMEM_BYTES, dimension_semantics=('arbitrary',) * n_grid if n_grid else None, **kw)

    def device_body(tok_ids, resid_in, cot_out, tables, w_up, w_down, w_gate, w_proj):
        n_layers, range_rows, e_dim = tables.shape
        tok = tok_ids.shape[0]
        dim, ffn = w_up.shape[1:]
        n_slots, n_serve = n_dev * CAP, n_emb * CAP
        my_emb, my_dp = lax.axis_index('emb'), lax.axis_index('dp')

        lanes = 128
        per_dot, dots = 32, 2
        dma = pltpu.SemaphoreType.DMA
        _, recv_loc, counts, pick, slot_row, slot_col = pl.pallas_call(
            functools.partial(plan_kernel, (n_dp, n_emb, CAP, range_rows, per_dot)),
            out_shape=[jax.ShapeDtypeStruct(shape, I32) for shape in (
                (n_dev, tok // lanes, lanes), (n_dev, CAP), (n_dev, lanes), (n_serve, 1), (1, tok), (tok, 1))],
            in_specs=[vm], out_specs=[vm] * 6,
            scratch_shapes=[pltpu.VMEM((n_dev, tok), F32), dma((n_dev - 1,)), dma((n_dev - 1,))],
            compiler_params=pltpu.CompilerParams(collective_id=0, has_side_effects=True),
            name='plan',
        )(tok_ids.reshape(tok // lanes, lanes))
        slot_bits = (n_slots - 1).bit_length()
        tab_shape = (n_layers, range_rows // 8, e_dim // 128, 8, 128)
        z_rows = 167
        z_chunks = tab_shape[1] // z_rows
        words = [jax.ShapeDtypeStruct((n_dev, CAP), I32)] * 3 + [jax.ShapeDtypeStruct((n_dev, lanes), I32)]
        served, dtab, read_word, write_word, group_word, meta = pl.pallas_call(
            functools.partial(gather_kernel, (n_layers, n_emb, CAP, per_dot, dots, z_chunks, slot_bits)),
            out_shape=[jax.ShapeDtypeStruct((n_layers, n_serve, e_dim), BF), jax.ShapeDtypeStruct(tab_shape, F32)] + words,
            in_specs=[sm, sm, vm, vm, vm, hbm],
            out_specs=[vm, hbm, vm, vm, vm, vm],
            scratch_shapes=[pltpu.VMEM((n_layers, n_serve * 8, e_dim), BF), pltpu.VMEM((z_rows,) + tab_shape[2:], F32), dma((n_emb,)), dma],
            compiler_params=params(0),
            name='table_rows',
        )(recv_loc, counts, recv_loc, counts, pick, tables)

        fb = 1024
        n_blk = ffn // fb
        cw, nw, slab = 512, 512, 32
        n_back = n_layers - 1
        z_per = z_chunks // n_blk
        assert z_chunks * z_rows == tab_shape[1] and z_per * n_blk == z_chunks
        matmul_flops = 4 * tok * dim * ffn
        w_bufs = [pltpu.VMEM((2, dim, fb), BF), pltpu.VMEM((2, fb, dim), BF), pltpu.VMEM((dim, e_dim), BF), pltpu.VMEM((e_dim, dim), BF)]
        x1, gate0, fetched = pl.pallas_call(
            functools.partial(first_kernel, (n_dp, n_emb, CAP, n_blk, cw, nw, slab)),
            out_shape=[
                jax.ShapeDtypeStruct((tok, dim), BF),
                jax.ShapeDtypeStruct((1, tok, e_dim), F32),
                jax.ShapeDtypeStruct((n_layers, tok, e_dim), BF),
            ],
            in_specs=[hbm] * 7,
            out_specs=[hbm] * 3,
            scratch_shapes=[
                pltpu.VMEM((tok, dim), BF), pltpu.VMEM((tok, 1), I32), pltpu.VMEM((1, tok, e_dim), F32), pltpu.VMEM((n_layers, tok, e_dim), BF),
                pltpu.VMEM((tok, dim), BF), pltpu.VMEM((tok, dim), F32), pltpu.VMEM((tok, fb), BF), pltpu.VMEM((tok, fb), F32),
                pltpu.VMEM((n_layers, n_serve, e_dim), BF), *w_bufs,
                dma((4,)), dma((4,)), dma((2, 2)), dma, dma((n_emb - 1,)), dma((n_emb - 1,)),
            ],
            compiler_params=params(0, collective_id=1, has_side_effects=True),
            cost_estimate=pl.CostEstimate(flops=matmul_flops, bytes_accessed=100 << 20, transcendentals=0),
            name='first_layer',
        )(resid_in, slot_col, served, w_gate, w_proj, w_up, w_down)

        out, saved, ups, gates, dtab, scales = pl.pallas_call(
            functools.partial(forward_kernel, (n_back, n_blk, cw, nw, slab, z_per, z_chunks)),
            out_shape=[
                jax.ShapeDtypeStruct((tok, dim), BF),
                jax.ShapeDtypeStruct((n_back - 1, tok, dim), BF),
                jax.ShapeDtypeStruct((n_back, tok, ffn), F32),
                jax.ShapeDtypeStruct((n_back, tok, e_dim), F32),
                jax.ShapeDtypeStruct(tab_shape, F32),
                jax.ShapeDtypeStruct((n_back, tok, lanes), F32),
            ],
            in_specs=[hbm] * 7,
            out_specs=[hbm] * 6,
            input_output_aliases={6: 4},
            scratch_shapes=[
                pltpu.VMEM((tok, dim), BF), pltpu.VMEM((tok, dim), BF), pltpu.VMEM((tok, dim), F32), pltpu.VMEM((tok, fb), BF),
                pltpu.VMEM((2, tok, fb), F32), pltpu.VMEM((z_rows,) + tab_shape[2:], F32),
                pltpu.VMEM((n_layers, tok, e_dim), BF), pltpu.VMEM((n_back, tok, e_dim), F32), pltpu.VMEM((n_back, tok, lanes), F32), *w_bufs,
                dma((4,)), dma((2, 2)), dma((2,)), dma((4,)), dma((z_per,)),
            ],
            compiler_params=params(0),
            cost_estimate=pl.CostEstimate(flops=n_back * matmul_flops, bytes_accessed=400 << 20, transcendentals=0),
            name='forward',
        )(x1, fetched, w_gate, w_proj, w_up, w_down, dtab)

        got, got_gate, mixed0 = pl.pallas_call(
            functools.partial(backward_kernel, (n_back, n_blk, n_dp, n_emb, CAP, cw, nw, slab)),
            out_shape=[jax.ShapeDtypeStruct((n_back, n_slots // 8, e_dim // 128, 8, 128), F32), jax.ShapeDtypeStruct((n_slots // 8, e_dim // 128, 8, 128), F32),
                       jax.ShapeDtypeStruct((n_slots, e_dim), BF)],
            in_specs=[hbm] * 13,
            out_specs=[hbm, hbm, hbm],
            scratch_shapes=[
                pltpu.VMEM((tok, dim), BF), pltpu.VMEM((tok, dim), BF), pltpu.VMEM((tok, dim), F32), pltpu.VMEM((tok, fb), BF), pltpu.VMEM((tok, fb), BF),
                pltpu.VMEM((tok, dim), BF), pltpu.VMEM((n_serve // 8, e_dim // 128, 8, 128), F32), pltpu.VMEM((n_serve // 8, e_dim // 128, 8, 128), F32),
                pltpu.VMEM((n_serve, e_dim), BF), pltpu.VMEM((tok, e_dim), F32), pltpu.VMEM((tok, e_dim), BF), pltpu.VMEM((1, tok), I32),
                pltpu.VMEM((1, tok, e_dim), F32), pltpu.VMEM((n_back, tok, e_dim), F32), pltpu.VMEM((n_layers, tok, e_dim), BF),
                pltpu.VMEM((n_back, tok, lanes), F32), pltpu.VMEM((2, tok, fb), F32), *w_bufs,
                dma((11,)), dma((2, 2)), dma((2,)), dma((3, n_dev - 1)), dma((3,)), dma((n_back + 2, n_dev - 1)),
            ],
            compiler_params=params(0, collective_id=2, has_side_effects=True),
            cost_estimate=pl.CostEstimate(flops=n_back * matmul_flops, bytes_accessed=400 << 20, transcendentals=0),
            name='backward',
        )(cot_out, x1, saved, slot_row, gate0, gates, fetched, scales, ups, w_up, w_down, w_gate, w_proj)

        dtab = pl.pallas_call(
            functools.partial(scatter_kernel, (8, 32)),
            out_shape=jax.ShapeDtypeStruct(dtab.shape, F32),
            in_specs=[sm, sm, sm, sm, hbm, hbm, hbm, hbm],
            out_specs=hbm,
            input_output_aliases={7: 0},
            scratch_shapes=[pltpu.VMEM((n_back, n_slots * 2, 128), F32), pltpu.VMEM((n_slots // 8,) + tab_shape[2:], F32),
                            pltpu.VMEM((n_slots, e_dim), BF), pltpu.VMEM((2, n_layers, CAP) + tab_shape[2:], F32),
                            pltpu.VMEM((n_slots // 8,) + tab_shape[2:], F32), pltpu.SMEM((CAP,), I32), dma((2,)), dma((3,))],
            compiler_params=params(0),
            name='scatter',
        )(read_word, write_word, group_word, meta, got.reshape(n_back, n_slots * 2, 128), got_gate, mixed0, dtab)
        dtab = dtab.transpose(0, 1, 3, 2, 4).reshape(n_layers, range_rows, e_dim)
        return out, dtab

    return jax.shard_map(device_body, mesh=mesh, in_specs=(tok_spec, act_spec, act_spec, table_spec, full_spec, full_spec, full_spec, full_spec), out_specs=(act_spec, table_spec), check_vma=False)
```

```python
import functools

import jax
import jax.numpy as jnp
from jax import lax
from jax.experimental import pallas as pl
from jax.experimental.pallas import tpu as pltpu
from jax.sharding import PartitionSpec as P

NORM_EPS = 1e-6
BF = jnp.bfloat16
F32 = jnp.float32
I32 = jnp.int32
VMEM_BYTES = 67043328
GELU_C = 0.7978845608028654
GELU_A = 0.044715

MESH_AXES = ('dp', 'emb')
CAP = 256


def gelu(x):
    return 0.5 * x * (1.0 + jnp.tanh(GELU_C * (x + GELU_A * (x * x * x))))


def gelu_slope(x):
    sq = x * x
    th = jnp.tanh(GELU_C * (x + GELU_A * (x * sq)))
    return 0.5 * (1.0 + th) + (0.5 * GELU_C) * x * (1.0 - th * th) * (1.0 + (3 * GELU_A) * sq)


def dot(a, b):
    return jnp.dot(a, b, preferred_element_type=F32)


def dot_t(a, b):
    return lax.dot_general(a, b, (((1,), (1,)), ((), ())), preferred_element_type=F32)


def row_loop(rows, slab, unroll=1):
    def run(body):
        def step(i, carry):
            body(pl.ds(pl.multiple_of(i * slab, slab), slab))
            return carry

        lax.fori_loop(0, rows // slab, step, 0, unroll=unroll)

    return run


def peer_of(n_emb, index):
    dp = index // n_emb
    return {'dp': dp, 'emb': index - dp * n_emb}


def remote(src, dst, send_sem, recv_sem, device):
    return pltpu.make_async_remote_copy(src_ref=src, dst_ref=dst, send_sem=send_sem, recv_sem=recv_sem,
                                        device_id=device, device_id_type=pl.DeviceIdType.MESH)


def meet(devices):
    barrier = pltpu.get_barrier_semaphore()
    for device in devices:
        pl.semaphore_signal(barrier, inc=1, device_id=device, device_id_type=pl.DeviceIdType.MESH)
    pl.semaphore_wait(barrier, len(devices))


def plan_kernel(cfg, in_ref, ids_ref, recv_ref, counts_ref, pick_ref, slot_row_ref, slot_col_ref, rank_s, send_sem, recv_sem):
    n_dp, n_emb, cap, range_rows, per_dot = cfg
    n_dev = n_dp * n_emb
    my_dp, my_emb = lax.axis_index('dp'), lax.axis_index('emb')
    me = my_dp * n_emb + my_emb
    n_sub, lanes = in_ref.shape
    tok = n_sub * lanes
    peers = [peer_of(n_emb, lax.rem(me + k, n_dev)) for k in range(1, n_dev)]
    meet(peers)
    copies = [remote(in_ref, ids_ref.at[me], send_sem.at[k], recv_sem.at[k], peer) for k, peer in enumerate(peers)]
    start(copies)
    ids_ref[me] = in_ref[...]

    def line(ref):
        return jnp.concatenate([ref[..., j, :] for j in range(n_sub)], axis=-1)

    def ones(cond):
        return jnp.where(cond, 1.0, 0.0)

    def digits(x):
        return jnp.concatenate([jnp.right_shift(x, 8), jnp.bitwise_and(x, 255)], axis=0).astype(F32).astype(BF)

    square = (tok, tok)
    down, right = lax.broadcasted_iota(I32, square, 0), lax.broadcasted_iota(I32, square, 1)
    earlier = ones(down < right).astype(BF)
    own = jnp.broadcast_to(jnp.concatenate([in_ref[j:j + 1, :] for j in range(n_sub)], axis=-1), (8, tok))
    owner = sum(jnp.where(own >= e * range_rows, 1, 0) for e in range(1, n_emb))
    is_owner = owner == lax.broadcasted_iota(I32, (8, tok), 0)
    own_rank = dot(ones(is_owner).astype(BF), earlier).astype(I32)
    slot_row = jnp.sum(jnp.where(is_owner, own_rank + owner * cap, 0).astype(F32), axis=0, keepdims=True).astype(I32)
    slot_row_ref[...] = slot_row
    turned = dot_t(ones(down == right).astype(BF), digits(jnp.broadcast_to(slot_row, (8, tok))))
    slot_col_ref[...] = (turned[:, 0:1] * 256.0 + turned[:, 8:9]).astype(I32)

    wait(copies)
    ids8 = line(ids_ref)
    low = my_emb * range_rows
    mine = jnp.logical_and(ids8 >= low, ids8 < low + range_rows)
    mine_f = ones(mine)
    rank_s[...] = jnp.where(mine, dot(mine_f.astype(BF), earlier), -1.0)
    counts = jnp.sum(mine_f, axis=1, keepdims=True).astype(I32)
    counts_ref[...] = jnp.broadcast_to(counts, counts_ref.shape)
    loc = digits(jnp.where(mine, ids8 - low, 0))
    c_iota = lax.broadcasted_iota(I32, (cap, tok), 0).astype(F32)
    dev_iota = lax.broadcasted_iota(I32, (n_dev, cap), 0)
    recv = jnp.zeros((n_dev, cap), F32)
    for d in range(n_dev):
        found = dot_t(loc, ones(rank_s[d:d + 1, :] == c_iota).astype(BF))
        recv = jnp.where(dev_iota == d, found[:n_dev] * 256.0 + found[n_dev:], recv)
    slot = dev_iota * cap + lax.broadcasted_iota(I32, (n_dev, cap), 1)
    recv_ref[...] = jnp.where(slot - dev_iota * cap < counts, recv.astype(I32), slot * 8)
    lane16 = lax.broadcasted_iota(I32, (cap, 2 * n_dev), 1)
    row1 = lax.broadcasted_iota(I32, (cap, 1), 0)
    for e in range(n_emb):
        d = my_dp * n_emb + e
        found = dot_t(ones(rank_s[pl.ds(d, 1), :] == c_iota).astype(BF), loc)
        low8 = jnp.sum(jnp.where(lane16 == n_dev + d, found, 0.0), axis=1, keepdims=True).astype(I32)
        pick_ref[e * cap:(e + 1) * cap, :] = jnp.bitwise_and(low8, 7) + 8 * jnp.bitwise_and(row1, per_dot - 1)


def gather_kernel(cfg, loc_ref, counts_ref, recv_ref, tally_ref, pick_ref, tables_hbm,
                  out_ref, dtab_hbm, read_ref, write_ref, group_ref, meta_ref, buf, zero_s, sems, z_sem):
    n_layers, n_dest, cap, per_dot, group, z_chunks, slot_bits = cfg
    trip = per_dot * group
    z_rows = zero_s.shape[0]
    first = lax.axis_index('dp') * n_dest
    n_trips = [(counts_ref[first + d, 0] + (trip - 1)) // trip for d in range(n_dest)]

    def row_copy(d, c):
        base = pl.multiple_of(jnp.left_shift(jnp.right_shift(loc_ref[first + d, c], 3), 3), 8)
        at = pl.multiple_of(d * cap * 8 + c * 8, 8)
        return pltpu.make_async_copy(tables_hbm.at[:, pl.ds(base, 8), :], buf.at[:, pl.ds(at, 8), :], sems.at[d])

    def z_copy(c):
        return pltpu.make_async_copy(zero_s, dtab_hbm.at[0, pl.ds(c * z_rows, z_rows)], z_sem)

    for d in range(n_dest):
        def issue(i, carry, d=d):
            for k in range(8):
                row_copy(d, i * 8 + k).start()
            return carry

        lax.fori_loop(0, n_trips[d] * (trip // 8), issue, 0)

    clear_rows(zero_s)

    def z_start(c, carry):
        z_copy(c).start(priority=1)
        return carry

    lax.fori_loop(0, z_chunks, z_start, 0)
    order_rows(recv_ref, tally_ref, slot_bits, read_ref, write_ref, group_ref, meta_ref)
    for d in range(n_dest):
        def drain(i, carry, d=d):
            part = buf.at[:, pl.ds(pl.multiple_of((d * cap + i * trip) * 8, 8), trip * 8), :]
            pltpu.make_async_copy(part, part, sems.at[d]).wait()
            return carry

        lax.fori_loop(0, n_trips[d], drain, 0)

        def pick(i, carry, d=d):
            for k in range(group):
                s0 = pl.multiple_of(d * cap + i * trip + k * per_dot, per_dot)
                want = pick_ref[pl.ds(s0, per_dot), :]
                sel = (lax.broadcasted_iota(I32, (per_dot, per_dot * 8), 1) == want).astype(BF)
                for l in range(n_layers):
                    rows = buf[l, pl.ds(pl.multiple_of(s0 * 8, 8), per_dot * 8), :]
                    out_ref[l, pl.ds(s0, per_dot), :] = dot(sel, rows).astype(BF)
            return carry

        lax.fori_loop(0, n_trips[d], pick, 0)

        def blank(i, carry, d=d):
            s0 = pl.multiple_of(d * cap + i * trip, trip)
            for l in range(n_layers):
                out_ref[l, pl.ds(s0, trip), :] = jnp.zeros((trip, out_ref.shape[2]), BF)
            return carry

        lax.fori_loop(n_trips[d], cap // trip, blank, 0)

    def z_wait(c, carry):
        z_copy(c).wait()
        return carry

    lax.fori_loop(0, z_chunks, z_wait, 0)


def clear_rows(ref):
    def clear(i, carry):
        ref[i] = jnp.zeros(ref.shape[1:], F32)
        return carry

    lax.fori_loop(0, ref.shape[0], clear, 0)


def weight_copies(wu_hbm, wd_hbm, wu_s, wd_s, sems):
    fb = wu_s.shape[2]

    def copies(layer, blk, slot):
        at = pl.multiple_of(blk * fb, fb)
        return (pltpu.make_async_copy(wu_hbm.at[layer, :, pl.ds(at, fb)], wu_s.at[slot], sems.at[0, slot]),
                pltpu.make_async_copy(wd_hbm.at[layer, pl.ds(at, fb), :], wd_s.at[slot], sems.at[1, slot]))

    return copies


def start(copies):
    for copy in copies:
        copy.start()


def wait(copies):
    for copy in copies:
        copy.wait()


def mlp_block(cfg, u_s, h_s, acc_s, wu_ref, wd_ref, up_ref, second=None):
    cw, nw = cfg
    gw = 128
    n_c = wu_ref.shape[1] // cw

    def act(c):
        for g in range(cw // gw):
            gs = slice(c * cw + g * gw, c * cw + (g + 1) * gw)
            h_s[:, gs] = gelu(up_ref[:, gs]).astype(BF)

    for c in range(n_c):
        cs = slice(c * cw, (c + 1) * cw)
        up_ref[:, cs] = dot(u_s[...], wu_ref[:, cs])
        if c > 0:
            act(c - 1)
    if second is not None:
        second.wait()
    for c in range(n_c):
        cs = slice(c * cw, (c + 1) * cw)
        for n in range(acc_s.shape[1] // nw):
            ns = slice(n * nw, (n + 1) * nw)
            acc_s[:, ns] += dot(h_s[:, cs], wd_ref[cs, ns])
        if c == 0:
            act(n_c - 1)


def norm_rows(x, sl, u_s, acc_s, scale_ref=None):
    scale = lax.rsqrt(jnp.mean(x * x, axis=-1, keepdims=True) + NORM_EPS)
    u_s[sl, :] = (x * scale).astype(BF)
    acc_s[sl, :] = x
    if scale_ref is not None:
        scale_ref[sl, :] = jnp.broadcast_to(scale, (scale.shape[0], scale_ref.shape[1]))


def add_proj(nw, acc_s, mixed, wp_ref):
    for n in range(acc_s.shape[1] // nw):
        ns = slice(n * nw, (n + 1) * nw)
        acc_s[:, ns] += dot(mixed, wp_ref[:, ns])


def first_kernel(cfg, x_hbm, slot_hbm, served_hbm, wg_hbm, wp_hbm, wu_hbm, wd_hbm,
                 x_out_hbm, gate_hbm, fet_hbm,
                 x_s, slot_s, gate_s, fet_s, u_s, acc_s, h_s, up_s, ret_s, wu_s, wd_s, wg_s, wp_s,
                 in_sem, out_sem, w_sem, self_sem, send_sem, recv_sem):
    n_dp, n_emb, cap, n_blk, cw, nw, slab = cfg
    tok, dim = u_s.shape
    my_emb = lax.axis_index('emb')
    my_dp = lax.axis_index('dp')
    here = ret_s.at[:, pl.ds(pl.multiple_of(my_emb * cap, cap), cap), :]
    own = pltpu.make_async_copy(served_hbm.at[:, pl.ds(pl.multiple_of(my_emb * cap, cap), cap), :], here, self_sem)
    peers = [lax.rem(my_emb + k, n_emb) for k in range(1, n_emb)]
    copies = [remote(served_hbm.at[:, pl.ds(pl.multiple_of(p * cap, cap), cap), :], here,
                     send_sem.at[k], recv_sem.at[k], {'dp': my_dp, 'emb': p}) for k, p in enumerate(peers)]
    weights = weight_copies(wu_hbm, wd_hbm, wu_s, wd_s, w_sem)
    first = [pltpu.make_async_copy(x_hbm, x_s, in_sem.at[0]),
             pltpu.make_async_copy(wg_hbm.at[0], wg_s, in_sem.at[1]),
             pltpu.make_async_copy(wp_hbm.at[0], wp_s, in_sem.at[2]),
             pltpu.make_async_copy(slot_hbm, slot_s, in_sem.at[3])]
    start(first[:2])
    start(weights(0, 0, 0))
    start(first[2:])
    meet([{'dp': my_dp, 'emb': p} for p in peers])
    own.start()
    start(copies)
    first[0].wait()
    row_loop(tok, slab)(lambda sl: norm_rows(x_s[sl, :].astype(F32), sl, u_s, acc_s))
    first[1].wait()
    gate_s[0] = dot(u_s[...], wg_s[...])
    gate_out = pltpu.make_async_copy(gate_s, gate_hbm, out_sem.at[0])
    gate_out.start()

    def block(f, carry):
        slot = lax.rem(f, 2)

        @pl.when(f + 1 < n_blk)
        def _():
            start(weights(0, f + 1, 1 - slot))

        up_w, down_w = weights(0, f, slot)
        up_w.wait()
        mlp_block((cw, nw), u_s, h_s, acc_s, wu_s.at[slot], wd_s.at[slot], up_s, down_w)
        return carry

    lax.fori_loop(0, n_blk, block, 0)
    own.wait()
    wait(copies)
    wait(first[2:])
    sel = (lax.broadcasted_iota(I32, (tok, n_emb * cap), 1) == slot_s[...]).astype(BF)
    for l in range(fet_s.shape[0]):
        fet_s[l] = dot(sel, ret_s[l]).astype(BF)
    add_proj(nw, acc_s, (gelu(gate_s[0]) * fet_s[0].astype(F32)).astype(BF), wp_s)
    fet_out = pltpu.make_async_copy(fet_s, fet_hbm, out_sem.at[1])
    fet_out.start()
    outs = []
    for half in range(2):
        rows = pl.ds(half * (tok // 2), tok // 2)

        def finish(sl, half=half):
            sl = pl.ds(sl.start + half * (tok // 2), slab)
            x_s[sl, :] = acc_s[sl, :].astype(BF)

        row_loop(tok // 2, slab)(finish)
        outs.append(pltpu.make_async_copy(x_s.at[rows], x_out_hbm.at[rows], out_sem.at[2 + half]))
        outs[-1].start()
    gate_out.wait()
    fet_out.wait()
    wait(outs)


def forward_kernel(cfg, x_hbm, fet_hbm, wg_hbm, wp_hbm, wu_hbm, wd_hbm, dt_in,
                   out_hbm, saved_hbm, ups_hbm, gate_hbm, dtab_hbm, scale_hbm,
                   x_s, u_s, acc_s, h_s, up_s, zero_s, fet_ref, gate_ref, scale_ref, wu_s, wd_s, wg_s, wp_s,
                   in_sem, w_sem, up_sem, out_sem, z_sem):
    n_layers, n_blk, cw, nw, slab, z_per, z_chunks = cfg
    tok, dim = x_s.shape
    fb = wu_s.shape[2]
    z_rows = zero_s.shape[0]
    n_steps = n_layers * n_blk
    weights = weight_copies(wu_hbm, wd_hbm, wu_s, wd_s, w_sem)

    def z_copies(step):
        found = []
        for j in range(z_per):
            c = step * z_per + j
            zl = c // z_chunks
            found.append(pltpu.make_async_copy(zero_s, dtab_hbm.at[zl + 1, pl.ds((c - zl * z_chunks) * z_rows, z_rows)], z_sem.at[j]))
        return found

    def up_copy(layer, blk, slot):
        return pltpu.make_async_copy(up_s.at[slot], ups_hbm.at[layer, :, pl.ds(pl.multiple_of(blk * fb, fb), fb)], up_sem.at[slot])

    def gate_copy(layer):
        return pltpu.make_async_copy(wg_hbm.at[layer + 1], wg_s, in_sem.at[1])

    def proj_copy(layer):
        return pltpu.make_async_copy(wp_hbm.at[layer + 1], wp_s, in_sem.at[2])

    fetch = pltpu.make_async_copy(x_hbm, x_s, in_sem.at[0])
    fetch.start()
    gate_copy(0).start()
    start(weights(1, 0, 0))
    proj_copy(0).start()
    get_fet = pltpu.make_async_copy(fet_hbm, fet_ref, in_sem.at[3])
    get_fet.start()
    put_scales = pltpu.make_async_copy(scale_ref, scale_hbm, out_sem.at[1])

    def put_gate(layer):
        return pltpu.make_async_copy(gate_ref.at[layer], gate_hbm.at[layer], out_sem.at[2])

    clear_rows(zero_s)
    fetch.wait()
    row_loop(tok, slab)(lambda sl: norm_rows(x_s[sl, :].astype(F32), sl, u_s, acc_s, scale_ref.at[0]))

    def one_layer(layer, carry):
        gate_copy(layer).wait()
        gate_ref[layer] = dot(u_s[...], wg_s[...])
        put_gate(layer).start()

        @pl.when(layer == n_layers - 1)
        def _():
            put_scales.start()

        @pl.when(layer + 1 < n_layers)
        def _():
            gate_copy(layer + 1).start()

        def block(f, carry):
            step = layer * n_blk + f
            slot = lax.rem(step, 2)

            @pl.when(step + 1 < n_steps)
            def _():
                nxt = step + 1
                start(weights(1 + nxt // n_blk, lax.rem(nxt, n_blk), 1 - slot))

            @pl.when(step > 0)
            def _():
                wait(z_copies(step - 1))

            for copy in z_copies(step):
                copy.start(priority=1)

            @pl.when(step > 1)
            def _():
                up_copy(layer, f, slot).wait()

            wait(weights(1 + layer, f, slot))
            mlp_block((cw, nw), u_s, h_s, acc_s, wu_s.at[slot], wd_s.at[slot], up_s.at[slot])
            up_copy(layer, f, slot).start(priority=1)
            return carry

        lax.fori_loop(0, n_blk, block, 0)
        proj_copy(layer).wait()
        put_gate(layer).wait()

        @pl.when(layer == 0)
        def _():
            get_fet.wait()

        add_proj(nw, acc_s, (gelu(gate_ref[layer]) * fet_ref[layer + 1].astype(F32)).astype(BF), wp_s)

        @pl.when(layer > 0)
        def _():
            pltpu.make_async_copy(x_s, saved_hbm.at[layer - 1], out_sem.at[0]).wait()

        def next_rows(sl):
            x_new = acc_s[sl, :].astype(BF)
            x_s[sl, :] = x_new
            norm_rows(x_new.astype(F32), sl, u_s, acc_s, scale_ref.at[jnp.minimum(layer + 1, n_layers - 1)])

        @pl.when(layer < n_layers - 1)
        def _():
            row_loop(tok, slab)(next_rows)

        @pl.when(layer < n_layers - 1)
        def _():
            pltpu.make_async_copy(x_s, saved_hbm.at[layer], out_sem.at[0]).start()
            proj_copy(layer + 1).start()

        return carry

    lax.fori_loop(0, n_layers, one_layer, 0)
    outs = []
    for half in range(2):
        rows = pl.ds(half * (tok // 2), tok // 2)

        def last_rows(sl, half=half):
            sl = pl.ds(sl.start + half * (tok // 2), slab)
            x_s[sl, :] = acc_s[sl, :].astype(BF)

        row_loop(tok // 2, slab)(last_rows)
        outs.append(pltpu.make_async_copy(x_s.at[rows], out_hbm.at[rows], out_sem.at[2 * half]))
        outs[-1].start()
    wait(z_copies(n_steps - 1))
    up_copy(0, 0, 0).wait()
    up_copy(0, 0, 1).wait()
    put_scales.wait()
    wait(outs)


def gate_grads(gate_pre, fetched, d_mixed, rows_ref, dgp_ref):
    rows_ref[...] = gelu(gate_pre) * d_mixed
    dgp_ref[...] = (d_mixed * fetched.astype(F32) * gelu_slope(gate_pre)).astype(BF)


def to_slots(rows, slot_ref, slots_s):
    hi = rows.astype(BF)
    rest = rows - hi.astype(F32)
    mid = rest.astype(BF)
    low = (rest - mid.astype(F32)).astype(BF)
    n = slots_s.shape[0] * slots_s.shape[2]
    sel = slot_pick(n, slot_ref)
    slots = (dot(sel, hi) + dot(sel, mid)) + dot(sel, low)
    for h in range(slots_s.shape[1]):
        slots_s[:, h] = slots[:, h * 128:(h + 1) * 128].reshape(n // 8, 8, 128)


def slot_pick(n, slot_ref):
    return (lax.broadcasted_iota(I32, (n, slot_ref.shape[1]), 0) == slot_ref[...]).astype(BF)


def backward_kernel(cfg, cot_hbm, x1_hbm, saved_hbm, slot_hbm, gate0_hbm, gates_hbm, fet_hbm, scale_hbm,
                    ups_hbm, wu_hbm, wd_hbm, wg_hbm, wp_hbm,
                    got_hbm, gate_hbm, mixed_hbm,
                    cot_s, x_s, acc_s, dup_s, dh_s, dng_s, slots_s, gslots_s, dslots_s, rows_s, dgp_s, slot_ref, gate0_ref, gate_ref, fet_ref, scale_ref, up_s, wu_s, wd_s, wg_s, wp_s,
                    in_sem, w_sem, up_sem, send_sem, self_sem, recv_sem):
    n_layers, n_blk, n_dp, n_emb, cap, cw, nw, slab = cfg
    tok, dim = cot_s.shape
    fb = wu_s.shape[2]
    gw = 128
    n_dev = n_dp * n_emb
    n_steps = n_layers * n_blk
    my_emb = lax.axis_index('emb')
    me = lax.axis_index('dp') * n_emb + my_emb
    peers = [peer_of(n_emb, lax.rem(me + k, n_dev)) for k in range(1, n_dev)]
    weights = weight_copies(wu_hbm, wd_hbm, wu_s, wd_s, w_sem)

    def part(ref, emb):
        return ref.at[pl.ds(emb * (cap // 8), cap // 8)]

    def sends(ref, there, which, got):
        return [pltpu.make_async_copy(part(ref, my_emb), there, self_sem.at[which])] + [
            remote(part(ref, peer['emb']), there, send_sem.at[which, k], recv_sem.at[got, k], peer) for k, peer in enumerate(peers)]

    def row_sends(i):
        return sends(slots_s, part(got_hbm.at[n_layers - 1 - i], me), 0, i)

    gate_sends = sends(gslots_s, part(gate_hbm, me), 1, n_layers)

    def flat(ref, dev):
        return ref.at[pl.ds(pl.multiple_of(dev * cap, cap), cap), :]

    mixed_sends = [pltpu.make_async_copy(flat(dslots_s, my_emb), flat(mixed_hbm, me), self_sem.at[2])] + [
        remote(flat(dslots_s, peer['emb']), flat(mixed_hbm, me), send_sem.at[2, k], recv_sem.at[n_layers + 1, k], peer)
        for k, peer in enumerate(peers)]

    def up_copy(step, slot):
        i = step // n_blk
        blk = step - i * n_blk
        return pltpu.make_async_copy(ups_hbm.at[n_layers - 1 - i, :, pl.ds(pl.multiple_of(blk * fb, fb), fb)], up_s.at[slot], up_sem.at[slot])

    def load(step, slot):
        i = step // n_blk
        return weights(n_layers - i, step - i * n_blk, slot) + (up_copy(step, slot),)

    def gate_copy(i):
        return pltpu.make_async_copy(wg_hbm.at[n_layers - i], wg_s, in_sem.at[1])

    def proj_copy(i):
        return pltpu.make_async_copy(wp_hbm.at[n_layers - 1 - i], wp_s, in_sem.at[2])

    def x_copy(i):
        return pltpu.make_async_copy(saved_hbm.at[n_layers - 2 - i], x_s, in_sem.at[3])

    fetch = pltpu.make_async_copy(cot_hbm, cot_s, in_sem.at[0])
    top = n_layers - 1
    soon = [pltpu.make_async_copy(src, dst, in_sem.at[4 + k]) for k, (src, dst) in enumerate(
        ((gate0_hbm, gate0_ref), (slot_hbm, slot_ref), (gates_hbm.at[top], gate_ref.at[top]), (fet_hbm.at[top + 1], fet_ref.at[top + 1])))]
    later = [pltpu.make_async_copy(src, dst, in_sem.at[8 + k]) for k, (src, dst) in enumerate(
        ((gates_hbm.at[pl.ds(0, top)], gate_ref.at[pl.ds(0, top)]), (fet_hbm.at[pl.ds(0, top + 1)], fet_ref.at[pl.ds(0, top + 1)]),
         (scale_hbm, scale_ref)))]
    start(soon[:2])
    fetch.start()
    proj_copy(-1).start()
    start(soon[2:])
    gate_copy(0).start()
    start(load(0, 0))
    start(later)

    def clear(sl):
        acc_s[sl, :] = jnp.zeros((slab, dim), F32)

    row_loop(tok, slab)(clear)
    meet(peers)
    wait(soon[:2])
    to_slots(gelu(gate0_ref[0]), slot_ref, gslots_s)
    fetch.wait()
    proj_copy(-1).wait()
    wait(soon[2:])
    gate_grads(gate_ref[n_layers - 1], fet_ref[n_layers], dot_t(cot_s[...], wp_s[...]).astype(BF).astype(F32), rows_s, dgp_s)
    proj_copy(0).start()

    def one_layer(i, carry):
        @pl.when(i < n_layers - 1)
        def _():
            x_copy(i).start()

        @pl.when(i == n_layers - 1)
        def _():
            pltpu.make_async_copy(x1_hbm, x_s, in_sem.at[3]).start()

        gate_copy(i).wait()
        to_slots(rows_s[...], slot_ref, slots_s)
        for n in range(dim // nw):
            ns = slice(n * nw, (n + 1) * nw)
            dng_s[:, ns] = dot_t(dgp_s[...], wg_s[ns, :]).astype(BF)
        start(row_sends(i))

        @pl.when(i < n_layers - 1)
        def _():
            gate_copy(i + 1).start()

        @pl.when(i == 0)
        def _():
            start(gate_sends)

        def block(f, carry):
            step = i * n_blk + f
            slot = lax.rem(step, 2)

            @pl.when(step + 1 < n_steps)
            def _():
                start(load(step + 1, 1 - slot))

            wait(load(step, slot))
            wu_ref, wd_ref, up_ref = wu_s.at[slot], wd_s.at[slot], up_s.at[slot]

            def act(c):
                for g in range(cw // gw):
                    gs = slice(c * cw + g * gw, c * cw + (g + 1) * gw)
                    dup_s[:, gs] = (dh_s[:, gs].astype(F32) * gelu_slope(up_ref[:, gs])).astype(BF)

            n_c = fb // cw
            for c in range(n_c):
                cs = slice(c * cw, (c + 1) * cw)
                dh_s[:, cs] = dot_t(cot_s[...], wd_ref[cs, :]).astype(BF)
                if c > 0:
                    act(c - 1)
            for c in range(n_c):
                cs = slice(c * cw, (c + 1) * cw)
                for n in range(dim // nw):
                    ns = slice(n * nw, (n + 1) * nw)
                    acc_s[:, ns] += dot_t(dup_s[:, cs], wu_ref[ns, cs])
                if c == 0:
                    act(n_c - 1)
            return carry

        lax.fori_loop(0, n_blk, block, 0)
        pltpu.make_async_copy(x1_hbm, x_s, in_sem.at[3]).wait()

        @pl.when(i == 0)
        def _():
            wait(later)


        def rows_back(sl):
            x = x_s[sl, :].astype(F32)
            scale = scale_ref[n_layers - 1 - i, sl, 0:1]
            d_n = (acc_s[sl, :].astype(BF) + dng_s[sl, :]).astype(F32)
            acc_s[sl, :] = jnp.zeros((slab, dim), F32)
            proj = jnp.mean(d_n * x, axis=-1, keepdims=True)
            d_x = d_n * scale - x * (proj * (scale * scale * scale))
            cot_s[sl, :] = (cot_s[sl, :].astype(F32) + d_x).astype(BF)

        row_loop(tok, slab)(rows_back)
        proj_copy(i).wait()
        d_mixed = dot_t(cot_s[...], wp_s[...]).astype(BF)

        @pl.when(i == n_layers - 1)
        def _():
            dslots_s[...] = dot(slot_pick(n_emb * cap, slot_ref), d_mixed).astype(BF)

        wait(row_sends(i))

        @pl.when(i < n_layers - 1)
        def _():
            proj_copy(i + 1).start()
            gate_grads(gate_ref[jnp.maximum(n_layers - 2 - i, 0)], fet_ref[n_layers - 1 - i], d_mixed.astype(F32), rows_s, dgp_s)

        return carry

    lax.fori_loop(0, n_layers, one_layer, 0)
    start(mixed_sends)
    wait(gate_sends)
    wait(mixed_sends)


def order_rows(recv_ref, counts_ref, slot_bits, read_ref, write_ref, group_ref, meta_ref):
    n_dev, cap = recv_ref.shape
    shape = (n_dev, cap)
    square = (cap, cap)
    dev, lane = lax.broadcasted_iota(I32, shape, 0), lax.broadcasted_iota(I32, shape, 1)
    down, right = lax.broadcasted_iota(I32, square, 0), lax.broadcasted_iota(I32, square, 1)
    counts = counts_ref[:, 0:1]
    key = jnp.where(lane < counts, jnp.left_shift(recv_ref[...], slot_bits), 1 << 30) + dev * cap + lane

    def ones(cond):
        return jnp.where(cond, 1.0, 0.0)

    def digit(k):
        return jnp.bitwise_and(jnp.right_shift(key, 8 * k), 255).astype(F32).astype(BF)

    digits = [digit(k) for k in range(4)]
    same = ones(down == right).astype(BF)
    turned = sum(jnp.left_shift(dot_t(same, d).astype(I32), 8 * k) for k, d in enumerate(digits))
    rows = jnp.concatenate([d[None] for d in digits], axis=0)
    found = [jnp.zeros((8, cap), F32) for _ in range(n_dev)]
    for d in range(n_dev):
        column = turned[:, d:d + 1]
        smaller = sum(ones(key[e:e + 1, :] < column) for e in range(n_dev))
        rank = jnp.sum(smaller, axis=1, keepdims=True)
        mine = jnp.concatenate([rows[k, d:d + 1, :] for k in range(4)] * 2, axis=0)
        for w in range(n_dev):
            found[w] = found[w] + dot(mine, ones(rank - (w * cap) == right.astype(F32)).astype(BF))
    merged = [sum(jnp.left_shift(f[k:k + 1].astype(I32), 8 * k) for k in range(4)) for f in found]
    ordered = jnp.concatenate(merged, axis=0)

    before = pltpu.roll(ordered, 1, 1)
    before = jnp.where(lane == 0, pltpu.roll(before, 1, 0), before)
    after = pltpu.roll(ordered, cap - 1, 1)
    after = jnp.where(lane == cap - 1, pltpu.roll(after, n_dev - 1, 0), after)
    total = jnp.sum(counts_ref[...].astype(F32), axis=0, keepdims=True).astype(I32)
    place_in = dev * cap + lane
    live = place_in < total[:, 0:1]
    slot = jnp.bitwise_and(ordered, (1 << slot_bits) - 1)
    row = jnp.right_shift(ordered, slot_bits)
    group = jnp.right_shift(ordered, slot_bits + 3)
    begin, end = place_in == 0, place_in == n_dev * cap - 1
    same_row = jnp.logical_and(row == jnp.right_shift(before, slot_bits), jnp.logical_not(begin))
    fresh = jnp.logical_or(group != jnp.right_shift(before, slot_bits + 3), begin)
    last = jnp.logical_and(jnp.logical_or(group != jnp.right_shift(after, slot_bits + 3), end), live)
    place = dot(ones(fresh).astype(BF), ones(down <= right).astype(BF)).astype(I32)
    place = place - place[:, 0:1]
    read_ref[...] = jnp.right_shift(slot, 3) * 16 + jnp.bitwise_and(slot, 7) + jnp.where(same_row, -(1 << 31), 0)
    write_ref[...] = place * 16 + jnp.bitwise_and(row, 7)
    group_ref[...] = jnp.where(live, group, 0)
    n_out = jnp.sum(ones(last), axis=1, keepdims=True).astype(I32)
    goes_on = jnp.where(jnp.logical_and(jnp.logical_not(fresh), live), 1, 0)[:, 0:1]
    meta_lane = lax.broadcasted_iota(I32, meta_ref.shape, 1)
    meta = jnp.where(meta_lane == 0, n_out, jnp.where(meta_lane == 1, place[:, cap - 1:cap], goes_on))
    meta_ref[...] = jnp.where(meta_lane == 3, total, meta)


def scatter_kernel(cfg, read_ref, write_ref, group_ref, meta_ref, rows_hbm, gate_hbm, mixed_hbm, dt_in, dt_out,
                   rows_ref, gate_ref, mixed_ref, groups, prod, spots, sems, in_sem):
    unroll, bulk = cfg
    n_layers, window = groups.shape[1:3]
    n_slots = mixed_ref.shape[0]
    n_win = n_slots // window
    count = meta_ref[0, 3]
    loads = [pltpu.make_async_copy(src, dst, in_sem.at[k]) for k, (src, dst) in enumerate(
        ((gate_hbm, gate_ref), (mixed_hbm, mixed_ref), (rows_hbm, rows_ref)))]
    start(loads)

    def product(i, carry):
        step = 64
        mixed = mixed_ref[pl.ds(pl.multiple_of(i * step, step), step), :].astype(F32)
        for h in range(2):
            at = pl.ds(i * (step // 8), step // 8)
            prod[at, h] = gate_ref[at, h] * mixed[:, h * 128:(h + 1) * 128].reshape(step // 8, 8, 128)
        return carry

    def move(buf, spot, group, n):
        return pltpu.make_async_copy(groups.at[buf, :, pl.ds(spot, n)], dt_out.at[:, pl.ds(group, n)], sems.at[buf])

    def each(n, k, body):
        def trip(t, carry):
            for i in range(k):
                body(t * k + i)
            return carry

        def one(i, carry):
            body(i)
            return carry

        full = n // k
        lax.fori_loop(0, full, trip, 0)
        lax.fori_loop(full * k, n, one, 0)

    def settle(w):
        n = meta_ref[w, 0]

        def drain_bulk(j, carry):
            move(w % 2, 0, 0, bulk).wait()
            return carry

        def drain(j, carry):
            move(w % 2, 0, 0, 1).wait()
            return carry

        lax.fori_loop(0, n // bulk, drain_bulk, 0)
        lax.fori_loop(0, lax.rem(n, bulk), drain, 0)

    blank = jnp.zeros(groups.shape[3:], F32)

    def clear_groups(w):
        def clear(u):
            for l in range(n_layers):
                groups[w % 2, l, u] = blank

        each(jnp.where(count > w * window, jnp.minimum(meta_ref[w, 0] + 1, window), 0), 4, clear)

    clear_groups(0)
    clear_groups(1)
    wait(loads[:2])
    lax.fori_loop(0, n_slots // 64, product, 0, unroll=4)
    wait(loads[2:])
    accs = tuple(jnp.zeros((2, 128), F32) for _ in range(n_layers))
    for w in range(n_win):
        buf = w % 2
        if w >= 2:
            settle(w - 2)
            clear_groups(w)
        left = jnp.clip(count - w * window, 0, window)
        trips = (left + (unroll - 1)) // unroll
        n_out = meta_ref[w, 0]
        if w > 0:
            @pl.when(meta_ref[w, 2] > 0)
            def _(w=w, buf=buf):
                for l in range(n_layers):
                    groups[buf, l, 0] = groups[1 - buf, l, meta_ref[w - 1, 1]]

        sums = [groups.at[buf, l].reshape(window * 16, 128) for l in range(n_layers)]
        rows = [prod.reshape(n_slots * 2, 128)] + [rows_ref.at[l] for l in range(n_layers - 1)]

        def add(t, accs, w=w, sums=sums, rows=rows):
            for k in range(unroll):
                j = t * unroll + k
                word = read_ref[w, j]
                at = jnp.bitwise_and(word, n_slots * 2 - 1)
                same = word < 0
                to = write_ref[w, j]
                spots[jnp.right_shift(to, 4)] = group_ref[w, j]
                accs = tuple(jnp.where(same, acc, 0.0) + src[pl.ds(at, 2, stride=8), :] for acc, src in zip(accs, rows))
                for acc, dst in zip(accs, sums):
                    dst[pl.ds(to, 2, stride=8), :] = acc
            return accs

        accs = lax.fori_loop(0, trips, add, accs)
        each(n_out, 8, lambda u, buf=buf: move(buf, u, spots[u], 1).start())
    for w in range(max(n_win - 2, 0), n_win):
        settle(w)


def solution(mesh):
    n_emb, n_dp = mesh.shape['emb'], mesh.shape['dp']
    n_dev = n_emb * n_dp
    tok_spec = P(('dp', 'emb'))
    act_spec = P(('dp', 'emb'), None)
    table_spec = P(None, 'emb', None)
    full_spec = P(None, None, None)
    hbm = pl.BlockSpec(memory_space=pl.ANY)
    vm = pl.BlockSpec(memory_space=pltpu.VMEM)
    sm = pl.BlockSpec(memory_space=pltpu.SMEM)
    big = jnp.iinfo(jnp.int32).max

    def params(n_grid, **kw):
        return pltpu.CompilerParams(vmem_limit_bytes=VMEM_BYTES, dimension_semantics=('arbitrary',) * n_grid if n_grid else None, **kw)

    def device_body(tok_ids, resid_in, cot_out, tables, w_up, w_down, w_gate, w_proj):
        n_layers, range_rows, e_dim = tables.shape
        tok = tok_ids.shape[0]
        dim, ffn = w_up.shape[1:]
        n_slots, n_serve = n_dev * CAP, n_emb * CAP
        my_emb, my_dp = lax.axis_index('emb'), lax.axis_index('dp')

        lanes = 128
        per_dot, dots = 32, 2
        dma = pltpu.SemaphoreType.DMA
        _, recv_loc, counts, pick, slot_row, slot_col = pl.pallas_call(
            functools.partial(plan_kernel, (n_dp, n_emb, CAP, range_rows, per_dot)),
            out_shape=[jax.ShapeDtypeStruct(shape, I32) for shape in (
                (n_dev, tok // lanes, lanes), (n_dev, CAP), (n_dev, lanes), (n_serve, 1), (1, tok), (tok, 1))],
            in_specs=[vm], out_specs=[vm] * 6,
            scratch_shapes=[pltpu.VMEM((n_dev, tok), F32), dma((n_dev - 1,)), dma((n_dev - 1,))],
            compiler_params=pltpu.CompilerParams(collective_id=0, has_side_effects=True),
            name='plan',
        )(tok_ids.reshape(tok // lanes, lanes))
        slot_bits = (n_slots - 1).bit_length()
        tab_shape = (n_layers, range_rows // 8, e_dim // 128, 8, 128)
        z_rows = 167
        z_chunks = tab_shape[1] // z_rows
        words = [jax.ShapeDtypeStruct((n_dev, CAP), I32)] * 3 + [jax.ShapeDtypeStruct((n_dev, lanes), I32)]
        served, dtab, read_word, write_word, group_word, meta = pl.pallas_call(
            functools.partial(gather_kernel, (n_layers, n_emb, CAP, per_dot, dots, z_chunks, slot_bits)),
            out_shape=[jax.ShapeDtypeStruct((n_layers, n_serve, e_dim), BF), jax.ShapeDtypeStruct(tab_shape, F32)] + words,
            in_specs=[sm, sm, vm, vm, vm, hbm],
            out_specs=[vm, hbm, vm, vm, vm, vm],
            scratch_shapes=[pltpu.VMEM((n_layers, n_serve * 8, e_dim), BF), pltpu.VMEM((z_rows,) + tab_shape[2:], F32), dma((n_emb,)), dma],
            compiler_params=params(0),
            name='table_rows',
        )(recv_loc, counts, recv_loc, counts, pick, tables)

        fb = 1024
        n_blk = ffn // fb
        cw, nw, slab = 512, 512, 32
        n_back = n_layers - 1
        z_per = z_chunks // n_blk
        assert z_chunks * z_rows == tab_shape[1] and z_per * n_blk == z_chunks
        matmul_flops = 4 * tok * dim * ffn
        w_bufs = [pltpu.VMEM((2, dim, fb), BF), pltpu.VMEM((2, fb, dim), BF), pltpu.VMEM((dim, e_dim), BF), pltpu.VMEM((e_dim, dim), BF)]
        x1, gate0, fetched = pl.pallas_call(
            functools.partial(first_kernel, (n_dp, n_emb, CAP, n_blk, cw, nw, slab)),
            out_shape=[
                jax.ShapeDtypeStruct((tok, dim), BF),
                jax.ShapeDtypeStruct((1, tok, e_dim), F32),
                jax.ShapeDtypeStruct((n_layers, tok, e_dim), BF),
            ],
            in_specs=[hbm] * 7,
            out_specs=[hbm] * 3,
            scratch_shapes=[
                pltpu.VMEM((tok, dim), BF), pltpu.VMEM((tok, 1), I32), pltpu.VMEM((1, tok, e_dim), F32), pltpu.VMEM((n_layers, tok, e_dim), BF),
                pltpu.VMEM((tok, dim), BF), pltpu.VMEM((tok, dim), F32), pltpu.VMEM((tok, fb), BF), pltpu.VMEM((tok, fb), F32),
                pltpu.VMEM((n_layers, n_serve, e_dim), BF), *w_bufs,
                dma((4,)), dma((4,)), dma((2, 2)), dma, dma((n_emb - 1,)), dma((n_emb - 1,)),
            ],
            compiler_params=params(0, collective_id=1, has_side_effects=True),
            cost_estimate=pl.CostEstimate(flops=matmul_flops, bytes_accessed=100 << 20, transcendentals=0),
            name='first_layer',
        )(resid_in, slot_col, served, w_gate, w_proj, w_up, w_down)

        out, saved, ups, gates, dtab, scales = pl.pallas_call(
            functools.partial(forward_kernel, (n_back, n_blk, cw, nw, slab, z_per, z_chunks)),
            out_shape=[
                jax.ShapeDtypeStruct((tok, dim), BF),
                jax.ShapeDtypeStruct((n_back - 1, tok, dim), BF),
                jax.ShapeDtypeStruct((n_back, tok, ffn), F32),
                jax.ShapeDtypeStruct((n_back, tok, e_dim), F32),
                jax.ShapeDtypeStruct(tab_shape, F32),
                jax.ShapeDtypeStruct((n_back, tok, lanes), F32),
            ],
            in_specs=[hbm] * 7,
            out_specs=[hbm] * 6,
            input_output_aliases={6: 4},
            scratch_shapes=[
                pltpu.VMEM((tok, dim), BF), pltpu.VMEM((tok, dim), BF), pltpu.VMEM((tok, dim), F32), pltpu.VMEM((tok, fb), BF),
                pltpu.VMEM((2, tok, fb), F32), pltpu.VMEM((z_rows,) + tab_shape[2:], F32),
                pltpu.VMEM((n_layers, tok, e_dim), BF), pltpu.VMEM((n_back, tok, e_dim), F32), pltpu.VMEM((n_back, tok, lanes), F32), *w_bufs,
                dma((4,)), dma((2, 2)), dma((2,)), dma((4,)), dma((z_per,)),
            ],
            compiler_params=params(0),
            cost_estimate=pl.CostEstimate(flops=n_back * matmul_flops, bytes_accessed=400 << 20, transcendentals=0),
            name='forward',
        )(x1, fetched, w_gate, w_proj, w_up, w_down, dtab)

        got, got_gate, mixed0 = pl.pallas_call(
            functools.partial(backward_kernel, (n_back, n_blk, n_dp, n_emb, CAP, cw, nw, slab)),
            out_shape=[jax.ShapeDtypeStruct((n_back, n_slots // 8, e_dim // 128, 8, 128), F32), jax.ShapeDtypeStruct((n_slots // 8, e_dim // 128, 8, 128), F32),
                       jax.ShapeDtypeStruct((n_slots, e_dim), BF)],
            in_specs=[hbm] * 13,
            out_specs=[hbm, hbm, hbm],
            scratch_shapes=[
                pltpu.VMEM((tok, dim), BF), pltpu.VMEM((tok, dim), BF), pltpu.VMEM((tok, dim), F32), pltpu.VMEM((tok, fb), BF), pltpu.VMEM((tok, fb), BF),
                pltpu.VMEM((tok, dim), BF), pltpu.VMEM((n_serve // 8, e_dim // 128, 8, 128), F32), pltpu.VMEM((n_serve // 8, e_dim // 128, 8, 128), F32),
                pltpu.VMEM((n_serve, e_dim), BF), pltpu.VMEM((tok, e_dim), F32), pltpu.VMEM((tok, e_dim), BF), pltpu.VMEM((1, tok), I32),
                pltpu.VMEM((1, tok, e_dim), F32), pltpu.VMEM((n_back, tok, e_dim), F32), pltpu.VMEM((n_layers, tok, e_dim), BF),
                pltpu.VMEM((n_back, tok, lanes), F32), pltpu.VMEM((2, tok, fb), F32), *w_bufs,
                dma((11,)), dma((2, 2)), dma((2,)), dma((3, n_dev - 1)), dma((3,)), dma((n_back + 2, n_dev - 1)),
            ],
            compiler_params=params(0, collective_id=2, has_side_effects=True),
            cost_estimate=pl.CostEstimate(flops=n_back * matmul_flops, bytes_accessed=400 << 20, transcendentals=0),
            name='backward',
        )(cot_out, x1, saved, slot_row, gate0, gates, fetched, scales, ups, w_up, w_down, w_gate, w_proj)

        dtab = pl.pallas_call(
            functools.partial(scatter_kernel, (8, 32)),
            out_shape=jax.ShapeDtypeStruct(dtab.shape, F32),
            in_specs=[sm, sm, sm, sm, hbm, hbm, hbm, hbm],
            out_specs=hbm,
            input_output_aliases={7: 0},
            scratch_shapes=[pltpu.VMEM((n_back, n_slots * 2, 128), F32), pltpu.VMEM((n_slots // 8,) + tab_shape[2:], F32),
                            pltpu.VMEM((n_slots, e_dim), BF), pltpu.VMEM((2, n_layers, CAP) + tab_shape[2:], F32),
                            pltpu.VMEM((n_slots // 8,) + tab_shape[2:], F32), pltpu.SMEM((CAP,), I32), dma((2,)), dma((3,))],
            compiler_params=params(0),
            name='scatter',
        )(read_word, write_word, group_word, meta, got.reshape(n_back, n_slots * 2, 128), got_gate, mixed0, dtab)
        dtab = dtab.transpose(0, 1, 3, 2, 4).reshape(n_layers, range_rows, e_dim)
        return out, dtab

    return jax.shard_map(device_body, mesh=mesh, in_specs=(tok_spec, act_spec, act_spec, table_spec, full_spec, full_spec, full_spec, full_spec), out_specs=(act_spec, table_spec), check_vma=False)
```

```python
import functools

import jax
import jax.numpy as jnp
from jax import lax
from jax.experimental import pallas as pl
from jax.experimental.pallas import tpu as pltpu
from jax.sharding import PartitionSpec as P

NORM_EPS = 1e-6
BF = jnp.bfloat16
F32 = jnp.float32
I32 = jnp.int32
VMEM_BYTES = 67043328
GELU_C = 0.7978845608028654
GELU_A = 0.044715

MESH_AXES = ('dp', 'emb')
CAP = 256


def gelu(x):
    return 0.5 * x * (1.0 + jnp.tanh(GELU_C * (x + GELU_A * (x * x * x))))


def gelu_slope(x):
    sq = x * x
    th = jnp.tanh(GELU_C * (x + GELU_A * (x * sq)))
    return 0.5 * (1.0 + th) + (0.5 * GELU_C) * x * (1.0 - th * th) * (1.0 + (3 * GELU_A) * sq)


def dot(a, b):
    return jnp.dot(a, b, preferred_element_type=F32)


def dot_t(a, b):
    return lax.dot_general(a, b, (((1,), (1,)), ((), ())), preferred_element_type=F32)


def row_loop(rows, slab, unroll=1):
    def run(body):
        def step(i, carry):
            body(pl.ds(pl.multiple_of(i * slab, slab), slab))
            return carry

        lax.fori_loop(0, rows // slab, step, 0, unroll=unroll)

    return run


def peer_of(n_emb, index):
    dp = index // n_emb
    return {'dp': dp, 'emb': index - dp * n_emb}


def remote(src, dst, send_sem, recv_sem, device):
    return pltpu.make_async_remote_copy(src_ref=src, dst_ref=dst, send_sem=send_sem, recv_sem=recv_sem,
                                        device_id=device, device_id_type=pl.DeviceIdType.MESH)


def meet(devices):
    barrier = pltpu.get_barrier_semaphore()
    for device in devices:
        pl.semaphore_signal(barrier, inc=1, device_id=device, device_id_type=pl.DeviceIdType.MESH)
    pl.semaphore_wait(barrier, len(devices))


def plan_kernel(cfg, in_ref, ids_ref, recv_ref, counts_ref, pick_ref, slot_row_ref, slot_col_ref, rank_s, send_sem, recv_sem):
    n_dp, n_emb, cap, range_rows, per_dot = cfg
    n_dev = n_dp * n_emb
    my_dp, my_emb = lax.axis_index('dp'), lax.axis_index('emb')
    me = my_dp * n_emb + my_emb
    n_sub, lanes = in_ref.shape
    tok = n_sub * lanes
    peers = [peer_of(n_emb, lax.rem(me + k, n_dev)) for k in range(1, n_dev)]
    meet(peers)
    copies = [remote(in_ref, ids_ref.at[me], send_sem.at[k], recv_sem.at[k], peer) for k, peer in enumerate(peers)]
    start(copies)
    ids_ref[me] = in_ref[...]

    def line(ref):
        return jnp.concatenate([ref[..., j, :] for j in range(n_sub)], axis=-1)

    def ones(cond):
        return jnp.where(cond, 1.0, 0.0)

    def digits(x):
        return jnp.concatenate([jnp.right_shift(x, 8), jnp.bitwise_and(x, 255)], axis=0).astype(F32).astype(BF)

    square = (tok, tok)
    down, right = lax.broadcasted_iota(I32, square, 0), lax.broadcasted_iota(I32, square, 1)
    earlier = ones(down < right).astype(BF)
    own = jnp.broadcast_to(jnp.concatenate([in_ref[j:j + 1, :] for j in range(n_sub)], axis=-1), (8, tok))
    owner = sum(jnp.where(own >= e * range_rows, 1, 0) for e in range(1, n_emb))
    is_owner = owner == lax.broadcasted_iota(I32, (8, tok), 0)
    own_rank = dot(ones(is_owner).astype(BF), earlier).astype(I32)
    slot_row = jnp.sum(jnp.where(is_owner, own_rank + owner * cap, 0).astype(F32), axis=0, keepdims=True).astype(I32)
    slot_row_ref[...] = slot_row
    turned = dot_t(ones(down == right).astype(BF), digits(jnp.broadcast_to(slot_row, (8, tok))))
    slot_col_ref[...] = (turned[:, 0:1] * 256.0 + turned[:, 8:9]).astype(I32)

    wait(copies)
    ids8 = line(ids_ref)
    low = my_emb * range_rows
    mine = jnp.logical_and(ids8 >= low, ids8 < low + range_rows)
    mine_f = ones(mine)
    rank_s[...] = jnp.where(mine, dot(mine_f.astype(BF), earlier), -1.0)
    counts = jnp.sum(mine_f, axis=1, keepdims=True).astype(I32)
    counts_ref[...] = jnp.broadcast_to(counts, counts_ref.shape)
    loc = digits(jnp.where(mine, ids8 - low, 0))
    c_iota = lax.broadcasted_iota(I32, (cap, tok), 0).astype(F32)
    dev_iota = lax.broadcasted_iota(I32, (n_dev, cap), 0)
    recv = jnp.zeros((n_dev, cap), F32)
    for d in range(n_dev):
        found = dot_t(loc, ones(rank_s[d:d + 1, :] == c_iota).astype(BF))
        recv = jnp.where(dev_iota == d, found[:n_dev] * 256.0 + found[n_dev:], recv)
    slot = dev_iota * cap + lax.broadcasted_iota(I32, (n_dev, cap), 1)
    recv_ref[...] = jnp.where(slot - dev_iota * cap < counts, recv.astype(I32), slot * 8)
    lane16 = lax.broadcasted_iota(I32, (cap, 2 * n_dev), 1)
    row1 = lax.broadcasted_iota(I32, (cap, 1), 0)
    for e in range(n_emb):
        d = my_dp * n_emb + e
        found = dot_t(ones(rank_s[pl.ds(d, 1), :] == c_iota).astype(BF), loc)
        low8 = jnp.sum(jnp.where(lane16 == n_dev + d, found, 0.0), axis=1, keepdims=True).astype(I32)
        pick_ref[e * cap:(e + 1) * cap, :] = jnp.bitwise_and(low8, 7) + 8 * jnp.bitwise_and(row1, per_dot - 1)


def gather_kernel(cfg, loc_ref, counts_ref, recv_ref, tally_ref, pick_ref, tables_hbm,
                  out_ref, dtab_hbm, read_ref, write_ref, group_ref, meta_ref, buf, zero_s, sems, z_sem):
    n_layers, n_dest, cap, per_dot, group, z_chunks, slot_bits = cfg
    trip = per_dot * group
    z_rows = zero_s.shape[0]
    first = lax.axis_index('dp') * n_dest
    n_trips = [(counts_ref[first + d, 0] + (trip - 1)) // trip for d in range(n_dest)]

    def row_copy(d, c):
        base = pl.multiple_of(jnp.left_shift(jnp.right_shift(loc_ref[first + d, c], 3), 3), 8)
        at = pl.multiple_of(d * cap * 8 + c * 8, 8)
        return pltpu.make_async_copy(tables_hbm.at[:, pl.ds(base, 8), :], buf.at[:, pl.ds(at, 8), :], sems.at[d])

    def z_copy(c):
        return pltpu.make_async_copy(zero_s, dtab_hbm.at[0, pl.ds(c * z_rows, z_rows)], z_sem)

    for d in range(n_dest):
        def issue(i, carry, d=d):
            for k in range(8):
                row_copy(d, i * 8 + k).start()
            return carry

        lax.fori_loop(0, n_trips[d] * (trip // 8), issue, 0)

    clear_rows(zero_s)

    def z_start(c, carry):
        z_copy(c).start(priority=1)
        return carry

    lax.fori_loop(0, z_chunks, z_start, 0)
    order_rows(recv_ref, tally_ref, slot_bits, read_ref, write_ref, group_ref, meta_ref)
    for d in range(n_dest):
        def drain(i, carry, d=d):
            part = buf.at[:, pl.ds(pl.multiple_of((d * cap + i * trip) * 8, 8), trip * 8), :]
            pltpu.make_async_copy(part, part, sems.at[d]).wait()
            return carry

        lax.fori_loop(0, n_trips[d], drain, 0)

        def pick(i, carry, d=d):
            for k in range(group):
                s0 = pl.multiple_of(d * cap + i * trip + k * per_dot, per_dot)
                want = pick_ref[pl.ds(s0, per_dot), :]
                sel = (lax.broadcasted_iota(I32, (per_dot, per_dot * 8), 1) == want).astype(BF)
                for l in range(n_layers):
                    rows = buf[l, pl.ds(pl.multiple_of(s0 * 8, 8), per_dot * 8), :]
                    out_ref[l, pl.ds(s0, per_dot), :] = dot(sel, rows).astype(BF)
            return carry

        lax.fori_loop(0, n_trips[d], pick, 0)

        def blank(i, carry, d=d):
            s0 = pl.multiple_of(d * cap + i * trip, trip)
            for l in range(n_layers):
                out_ref[l, pl.ds(s0, trip), :] = jnp.zeros((trip, out_ref.shape[2]), BF)
            return carry

        lax.fori_loop(n_trips[d], cap // trip, blank, 0)

    def z_wait(c, carry):
        z_copy(c).wait()
        return carry

    lax.fori_loop(0, z_chunks, z_wait, 0)


def clear_rows(ref):
    def clear(i, carry):
        ref[i] = jnp.zeros(ref.shape[1:], F32)
        return carry

    lax.fori_loop(0, ref.shape[0], clear, 0)


def weight_copies(wu_hbm, wd_hbm, wu_s, wd_s, sems):
    fb = wu_s.shape[2]

    def copies(layer, blk, slot):
        at = pl.multiple_of(blk * fb, fb)
        return (pltpu.make_async_copy(wu_hbm.at[layer, :, pl.ds(at, fb)], wu_s.at[slot], sems.at[0, slot]),
                pltpu.make_async_copy(wd_hbm.at[layer, pl.ds(at, fb), :], wd_s.at[slot], sems.at[1, slot]))

    return copies


def start(copies):
    for copy in copies:
        copy.start()


def wait(copies):
    for copy in copies:
        copy.wait()


def mlp_block(cfg, u_s, h_s, acc_s, wu_ref, wd_ref, up_ref, second=None):
    cw, nw = cfg
    gw = 128
    n_c = wu_ref.shape[1] // cw

    def act(c):
        for g in range(cw // gw):
            gs = slice(c * cw + g * gw, c * cw + (g + 1) * gw)
            h_s[:, gs] = gelu(up_ref[:, gs]).astype(BF)

    for c in range(n_c):
        cs = slice(c * cw, (c + 1) * cw)
        up_ref[:, cs] = dot(u_s[...], wu_ref[:, cs])
        if c > 0:
            act(c - 1)
    if second is not None:
        second.wait()
    for c in range(n_c):
        cs = slice(c * cw, (c + 1) * cw)
        for n in range(acc_s.shape[1] // nw):
            ns = slice(n * nw, (n + 1) * nw)
            acc_s[:, ns] += dot(h_s[:, cs], wd_ref[cs, ns])
        if c == 0:
            act(n_c - 1)


def norm_rows(x, sl, u_s, acc_s, scale_ref=None):
    scale = lax.rsqrt(jnp.mean(x * x, axis=-1, keepdims=True) + NORM_EPS)
    u_s[sl, :] = (x * scale).astype(BF)
    acc_s[sl, :] = x
    if scale_ref is not None:
        scale_ref[sl, :] = jnp.broadcast_to(scale, (scale.shape[0], scale_ref.shape[1]))


def add_proj(nw, acc_s, mixed, wp_ref):
    for n in range(acc_s.shape[1] // nw):
        ns = slice(n * nw, (n + 1) * nw)
        acc_s[:, ns] += dot(mixed, wp_ref[:, ns])


def first_kernel(cfg, x_hbm, slot_hbm, served_hbm, wg_hbm, wp_hbm, wu_hbm, wd_hbm,
                 x_out_hbm, gate_hbm, fet_hbm,
                 x_s, slot_s, gate_s, fet_s, u_s, acc_s, h_s, up_s, ret_s, wu_s, wd_s, wg_s, wp_s,
                 in_sem, out_sem, w_sem, self_sem, send_sem, recv_sem):
    n_dp, n_emb, cap, n_blk, cw, nw, slab = cfg
    tok, dim = u_s.shape
    my_emb = lax.axis_index('emb')
    my_dp = lax.axis_index('dp')
    here = ret_s.at[:, pl.ds(pl.multiple_of(my_emb * cap, cap), cap), :]
    own = pltpu.make_async_copy(served_hbm.at[:, pl.ds(pl.multiple_of(my_emb * cap, cap), cap), :], here, self_sem)
    peers = [lax.rem(my_emb + k, n_emb) for k in range(1, n_emb)]
    copies = [remote(served_hbm.at[:, pl.ds(pl.multiple_of(p * cap, cap), cap), :], here,
                     send_sem.at[k], recv_sem.at[k], {'dp': my_dp, 'emb': p}) for k, p in enumerate(peers)]
    weights = weight_copies(wu_hbm, wd_hbm, wu_s, wd_s, w_sem)
    first = [pltpu.make_async_copy(x_hbm, x_s, in_sem.at[0]),
             pltpu.make_async_copy(wg_hbm.at[0], wg_s, in_sem.at[1]),
             pltpu.make_async_copy(wp_hbm.at[0], wp_s, in_sem.at[2]),
             pltpu.make_async_copy(slot_hbm, slot_s, in_sem.at[3])]
    start(first[:2])
    start(weights(0, 0, 0))
    start(first[2:])
    meet([{'dp': my_dp, 'emb': p} for p in peers])
    own.start()
    start(copies)
    first[0].wait()
    row_loop(tok, slab)(lambda sl: norm_rows(x_s[sl, :].astype(F32), sl, u_s, acc_s))
    first[1].wait()
    gate_s[0] = dot(u_s[...], wg_s[...])
    gate_out = pltpu.make_async_copy(gate_s, gate_hbm, out_sem.at[0])
    gate_out.start()

    def block(f, carry):
        slot = lax.rem(f, 2)

        @pl.when(f + 1 < n_blk)
        def _():
            start(weights(0, f + 1, 1 - slot))

        up_w, down_w = weights(0, f, slot)
        up_w.wait()
        mlp_block((cw, nw), u_s, h_s, acc_s, wu_s.at[slot], wd_s.at[slot], up_s, down_w)
        return carry

    lax.fori_loop(0, n_blk, block, 0)
    own.wait()
    wait(copies)
    wait(first[2:])
    sel = (lax.broadcasted_iota(I32, (tok, n_emb * cap), 1) == slot_s[...]).astype(BF)
    for l in range(fet_s.shape[0]):
        fet_s[l] = dot(sel, ret_s[l]).astype(BF)
    add_proj(nw, acc_s, (gelu(gate_s[0]) * fet_s[0].astype(F32)).astype(BF), wp_s)
    fet_out = pltpu.make_async_copy(fet_s, fet_hbm, out_sem.at[1])
    fet_out.start()
    outs = []
    for half in range(2):
        rows = pl.ds(half * (tok // 2), tok // 2)

        def finish(sl, half=half):
            sl = pl.ds(sl.start + half * (tok // 2), slab)
            x_s[sl, :] = acc_s[sl, :].astype(BF)

        row_loop(tok // 2, slab)(finish)
        outs.append(pltpu.make_async_copy(x_s.at[rows], x_out_hbm.at[rows], out_sem.at[2 + half]))
        outs[-1].start()
    gate_out.wait()
    fet_out.wait()
    wait(outs)


def forward_kernel(cfg, x_hbm, fet_hbm, wg_hbm, wp_hbm, wu_hbm, wd_hbm, dt_in,
                   out_hbm, saved_hbm, ups_hbm, gate_hbm, dtab_hbm, scale_hbm,
                   x_s, u_s, acc_s, h_s, up_s, zero_s, fet_ref, gate_ref, scale_ref, wu_s, wd_s, wg_s, wp_s,
                   in_sem, w_sem, up_sem, out_sem, z_sem):
    n_layers, n_blk, cw, nw, slab, z_per, z_chunks, z_first, z_gap = cfg
    tok, dim = x_s.shape
    fb = wu_s.shape[2]
    z_rows = zero_s.shape[0]
    n_steps = n_layers * n_blk
    weights = weight_copies(wu_hbm, wd_hbm, wu_s, wd_s, w_sem)

    def z_copies(step):
        found = []
        for j in range(z_per):
            c = step * z_per + j
            zl = c // z_chunks
            found.append(pltpu.make_async_copy(zero_s, dtab_hbm.at[zl + 1, pl.ds((c - zl * z_chunks) * z_rows, z_rows)], z_sem.at[j]))
        return found

    def gap_copies(layer):
        return [pltpu.make_async_copy(zero_s, dtab_hbm.at[0, pl.ds((z_first + layer * z_gap + j) * z_rows, z_rows)], z_sem.at[z_per + j])
                for j in range(z_gap)]

    def up_copy(layer, blk, slot):
        return pltpu.make_async_copy(up_s.at[slot], ups_hbm.at[layer, :, pl.ds(pl.multiple_of(blk * fb, fb), fb)], up_sem.at[slot])

    def gate_copy(layer):
        return pltpu.make_async_copy(wg_hbm.at[layer + 1], wg_s, in_sem.at[1])

    def proj_copy(layer):
        return pltpu.make_async_copy(wp_hbm.at[layer + 1], wp_s, in_sem.at[2])

    fetch = pltpu.make_async_copy(x_hbm, x_s, in_sem.at[0])
    fetch.start()
    gate_copy(0).start()
    start(weights(1, 0, 0))
    proj_copy(0).start()
    get_fet = pltpu.make_async_copy(fet_hbm, fet_ref, in_sem.at[3])
    get_fet.start()
    put_scales = pltpu.make_async_copy(scale_ref, scale_hbm, out_sem.at[1])

    def put_gate(layer):
        return pltpu.make_async_copy(gate_ref.at[layer], gate_hbm.at[layer], out_sem.at[2])

    clear_rows(zero_s)
    fetch.wait()
    row_loop(tok, slab)(lambda sl: norm_rows(x_s[sl, :].astype(F32), sl, u_s, acc_s, scale_ref.at[0]))

    def one_layer(layer, carry):
        gate_copy(layer).wait()
        gate_ref[layer] = dot(u_s[...], wg_s[...])
        put_gate(layer).start()

        @pl.when(layer == n_layers - 1)
        def _():
            put_scales.start()

        @pl.when(layer + 1 < n_layers)
        def _():
            gate_copy(layer + 1).start()

        def block(f, carry):
            step = layer * n_blk + f
            slot = lax.rem(step, 2)

            @pl.when(step + 1 < n_steps)
            def _():
                nxt = step + 1
                start(weights(1 + nxt // n_blk, lax.rem(nxt, n_blk), 1 - slot))

            @pl.when(step > 0)
            def _():
                wait(z_copies(step - 1))

            for copy in z_copies(step):
                copy.start(priority=1)

            @pl.when(step > 1)
            def _():
                up_copy(layer, f, slot).wait()

            wait(weights(1 + layer, f, slot))
            mlp_block((cw, nw), u_s, h_s, acc_s, wu_s.at[slot], wd_s.at[slot], up_s.at[slot])
            up_copy(layer, f, slot).start(priority=1)
            return carry

        lax.fori_loop(0, n_blk, block, 0)

        @pl.when(layer > 0)
        def _():
            wait(gap_copies(layer - 1))

        @pl.when(layer < n_layers - 1)
        def _():
            for copy in gap_copies(layer):
                copy.start(priority=1)

        proj_copy(layer).wait()
        put_gate(layer).wait()

        @pl.when(layer == 0)
        def _():
            get_fet.wait()

        add_proj(nw, acc_s, (gelu(gate_ref[layer]) * fet_ref[layer + 1].astype(F32)).astype(BF), wp_s)

        @pl.when(layer > 0)
        def _():
            pltpu.make_async_copy(x_s, saved_hbm.at[layer - 1], out_sem.at[0]).wait()

        def next_rows(sl):
            x_new = acc_s[sl, :].astype(BF)
            x_s[sl, :] = x_new
            norm_rows(x_new.astype(F32), sl, u_s, acc_s, scale_ref.at[jnp.minimum(layer + 1, n_layers - 1)])

        @pl.when(layer < n_layers - 1)
        def _():
            row_loop(tok, slab)(next_rows)

        @pl.when(layer < n_layers - 1)
        def _():
            pltpu.make_async_copy(x_s, saved_hbm.at[layer], out_sem.at[0]).start()
            proj_copy(layer + 1).start()

        return carry

    lax.fori_loop(0, n_layers, one_layer, 0)
    outs = []
    for half in range(2):
        rows = pl.ds(half * (tok // 2), tok // 2)

        def last_rows(sl, half=half):
            sl = pl.ds(sl.start + half * (tok // 2), slab)
            x_s[sl, :] = acc_s[sl, :].astype(BF)

        row_loop(tok // 2, slab)(last_rows)
        outs.append(pltpu.make_async_copy(x_s.at[rows], out_hbm.at[rows], out_sem.at[2 * half]))
        outs[-1].start()
    wait(z_copies(n_steps - 1))
    up_copy(0, 0, 0).wait()
    up_copy(0, 0, 1).wait()
    put_scales.wait()
    wait(outs)


def gate_grads(gate_pre, fetched, d_mixed, rows_ref, dgp_ref):
    rows_ref[...] = gelu(gate_pre) * d_mixed
    dgp_ref[...] = (d_mixed * fetched.astype(F32) * gelu_slope(gate_pre)).astype(BF)


def to_slots(rows, slot_ref, slots_s):
    hi = rows.astype(BF)
    rest = rows - hi.astype(F32)
    mid = rest.astype(BF)
    low = (rest - mid.astype(F32)).astype(BF)
    n = slots_s.shape[0] * slots_s.shape[2]
    sel = slot_pick(n, slot_ref)
    slots = (dot(sel, hi) + dot(sel, mid)) + dot(sel, low)
    for h in range(slots_s.shape[1]):
        slots_s[:, h] = slots[:, h * 128:(h + 1) * 128].reshape(n // 8, 8, 128)


def slot_pick(n, slot_ref):
    return (lax.broadcasted_iota(I32, (n, slot_ref.shape[1]), 0) == slot_ref[...]).astype(BF)


def backward_kernel(cfg, cot_hbm, x1_hbm, saved_hbm, slot_hbm, gate0_hbm, gates_hbm, fet_hbm, scale_hbm,
                    ups_hbm, wu_hbm, wd_hbm, wg_hbm, wp_hbm,
                    got_hbm, gate_hbm, mixed_hbm,
                    cot_s, x_s, acc_s, dup_s, dh_s, dng_s, slots_s, gslots_s, dslots_s, rows_s, dgp_s, slot_ref, gate0_ref, gate_ref, fet_ref, scale_ref, up_s, wu_s, wd_s, wg_s, wp_s,
                    in_sem, w_sem, up_sem, send_sem, self_sem, recv_sem):
    n_layers, n_blk, n_dp, n_emb, cap, cw, nw, slab = cfg
    tok, dim = cot_s.shape
    fb = wu_s.shape[2]
    gw = 128
    n_dev = n_dp * n_emb
    n_steps = n_layers * n_blk
    my_emb = lax.axis_index('emb')
    me = lax.axis_index('dp') * n_emb + my_emb
    peers = [peer_of(n_emb, lax.rem(me + k, n_dev)) for k in range(1, n_dev)]
    weights = weight_copies(wu_hbm, wd_hbm, wu_s, wd_s, w_sem)

    def part(ref, emb):
        return ref.at[pl.ds(emb * (cap // 8), cap // 8)]

    def sends(ref, there, which, got):
        return [pltpu.make_async_copy(part(ref, my_emb), there, self_sem.at[which])] + [
            remote(part(ref, peer['emb']), there, send_sem.at[which, k], recv_sem.at[got, k], peer) for k, peer in enumerate(peers)]

    def row_sends(i):
        return sends(slots_s, part(got_hbm.at[n_layers - 1 - i], me), 0, i)

    gate_sends = sends(gslots_s, part(gate_hbm, me), 1, n_layers)

    def flat(ref, dev):
        return ref.at[pl.ds(pl.multiple_of(dev * cap, cap), cap), :]

    mixed_sends = [pltpu.make_async_copy(flat(dslots_s, my_emb), flat(mixed_hbm, me), self_sem.at[2])] + [
        remote(flat(dslots_s, peer['emb']), flat(mixed_hbm, me), send_sem.at[2, k], recv_sem.at[n_layers + 1, k], peer)
        for k, peer in enumerate(peers)]

    def up_copy(step, slot):
        i = step // n_blk
        blk = step - i * n_blk
        return pltpu.make_async_copy(ups_hbm.at[n_layers - 1 - i, :, pl.ds(pl.multiple_of(blk * fb, fb), fb)], up_s.at[slot], up_sem.at[slot])

    def load(step, slot):
        i = step // n_blk
        return weights(n_layers - i, step - i * n_blk, slot) + (up_copy(step, slot),)

    def gate_copy(i):
        return pltpu.make_async_copy(wg_hbm.at[n_layers - i], wg_s, in_sem.at[1])

    def proj_copy(i):
        return pltpu.make_async_copy(wp_hbm.at[n_layers - 1 - i], wp_s, in_sem.at[2])

    def x_copy(i):
        return pltpu.make_async_copy(saved_hbm.at[n_layers - 2 - i], x_s, in_sem.at[3])

    fetch = pltpu.make_async_copy(cot_hbm, cot_s, in_sem.at[0])
    top = n_layers - 1
    soon = [pltpu.make_async_copy(src, dst, in_sem.at[4 + k]) for k, (src, dst) in enumerate(
        ((gate0_hbm, gate0_ref), (slot_hbm, slot_ref), (gates_hbm.at[top], gate_ref.at[top]), (fet_hbm.at[top + 1], fet_ref.at[top + 1])))]
    later = [pltpu.make_async_copy(src, dst, in_sem.at[8 + k]) for k, (src, dst) in enumerate(
        ((gates_hbm.at[pl.ds(0, top)], gate_ref.at[pl.ds(0, top)]), (fet_hbm.at[pl.ds(0, top + 1)], fet_ref.at[pl.ds(0, top + 1)]),
         (scale_hbm, scale_ref)))]
    start(soon[:2])
    fetch.start()
    proj_copy(-1).start()
    start(soon[2:])
    gate_copy(0).start()
    start(load(0, 0))
    start(later)

    def clear(sl):
        acc_s[sl, :] = jnp.zeros((slab, dim), F32)

    row_loop(tok, slab)(clear)
    meet(peers)
    wait(soon[:2])
    to_slots(gelu(gate0_ref[0]), slot_ref, gslots_s)
    fetch.wait()
    proj_copy(-1).wait()
    wait(soon[2:])
    gate_grads(gate_ref[n_layers - 1], fet_ref[n_layers], dot_t(cot_s[...], wp_s[...]).astype(BF).astype(F32), rows_s, dgp_s)
    proj_copy(0).start()

    def one_layer(i, carry):
        @pl.when(i < n_layers - 1)
        def _():
            x_copy(i).start()

        @pl.when(i == n_layers - 1)
        def _():
            pltpu.make_async_copy(x1_hbm, x_s, in_sem.at[3]).start()

        gate_copy(i).wait()
        to_slots(rows_s[...], slot_ref, slots_s)
        for n in range(dim // nw):
            ns = slice(n * nw, (n + 1) * nw)
            dng_s[:, ns] = dot_t(dgp_s[...], wg_s[ns, :]).astype(BF)
        start(row_sends(i))

        @pl.when(i < n_layers - 1)
        def _():
            gate_copy(i + 1).start()

        @pl.when(i == 0)
        def _():
            start(gate_sends)

        def block(f, carry):
            step = i * n_blk + f
            slot = lax.rem(step, 2)

            @pl.when(step + 1 < n_steps)
            def _():
                start(load(step + 1, 1 - slot))

            wait(load(step, slot))
            wu_ref, wd_ref, up_ref = wu_s.at[slot], wd_s.at[slot], up_s.at[slot]

            def act(c):
                for g in range(cw // gw):
                    gs = slice(c * cw + g * gw, c * cw + (g + 1) * gw)
                    dup_s[:, gs] = (dh_s[:, gs].astype(F32) * gelu_slope(up_ref[:, gs])).astype(BF)

            n_c = fb // cw
            for c in range(n_c):
                cs = slice(c * cw, (c + 1) * cw)
                dh_s[:, cs] = dot_t(cot_s[...], wd_ref[cs, :]).astype(BF)
                if c > 0:
                    act(c - 1)
            for c in range(n_c):
                cs = slice(c * cw, (c + 1) * cw)
                for n in range(dim // nw):
                    ns = slice(n * nw, (n + 1) * nw)
                    acc_s[:, ns] += dot_t(dup_s[:, cs], wu_ref[ns, cs])
                if c == 0:
                    act(n_c - 1)
            return carry

        lax.fori_loop(0, n_blk, block, 0)
        pltpu.make_async_copy(x1_hbm, x_s, in_sem.at[3]).wait()

        @pl.when(i == 0)
        def _():
            wait(later)


        def rows_back(sl):
            x = x_s[sl, :].astype(F32)
            scale = scale_ref[n_layers - 1 - i, sl, 0:1]
            d_n = (acc_s[sl, :].astype(BF) + dng_s[sl, :]).astype(F32)
            acc_s[sl, :] = jnp.zeros((slab, dim), F32)
            proj = jnp.mean(d_n * x, axis=-1, keepdims=True)
            d_x = d_n * scale - x * (proj * (scale * scale * scale))
            cot_s[sl, :] = (cot_s[sl, :].astype(F32) + d_x).astype(BF)

        row_loop(tok, slab)(rows_back)
        proj_copy(i).wait()
        d_mixed = dot_t(cot_s[...], wp_s[...]).astype(BF)

        @pl.when(i == n_layers - 1)
        def _():
            dslots_s[...] = dot(slot_pick(n_emb * cap, slot_ref), d_mixed).astype(BF)

        wait(row_sends(i))

        @pl.when(i < n_layers - 1)
        def _():
            proj_copy(i + 1).start()
            gate_grads(gate_ref[jnp.maximum(n_layers - 2 - i, 0)], fet_ref[n_layers - 1 - i], d_mixed.astype(F32), rows_s, dgp_s)

        return carry

    lax.fori_loop(0, n_layers, one_layer, 0)
    start(mixed_sends)
    wait(gate_sends)
    wait(mixed_sends)


def order_rows(recv_ref, counts_ref, slot_bits, read_ref, write_ref, group_ref, meta_ref):
    n_dev, cap = recv_ref.shape
    shape = (n_dev, cap)
    square = (cap, cap)
    dev, lane = lax.broadcasted_iota(I32, shape, 0), lax.broadcasted_iota(I32, shape, 1)
    down, right = lax.broadcasted_iota(I32, square, 0), lax.broadcasted_iota(I32, square, 1)
    counts = counts_ref[:, 0:1]
    key = jnp.where(lane < counts, jnp.left_shift(recv_ref[...], slot_bits), 1 << 30) + dev * cap + lane

    def ones(cond):
        return jnp.where(cond, 1.0, 0.0)

    def digit(k):
        return jnp.bitwise_and(jnp.right_shift(key, 8 * k), 255).astype(F32).astype(BF)

    digits = [digit(k) for k in range(4)]
    same = ones(down == right).astype(BF)
    turned = sum(jnp.left_shift(dot_t(same, d).astype(I32), 8 * k) for k, d in enumerate(digits))
    rows = jnp.concatenate([d[None] for d in digits], axis=0)
    found = [jnp.zeros((8, cap), F32) for _ in range(n_dev)]
    for d in range(n_dev):
        column = turned[:, d:d + 1]
        smaller = sum(ones(key[e:e + 1, :] < column) for e in range(n_dev))
        rank = jnp.sum(smaller, axis=1, keepdims=True)
        mine = jnp.concatenate([rows[k, d:d + 1, :] for k in range(4)] * 2, axis=0)
        for w in range(n_dev):
            found[w] = found[w] + dot(mine, ones(rank - (w * cap) == right.astype(F32)).astype(BF))
    merged = [sum(jnp.left_shift(f[k:k + 1].astype(I32), 8 * k) for k in range(4)) for f in found]
    ordered = jnp.concatenate(merged, axis=0)

    before = pltpu.roll(ordered, 1, 1)
    before = jnp.where(lane == 0, pltpu.roll(before, 1, 0), before)
    after = pltpu.roll(ordered, cap - 1, 1)
    after = jnp.where(lane == cap - 1, pltpu.roll(after, n_dev - 1, 0), after)
    total = jnp.sum(counts_ref[...].astype(F32), axis=0, keepdims=True).astype(I32)
    place_in = dev * cap + lane
    live = place_in < total[:, 0:1]
    slot = jnp.bitwise_and(ordered, (1 << slot_bits) - 1)
    row = jnp.right_shift(ordered, slot_bits)
    group = jnp.right_shift(ordered, slot_bits + 3)
    begin, end = place_in == 0, place_in == n_dev * cap - 1
    same_row = jnp.logical_and(row == jnp.right_shift(before, slot_bits), jnp.logical_not(begin))
    fresh = jnp.logical_or(group != jnp.right_shift(before, slot_bits + 3), begin)
    last = jnp.logical_and(jnp.logical_or(group != jnp.right_shift(after, slot_bits + 3), end), live)
    place = dot(ones(fresh).astype(BF), ones(down <= right).astype(BF)).astype(I32)
    place = place - place[:, 0:1]
    read_ref[...] = jnp.right_shift(slot, 3) * 16 + jnp.bitwise_and(slot, 7) + jnp.where(same_row, -(1 << 31), 0)
    write_ref[...] = place * 16 + jnp.bitwise_and(row, 7)
    group_ref[...] = jnp.where(live, group, 0)
    n_out = jnp.sum(ones(last), axis=1, keepdims=True).astype(I32)
    goes_on = jnp.where(jnp.logical_and(jnp.logical_not(fresh), live), 1, 0)[:, 0:1]
    meta_lane = lax.broadcasted_iota(I32, meta_ref.shape, 1)
    meta = jnp.where(meta_lane == 0, n_out, jnp.where(meta_lane == 1, place[:, cap - 1:cap], goes_on))
    meta_ref[...] = jnp.where(meta_lane == 3, total, meta)


def scatter_kernel(cfg, read_ref, write_ref, group_ref, meta_ref, rows_hbm, gate_hbm, mixed_hbm, dt_in, dt_out,
                   rows_ref, gate_ref, mixed_ref, groups, prod, spots, sems, in_sem):
    unroll, bulk = cfg
    n_layers, window = groups.shape[1:3]
    n_slots = mixed_ref.shape[0]
    n_win = n_slots // window
    count = meta_ref[0, 3]
    loads = [pltpu.make_async_copy(src, dst, in_sem.at[k]) for k, (src, dst) in enumerate(
        ((gate_hbm, gate_ref), (mixed_hbm, mixed_ref), (rows_hbm, rows_ref)))]
    start(loads)

    def product(i, carry):
        step = 64
        mixed = mixed_ref[pl.ds(pl.multiple_of(i * step, step), step), :].astype(F32)
        for h in range(2):
            at = pl.ds(i * (step // 8), step // 8)
            prod[at, h] = gate_ref[at, h] * mixed[:, h * 128:(h + 1) * 128].reshape(step // 8, 8, 128)
        return carry

    def move(buf, spot, group, n):
        return pltpu.make_async_copy(groups.at[buf, :, pl.ds(spot, n)], dt_out.at[:, pl.ds(group, n)], sems.at[buf])

    def each(n, k, body):
        def trip(t, carry):
            for i in range(k):
                body(t * k + i)
            return carry

        def one(i, carry):
            body(i)
            return carry

        full = n // k
        lax.fori_loop(0, full, trip, 0)
        lax.fori_loop(full * k, n, one, 0)

    def settle(w):
        n = meta_ref[w, 0]

        def drain_bulk(j, carry):
            move(w % 2, 0, 0, bulk).wait()
            return carry

        def drain(j, carry):
            move(w % 2, 0, 0, 1).wait()
            return carry

        lax.fori_loop(0, n // bulk, drain_bulk, 0)
        lax.fori_loop(0, lax.rem(n, bulk), drain, 0)

    blank = jnp.zeros(groups.shape[3:], F32)

    def clear_groups(w):
        def clear(u):
            for l in range(n_layers):
                groups[w % 2, l, u] = blank

        each(jnp.where(count > w * window, jnp.minimum(meta_ref[w, 0] + 1, window), 0), 4, clear)

    clear_groups(0)
    clear_groups(1)
    wait(loads[:2])
    lax.fori_loop(0, n_slots // 64, product, 0, unroll=4)
    wait(loads[2:])
    accs = tuple(jnp.zeros((2, 128), F32) for _ in range(n_layers))
    for w in range(n_win):
        buf = w % 2
        if w >= 2:
            settle(w - 2)
            clear_groups(w)
        left = jnp.clip(count - w * window, 0, window)
        trips = (left + (unroll - 1)) // unroll
        n_out = meta_ref[w, 0]
        if w > 0:
            @pl.when(meta_ref[w, 2] > 0)
            def _(w=w, buf=buf):
                for l in range(n_layers):
                    groups[buf, l, 0] = groups[1 - buf, l, meta_ref[w - 1, 1]]

        sums = [groups.at[buf, l].reshape(window * 16, 128) for l in range(n_layers)]
        rows = [prod.reshape(n_slots * 2, 128)] + [rows_ref.at[l] for l in range(n_layers - 1)]

        def add(t, accs, w=w, sums=sums, rows=rows):
            for k in range(unroll):
                j = t * unroll + k
                word = read_ref[w, j]
                at = jnp.bitwise_and(word, n_slots * 2 - 1)
                same = word < 0
                to = write_ref[w, j]
                spots[jnp.right_shift(to, 4)] = group_ref[w, j]
                accs = tuple(jnp.where(same, acc, 0.0) + src[pl.ds(at, 2, stride=8), :] for acc, src in zip(accs, rows))
                for acc, dst in zip(accs, sums):
                    dst[pl.ds(to, 2, stride=8), :] = acc
            return accs

        accs = lax.fori_loop(0, trips, add, accs)
        each(n_out, 8, lambda u, buf=buf: move(buf, u, spots[u], 1).start())
    for w in range(max(n_win - 2, 0), n_win):
        settle(w)


def solution(mesh):
    n_emb, n_dp = mesh.shape['emb'], mesh.shape['dp']
    n_dev = n_emb * n_dp
    tok_spec = P(('dp', 'emb'))
    act_spec = P(('dp', 'emb'), None)
    table_spec = P(None, 'emb', None)
    full_spec = P(None, None, None)
    hbm = pl.BlockSpec(memory_space=pl.ANY)
    vm = pl.BlockSpec(memory_space=pltpu.VMEM)
    sm = pl.BlockSpec(memory_space=pltpu.SMEM)
    big = jnp.iinfo(jnp.int32).max

    def params(n_grid, **kw):
        return pltpu.CompilerParams(vmem_limit_bytes=VMEM_BYTES, dimension_semantics=('arbitrary',) * n_grid if n_grid else None, **kw)

    def device_body(tok_ids, resid_in, cot_out, tables, w_up, w_down, w_gate, w_proj):
        n_layers, range_rows, e_dim = tables.shape
        tok = tok_ids.shape[0]
        dim, ffn = w_up.shape[1:]
        n_slots, n_serve = n_dev * CAP, n_emb * CAP
        my_emb, my_dp = lax.axis_index('emb'), lax.axis_index('dp')

        lanes = 128
        per_dot, dots = 32, 2
        dma = pltpu.SemaphoreType.DMA
        _, recv_loc, counts, pick, slot_row, slot_col = pl.pallas_call(
            functools.partial(plan_kernel, (n_dp, n_emb, CAP, range_rows, per_dot)),
            out_shape=[jax.ShapeDtypeStruct(shape, I32) for shape in (
                (n_dev, tok // lanes, lanes), (n_dev, CAP), (n_dev, lanes), (n_serve, 1), (1, tok), (tok, 1))],
            in_specs=[vm], out_specs=[vm] * 6,
            scratch_shapes=[pltpu.VMEM((n_dev, tok), F32), dma((n_dev - 1,)), dma((n_dev - 1,))],
            compiler_params=pltpu.CompilerParams(collective_id=0, has_side_effects=True),
            name='plan',
        )(tok_ids.reshape(tok // lanes, lanes))
        slot_bits = (n_slots - 1).bit_length()
        tab_shape = (n_layers, range_rows // 8, e_dim // 128, 8, 128)
        z_rows = 167
        z_chunks = tab_shape[1] // z_rows
        z_gap = 8
        z_first = z_chunks - (n_layers - 2) * z_gap
        words = [jax.ShapeDtypeStruct((n_dev, CAP), I32)] * 3 + [jax.ShapeDtypeStruct((n_dev, lanes), I32)]
        served, dtab, read_word, write_word, group_word, meta = pl.pallas_call(
            functools.partial(gather_kernel, (n_layers, n_emb, CAP, per_dot, dots, z_first, slot_bits)),
            out_shape=[jax.ShapeDtypeStruct((n_layers, n_serve, e_dim), BF), jax.ShapeDtypeStruct(tab_shape, F32)] + words,
            in_specs=[sm, sm, vm, vm, vm, hbm],
            out_specs=[vm, hbm, vm, vm, vm, vm],
            scratch_shapes=[pltpu.VMEM((n_layers, n_serve * 8, e_dim), BF), pltpu.VMEM((z_rows,) + tab_shape[2:], F32), dma((n_emb,)), dma],
            compiler_params=params(0),
            name='table_rows',
        )(recv_loc, counts, recv_loc, counts, pick, tables)

        fb = 1024
        n_blk = ffn // fb
        cw, nw, slab = 512, 512, 32
        n_back = n_layers - 1
        z_per = z_chunks // n_blk
        assert z_chunks * z_rows == tab_shape[1] and z_per * n_blk == z_chunks
        matmul_flops = 4 * tok * dim * ffn
        w_bufs = [pltpu.VMEM((2, dim, fb), BF), pltpu.VMEM((2, fb, dim), BF), pltpu.VMEM((dim, e_dim), BF), pltpu.VMEM((e_dim, dim), BF)]
        x1, gate0, fetched = pl.pallas_call(
            functools.partial(first_kernel, (n_dp, n_emb, CAP, n_blk, cw, nw, slab)),
            out_shape=[
                jax.ShapeDtypeStruct((tok, dim), BF),
                jax.ShapeDtypeStruct((1, tok, e_dim), F32),
                jax.ShapeDtypeStruct((n_layers, tok, e_dim), BF),
            ],
            in_specs=[hbm] * 7,
            out_specs=[hbm] * 3,
            scratch_shapes=[
                pltpu.VMEM((tok, dim), BF), pltpu.VMEM((tok, 1), I32), pltpu.VMEM((1, tok, e_dim), F32), pltpu.VMEM((n_layers, tok, e_dim), BF),
                pltpu.VMEM((tok, dim), BF), pltpu.VMEM((tok, dim), F32), pltpu.VMEM((tok, fb), BF), pltpu.VMEM((tok, fb), F32),
                pltpu.VMEM((n_layers, n_serve, e_dim), BF), *w_bufs,
                dma((4,)), dma((4,)), dma((2, 2)), dma, dma((n_emb - 1,)), dma((n_emb - 1,)),
            ],
            compiler_params=params(0, collective_id=1, has_side_effects=True),
            cost_estimate=pl.CostEstimate(flops=matmul_flops, bytes_accessed=100 << 20, transcendentals=0),
            name='first_layer',
        )(resid_in, slot_col, served, w_gate, w_proj, w_up, w_down)

        out, saved, ups, gates, dtab, scales = pl.pallas_call(
            functools.partial(forward_kernel, (n_back, n_blk, cw, nw, slab, z_per, z_chunks, z_first, z_gap)),
            out_shape=[
                jax.ShapeDtypeStruct((tok, dim), BF),
                jax.ShapeDtypeStruct((n_back - 1, tok, dim), BF),
                jax.ShapeDtypeStruct((n_back, tok, ffn), F32),
                jax.ShapeDtypeStruct((n_back, tok, e_dim), F32),
                jax.ShapeDtypeStruct(tab_shape, F32),
                jax.ShapeDtypeStruct((n_back, tok, lanes), F32),
            ],
            in_specs=[hbm] * 7,
            out_specs=[hbm] * 6,
            input_output_aliases={6: 4},
            scratch_shapes=[
                pltpu.VMEM((tok, dim), BF), pltpu.VMEM((tok, dim), BF), pltpu.VMEM((tok, dim), F32), pltpu.VMEM((tok, fb), BF),
                pltpu.VMEM((2, tok, fb), F32), pltpu.VMEM((z_rows,) + tab_shape[2:], F32),
                pltpu.VMEM((n_layers, tok, e_dim), BF), pltpu.VMEM((n_back, tok, e_dim), F32), pltpu.VMEM((n_back, tok, lanes), F32), *w_bufs,
                dma((4,)), dma((2, 2)), dma((2,)), dma((4,)), dma((z_per + z_gap,)),
            ],
            compiler_params=params(0),
            cost_estimate=pl.CostEstimate(flops=n_back * matmul_flops, bytes_accessed=400 << 20, transcendentals=0),
            name='forward',
        )(x1, fetched, w_gate, w_proj, w_up, w_down, dtab)

        got, got_gate, mixed0 = pl.pallas_call(
            functools.partial(backward_kernel, (n_back, n_blk, n_dp, n_emb, CAP, cw, nw, slab)),
            out_shape=[jax.ShapeDtypeStruct((n_back, n_slots // 8, e_dim // 128, 8, 128), F32), jax.ShapeDtypeStruct((n_slots // 8, e_dim // 128, 8, 128), F32),
                       jax.ShapeDtypeStruct((n_slots, e_dim), BF)],
            in_specs=[hbm] * 13,
            out_specs=[hbm, hbm, hbm],
            scratch_shapes=[
                pltpu.VMEM((tok, dim), BF), pltpu.VMEM((tok, dim), BF), pltpu.VMEM((tok, dim), F32), pltpu.VMEM((tok, fb), BF), pltpu.VMEM((tok, fb), BF),
                pltpu.VMEM((tok, dim), BF), pltpu.VMEM((n_serve // 8, e_dim // 128, 8, 128), F32), pltpu.VMEM((n_serve // 8, e_dim // 128, 8, 128), F32),
                pltpu.VMEM((n_serve, e_dim), BF), pltpu.VMEM((tok, e_dim), F32), pltpu.VMEM((tok, e_dim), BF), pltpu.VMEM((1, tok), I32),
                pltpu.VMEM((1, tok, e_dim), F32), pltpu.VMEM((n_back, tok, e_dim), F32), pltpu.VMEM((n_layers, tok, e_dim), BF),
                pltpu.VMEM((n_back, tok, lanes), F32), pltpu.VMEM((2, tok, fb), F32), *w_bufs,
                dma((11,)), dma((2, 2)), dma((2,)), dma((3, n_dev - 1)), dma((3,)), dma((n_back + 2, n_dev - 1)),
            ],
            compiler_params=params(0, collective_id=2, has_side_effects=True),
            cost_estimate=pl.CostEstimate(flops=n_back * matmul_flops, bytes_accessed=400 << 20, transcendentals=0),
            name='backward',
        )(cot_out, x1, saved, slot_row, gate0, gates, fetched, scales, ups, w_up, w_down, w_gate, w_proj)

        dtab = pl.pallas_call(
            functools.partial(scatter_kernel, (8, 32)),
            out_shape=jax.ShapeDtypeStruct(dtab.shape, F32),
            in_specs=[sm, sm, sm, sm, hbm, hbm, hbm, hbm],
            out_specs=hbm,
            input_output_aliases={7: 0},
            scratch_shapes=[pltpu.VMEM((n_back, n_slots * 2, 128), F32), pltpu.VMEM((n_slots // 8,) + tab_shape[2:], F32),
                            pltpu.VMEM((n_slots, e_dim), BF), pltpu.VMEM((2, n_layers, CAP) + tab_shape[2:], F32),
                            pltpu.VMEM((n_slots // 8,) + tab_shape[2:], F32), pltpu.SMEM((CAP,), I32), dma((2,)), dma((3,))],
            compiler_params=params(0),
            name='scatter',
        )(read_word, write_word, group_word, meta, got.reshape(n_back, n_slots * 2, 128), got_gate, mixed0, dtab)
        dtab = dtab.transpose(0, 1, 3, 2, 4).reshape(n_layers, range_rows, e_dim)
        return out, dtab

    return jax.shard_map(device_body, mesh=mesh, in_specs=(tok_spec, act_spec, act_spec, table_spec, full_spec, full_spec, full_spec, full_spec), out_specs=(act_spec, table_spec), check_vma=False)
```

```python
import functools

import jax
import jax.numpy as jnp
from jax import lax
from jax.experimental import pallas as pl
from jax.experimental.pallas import tpu as pltpu
from jax.sharding import PartitionSpec as P

NORM_EPS = 1e-6
BF = jnp.bfloat16
F32 = jnp.float32
I32 = jnp.int32
VMEM_BYTES = 67043328
GELU_C = 0.7978845608028654
GELU_A = 0.044715

MESH_AXES = ('dp', 'emb')
CAP = 256


def gelu(x):
    return 0.5 * x * (1.0 + jnp.tanh(GELU_C * (x + GELU_A * (x * x * x))))


def gelu_slope(x):
    sq = x * x
    th = jnp.tanh(GELU_C * (x + GELU_A * (x * sq)))
    return 0.5 * (1.0 + th) + (0.5 * GELU_C) * x * (1.0 - th * th) * (1.0 + (3 * GELU_A) * sq)


def dot(a, b):
    return jnp.dot(a, b, preferred_element_type=F32)


def dot_t(a, b):
    return lax.dot_general(a, b, (((1,), (1,)), ((), ())), preferred_element_type=F32)


def row_loop(rows, slab, unroll=1):
    def run(body):
        def step(i, carry):
            body(pl.ds(pl.multiple_of(i * slab, slab), slab))
            return carry

        lax.fori_loop(0, rows // slab, step, 0, unroll=unroll)

    return run


def peer_of(n_emb, index):
    dp = index // n_emb
    return {'dp': dp, 'emb': index - dp * n_emb}


def remote(src, dst, send_sem, recv_sem, device):
    return pltpu.make_async_remote_copy(src_ref=src, dst_ref=dst, send_sem=send_sem, recv_sem=recv_sem,
                                        device_id=device, device_id_type=pl.DeviceIdType.MESH)


def meet(devices):
    barrier = pltpu.get_barrier_semaphore()
    for device in devices:
        pl.semaphore_signal(barrier, inc=1, device_id=device, device_id_type=pl.DeviceIdType.MESH)
    pl.semaphore_wait(barrier, len(devices))


def plan_kernel(cfg, in_ref, ids_ref, recv_ref, counts_ref, pick_ref, slot_row_ref, slot_col_ref, rank_s, send_sem, recv_sem):
    n_dp, n_emb, cap, range_rows, per_dot = cfg
    n_dev = n_dp * n_emb
    my_dp, my_emb = lax.axis_index('dp'), lax.axis_index('emb')
    me = my_dp * n_emb + my_emb
    n_sub, lanes = in_ref.shape
    tok = n_sub * lanes
    peers = [peer_of(n_emb, lax.rem(me + k, n_dev)) for k in range(1, n_dev)]
    meet(peers)
    copies = [remote(in_ref, ids_ref.at[me], send_sem.at[k], recv_sem.at[k], peer) for k, peer in enumerate(peers)]
    start(copies)
    ids_ref[me] = in_ref[...]

    def line(ref):
        return jnp.concatenate([ref[..., j, :] for j in range(n_sub)], axis=-1)

    def ones(cond):
        return jnp.where(cond, 1.0, 0.0)

    def digits(x):
        return jnp.concatenate([jnp.right_shift(x, 8), jnp.bitwise_and(x, 255)], axis=0).astype(F32).astype(BF)

    square = (tok, tok)
    down, right = lax.broadcasted_iota(I32, square, 0), lax.broadcasted_iota(I32, square, 1)
    earlier = ones(down < right).astype(BF)
    own = jnp.broadcast_to(jnp.concatenate([in_ref[j:j + 1, :] for j in range(n_sub)], axis=-1), (8, tok))
    owner = sum(jnp.where(own >= e * range_rows, 1, 0) for e in range(1, n_emb))
    is_owner = owner == lax.broadcasted_iota(I32, (8, tok), 0)
    own_rank = dot(ones(is_owner).astype(BF), earlier).astype(I32)
    slot_row = jnp.sum(jnp.where(is_owner, own_rank + owner * cap, 0).astype(F32), axis=0, keepdims=True).astype(I32)
    slot_row_ref[...] = slot_row
    turned = dot_t(ones(down == right).astype(BF), digits(jnp.broadcast_to(slot_row, (8, tok))))
    slot_col_ref[...] = (turned[:, 0:1] * 256.0 + turned[:, 8:9]).astype(I32)

    wait(copies)
    ids8 = line(ids_ref)
    low = my_emb * range_rows
    mine = jnp.logical_and(ids8 >= low, ids8 < low + range_rows)
    mine_f = ones(mine)
    rank_s[...] = jnp.where(mine, dot(mine_f.astype(BF), earlier), -1.0)
    counts = jnp.sum(mine_f, axis=1, keepdims=True).astype(I32)
    counts_ref[...] = jnp.broadcast_to(counts, counts_ref.shape)
    loc = digits(jnp.where(mine, ids8 - low, 0))
    c_iota = lax.broadcasted_iota(I32, (cap, tok), 0).astype(F32)
    dev_iota = lax.broadcasted_iota(I32, (n_dev, cap), 0)
    recv = jnp.zeros((n_dev, cap), F32)
    for d in range(n_dev):
        found = dot_t(loc, ones(rank_s[d:d + 1, :] == c_iota).astype(BF))
        recv = jnp.where(dev_iota == d, found[:n_dev] * 256.0 + found[n_dev:], recv)
    slot = dev_iota * cap + lax.broadcasted_iota(I32, (n_dev, cap), 1)
    recv_ref[...] = jnp.where(slot - dev_iota * cap < counts, recv.astype(I32), slot * 8)
    lane16 = lax.broadcasted_iota(I32, (cap, 2 * n_dev), 1)
    row1 = lax.broadcasted_iota(I32, (cap, 1), 0)
    for e in range(n_emb):
        d = my_dp * n_emb + e
        found = dot_t(ones(rank_s[pl.ds(d, 1), :] == c_iota).astype(BF), loc)
        low8 = jnp.sum(jnp.where(lane16 == n_dev + d, found, 0.0), axis=1, keepdims=True).astype(I32)
        pick_ref[e * cap:(e + 1) * cap, :] = jnp.bitwise_and(low8, 7) + 8 * jnp.bitwise_and(row1, per_dot - 1)


def gather_kernel(cfg, loc_ref, counts_ref, recv_ref, tally_ref, pick_ref, tables_hbm,
                  out_hbm, dtab_hbm, read_ref, write_ref, group_ref, meta_ref, out_ref, buf, zero_s, sems, z_sem, out_sem):
    n_layers, n_dest, cap, per_dot, group, z_chunks, slot_bits = cfg
    trip = per_dot * group
    z_rows = zero_s.shape[0]
    first = lax.axis_index('dp') * n_dest
    n_trips = [(counts_ref[first + d, 0] + (trip - 1)) // trip for d in range(n_dest)]

    def row_copy(d, c):
        base = pl.multiple_of(jnp.left_shift(jnp.right_shift(loc_ref[first + d, c], 3), 3), 8)
        at = pl.multiple_of(d * cap * 8 + c * 8, 8)
        return pltpu.make_async_copy(tables_hbm.at[:, pl.ds(base, 8), :], buf.at[:, pl.ds(at, 8), :], sems.at[d])

    def z_copy(c):
        return pltpu.make_async_copy(zero_s, dtab_hbm.at[0, pl.ds(c * z_rows, z_rows)], z_sem)

    def served(d):
        at = pl.ds(d * cap, cap)
        return pltpu.make_async_copy(out_ref.at[:, at], out_hbm.at[:, at], out_sem.at[d])

    for d in range(n_dest):
        def issue(i, carry, d=d):
            for k in range(8):
                row_copy(d, i * 8 + k).start()
            return carry

        lax.fori_loop(0, n_trips[d] * (trip // 8), issue, 0)

    clear_rows(zero_s)

    def z_start(c, carry):
        z_copy(c).start(priority=1)
        return carry

    lax.fori_loop(0, z_chunks, z_start, 0)
    order_rows(recv_ref, tally_ref, slot_bits, read_ref, write_ref, group_ref, meta_ref)
    for d in range(n_dest):
        def drain(i, carry, d=d):
            part = buf.at[:, pl.ds(pl.multiple_of((d * cap + i * trip) * 8, 8), trip * 8), :]
            pltpu.make_async_copy(part, part, sems.at[d]).wait()
            return carry

        lax.fori_loop(0, n_trips[d], drain, 0)

        def pick(i, carry, d=d):
            for k in range(group):
                s0 = pl.multiple_of(d * cap + i * trip + k * per_dot, per_dot)
                want = pick_ref[pl.ds(s0, per_dot), :]
                sel = (lax.broadcasted_iota(I32, (per_dot, per_dot * 8), 1) == want).astype(BF)
                for l in range(n_layers):
                    rows = buf[l, pl.ds(pl.multiple_of(s0 * 8, 8), per_dot * 8), :]
                    out_ref[l, pl.ds(s0, per_dot), :] = dot(sel, rows).astype(BF)
            return carry

        lax.fori_loop(0, n_trips[d], pick, 0)

        def blank(i, carry, d=d):
            s0 = pl.multiple_of(d * cap + i * trip, trip)
            for l in range(n_layers):
                out_ref[l, pl.ds(s0, trip), :] = jnp.zeros((trip, out_ref.shape[2]), BF)
            return carry

        lax.fori_loop(n_trips[d], cap // trip, blank, 0)
        served(d).start()

    def z_wait(c, carry):
        z_copy(c).wait()
        return carry

    lax.fori_loop(0, z_chunks, z_wait, 0)
    for d in range(n_dest):
        served(d).wait()


def clear_rows(ref):
    def clear(i, carry):
        ref[i] = jnp.zeros(ref.shape[1:], F32)
        return carry

    lax.fori_loop(0, ref.shape[0], clear, 0)


def weight_copies(wu_hbm, wd_hbm, wu_s, wd_s, sems):
    fb = wu_s.shape[2]

    def copies(layer, blk, slot):
        at = pl.multiple_of(blk * fb, fb)
        return (pltpu.make_async_copy(wu_hbm.at[layer, :, pl.ds(at, fb)], wu_s.at[slot], sems.at[0, slot]),
                pltpu.make_async_copy(wd_hbm.at[layer, pl.ds(at, fb), :], wd_s.at[slot], sems.at[1, slot]))

    return copies


def start(copies):
    for copy in copies:
        copy.start()


def wait(copies):
    for copy in copies:
        copy.wait()


def mlp_block(cfg, u_s, h_s, acc_s, wu_ref, wd_ref, up_ref, second=None):
    cw, nw = cfg
    gw = 128
    n_c = wu_ref.shape[1] // cw

    def act(c):
        for g in range(cw // gw):
            gs = slice(c * cw + g * gw, c * cw + (g + 1) * gw)
            h_s[:, gs] = gelu(up_ref[:, gs]).astype(BF)

    for c in range(n_c):
        cs = slice(c * cw, (c + 1) * cw)
        up_ref[:, cs] = dot(u_s[...], wu_ref[:, cs])
        if c > 0:
            act(c - 1)
    if second is not None:
        second.wait()
    for c in range(n_c):
        cs = slice(c * cw, (c + 1) * cw)
        for n in range(acc_s.shape[1] // nw):
            ns = slice(n * nw, (n + 1) * nw)
            acc_s[:, ns] += dot(h_s[:, cs], wd_ref[cs, ns])
        if c == 0:
            act(n_c - 1)


def norm_rows(x, sl, u_s, acc_s, scale_ref=None):
    scale = lax.rsqrt(jnp.mean(x * x, axis=-1, keepdims=True) + NORM_EPS)
    u_s[sl, :] = (x * scale).astype(BF)
    acc_s[sl, :] = x
    if scale_ref is not None:
        scale_ref[sl, :] = jnp.broadcast_to(scale, (scale.shape[0], scale_ref.shape[1]))


def add_proj(nw, acc_s, mixed, wp_ref):
    for n in range(acc_s.shape[1] // nw):
        ns = slice(n * nw, (n + 1) * nw)
        acc_s[:, ns] += dot(mixed, wp_ref[:, ns])


def first_kernel(cfg, x_hbm, slot_hbm, served_hbm, wg_hbm, wp_hbm, wu_hbm, wd_hbm,
                 x_out_hbm, gate_hbm, fet_hbm,
                 x_s, slot_s, gate_s, fet_s, u_s, acc_s, h_s, up_s, ret_s, wu_s, wd_s, wg_s, wp_s,
                 in_sem, out_sem, w_sem, self_sem, send_sem, recv_sem):
    n_dp, n_emb, cap, n_blk, cw, nw, slab = cfg
    tok, dim = u_s.shape
    my_emb = lax.axis_index('emb')
    my_dp = lax.axis_index('dp')
    here = ret_s.at[:, pl.ds(pl.multiple_of(my_emb * cap, cap), cap), :]
    own = pltpu.make_async_copy(served_hbm.at[:, pl.ds(pl.multiple_of(my_emb * cap, cap), cap), :], here, self_sem)
    peers = [lax.rem(my_emb + k, n_emb) for k in range(1, n_emb)]
    copies = [remote(served_hbm.at[:, pl.ds(pl.multiple_of(p * cap, cap), cap), :], here,
                     send_sem.at[k], recv_sem.at[k], {'dp': my_dp, 'emb': p}) for k, p in enumerate(peers)]
    weights = weight_copies(wu_hbm, wd_hbm, wu_s, wd_s, w_sem)
    first = [pltpu.make_async_copy(x_hbm, x_s, in_sem.at[0]),
             pltpu.make_async_copy(wg_hbm.at[0], wg_s, in_sem.at[1]),
             pltpu.make_async_copy(wp_hbm.at[0], wp_s, in_sem.at[2]),
             pltpu.make_async_copy(slot_hbm, slot_s, in_sem.at[3])]
    start(first[:2])
    start(weights(0, 0, 0))
    start(first[2:])
    meet([{'dp': my_dp, 'emb': p} for p in peers])
    own.start()
    start(copies)
    first[0].wait()
    row_loop(tok, slab)(lambda sl: norm_rows(x_s[sl, :].astype(F32), sl, u_s, acc_s))
    first[1].wait()
    gate_s[0] = dot(u_s[...], wg_s[...])
    gate_out = pltpu.make_async_copy(gate_s, gate_hbm, out_sem.at[0])
    gate_out.start()

    def block(f, carry):
        slot = lax.rem(f, 2)

        @pl.when(f + 1 < n_blk)
        def _():
            start(weights(0, f + 1, 1 - slot))

        up_w, down_w = weights(0, f, slot)
        up_w.wait()
        mlp_block((cw, nw), u_s, h_s, acc_s, wu_s.at[slot], wd_s.at[slot], up_s, down_w)
        return carry

    lax.fori_loop(0, n_blk, block, 0)
    own.wait()
    wait(copies)
    wait(first[2:])
    sel = (lax.broadcasted_iota(I32, (tok, n_emb * cap), 1) == slot_s[...]).astype(BF)
    for l in range(fet_s.shape[0]):
        fet_s[l] = dot(sel, ret_s[l]).astype(BF)
    add_proj(nw, acc_s, (gelu(gate_s[0]) * fet_s[0].astype(F32)).astype(BF), wp_s)
    fet_out = pltpu.make_async_copy(fet_s, fet_hbm, out_sem.at[1])
    fet_out.start()
    outs = []
    for half in range(2):
        rows = pl.ds(half * (tok // 2), tok // 2)

        def finish(sl, half=half):
            sl = pl.ds(sl.start + half * (tok // 2), slab)
            x_s[sl, :] = acc_s[sl, :].astype(BF)

        row_loop(tok // 2, slab)(finish)
        outs.append(pltpu.make_async_copy(x_s.at[rows], x_out_hbm.at[rows], out_sem.at[2 + half]))
        outs[-1].start()
    gate_out.wait()
    fet_out.wait()
    wait(outs)


def forward_kernel(cfg, x_hbm, fet_hbm, wg_hbm, wp_hbm, wu_hbm, wd_hbm, dt_in,
                   out_hbm, saved_hbm, ups_hbm, gate_hbm, dtab_hbm, scale_hbm,
                   x_s, u_s, acc_s, h_s, up_s, zero_s, fet_ref, gate_ref, scale_ref, wu_s, wd_s, wg_s, wp_s,
                   in_sem, w_sem, up_sem, out_sem, z_sem):
    n_layers, n_blk, cw, nw, slab, z_per, z_chunks, z_first, z_gap = cfg
    tok, dim = x_s.shape
    fb = wu_s.shape[2]
    z_rows = zero_s.shape[0]
    n_steps = n_layers * n_blk
    weights = weight_copies(wu_hbm, wd_hbm, wu_s, wd_s, w_sem)

    def z_copies(step):
        found = []
        for j in range(z_per):
            c = step * z_per + j
            zl = c // z_chunks
            found.append(pltpu.make_async_copy(zero_s, dtab_hbm.at[zl + 1, pl.ds((c - zl * z_chunks) * z_rows, z_rows)], z_sem.at[j]))
        return found

    def gap_copies(layer):
        return [pltpu.make_async_copy(zero_s, dtab_hbm.at[0, pl.ds((z_first + layer * z_gap + j) * z_rows, z_rows)], z_sem.at[z_per + j])
                for j in range(z_gap)]

    def up_copy(layer, blk, slot):
        return pltpu.make_async_copy(up_s.at[slot], ups_hbm.at[layer, :, pl.ds(pl.multiple_of(blk * fb, fb), fb)], up_sem.at[slot])

    def gate_copy(layer):
        return pltpu.make_async_copy(wg_hbm.at[layer + 1], wg_s, in_sem.at[1])

    def proj_copy(layer):
        return pltpu.make_async_copy(wp_hbm.at[layer + 1], wp_s, in_sem.at[2])

    fetch = pltpu.make_async_copy(x_hbm, x_s, in_sem.at[0])
    fetch.start()
    gate_copy(0).start()
    start(weights(1, 0, 0))
    proj_copy(0).start()
    get_fet = pltpu.make_async_copy(fet_hbm, fet_ref, in_sem.at[3])
    get_fet.start()
    put_scales = pltpu.make_async_copy(scale_ref, scale_hbm, out_sem.at[1])

    def put_gate(layer):
        return pltpu.make_async_copy(gate_ref.at[layer], gate_hbm.at[layer], out_sem.at[2])

    clear_rows(zero_s)
    fetch.wait()
    row_loop(tok, slab)(lambda sl: norm_rows(x_s[sl, :].astype(F32), sl, u_s, acc_s, scale_ref.at[0]))

    def one_layer(layer, carry):
        gate_copy(layer).wait()
        gate_ref[layer] = dot(u_s[...], wg_s[...])
        put_gate(layer).start()

        @pl.when(layer == n_layers - 1)
        def _():
            put_scales.start()

        @pl.when(layer + 1 < n_layers)
        def _():
            gate_copy(layer + 1).start()

        def block(f, carry):
            step = layer * n_blk + f
            slot = lax.rem(step, 2)

            @pl.when(step + 1 < n_steps)
            def _():
                nxt = step + 1
                start(weights(1 + nxt // n_blk, lax.rem(nxt, n_blk), 1 - slot))

            @pl.when(step > 0)
            def _():
                wait(z_copies(step - 1))

            for copy in z_copies(step):
                copy.start(priority=1)

            @pl.when(step > 1)
            def _():
                up_copy(layer, f, slot).wait()

            wait(weights(1 + layer, f, slot))
            mlp_block((cw, nw), u_s, h_s, acc_s, wu_s.at[slot], wd_s.at[slot], up_s.at[slot])
            up_copy(layer, f, slot).start(priority=1)
            return carry

        lax.fori_loop(0, n_blk, block, 0)

        @pl.when(layer > 0)
        def _():
            wait(gap_copies(layer - 1))

        @pl.when(layer < n_layers - 1)
        def _():
            for copy in gap_copies(layer):
                copy.start(priority=1)

        proj_copy(layer).wait()
        put_gate(layer).wait()

        @pl.when(layer == 0)
        def _():
            get_fet.wait()

        add_proj(nw, acc_s, (gelu(gate_ref[layer]) * fet_ref[layer + 1].astype(F32)).astype(BF), wp_s)

        @pl.when(layer > 0)
        def _():
            pltpu.make_async_copy(x_s, saved_hbm.at[layer - 1], out_sem.at[0]).wait()

        def next_rows(sl):
            x_new = acc_s[sl, :].astype(BF)
            x_s[sl, :] = x_new
            norm_rows(x_new.astype(F32), sl, u_s, acc_s, scale_ref.at[jnp.minimum(layer + 1, n_layers - 1)])

        @pl.when(layer < n_layers - 1)
        def _():
            row_loop(tok, slab)(next_rows)

        @pl.when(layer < n_layers - 1)
        def _():
            pltpu.make_async_copy(x_s, saved_hbm.at[layer], out_sem.at[0]).start()
            proj_copy(layer + 1).start()

        return carry

    lax.fori_loop(0, n_layers, one_layer, 0)
    outs = []
    for half in range(2):
        rows = pl.ds(half * (tok // 2), tok // 2)

        def last_rows(sl, half=half):
            sl = pl.ds(sl.start + half * (tok // 2), slab)
            x_s[sl, :] = acc_s[sl, :].astype(BF)

        row_loop(tok // 2, slab)(last_rows)
        outs.append(pltpu.make_async_copy(x_s.at[rows], out_hbm.at[rows], out_sem.at[2 * half]))
        outs[-1].start()
    wait(z_copies(n_steps - 1))
    up_copy(0, 0, 0).wait()
    up_copy(0, 0, 1).wait()
    put_scales.wait()
    wait(outs)


def gate_grads(gate_pre, fetched, d_mixed, rows_ref, dgp_ref):
    rows_ref[...] = gelu(gate_pre) * d_mixed
    dgp_ref[...] = (d_mixed * fetched.astype(F32) * gelu_slope(gate_pre)).astype(BF)


def to_slots(rows, slot_ref, slots_s):
    hi = rows.astype(BF)
    rest = rows - hi.astype(F32)
    mid = rest.astype(BF)
    low = (rest - mid.astype(F32)).astype(BF)
    n = slots_s.shape[0] * slots_s.shape[2]
    sel = slot_pick(n, slot_ref)
    slots = (dot(sel, hi) + dot(sel, mid)) + dot(sel, low)
    for h in range(slots_s.shape[1]):
        slots_s[:, h] = slots[:, h * 128:(h + 1) * 128].reshape(n // 8, 8, 128)


def slot_pick(n, slot_ref):
    return (lax.broadcasted_iota(I32, (n, slot_ref.shape[1]), 0) == slot_ref[...]).astype(BF)


def backward_kernel(cfg, cot_hbm, x1_hbm, saved_hbm, slot_hbm, gate0_hbm, gates_hbm, fet_hbm, scale_hbm,
                    ups_hbm, wu_hbm, wd_hbm, wg_hbm, wp_hbm,
                    got_hbm, gate_hbm, mixed_hbm,
                    cot_s, x_s, acc_s, dup_s, dh_s, dng_s, slots_s, gslots_s, dslots_s, rows_s, dgp_s, slot_ref, gate0_ref, gate_ref, fet_ref, scale_ref, up_s, wu_s, wd_s, wg_s, wp_s,
                    in_sem, w_sem, up_sem, send_sem, self_sem, recv_sem):
    n_layers, n_blk, n_dp, n_emb, cap, cw, nw, slab = cfg
    tok, dim = cot_s.shape
    fb = wu_s.shape[2]
    gw = 128
    n_dev = n_dp * n_emb
    n_steps = n_layers * n_blk
    my_emb = lax.axis_index('emb')
    me = lax.axis_index('dp') * n_emb + my_emb
    peers = [peer_of(n_emb, lax.rem(me + k, n_dev)) for k in range(1, n_dev)]
    weights = weight_copies(wu_hbm, wd_hbm, wu_s, wd_s, w_sem)

    def part(ref, emb):
        return ref.at[pl.ds(emb * (cap // 8), cap // 8)]

    def sends(ref, there, which, got):
        return [pltpu.make_async_copy(part(ref, my_emb), there, self_sem.at[which])] + [
            remote(part(ref, peer['emb']), there, send_sem.at[which, k], recv_sem.at[got, k], peer) for k, peer in enumerate(peers)]

    def row_sends(i):
        return sends(slots_s, part(got_hbm.at[n_layers - 1 - i], me), 0, i)

    gate_sends = sends(gslots_s, part(gate_hbm, me), 1, n_layers)

    def flat(ref, dev):
        return ref.at[pl.ds(pl.multiple_of(dev * cap, cap), cap), :]

    mixed_sends = [pltpu.make_async_copy(flat(dslots_s, my_emb), flat(mixed_hbm, me), self_sem.at[2])] + [
        remote(flat(dslots_s, peer['emb']), flat(mixed_hbm, me), send_sem.at[2, k], recv_sem.at[n_layers + 1, k], peer)
        for k, peer in enumerate(peers)]

    def up_copy(step, slot):
        i = step // n_blk
        blk = step - i * n_blk
        return pltpu.make_async_copy(ups_hbm.at[n_layers - 1 - i, :, pl.ds(pl.multiple_of(blk * fb, fb), fb)], up_s.at[slot], up_sem.at[slot])

    def load(step, slot):
        i = step // n_blk
        return weights(n_layers - i, step - i * n_blk, slot) + (up_copy(step, slot),)

    def gate_copy(i):
        return pltpu.make_async_copy(wg_hbm.at[n_layers - i], wg_s, in_sem.at[1])

    def proj_copy(i):
        return pltpu.make_async_copy(wp_hbm.at[n_layers - 1 - i], wp_s, in_sem.at[2])

    def x_copy(i):
        return pltpu.make_async_copy(saved_hbm.at[n_layers - 2 - i], x_s, in_sem.at[3])

    fetch = pltpu.make_async_copy(cot_hbm, cot_s, in_sem.at[0])
    top = n_layers - 1
    soon = [pltpu.make_async_copy(src, dst, in_sem.at[4 + k]) for k, (src, dst) in enumerate(
        ((gate0_hbm, gate0_ref), (slot_hbm, slot_ref), (gates_hbm.at[top], gate_ref.at[top]), (fet_hbm.at[top + 1], fet_ref.at[top + 1])))]
    later = [pltpu.make_async_copy(src, dst, in_sem.at[8 + k]) for k, (src, dst) in enumerate(
        ((gates_hbm.at[pl.ds(0, top)], gate_ref.at[pl.ds(0, top)]), (fet_hbm.at[pl.ds(0, top + 1)], fet_ref.at[pl.ds(0, top + 1)]),
         (scale_hbm, scale_ref)))]
    start(soon[:2])
    fetch.start()
    proj_copy(-1).start()
    start(soon[2:])
    gate_copy(0).start()
    start(load(0, 0))
    start(later)

    def clear(sl):
        acc_s[sl, :] = jnp.zeros((slab, dim), F32)

    row_loop(tok, slab)(clear)
    meet(peers)
    wait(soon[:2])
    to_slots(gelu(gate0_ref[0]), slot_ref, gslots_s)
    fetch.wait()
    proj_copy(-1).wait()
    wait(soon[2:])
    gate_grads(gate_ref[n_layers - 1], fet_ref[n_layers], dot_t(cot_s[...], wp_s[...]).astype(BF).astype(F32), rows_s, dgp_s)
    proj_copy(0).start()

    def one_layer(i, carry):
        @pl.when(i < n_layers - 1)
        def _():
            x_copy(i).start()

        @pl.when(i == n_layers - 1)
        def _():
            pltpu.make_async_copy(x1_hbm, x_s, in_sem.at[3]).start()

        gate_copy(i).wait()
        to_slots(rows_s[...], slot_ref, slots_s)
        for n in range(dim // nw):
            ns = slice(n * nw, (n + 1) * nw)
            dng_s[:, ns] = dot_t(dgp_s[...], wg_s[ns, :]).astype(BF)
        start(row_sends(i))

        @pl.when(i < n_layers - 1)
        def _():
            gate_copy(i + 1).start()

        @pl.when(i == 0)
        def _():
            start(gate_sends)

        def block(f, carry):
            step = i * n_blk + f
            slot = lax.rem(step, 2)

            @pl.when(step + 1 < n_steps)
            def _():
                start(load(step + 1, 1 - slot))

            wait(load(step, slot))
            wu_ref, wd_ref, up_ref = wu_s.at[slot], wd_s.at[slot], up_s.at[slot]

            def act(c):
                for g in range(cw // gw):
                    gs = slice(c * cw + g * gw, c * cw + (g + 1) * gw)
                    dup_s[:, gs] = (dh_s[:, gs].astype(F32) * gelu_slope(up_ref[:, gs])).astype(BF)

            n_c = fb // cw
            for c in range(n_c):
                cs = slice(c * cw, (c + 1) * cw)
                dh_s[:, cs] = dot_t(cot_s[...], wd_ref[cs, :]).astype(BF)
                if c > 0:
                    act(c - 1)
            for c in range(n_c):
                cs = slice(c * cw, (c + 1) * cw)
                for n in range(dim // nw):
                    ns = slice(n * nw, (n + 1) * nw)
                    acc_s[:, ns] += dot_t(dup_s[:, cs], wu_ref[ns, cs])
                if c == 0:
                    act(n_c - 1)
            return carry

        lax.fori_loop(0, n_blk, block, 0)
        pltpu.make_async_copy(x1_hbm, x_s, in_sem.at[3]).wait()

        @pl.when(i == 0)
        def _():
            wait(later)


        def rows_back(sl):
            x = x_s[sl, :].astype(F32)
            scale = scale_ref[n_layers - 1 - i, sl, 0:1]
            d_n = (acc_s[sl, :].astype(BF) + dng_s[sl, :]).astype(F32)
            acc_s[sl, :] = jnp.zeros((slab, dim), F32)
            proj = jnp.mean(d_n * x, axis=-1, keepdims=True)
            d_x = d_n * scale - x * (proj * (scale * scale * scale))
            cot_s[sl, :] = (cot_s[sl, :].astype(F32) + d_x).astype(BF)

        row_loop(tok, slab)(rows_back)
        proj_copy(i).wait()
        d_mixed = dot_t(cot_s[...], wp_s[...]).astype(BF)

        @pl.when(i == n_layers - 1)
        def _():
            dslots_s[...] = dot(slot_pick(n_emb * cap, slot_ref), d_mixed).astype(BF)

        wait(row_sends(i))

        @pl.when(i < n_layers - 1)
        def _():
            proj_copy(i + 1).start()
            gate_grads(gate_ref[jnp.maximum(n_layers - 2 - i, 0)], fet_ref[n_layers - 1 - i], d_mixed.astype(F32), rows_s, dgp_s)

        return carry

    lax.fori_loop(0, n_layers, one_layer, 0)
    start(mixed_sends)
    wait(gate_sends)
    wait(mixed_sends)


def order_rows(recv_ref, counts_ref, slot_bits, read_ref, write_ref, group_ref, meta_ref):
    n_dev, cap = recv_ref.shape
    shape = (n_dev, cap)
    square = (cap, cap)
    dev, lane = lax.broadcasted_iota(I32, shape, 0), lax.broadcasted_iota(I32, shape, 1)
    down, right = lax.broadcasted_iota(I32, square, 0), lax.broadcasted_iota(I32, square, 1)
    counts = counts_ref[:, 0:1]
    key = jnp.where(lane < counts, jnp.left_shift(recv_ref[...], slot_bits), 1 << 30) + dev * cap + lane

    def ones(cond):
        return jnp.where(cond, 1.0, 0.0)

    def digit(k):
        return jnp.bitwise_and(jnp.right_shift(key, 8 * k), 255).astype(F32).astype(BF)

    digits = [digit(k) for k in range(4)]
    same = ones(down == right).astype(BF)
    turned = sum(jnp.left_shift(dot_t(same, d).astype(I32), 8 * k) for k, d in enumerate(digits))
    rows = jnp.concatenate([d[None] for d in digits], axis=0)
    found = [jnp.zeros((8, cap), F32) for _ in range(n_dev)]
    for d in range(n_dev):
        column = turned[:, d:d + 1]
        smaller = sum(ones(key[e:e + 1, :] < column) for e in range(n_dev))
        rank = jnp.sum(smaller, axis=1, keepdims=True)
        mine = jnp.concatenate([rows[k, d:d + 1, :] for k in range(4)] * 2, axis=0)
        for w in range(n_dev):
            found[w] = found[w] + dot(mine, ones(rank - (w * cap) == right.astype(F32)).astype(BF))
    merged = [sum(jnp.left_shift(f[k:k + 1].astype(I32), 8 * k) for k in range(4)) for f in found]
    ordered = jnp.concatenate(merged, axis=0)

    before = pltpu.roll(ordered, 1, 1)
    before = jnp.where(lane == 0, pltpu.roll(before, 1, 0), before)
    after = pltpu.roll(ordered, cap - 1, 1)
    after = jnp.where(lane == cap - 1, pltpu.roll(after, n_dev - 1, 0), after)
    total = jnp.sum(counts_ref[...].astype(F32), axis=0, keepdims=True).astype(I32)
    place_in = dev * cap + lane
    live = place_in < total[:, 0:1]
    slot = jnp.bitwise_and(ordered, (1 << slot_bits) - 1)
    row = jnp.right_shift(ordered, slot_bits)
    group = jnp.right_shift(ordered, slot_bits + 3)
    begin, end = place_in == 0, place_in == n_dev * cap - 1
    same_row = jnp.logical_and(row == jnp.right_shift(before, slot_bits), jnp.logical_not(begin))
    fresh = jnp.logical_or(group != jnp.right_shift(before, slot_bits + 3), begin)
    last = jnp.logical_and(jnp.logical_or(group != jnp.right_shift(after, slot_bits + 3), end), live)
    place = dot(ones(fresh).astype(BF), ones(down <= right).astype(BF)).astype(I32)
    place = place - place[:, 0:1]
    read_ref[...] = jnp.right_shift(slot, 3) * 16 + jnp.bitwise_and(slot, 7) + jnp.where(same_row, -(1 << 31), 0)
    write_ref[...] = place * 16 + jnp.bitwise_and(row, 7)
    group_ref[...] = jnp.where(live, group, 0)
    n_out = jnp.sum(ones(last), axis=1, keepdims=True).astype(I32)
    goes_on = jnp.where(jnp.logical_and(jnp.logical_not(fresh), live), 1, 0)[:, 0:1]
    meta_lane = lax.broadcasted_iota(I32, meta_ref.shape, 1)
    meta = jnp.where(meta_lane == 0, n_out, jnp.where(meta_lane == 1, place[:, cap - 1:cap], goes_on))
    meta_ref[...] = jnp.where(meta_lane == 3, total, meta)


def scatter_kernel(cfg, read_ref, write_ref, group_ref, meta_ref, rows_hbm, gate_hbm, mixed_hbm, dt_in, dt_out,
                   rows_ref, gate_ref, mixed_ref, groups, prod, spots, sems, in_sem):
    unroll, bulk = cfg
    n_layers, window = groups.shape[1:3]
    n_slots = mixed_ref.shape[0]
    n_win = n_slots // window
    count = meta_ref[0, 3]
    loads = [pltpu.make_async_copy(src, dst, in_sem.at[k]) for k, (src, dst) in enumerate(
        ((gate_hbm, gate_ref), (mixed_hbm, mixed_ref), (rows_hbm, rows_ref)))]
    start(loads)

    def product(i, carry):
        step = 64
        mixed = mixed_ref[pl.ds(pl.multiple_of(i * step, step), step), :].astype(F32)
        for h in range(2):
            at = pl.ds(i * (step // 8), step // 8)
            prod[at, h] = gate_ref[at, h] * mixed[:, h * 128:(h + 1) * 128].reshape(step // 8, 8, 128)
        return carry

    def move(buf, spot, group, n):
        return pltpu.make_async_copy(groups.at[buf, :, pl.ds(spot, n)], dt_out.at[:, pl.ds(group, n)], sems.at[buf])

    def each(n, k, body):
        def trip(t, carry):
            for i in range(k):
                body(t * k + i)
            return carry

        def one(i, carry):
            body(i)
            return carry

        full = n // k
        lax.fori_loop(0, full, trip, 0)
        lax.fori_loop(full * k, n, one, 0)

    def settle(w):
        n = meta_ref[w, 0]

        def drain_bulk(j, carry):
            move(w % 2, 0, 0, bulk).wait()
            return carry

        def drain(j, carry):
            move(w % 2, 0, 0, 1).wait()
            return carry

        lax.fori_loop(0, n // bulk, drain_bulk, 0)
        lax.fori_loop(0, lax.rem(n, bulk), drain, 0)

    blank = jnp.zeros(groups.shape[3:], F32)

    def clear_groups(w):
        def clear(u):
            for l in range(n_layers):
                groups[w % 2, l, u] = blank

        each(jnp.where(count > w * window, jnp.minimum(meta_ref[w, 0] + 1, window), 0), 4, clear)

    clear_groups(0)
    clear_groups(1)
    wait(loads[:2])
    lax.fori_loop(0, n_slots // 64, product, 0, unroll=4)
    wait(loads[2:])
    accs = tuple(jnp.zeros((2, 128), F32) for _ in range(n_layers))
    for w in range(n_win):
        buf = w % 2
        if w >= 2:
            settle(w - 2)
            clear_groups(w)
        left = jnp.clip(count - w * window, 0, window)
        trips = (left + (unroll - 1)) // unroll
        n_out = meta_ref[w, 0]
        if w > 0:
            @pl.when(meta_ref[w, 2] > 0)
            def _(w=w, buf=buf):
                for l in range(n_layers):
                    groups[buf, l, 0] = groups[1 - buf, l, meta_ref[w - 1, 1]]

        sums = [groups.at[buf, l].reshape(window * 16, 128) for l in range(n_layers)]
        rows = [prod.reshape(n_slots * 2, 128)] + [rows_ref.at[l] for l in range(n_layers - 1)]

        def add(t, accs, w=w, sums=sums, rows=rows):
            for k in range(unroll):
                j = t * unroll + k
                word = read_ref[w, j]
                at = jnp.bitwise_and(word, n_slots * 2 - 1)
                same = word < 0
                to = write_ref[w, j]
                spots[jnp.right_shift(to, 4)] = group_ref[w, j]
                accs = tuple(jnp.where(same, acc, 0.0) + src[pl.ds(at, 2, stride=8), :] for acc, src in zip(accs, rows))
                for acc, dst in zip(accs, sums):
                    dst[pl.ds(to, 2, stride=8), :] = acc
            return accs

        accs = lax.fori_loop(0, trips, add, accs)
        each(n_out, 8, lambda u, buf=buf: move(buf, u, spots[u], 1).start())
    for w in range(max(n_win - 2, 0), n_win):
        settle(w)


def solution(mesh):
    n_emb, n_dp = mesh.shape['emb'], mesh.shape['dp']
    n_dev = n_emb * n_dp
    tok_spec = P(('dp', 'emb'))
    act_spec = P(('dp', 'emb'), None)
    table_spec = P(None, 'emb', None)
    full_spec = P(None, None, None)
    hbm = pl.BlockSpec(memory_space=pl.ANY)
    vm = pl.BlockSpec(memory_space=pltpu.VMEM)
    sm = pl.BlockSpec(memory_space=pltpu.SMEM)
    big = jnp.iinfo(jnp.int32).max

    def params(n_grid, **kw):
        return pltpu.CompilerParams(vmem_limit_bytes=VMEM_BYTES, dimension_semantics=('arbitrary',) * n_grid if n_grid else None, **kw)

    def device_body(tok_ids, resid_in, cot_out, tables, w_up, w_down, w_gate, w_proj):
        n_layers, range_rows, e_dim = tables.shape
        tok = tok_ids.shape[0]
        dim, ffn = w_up.shape[1:]
        n_slots, n_serve = n_dev * CAP, n_emb * CAP
        my_emb, my_dp = lax.axis_index('emb'), lax.axis_index('dp')

        lanes = 128
        per_dot, dots = 32, 2
        dma = pltpu.SemaphoreType.DMA
        _, recv_loc, counts, pick, slot_row, slot_col = pl.pallas_call(
            functools.partial(plan_kernel, (n_dp, n_emb, CAP, range_rows, per_dot)),
            out_shape=[jax.ShapeDtypeStruct(shape, I32) for shape in (
                (n_dev, tok // lanes, lanes), (n_dev, CAP), (n_dev, lanes), (n_serve, 1), (1, tok), (tok, 1))],
            in_specs=[vm], out_specs=[vm] * 6,
            scratch_shapes=[pltpu.VMEM((n_dev, tok), F32), dma((n_dev - 1,)), dma((n_dev - 1,))],
            compiler_params=pltpu.CompilerParams(collective_id=0, has_side_effects=True),
            name='plan',
        )(tok_ids.reshape(tok // lanes, lanes))
        slot_bits = (n_slots - 1).bit_length()
        tab_shape = (n_layers, range_rows // 8, e_dim // 128, 8, 128)
        z_rows = 167
        z_chunks = tab_shape[1] // z_rows
        z_gap = 11
        z_first = z_chunks - (n_layers - 2) * z_gap
        words = [jax.ShapeDtypeStruct((n_dev, CAP), I32)] * 3 + [jax.ShapeDtypeStruct((n_dev, lanes), I32)]
        served, dtab, read_word, write_word, group_word, meta = pl.pallas_call(
            functools.partial(gather_kernel, (n_layers, n_emb, CAP, per_dot, dots, z_first, slot_bits)),
            out_shape=[jax.ShapeDtypeStruct((n_layers, n_serve, e_dim), BF), jax.ShapeDtypeStruct(tab_shape, F32)] + words,
            in_specs=[sm, sm, vm, vm, vm, hbm],
            out_specs=[hbm, hbm, vm, vm, vm, vm],
            scratch_shapes=[pltpu.VMEM((n_layers, n_serve, e_dim), BF), pltpu.VMEM((n_layers, n_serve * 8, e_dim), BF),
                            pltpu.VMEM((z_rows,) + tab_shape[2:], F32), dma((n_emb,)), dma, dma((n_emb,))],
            compiler_params=params(0),
            name='table_rows',
        )(recv_loc, counts, recv_loc, counts, pick, tables)

        fb = 1024
        n_blk = ffn // fb
        cw, nw, slab = 512, 512, 32
        n_back = n_layers - 1
        z_per = z_chunks // n_blk
        assert z_chunks * z_rows == tab_shape[1] and z_per * n_blk == z_chunks
        matmul_flops = 4 * tok * dim * ffn
        w_bufs = [pltpu.VMEM((2, dim, fb), BF), pltpu.VMEM((2, fb, dim), BF), pltpu.VMEM((dim, e_dim), BF), pltpu.VMEM((e_dim, dim), BF)]
        x1, gate0, fetched = pl.pallas_call(
            functools.partial(first_kernel, (n_dp, n_emb, CAP, n_blk, cw, nw, slab)),
            out_shape=[
                jax.ShapeDtypeStruct((tok, dim), BF),
                jax.ShapeDtypeStruct((1, tok, e_dim), F32),
                jax.ShapeDtypeStruct((n_layers, tok, e_dim), BF),
            ],
            in_specs=[hbm] * 7,
            out_specs=[hbm] * 3,
            scratch_shapes=[
                pltpu.VMEM((tok, dim), BF), pltpu.VMEM((tok, 1), I32), pltpu.VMEM((1, tok, e_dim), F32), pltpu.VMEM((n_layers, tok, e_dim), BF),
                pltpu.VMEM((tok, dim), BF), pltpu.VMEM((tok, dim), F32), pltpu.VMEM((tok, fb), BF), pltpu.VMEM((tok, fb), F32),
                pltpu.VMEM((n_layers, n_serve, e_dim), BF), *w_bufs,
                dma((4,)), dma((4,)), dma((2, 2)), dma, dma((n_emb - 1,)), dma((n_emb - 1,)),
            ],
            compiler_params=params(0, collective_id=1, has_side_effects=True),
            cost_estimate=pl.CostEstimate(flops=matmul_flops, bytes_accessed=100 << 20, transcendentals=0),
            name='first_layer',
        )(resid_in, slot_col, served, w_gate, w_proj, w_up, w_down)

        out, saved, ups, gates, dtab, scales = pl.pallas_call(
            functools.partial(forward_kernel, (n_back, n_blk, cw, nw, slab, z_per, z_chunks, z_first, z_gap)),
            out_shape=[
                jax.ShapeDtypeStruct((tok, dim), BF),
                jax.ShapeDtypeStruct((n_back - 1, tok, dim), BF),
                jax.ShapeDtypeStruct((n_back, tok, ffn), F32),
                jax.ShapeDtypeStruct((n_back, tok, e_dim), F32),
                jax.ShapeDtypeStruct(tab_shape, F32),
                jax.ShapeDtypeStruct((n_back, tok, lanes), F32),
            ],
            in_specs=[hbm] * 7,
            out_specs=[hbm] * 6,
            input_output_aliases={6: 4},
            scratch_shapes=[
                pltpu.VMEM((tok, dim), BF), pltpu.VMEM((tok, dim), BF), pltpu.VMEM((tok, dim), F32), pltpu.VMEM((tok, fb), BF),
                pltpu.VMEM((2, tok, fb), F32), pltpu.VMEM((z_rows,) + tab_shape[2:], F32),
                pltpu.VMEM((n_layers, tok, e_dim), BF), pltpu.VMEM((n_back, tok, e_dim), F32), pltpu.VMEM((n_back, tok, lanes), F32), *w_bufs,
                dma((4,)), dma((2, 2)), dma((2,)), dma((4,)), dma((z_per + z_gap,)),
            ],
            compiler_params=params(0),
            cost_estimate=pl.CostEstimate(flops=n_back * matmul_flops, bytes_accessed=400 << 20, transcendentals=0),
            name='forward',
        )(x1, fetched, w_gate, w_proj, w_up, w_down, dtab)

        got, got_gate, mixed0 = pl.pallas_call(
            functools.partial(backward_kernel, (n_back, n_blk, n_dp, n_emb, CAP, cw, nw, slab)),
            out_shape=[jax.ShapeDtypeStruct((n_back, n_slots // 8, e_dim // 128, 8, 128), F32), jax.ShapeDtypeStruct((n_slots // 8, e_dim // 128, 8, 128), F32),
                       jax.ShapeDtypeStruct((n_slots, e_dim), BF)],
            in_specs=[hbm] * 13,
            out_specs=[hbm, hbm, hbm],
            scratch_shapes=[
                pltpu.VMEM((tok, dim), BF), pltpu.VMEM((tok, dim), BF), pltpu.VMEM((tok, dim), F32), pltpu.VMEM((tok, fb), BF), pltpu.VMEM((tok, fb), BF),
                pltpu.VMEM((tok, dim), BF), pltpu.VMEM((n_serve // 8, e_dim // 128, 8, 128), F32), pltpu.VMEM((n_serve // 8, e_dim // 128, 8, 128), F32),
                pltpu.VMEM((n_serve, e_dim), BF), pltpu.VMEM((tok, e_dim), F32), pltpu.VMEM((tok, e_dim), BF), pltpu.VMEM((1, tok), I32),
                pltpu.VMEM((1, tok, e_dim), F32), pltpu.VMEM((n_back, tok, e_dim), F32), pltpu.VMEM((n_layers, tok, e_dim), BF),
                pltpu.VMEM((n_back, tok, lanes), F32), pltpu.VMEM((2, tok, fb), F32), *w_bufs,
                dma((11,)), dma((2, 2)), dma((2,)), dma((3, n_dev - 1)), dma((3,)), dma((n_back + 2, n_dev - 1)),
            ],
            compiler_params=params(0, collective_id=2, has_side_effects=True),
            cost_estimate=pl.CostEstimate(flops=n_back * matmul_flops, bytes_accessed=400 << 20, transcendentals=0),
            name='backward',
        )(cot_out, x1, saved, slot_row, gate0, gates, fetched, scales, ups, w_up, w_down, w_gate, w_proj)

        dtab = pl.pallas_call(
            functools.partial(scatter_kernel, (8, 32)),
            out_shape=jax.ShapeDtypeStruct(dtab.shape, F32),
            in_specs=[sm, sm, sm, sm, hbm, hbm, hbm, hbm],
            out_specs=hbm,
            input_output_aliases={7: 0},
            scratch_shapes=[pltpu.VMEM((n_back, n_slots * 2, 128), F32), pltpu.VMEM((n_slots // 8,) + tab_shape[2:], F32),
                            pltpu.VMEM((n_slots, e_dim), BF), pltpu.VMEM((2, n_layers, CAP) + tab_shape[2:], F32),
                            pltpu.VMEM((n_slots // 8,) + tab_shape[2:], F32), pltpu.SMEM((CAP,), I32), dma((2,)), dma((3,))],
            compiler_params=params(0),
            name='scatter',
        )(read_word, write_word, group_word, meta, got.reshape(n_back, n_slots * 2, 128), got_gate, mixed0, dtab)
        dtab = dtab.transpose(0, 1, 3, 2, 4).reshape(n_layers, range_rows, e_dim)
        return out, dtab

    return jax.shard_map(device_body, mesh=mesh, in_specs=(tok_spec, act_spec, act_spec, table_spec, full_spec, full_spec, full_spec, full_spec), out_specs=(act_spec, table_spec), check_vma=False)
```
